32 devices in a mesh: fsdp: 4 (over x, core), expert: 8 (over z, y).
Axes of the slice: x: 2, y: 2, z: 4, core: 2. Of those that a mesh axis runs over, the one named last changes fastest.
Arguments:
- hidden_in: bfloat16 [4096, 1536], P(('fsdp', 'expert')), may hold values from -6 to 6
- doc_ids: int32 [32, 128], P(('fsdp', 'expert')), may hold values from 0 to 1, never falling along the last dimension, each value on 1 to 80 neighbouring positions
- routes: int32 [4096, 8], P(('fsdp', 'expert')), may hold values from 0 to 39, all different within a row; in each aligned block of 128 rows (0 to 127, 128 to 255, ...) at most 48 rows name the same one
- gain_attn: float32 [1536], replicated, may hold values from 0.5 to 1.5
- w_query: bfloat16 [1536, 1536], P('fsdp'), may hold values from -0.15625 to 0.15625
- key_matrix: bfloat16 [1536, 512], P('fsdp'), may hold values from -0.15625 to 0.15625
- value_matrix: bfloat16 [1536, 512], P('fsdp'), may hold values from -0.15625 to 0.15625
- w_output: bfloat16 [1536, 1536], P('fsdp'), may hold values from -0.625 to 0.625
- gain_ffn: float32 [1536], replicated, may hold values from 0.5 to 1.5
- w_router: bfloat16 [1536, 40], P('fsdp'), may hold values from -0.046875 to 0.046875
- w_gateup: bfloat16 [80, 1536, 512], P('expert'), may hold values from -0.15625 to 0.15625
- w_down: bfloat16 [80, 256, 1536], P('expert'), may hold values from -2 to 2
- cotangent: bfloat16 [4096, 1536], P(('fsdp', 'expert')), may hold values from -6 to 6
Outputs:
- block_out: bfloat16 [4096, 1536], P(('fsdp', 'expert'))
- grad_input: float32 [4096, 1536], P(('fsdp', 'expert'))
- grad_query: float32 [1536, 1536], P('fsdp')
- grad_key: float32 [1536, 512], P('fsdp')
- grad_value: float32 [1536, 512], P('fsdp')
- grad_output: float32 [1536, 1536], P('fsdp')
- grad_router: float32 [1536, 40], P('fsdp')
- grad_gain_attn: float32 [1536], P('fsdp')
- grad_gain_ffn: float32 [1536], P('fsdp')
- grad_gateup: float32 [80, 1536, 512], P('expert', 'fsdp')
- grad_down: float32 [80, 256, 1536], P('expert', 'fsdp')
The draws below stay inside these ranges and needn't reach their ends.
Inputs may be any that keep to these rules, and one draw needn't show every extreme that they name: `doc_ids`: along each device's row the document numbers never fall; each document has 1 to 80 tokens. `routes`: A token names 8 different experts; among the 128 tokens of one device no expert is named by more than 48 slots.
All inputs are finite; a program needn't handle non-finite values.
Results may differ from the reference program's by a relative error of at most 0.015.
Values may be sent and summed in bfloat16 or wider, within the bound.
A program may use at most 320 MiB of HBM per device.

```python
import math
import jax
import jax.numpy as jnp
import numpy as np
from jax import lax

MODEL_WIDTH = 1536
QUERY_HEADS = 24
KEY_VALUE_HEADS = 8
HEAD_SIZE = 64
FF = 512
TOP = 8
EXPERT_COUNT = 40
PIECES = 80
HALF = 256
TOK_DEV = 128
CAP = 48
DOCS = 2
DOC_MOST = 80
TOKENS = 4096
N_FSDP = 4
N_EXPERT = 8
DEVICES = 32


def block_levels(rng, dims, cuts, low, high):
    loudness, own = 1.0, jax.random.fold_in(rng, 6)
    for dim, blocks in cuts:
        steps = jnp.exp(jax.random.uniform(jax.random.fold_in(own, dim), (blocks,), jnp.float32, low / len(cuts), high / len(cuts)))
        loudness = loudness * jnp.repeat(steps, dims[dim] // blocks).reshape([-1 if axis == dim else 1 for axis in range(len(dims))])
    return loudness


def length_profile(amount, total, most, slope):
    loads = [(1 << 20) // math.isqrt(grade ** slope) + 1 for grade in range(2, amount + 1)]
    rest, counts = total - most - (amount - 1), [1] * (amount - 1)
    while rest > 0:
        candidates = [i for i in range(amount - 1) if counts[i] < most]
        pool, budget = sum([loads[i] for i in candidates]), rest
        for i in candidates:
            more = min(most - counts[i], max(1, budget * loads[i] // pool), rest)
            counts[i] = counts[i] + more
            rest = rest - more
    return np.array([most] + counts)


def uneven_parts(rng, count, total, most, lean):
    if count == 2:
        one = jax.random.randint(rng, (), max(1, total - most), min(most, total - 1) + 1)
        return jnp.stack([one, total - one])
    sizes = jnp.asarray(length_profile(count, total, most, lean), jnp.int32)
    twos = (count - 1) // 2
    giver, sink = sizes[1:1 + 2 * twos:2], sizes[2:2 + 2 * twos:2]
    margin = jnp.minimum(giver - 1, most - sink)
    shifted = jax.random.randint(jax.random.fold_in(rng, 1), (twos,), 0, 1 << 20) % (margin + 1)
    sizes = sizes.at[1:1 + 2 * twos:2].set(giver - shifted).at[2:2 + 2 * twos:2].set(sink + shifted)
    return sizes[jax.random.permutation(jax.random.fold_in(rng, 2), count)]


def deal_out(own_key, own, number, rows, count, top, bound, lean):
    order = jax.random.permutation(own_key, count)
    packed, common = load_shares(count, rows * top, bound, lean, True), load_shares(count, rows * top, bound, lean, False)
    places = jnp.arange(count)

    def named(tallies, rotation):
        used = int((tallies > 0).sum())
        fixed = max(1, used // 4)
        passed = fixed + (places - fixed + rotation * (used - fixed)) % max(1, count - fixed)
        return jnp.zeros((count,), jnp.int32).at[order[jnp.where(places < fixed, places, passed)]].set(jnp.asarray(tallies, jnp.int32))

    tallies = jnp.where(number % 4 == 0, named(packed, number // 4), named(common, number - number // 4 - 1))
    mixed = jax.random.permutation(jax.random.fold_in(own, 3), count)
    giver, taker = mixed[0:count // 2 * 2:2], mixed[1:count // 2 * 2:2]
    slack = jnp.minimum(tallies[giver] - 1, bound - tallies[taker]) // 2
    slack = jnp.where((giver == order[0]) | (taker == order[0]) | (tallies[taker] == 0), 0, jnp.maximum(slack, 0))
    passed = jax.random.randint(jax.random.fold_in(own, 4), (count // 2,), 0, 1 << 20) % (slack + 1)
    tallies = tallies.at[giver].add(-passed).at[taker].add(passed)
    items = jnp.searchsorted(jnp.cumsum(tallies), jnp.arange(rows * top), side="right").astype(jnp.int32)
    table = items.reshape(top, rows).T
    table = table[jax.random.permutation(jax.random.fold_in(own, 1), rows)]
    rotation = jax.random.randint(jax.random.fold_in(own, 2), (rows, 1), 0, top)
    return jnp.take_along_axis(table, (jnp.arange(top)[None, :] + rotation) % top, axis=1)


def load_shares(number_of, total, most, skew, full):
    loads = [(1 << 20) // math.isqrt(standing ** skew) + 1 for standing in range(1, number_of + 1)]
    largest = most if full else min(most, max(-(-total // number_of), total * loads[0] // sum(loads)))
    least = 1 if total - largest >= number_of - 1 else 0
    holding, rest = [largest] + [least] * (number_of - 1), total - largest - least * (number_of - 1)
    while rest > 0:
        candidates = [i for i in range(1, number_of) if holding[i] < largest] or [i for i in range(1, number_of) if holding[i] < most]
        mass, left = sum([loads[i] for i in candidates]), rest
        for i in candidates:
            more = min(most - holding[i], max(1, left * loads[i] // mass), rest)
            holding[i] = holding[i] + more
            rest = rest - more
    return np.array(holding)


def gaussian(stream_key, extent, scale, most, cuts=(), held_as=jnp.bfloat16):
    drawn = scale * jax.random.normal(stream_key, extent, jnp.float32)
    if cuts:
        drawn = drawn * block_levels(stream_key, extent, cuts, -0.22, 0.18)
    return jnp.clip(drawn, -most, most).astype(held_as)


def setup_inputs(seed: int = 0) -> dict:
    key_of = jax.random.split(jax.random.key(seed), 14)
    hidden_in = gaussian(key_of[0], (TOKENS, MODEL_WIDTH), 1.0, 6.0, ((0, 32),))
    doc_ids = jax.vmap(lambda own: jnp.searchsorted(jnp.cumsum(uneven_parts(own, DOCS, TOK_DEV, DOC_MOST, 2)), jnp.arange(TOK_DEV), side="right"))(jax.random.split(key_of[1], DEVICES)).reshape((DEVICES, TOK_DEV)).astype(jnp.int32)
    routes_keys = jax.random.split(jax.random.fold_in(key_of[2], 1), TOKENS // TOK_DEV)
    routes_turns = jax.random.permutation(jax.random.fold_in(key_of[2], 3), TOKENS // TOK_DEV)
    routes = jax.vmap(lambda own, number: deal_out(jax.random.fold_in(key_of[2], 2), own, number, TOK_DEV, EXPERT_COUNT, TOP, CAP, 2))(routes_keys, routes_turns).reshape((TOKENS, TOP))
    gain_attn = jnp.clip(1.0 + 0.1 * jax.random.normal(key_of[3], (MODEL_WIDTH,), jnp.float32), 0.5, 1.5)
    w_query = gaussian(key_of[4], (MODEL_WIDTH, QUERY_HEADS * HEAD_SIZE), MODEL_WIDTH ** -0.5, 0.15625, ((0, 4),))
    key_matrix = gaussian(key_of[5], (MODEL_WIDTH, KEY_VALUE_HEADS * HEAD_SIZE), MODEL_WIDTH ** -0.5, 0.15625, ((0, 4),))
    value_matrix = gaussian(key_of[6], (MODEL_WIDTH, KEY_VALUE_HEADS * HEAD_SIZE), MODEL_WIDTH ** -0.5, 0.15625, ((0, 4),))
    w_output = gaussian(key_of[7], (QUERY_HEADS * HEAD_SIZE, MODEL_WIDTH), (QUERY_HEADS * HEAD_SIZE // 16) ** -0.5, 0.625, ((0, 4),))
    gain_ffn = jnp.clip(1.0 + 0.1 * jax.random.normal(key_of[8], (MODEL_WIDTH,), jnp.float32), 0.5, 1.5)
    w_router = gaussian(key_of[9], (MODEL_WIDTH, EXPERT_COUNT), (MODEL_WIDTH * 11) ** -0.5, 0.046875, ((0, 4),))
    w_gateup = gaussian(key_of[10], (PIECES, MODEL_WIDTH, FF), MODEL_WIDTH ** -0.5, 0.15625, ((0, 8),))
    w_down = gaussian(key_of[11], (PIECES, HALF, MODEL_WIDTH), (max(2, FF // 64)) ** -0.5, 2.0, ((0, 8),))
    cotangent = gaussian(key_of[12], (TOKENS, MODEL_WIDTH), 1.0, 6.0, ((0, 32),))
    return dict(hidden_in=hidden_in, doc_ids=doc_ids, routes=routes, gain_attn=gain_attn, w_query=w_query, key_matrix=key_matrix, value_matrix=value_matrix, w_output=w_output, gain_ffn=gain_ffn, w_router=w_router, w_gateup=w_gateup, w_down=w_down, cotangent=cotangent)


EPS = 1e-05
BASE = 10000.0
SCORE_SCALE = 0.015625
MASKED = -1e+30

def rope_tables(doc_row):
    document_length = doc_row.shape[0]
    places = jnp.arange(document_length, dtype=jnp.int32)
    same_doc = doc_row[:, None] == doc_row[None, :]
    starts = lax.optimization_barrier(jnp.min(jnp.where(same_doc, places[None, :], document_length), axis=1))
    position = (places - starts).astype(jnp.float32)
    half_width = HEAD_SIZE // 2
    inverse = jnp.exp(-math.log(BASE) * (2.0 * jnp.arange(half_width, dtype=jnp.float32) / HEAD_SIZE))
    angle = position[:, None] * inverse[None, :]
    allowed = same_doc & (places[None, :] <= places[:, None])
    return (jnp.cos(angle), jnp.sin(angle), allowed)

def rotate(tensor, cosine_table, sine_table):
    half_width = HEAD_SIZE // 2
    first_half = tensor[..., :half_width]
    second = tensor[..., half_width:]
    cos_part = cosine_table[:, None, :]
    sin_part = sine_table[:, None, :]
    return jnp.concatenate([first_half * cos_part - second * sin_part, second * cos_part + first_half * sin_part], axis=-1)

def inverse_rotation(tensor, cosine_table, sine_table):
    half_width = HEAD_SIZE // 2
    first_half = tensor[..., :half_width]
    second = tensor[..., half_width:]
    cos_part = cosine_table[:, None, :]
    sin_part = sine_table[:, None, :]
    return jnp.concatenate([first_half * cos_part + second * sin_part, second * cos_part - first_half * sin_part], axis=-1)

def norm_forward(value_rows, gain):
    scale_inv = lax.rsqrt(lax.optimization_barrier(jnp.mean(value_rows * value_rows, axis=-1, keepdims=True)) + EPS)
    normed = value_rows * scale_inv
    return ((normed * gain).astype(jnp.bfloat16), normed, scale_inv)

def norm_backward(grad_out, normed, scale_inv, gain):
    grad_normed = grad_out * gain
    grad_gain = lax.optimization_barrier(jnp.sum(grad_out * normed, axis=0))
    value_gradients = scale_inv * (grad_normed - normed * lax.optimization_barrier(jnp.mean(grad_normed * normed, axis=-1, keepdims=True)))
    return (value_gradients, grad_gain)

def scores_of(query_rows, key_rows, allowed):
    document_length = query_rows.shape[0]
    group_rows = query_rows.reshape(document_length, KEY_VALUE_HEADS, QUERY_HEADS // KEY_VALUE_HEADS, HEAD_SIZE).astype(jnp.float32)
    scores = jnp.einsum('qgrd,kgd->grqk', group_rows, key_rows.astype(jnp.float32)) * SCORE_SCALE
    return jnp.where(allowed[None, None], scores, MASKED)

def forward_local(hidden_rows, doc_row, route_rows, gain_attn, w_query, key_matrix, value_matrix, w_output, gain_ffn, w_router):
    document_length = hidden_rows.shape[0]
    hidden_f = hidden_rows.astype(jnp.float32)
    attention_input, normed_attn, scale_attn = norm_forward(hidden_f, gain_attn)
    cosine_table, sine_table, allowed = rope_tables(doc_row)
    query_rows = jnp.dot(attention_input, w_query, preferred_element_type=jnp.float32).reshape(document_length, QUERY_HEADS, HEAD_SIZE)
    key_rows = jnp.dot(attention_input, key_matrix, preferred_element_type=jnp.float32).reshape(document_length, KEY_VALUE_HEADS, HEAD_SIZE)
    value_rows = jnp.dot(attention_input, value_matrix, preferred_element_type=jnp.float32).astype(jnp.bfloat16).reshape(document_length, KEY_VALUE_HEADS, HEAD_SIZE)
    query_rows = rotate(query_rows, cosine_table, sine_table).astype(jnp.bfloat16)
    key_rows = rotate(key_rows, cosine_table, sine_table).astype(jnp.bfloat16)
    scores = scores_of(query_rows, key_rows, allowed)
    top_score = lax.optimization_barrier(jnp.max(scores, axis=-1, keepdims=True))
    log_total = top_score + jnp.log(lax.optimization_barrier(jnp.sum(jnp.exp(scores - top_score), axis=-1, keepdims=True)))
    weights = jnp.exp(scores - log_total).astype(jnp.bfloat16)
    attention_mixed = jnp.einsum('grqk,kgd->qgrd', weights.astype(jnp.float32), value_rows.astype(jnp.float32))
    attention_mixed = attention_mixed.reshape(document_length, QUERY_HEADS * HEAD_SIZE).astype(jnp.bfloat16)
    resid = hidden_f + jnp.dot(attention_mixed, w_output, preferred_element_type=jnp.float32)
    ffn_in, normed_ffn, scale_ffn = norm_forward(resid, gain_ffn)
    logits = jnp.dot(ffn_in, w_router, preferred_element_type=jnp.float32)
    probs = jax.nn.softmax(logits, axis=-1)
    picks = route_rows[:, :, None] == jnp.arange(probs.shape[1], dtype=jnp.int32)[None, None, :]
    gates = lax.optimization_barrier(jnp.sum(jnp.where(picks, probs[:, None, :], 0.0), axis=-1))
    return (normed_attn, scale_attn, attention_input, cosine_table, sine_table, allowed, query_rows, key_rows, value_rows, attention_mixed, log_total, resid, ffn_in, normed_ffn, scale_ffn, probs, gates)

def backward_local(state, route_rows, cot_rows, grad_ffn_in, grad_gates, gain_attn, w_query, key_matrix, value_matrix, w_output, gain_ffn, w_router):
    normed_attn, scale_attn, attention_input, cosine_table, sine_table, allowed, query_rows, key_rows, value_rows, attention_mixed, log_total, resid, ffn_in, normed_ffn, scale_ffn, probs, gates = state
    document_length = attention_input.shape[0]
    query_group = QUERY_HEADS // KEY_VALUE_HEADS
    picks = route_rows[:, :, None] == jnp.arange(probs.shape[1], dtype=jnp.int32)[None, None, :]
    grad_probs = lax.optimization_barrier(jnp.sum(jnp.where(picks, grad_gates[:, :, None], 0.0), axis=1))
    grad_logits = (probs * (grad_probs - lax.optimization_barrier(jnp.sum(probs * grad_probs, axis=-1, keepdims=True)))).astype(jnp.bfloat16)
    grad_router = jnp.dot(ffn_in.T, grad_logits, preferred_element_type=jnp.float32)
    grad_ffn_in = grad_ffn_in + jnp.dot(grad_logits, w_router.T, preferred_element_type=jnp.float32)
    grad_resid_part, grad_gain_ffn = norm_backward(grad_ffn_in, normed_ffn, scale_ffn, gain_ffn)
    grad_resid = cot_rows.astype(jnp.float32) + grad_resid_part
    grad_attn = grad_resid.astype(jnp.bfloat16)
    grad_output = jnp.dot(attention_mixed.T, grad_attn, preferred_element_type=jnp.float32)
    mixed_gradient = jnp.dot(grad_attn, w_output.T, preferred_element_type=jnp.float32).astype(jnp.bfloat16)
    scores = scores_of(query_rows, key_rows, allowed)
    weights = jnp.exp(scores - log_total)
    weights_low = weights.astype(jnp.bfloat16).astype(jnp.float32)
    gradient_by_group = mixed_gradient.reshape(document_length, KEY_VALUE_HEADS, query_group, HEAD_SIZE).astype(jnp.float32)
    mixed_by_group = attention_mixed.reshape(document_length, KEY_VALUE_HEADS, query_group, HEAD_SIZE).astype(jnp.float32)
    value_gradients = jnp.einsum('grqk,qgrd->kgd', weights_low, gradient_by_group)
    grad_weights = jnp.einsum('qgrd,kgd->grqk', gradient_by_group, value_rows.astype(jnp.float32))
    delta = jnp.transpose(lax.optimization_barrier(jnp.sum(gradient_by_group * mixed_by_group, axis=-1)), (1, 2, 0))
    grad_scores = (weights * (grad_weights - delta[..., None]) * SCORE_SCALE).astype(jnp.bfloat16).astype(jnp.float32)
    query_by_group = query_rows.reshape(document_length, KEY_VALUE_HEADS, query_group, HEAD_SIZE).astype(jnp.float32)
    grad_query_rows = jnp.einsum('grqk,kgd->qgrd', grad_scores, key_rows.astype(jnp.float32)).reshape(document_length, QUERY_HEADS, HEAD_SIZE)
    key_row_gradient = jnp.einsum('grqk,qgrd->kgd', grad_scores, query_by_group)
    grad_query_rows = inverse_rotation(grad_query_rows, cosine_table, sine_table).reshape(document_length, QUERY_HEADS * HEAD_SIZE).astype(jnp.bfloat16)
    key_row_gradient = inverse_rotation(key_row_gradient, cosine_table, sine_table).reshape(document_length, KEY_VALUE_HEADS * HEAD_SIZE).astype(jnp.bfloat16)
    value_row_gradient = value_gradients.reshape(document_length, KEY_VALUE_HEADS * HEAD_SIZE).astype(jnp.bfloat16)
    grad_query = jnp.dot(attention_input.T, grad_query_rows, preferred_element_type=jnp.float32)
    grad_key = jnp.dot(attention_input.T, key_row_gradient, preferred_element_type=jnp.float32)
    grad_value = jnp.dot(attention_input.T, value_row_gradient, preferred_element_type=jnp.float32)
    grad_attn_in = jnp.dot(grad_query_rows, w_query.T, preferred_element_type=jnp.float32)
    grad_attn_in = grad_attn_in + jnp.dot(key_row_gradient, key_matrix.T, preferred_element_type=jnp.float32)
    grad_attn_in = grad_attn_in + jnp.dot(value_row_gradient, value_matrix.T, preferred_element_type=jnp.float32)
    grad_hidden_part, grad_gain_attn = norm_backward(grad_attn_in, normed_attn, scale_attn, gain_attn)
    grad_in = grad_resid + grad_hidden_part
    return (grad_in, (grad_query, grad_key, grad_value, grad_output, grad_router, grad_gain_attn, grad_gain_ffn))

def reference(hidden_in, doc_ids, routes, gain_attn, w_query, key_matrix, value_matrix, w_output, gain_ffn, w_router, w_gateup, w_down, cotangent):
    devices = N_FSDP * N_EXPERT
    half_units = FF // 2
    hidden_dev = hidden_in.reshape(devices, TOK_DEV, MODEL_WIDTH)
    routes_dev = routes.reshape(devices, TOK_DEV, TOP)
    cot_dev = cotangent.reshape(devices, TOK_DEV, MODEL_WIDTH)
    weights_attn = (gain_attn, w_query, key_matrix, value_matrix, w_output, gain_ffn, w_router)

    def forward_one(pieces):
        hidden_rows, doc_row, route_rows = pieces
        state = forward_local(hidden_rows, doc_row, route_rows, *weights_attn)
        return (state[11], state[12], state[16])
    resid_dev, ffn_dev, gates_dev = lax.map(forward_one, (hidden_dev, doc_ids, routes_dev))
    resid_all = resid_dev.reshape(TOKENS, MODEL_WIDTH)
    slot_total = TOKENS * TOP
    limit = devices * CAP
    route_flat = routes.reshape(slot_total)
    ffn_pad = jnp.concatenate([ffn_dev.reshape(TOKENS, MODEL_WIDTH), jnp.zeros((1, MODEL_WIDTH), jnp.bfloat16)], axis=0)
    gates_pad = jnp.concatenate([gates_dev.reshape(slot_total), jnp.zeros((1,), jnp.float32)], axis=0)
    cot_pad = jnp.concatenate([cotangent.astype(jnp.float32), jnp.zeros((1, MODEL_WIDTH), jnp.float32)], axis=0)

    def expert_slots(expert):
        chosen = route_flat == expert
        order = jnp.cumsum(chosen.astype(jnp.int32)) - 1
        target = jnp.where(chosen, order, limit).astype(jnp.int32)
        slot_of = jnp.full((limit,), slot_total, jnp.int32).at[target].set(jnp.arange(slot_total, dtype=jnp.int32), mode='drop')
        return (slot_of, slot_of // TOP)

    def expert_forward(expert):
        slot_of, token_of = expert_slots(expert)
        rows = ffn_pad[token_of]
        made = jnp.zeros((limit, MODEL_WIDTH), jnp.float32)
        parts = []
        for half in range(2):
            piece = 2 * expert + half
            gate_up = jnp.dot(rows, w_gateup[piece], preferred_element_type=jnp.float32)
            gate_part = gate_up[:, :half_units]
            up_part = gate_up[:, half_units:]
            acted = (jax.nn.silu(gate_part) * up_part).astype(jnp.bfloat16)
            made_half = jnp.dot(acted, w_down[piece], preferred_element_type=jnp.float32).astype(jnp.bfloat16)
            made = made + made_half.astype(jnp.float32)
            parts.append((gate_part, up_part, acted))
        made = lax.optimization_barrier(made.astype(jnp.bfloat16)).astype(jnp.float32)
        return (slot_of, token_of, rows, parts, made)

    def step_forward(combined, expert):
        slot_of, token_of, rows, parts, made = expert_forward(expert)
        combined = combined.at[token_of].add(gates_pad[slot_of][:, None] * made)
        return (combined, None)
    combined, unused = lax.scan(step_forward, jnp.zeros((TOKENS + 1, MODEL_WIDTH), jnp.float32), jnp.arange(EXPERT_COUNT, dtype=jnp.int32))
    block_out = (resid_all + combined[:TOKENS]).astype(jnp.bfloat16)

    def step_backward(carry, expert):
        grad_ffn, grad_gates = carry
        slot_of, token_of, rows, parts, made = expert_forward(expert)
        cot_rows = cot_pad[token_of]
        grad_gates = grad_gates.at[slot_of].set(lax.optimization_barrier(jnp.sum(cot_rows * made, axis=-1)))
        grad_made = (gates_pad[slot_of][:, None] * cot_rows).astype(jnp.bfloat16)
        grad_rows_all = jnp.zeros((limit, MODEL_WIDTH), jnp.float32)
        gateup_list = []
        down_list = []
        for half in range(2):
            piece = 2 * expert + half
            gate_part, up_part, acted = parts[half]
            grad_acted = jnp.dot(grad_made, w_down[piece].T, preferred_element_type=jnp.float32)
            down_list.append(jnp.dot(acted.T, grad_made, preferred_element_type=jnp.float32))
            sigma = jax.nn.sigmoid(gate_part)
            grad_gate = grad_acted * up_part * sigma * (1.0 + gate_part * (1.0 - sigma))
            grad_up = grad_acted * gate_part * sigma
            grad_joined = jnp.concatenate([grad_gate, grad_up], axis=-1).astype(jnp.bfloat16)
            gateup_list.append(jnp.dot(rows.T, grad_joined, preferred_element_type=jnp.float32))
            grad_rows = jnp.dot(grad_joined, w_gateup[piece].T, preferred_element_type=jnp.float32).astype(jnp.bfloat16)
            grad_rows_all = grad_rows_all + grad_rows.astype(jnp.float32)
        grad_rows_all = lax.optimization_barrier(grad_rows_all.astype(jnp.bfloat16)).astype(jnp.float32)
        grad_ffn = grad_ffn.at[token_of].add(grad_rows_all)
        return ((grad_ffn, grad_gates), (jnp.stack(gateup_list), jnp.stack(down_list)))
    start_carry = (jnp.zeros((TOKENS + 1, MODEL_WIDTH), jnp.float32), jnp.zeros((slot_total + 1,), jnp.float32))
    (grad_ffn, grad_gates), (grad_gateup, grad_down) = lax.scan(step_backward, start_carry, jnp.arange(EXPERT_COUNT, dtype=jnp.int32))
    grad_gateup = grad_gateup.reshape(2 * EXPERT_COUNT, MODEL_WIDTH, FF)
    grad_down = grad_down.reshape(2 * EXPERT_COUNT, half_units, MODEL_WIDTH)
    grad_ffn_dev = grad_ffn[:TOKENS].reshape(devices, TOK_DEV, MODEL_WIDTH)
    grad_gates_dev = grad_gates[:slot_total].reshape(devices, TOK_DEV, TOP)

    def step_device(totals, pieces):
        hidden_rows, doc_row, route_rows, cot_rows, grad_ffn_rows, grad_gate_rows = pieces
        state = forward_local(hidden_rows, doc_row, route_rows, *weights_attn)
        grad_in, grads = backward_local(state, route_rows, cot_rows, grad_ffn_rows, grad_gate_rows, *weights_attn)
        totals = tuple((total + part for total, part in zip(totals, grads)))
        return (totals, grad_in)
    initial_totals = (jnp.zeros((MODEL_WIDTH, QUERY_HEADS * HEAD_SIZE), jnp.float32), jnp.zeros((MODEL_WIDTH, KEY_VALUE_HEADS * HEAD_SIZE), jnp.float32), jnp.zeros((MODEL_WIDTH, KEY_VALUE_HEADS * HEAD_SIZE), jnp.float32), jnp.zeros((QUERY_HEADS * HEAD_SIZE, MODEL_WIDTH), jnp.float32), jnp.zeros((MODEL_WIDTH, EXPERT_COUNT), jnp.float32), jnp.zeros((MODEL_WIDTH,), jnp.float32), jnp.zeros((MODEL_WIDTH,), jnp.float32))
    totals, grad_in_dev = lax.scan(step_device, initial_totals, (hidden_dev, doc_ids, routes_dev, cot_dev, grad_ffn_dev, grad_gates_dev))
    grad_input = grad_in_dev.reshape(TOKENS, MODEL_WIDTH)
    return (block_out, grad_input, totals[0], totals[1], totals[2], totals[3], totals[4], totals[5], totals[6], grad_gateup, grad_down)
```

```python
import functools
import math

import jax
import jax.numpy as jnp
from jax import lax
from jax.experimental import pallas as pl
from jax.experimental.pallas import tpu as pltpu
from jax.sharding import PartitionSpec as P

MODEL_WIDTH = 1536
QUERY_HEADS = 24
KEY_VALUE_HEADS = 8
HEAD_SIZE = 64
TOP = 8
CAP = 48


EPS = 1e-05
BASE = 10000.0
SCORE_SCALE = 0.015625
MASKED = -1e30


def rope_tables(doc_row):
    document_length = doc_row.shape[0]
    places = jnp.arange(document_length, dtype=jnp.int32)
    same_doc = doc_row[:, None] == doc_row[None, :]
    starts = jnp.min(jnp.where(same_doc, places[None, :], document_length), axis=1)
    position = (places - starts).astype(jnp.float32)
    half_width = HEAD_SIZE // 2
    inverse = jnp.exp(
        -math.log(BASE) * (2.0 * jnp.arange(half_width, dtype=jnp.float32) / HEAD_SIZE)
    )
    angle = position[:, None] * inverse[None, :]
    allowed = same_doc & (places[None, :] <= places[:, None])
    return (jnp.cos(angle), jnp.sin(angle), allowed)


def rotate(tensor, cosine_table, sine_table):
    half_width = HEAD_SIZE // 2
    first_half = tensor[..., :half_width]
    second = tensor[..., half_width:]
    cos_part = cosine_table[:, None, :]
    sin_part = sine_table[:, None, :]
    return jnp.concatenate(
        [first_half * cos_part - second * sin_part, second * cos_part + first_half * sin_part],
        axis=-1,
    )


def inverse_rotation(tensor, cosine_table, sine_table):
    half_width = HEAD_SIZE // 2
    first_half = tensor[..., :half_width]
    second = tensor[..., half_width:]
    cos_part = cosine_table[:, None, :]
    sin_part = sine_table[:, None, :]
    return jnp.concatenate(
        [first_half * cos_part + second * sin_part, second * cos_part - first_half * sin_part],
        axis=-1,
    )


def norm_forward(value_rows, gain):
    scale_inv = lax.rsqrt(jnp.mean(value_rows * value_rows, axis=-1, keepdims=True) + EPS)
    normed = value_rows * scale_inv
    return ((normed * gain).astype(jnp.bfloat16), normed, scale_inv)


def norm_backward(grad_out, normed, scale_inv, gain):
    grad_normed = grad_out * gain
    grad_gain = jnp.sum(grad_out * normed, axis=0)
    value_gradients = scale_inv * (
        grad_normed - normed * jnp.mean(grad_normed * normed, axis=-1, keepdims=True)
    )
    return (value_gradients, grad_gain)


def scores_of(query_rows, key_rows, allowed):
    document_length = query_rows.shape[0]
    group_rows = query_rows.reshape(
        document_length, KEY_VALUE_HEADS, QUERY_HEADS // KEY_VALUE_HEADS, HEAD_SIZE
    )
    scores = (
        jnp.einsum("qgrd,kgd->grqk", group_rows, key_rows, preferred_element_type=jnp.float32)
        * SCORE_SCALE
    )
    return jnp.where(allowed[None, None], scores, MASKED)


def forward_local(
    hidden_rows,
    doc_row,
    route_rows,
    gain_attn,
    w_query,
    key_matrix,
    value_matrix,
    w_output,
    gain_ffn,
    w_router,
):
    document_length = hidden_rows.shape[0]
    hidden_f = hidden_rows.astype(jnp.float32)
    attention_input, normed_attn, scale_attn = norm_forward(hidden_f, gain_attn)
    cosine_table, sine_table, allowed = rope_tables(doc_row)
    query_rows = jnp.dot(attention_input, w_query, preferred_element_type=jnp.float32).reshape(
        document_length, QUERY_HEADS, HEAD_SIZE
    )
    key_rows = jnp.dot(attention_input, key_matrix, preferred_element_type=jnp.float32).reshape(
        document_length, KEY_VALUE_HEADS, HEAD_SIZE
    )
    value_rows = (
        jnp.dot(attention_input, value_matrix, preferred_element_type=jnp.float32)
        .astype(jnp.bfloat16)
        .reshape(document_length, KEY_VALUE_HEADS, HEAD_SIZE)
    )
    query_rows = rotate(query_rows, cosine_table, sine_table).astype(jnp.bfloat16)
    key_rows = rotate(key_rows, cosine_table, sine_table).astype(jnp.bfloat16)
    scores = scores_of(query_rows, key_rows, allowed)
    top_score = jnp.max(scores, axis=-1, keepdims=True)
    log_total = top_score + jnp.log(jnp.sum(jnp.exp(scores - top_score), axis=-1, keepdims=True))
    weights = jnp.exp(scores - log_total).astype(jnp.bfloat16)
    attention_mixed = jnp.einsum(
        "grqk,kgd->qgrd", weights, value_rows, preferred_element_type=jnp.float32
    )
    attention_mixed = attention_mixed.reshape(document_length, QUERY_HEADS * HEAD_SIZE).astype(
        jnp.bfloat16
    )
    resid = hidden_f + jnp.dot(attention_mixed, w_output, preferred_element_type=jnp.float32)
    ffn_in, normed_ffn, scale_ffn = norm_forward(resid, gain_ffn)
    logits = jnp.dot(ffn_in, w_router, preferred_element_type=jnp.float32)
    probs = jax.nn.softmax(logits, axis=-1)
    picks = route_rows[:, :, None] == jnp.arange(probs.shape[1], dtype=jnp.int32)[None, None, :]
    gates = jnp.sum(jnp.where(picks, probs[:, None, :], 0.0), axis=-1)
    return (
        normed_attn,
        scale_attn,
        attention_input,
        cosine_table,
        sine_table,
        allowed,
        query_rows,
        key_rows,
        value_rows,
        attention_mixed,
        log_total,
        resid,
        ffn_in,
        normed_ffn,
        scale_ffn,
        probs,
        gates,
    )


def backward_local(
    state,
    route_rows,
    cot_rows,
    grad_ffn_in,
    grad_gates,
    gain_attn,
    w_query,
    key_matrix,
    value_matrix,
    w_output,
    gain_ffn,
    w_router,
):
    (
        normed_attn,
        scale_attn,
        attention_input,
        cosine_table,
        sine_table,
        allowed,
        query_rows,
        key_rows,
        value_rows,
        attention_mixed,
        log_total,
        resid,
        ffn_in,
        normed_ffn,
        scale_ffn,
        probs,
        gates,
    ) = state
    document_length = attention_input.shape[0]
    query_group = QUERY_HEADS // KEY_VALUE_HEADS
    grad_probs = jnp.where(route_rows, grad_gates, 0.0)
    grad_logits = (
        probs * (grad_probs - jnp.sum(probs * grad_probs, axis=-1, keepdims=True))
    ).astype(jnp.bfloat16)
    grad_router = jnp.dot(ffn_in.T, grad_logits, preferred_element_type=jnp.float32)
    grad_ffn_in = grad_ffn_in + jnp.dot(grad_logits, w_router.T, preferred_element_type=jnp.float32)
    grad_resid_part, grad_gain_ffn = norm_backward(grad_ffn_in, normed_ffn, scale_ffn, gain_ffn)
    grad_resid = cot_rows.astype(jnp.float32) + grad_resid_part
    grad_attn = grad_resid.astype(jnp.bfloat16)
    grad_output = jnp.dot(attention_mixed.T, grad_attn, preferred_element_type=jnp.float32)
    mixed_gradient = jnp.dot(grad_attn, w_output.T, preferred_element_type=jnp.float32).astype(
        jnp.bfloat16
    )
    scores = scores_of(query_rows, key_rows, allowed)
    weights = jnp.exp(scores - log_total)
    weights_low = weights.astype(jnp.bfloat16)
    gradient_by_group = mixed_gradient.reshape(
        document_length, KEY_VALUE_HEADS, query_group, HEAD_SIZE
    )
    mixed_by_group = attention_mixed.reshape(
        document_length, KEY_VALUE_HEADS, query_group, HEAD_SIZE
    )
    value_gradients = jnp.einsum(
        "grqk,qgrd->kgd", weights_low, gradient_by_group, preferred_element_type=jnp.float32
    )
    grad_weights = jnp.einsum(
        "qgrd,kgd->grqk", gradient_by_group, value_rows, preferred_element_type=jnp.float32
    )
    delta = jnp.transpose(
        jnp.sum(
            gradient_by_group.astype(jnp.float32) * mixed_by_group.astype(jnp.float32), axis=-1
        ),
        (1, 2, 0),
    )
    grad_scores = (weights * (grad_weights - delta[..., None]) * SCORE_SCALE).astype(jnp.bfloat16)
    query_by_group = query_rows.reshape(document_length, KEY_VALUE_HEADS, query_group, HEAD_SIZE)
    grad_query_rows = jnp.einsum(
        "grqk,kgd->qgrd", grad_scores, key_rows, preferred_element_type=jnp.float32
    ).reshape(document_length, QUERY_HEADS, HEAD_SIZE)
    key_row_gradient = jnp.einsum(
        "grqk,qgrd->kgd", grad_scores, query_by_group, preferred_element_type=jnp.float32
    )
    grad_query_rows = (
        inverse_rotation(grad_query_rows, cosine_table, sine_table)
        .reshape(document_length, QUERY_HEADS * HEAD_SIZE)
        .astype(jnp.bfloat16)
    )
    key_row_gradient = (
        inverse_rotation(key_row_gradient, cosine_table, sine_table)
        .reshape(document_length, KEY_VALUE_HEADS * HEAD_SIZE)
        .astype(jnp.bfloat16)
    )
    value_row_gradient = value_gradients.reshape(
        document_length, KEY_VALUE_HEADS * HEAD_SIZE
    ).astype(jnp.bfloat16)
    grad_query = jnp.dot(attention_input.T, grad_query_rows, preferred_element_type=jnp.float32)
    grad_key = jnp.dot(attention_input.T, key_row_gradient, preferred_element_type=jnp.float32)
    grad_value = jnp.dot(attention_input.T, value_row_gradient, preferred_element_type=jnp.float32)
    grad_attn_in = jnp.dot(grad_query_rows, w_query.T, preferred_element_type=jnp.float32)
    grad_attn_in = grad_attn_in + jnp.dot(
        key_row_gradient, key_matrix.T, preferred_element_type=jnp.float32
    )
    grad_attn_in = grad_attn_in + jnp.dot(
        value_row_gradient, value_matrix.T, preferred_element_type=jnp.float32
    )
    grad_hidden_part, grad_gain_attn = norm_backward(
        grad_attn_in, normed_attn, scale_attn, gain_attn
    )
    grad_in = grad_resid + grad_hidden_part
    return (
        grad_in,
        (grad_query, grad_key, grad_value, grad_output, grad_router, grad_gain_attn, grad_gain_ffn),
    )


MESH = pl.DeviceIdType.MESH
F32, BF16 = jnp.float32, jnp.bfloat16


def dot(a, b, da=1, db=0):
    return lax.dot_general(a, b, (((da,), (db,)), ((), ())), preferred_element_type=F32)


class Place:
    def __init__(self, shards, owners):
        self.shards, self.owners = shards, owners
        self.line = 4 if owners % 4 == 0 else 1
        self.side = owners // self.line
        self.chips = shards // 2
        self.f = lax.axis_index("fsdp")
        self.e = lax.axis_index("expert")
        self.a, self.b = self.e // self.side, self.e % self.side
        self.x, self.c = self.f // 2, self.f % 2

    def others(self):
        out = [((self.f, self.e + self.side), self.a < self.line - 1)]
        out.append(((self.f, self.e - self.side), self.a > 0))
        for i in range(1, self.side):
            out.append(((self.f, self.a * self.side + (self.b + i) % self.side), None))
        out.append(((self.x * 2 + 1 - self.c, self.e), None))
        for i in range(1, self.chips):
            out.append((((self.x + i) % self.chips * 2 + self.c, self.e), None))
        return out

    def meet(self):
        bar = pltpu.get_barrier_semaphore()
        for dev, cond in self.others():

            def signal(dev=dev):
                pl.semaphore_signal(bar, inc=1, device_id=dev, device_id_type=MESH)

            if cond is None:
                signal()
            else:
                pl.when(cond)(signal)
        count = self.side - 1 + 1 + self.chips - 1
        pl.semaphore_wait(
            bar,
            count
            + jnp.where(self.a < self.line - 1, 1, 0)
            + jnp.where(self.a > 0, 1, 0),
        )


def remote(src, dst, send, recv, dev):
    return pltpu.make_async_remote_copy(
        src_ref=src, dst_ref=dst, send_sem=send, recv_sem=recv, device_id=dev, device_id_type=MESH
    )


class LineGather:
    def __init__(self, at, buf, send, recv):
        self.at, self.buf, self.send, self.recv = at, buf, send, recv

    def up(self, k):
        at = self.at
        return remote(
            self.buf.at[k], self.buf.at[k], self.send.at[0, k], self.recv.at[k], (at.f, at.e + at.side)
        )

    def down(self, k):
        at = self.at
        return remote(
            self.buf.at[k], self.buf.at[k], self.send.at[1, k], self.recv.at[k], (at.f, at.e - at.side)
        )

    def across(self, k, i):
        at = self.at
        dev = (at.f, at.a * at.side + (at.b + i) % at.side)
        return remote(
            self.buf.at[k], self.buf.at[k], self.send.at[1 + i, k], self.recv.at[k], dev
        )

    def begin(self):
        at = self.at

        @pl.when(at.a < at.line - 1)
        def _():
            self.up(at.e).start()

        @pl.when(at.a > 0)
        def _():
            self.down(at.e).start()

        for i in range(1, at.side):
            self.across(at.e, i).start()

    def relay(self):
        at = self.at
        for s in range(1, at.line):

            @pl.when(at.a - s >= 0)
            def _(s=s):
                k = at.e - s * at.side
                self.down(k).wait_recv()

                @pl.when(at.a < at.line - 1)
                def _():
                    self.up(k).start()

                for i in range(1, at.side):
                    self.across(k, i).start()

            @pl.when(at.a + s < at.line)
            def _(s=s):
                k = at.e + s * at.side
                self.up(k).wait_recv()

                @pl.when(at.a > 0)
                def _():
                    self.down(k).start()

                for i in range(1, at.side):
                    self.across(k, i).start()

    def each(self, use):
        at = self.at

        def step(i, carry):
            k = (at.a + i) % at.line * at.side + (at.b + i // at.line) % at.side

            @pl.when(i >= at.line)
            def _():
                self.across(k, 1).wait_recv()

            use(k)
            return carry

        lax.fori_loop(0, at.owners, step, 0)

    def finish(self):
        at = self.at
        for s in range(at.line):
            k = s * at.side + at.b

            @pl.when((at.a < at.line - 1) & (at.a >= s))
            def _():
                self.up(k).wait_send()

            @pl.when((at.a > 0) & (at.a <= s))
            def _():
                self.down(k).wait_send()

            for i in range(1, at.side):
                self.across(k, i).wait_send()


class LineScatter:
    def __init__(self, at, part, side_in, line_in, own, sems):
        self.at, self.part, self.side_in, self.line_in, self.own = at, part, side_in, line_in, own
        self.ssend, self.srecv, self.lsend, self.lrecv = sems

    def across(self, s, i):
        at = self.at
        b = (at.b + i) % at.side
        j = at.side - 1 - i
        return remote(
            self.part.at[s * at.side + b],
            self.side_in.at[s, j],
            self.ssend.at[s, i - 1],
            self.srecv.at[s, j],
            (at.f, at.a * at.side + b),
        )

    def along(self, s, dev, slot):
        at = self.at
        return remote(
            self.part.at[s * at.side + at.b],
            self.line_in.at[slot],
            self.lsend.at[s],
            self.lrecv.at[slot],
            (at.f, dev),
        )

    def up(self, s):
        return self.along(s, self.at.e + self.at.side, s)

    def down(self, s):
        at = self.at
        return self.along(s, at.e - at.side, jnp.where(s == at.a - 1, at.line, s))

    def place(self, i):
        at = self.at
        return jnp.where(at.a < at.line // 2, at.line - 1 - i, i)

    def begin(self, make):
        at = self.at

        def step(n, carry):
            s, i = self.place(n % at.line), n // at.line + 1
            make(s * at.side + (at.b + i) % at.side)

            @pl.when(i < at.side)
            def _():
                self.across(s, i).start()

            return carry

        lax.fori_loop(0, at.owners, step, 0)

    def sum(self):
        at = self.at

        def step(n, carry):
            s = self.place(n)
            k = s * at.side + at.b
            for i in range(1, at.side):
                self.across(s, i).wait_recv()
            total = self.part[k].astype(F32)
            for j in range(at.side - 1):
                total = total + self.side_in[s, j].astype(F32)
            self.own[...] = total

            @pl.when(((s > at.a) & (at.a > 0)) | ((s < at.a) & (at.a < at.line - 1)))
            def _():
                self.along(s, at.e, s).wait_recv()
                self.own[...] += self.line_in[s].astype(F32)

            self.part[k] = self.own[...].astype(BF16)

            @pl.when(s > at.a)
            def _():
                self.up(s).start()

            @pl.when(s < at.a)
            def _():
                self.down(s).start()

            return carry

        lax.fori_loop(0, at.line, step, 0)
        total = self.part[at.e].astype(F32)
        self.own[...] = total

        @pl.when(at.a > 0)
        def _():
            self.along(at.a, at.e, at.a).wait_recv()
            self.own[...] += self.line_in[at.a].astype(F32)

        @pl.when(at.a < at.line - 1)
        def _():
            self.along(at.a, at.e, at.line).wait_recv()
            self.own[...] += self.line_in[at.line].astype(F32)

    def finish(self):
        at = self.at
        for s in range(at.line):
            for i in range(1, at.side):
                self.across(s, i).wait_send()

            @pl.when(at.a < s)
            def _(s=s):
                self.up(s).wait_send()

            @pl.when(at.a > s)
            def _(s=s):
                self.down(s).wait_send()


def moe_kernel(sizes, sent, cot, wgu, wd, comb_out, back_out, sums, far, *scratch):
    shards, owners, tokens, experts, held, pairing = sizes
    (rows_all, cot_all, taken, cots, slot_gate, place, wg_buf, wd_buf, gg, gd, from_core, to_far,
     own_sum, z_acc, dx_acc, dg_acc, side1, line1, side2, line2, own2,
     rs, rr, cs, cr, wsem, coresend, corerecv, farsend, farrecv, osem, free, s1, s2, s3, s4, t1, t2, t3, t4,
     ) = scratch
    at = Place(shards, owners)
    groups = held // pairing
    slots = groups * CAP
    half = wd.shape[1]
    rg, rd = MODEL_WIDTH // shards, half // shards
    width = MODEL_WIDTH + 128

    def weights(h, slot):
        return (
            pltpu.make_async_copy(wgu.at[h], wg_buf.at[slot], wsem.at[0, slot]),
            pltpu.make_async_copy(wd.at[h], wd_buf.at[slot], wsem.at[1, slot]),
        )

    for c in weights(0, 0):
        c.start()
    at.meet()
    rows = LineGather(at, rows_all, rs, rr)
    cotg = LineGather(at, cot_all, cs, cr)
    c1 = pltpu.make_async_copy(sent, rows_all.at[at.e], osem.at[0, 0])
    c2 = pltpu.make_async_copy(cot, cot_all.at[at.e], osem.at[0, 1])
    c1.start()
    c2.start()
    c1.wait()
    rows.begin()
    rows.relay()
    c2.wait()
    cotg.begin()

    lane = lax.broadcasted_iota(jnp.int32, (128, slots), 1)
    row = lax.broadcasted_iota(jnp.int32, (128, slots), 0)

    def expert_of(j):
        return (at.e * held + j // CAP * pairing) // 2

    e_lane = expert_of(lane)
    find_rank = (row == e_lane).astype(F32).astype(BF16)
    slot_rank = (lane % CAP).astype(F32)
    e_row = expert_of(lax.broadcasted_iota(jnp.int32, (slots, 128), 0))
    col = lax.broadcasted_iota(jnp.int32, (slots, 128), 1)
    pick_gate = (col == e_row + experts) | (col == e_row + 2 * experts)

    def dispatch_rows(k):
        rank_at = dot(rows_all[k, :, MODEL_WIDTH:], find_rank)
        pt = jnp.where(rank_at == slot_rank, 1.0, 0.0).astype(BF16)
        place[k] = pt
        got = dot(pt, rows_all[k], 0, 0)
        gate = jnp.sum(jnp.where(pick_gate, got[:, MODEL_WIDTH:], 0.0), axis=1, keepdims=True)
        gate = jnp.broadcast_to(gate, (slots, 128))
        to = pl.ds(k * CAP, CAP)
        for g in range(groups):
            taken[g, to, :] = got[g * CAP : (g + 1) * CAP, :MODEL_WIDTH].astype(BF16)
            slot_gate[g, to, :] = gate[g * CAP : (g + 1) * CAP]

    def dispatch_cot(k):
        got = dot(place[k], cot_all[k], 0, 0).astype(BF16)
        to = pl.ds(k * CAP, CAP)
        for g in range(groups):
            cots[g, to, :] = got[g * CAP : (g + 1) * CAP]

    rows.each(dispatch_rows)
    cotg.relay()
    cotg.each(dispatch_cot)

    def to_core(h, slot):
        out = []
        for i in range(at.chips):
            f = 2 * i + 1 - at.c
            for n, (buf, r, o) in enumerate(((gg, rg, 0), (gd, rd, 1))):
                out.append(
                    remote(
                        buf.at[slot, pl.ds(pl.multiple_of(f * r, r), r)],
                        from_core[o].at[slot, i],
                        coresend.at[slot, n, i],
                        corerecv.at[slot, n, i],
                        (at.x * 2 + 1 - at.c, at.e),
                    )
                )
        return out

    def to_chips(h):
        out = []
        for i in range(1, at.chips):
            j = at.chips - 1 - i
            dev = ((at.x + i) % at.chips * 2 + at.c, at.e)
            for n in range(2):
                out.append(
                    remote(
                        to_far[n].at[h, i - 1],
                        far[n].at[j, h],
                        farsend.at[n, i - 1, h],
                        farrecv.at[n, j, h],
                        dev,
                    )
                )
        return out

    def own_copy(h, slot):
        return [
            pltpu.make_async_copy(own_sum[n].at[slot], sums[n].at[h], osem.at[n, slot])
            for n in range(2)
        ]

    def add(h, slot):
        for c in to_core(h, slot):
            c.wait()

        @pl.when(h >= 2)
        def _():
            for c in own_copy(h, slot):
                c.wait()

        for i in range(at.chips):
            x = (at.x + i) % at.chips
            f = 2 * x + at.c
            for n, (buf, r) in enumerate(((gg, rg), (gd, rd))):
                mine = buf[slot, pl.ds(pl.multiple_of(f * r, r), r)].astype(F32)
                total = (mine + from_core[n][slot, x].astype(F32)).astype(BF16)
                if i == 0:
                    own_sum[n][slot] = total
                else:
                    to_far[n][h, i - 1] = total
        for c in to_chips(h):
            c.start()
        for c in own_copy(h, slot):
            c.start()

        @pl.when(h < held - 2)
        def _():
            pl.semaphore_signal(
                free, inc=1, device_id=(at.x * 2 + 1 - at.c, at.e), device_id_type=MESH
            )

    def step(h, carry):
        slot = h % 2
        g, m = h // pairing, h % pairing
        for c in weights(h, slot):
            c.wait()

        @pl.when(h + 1 < held)
        def _():
            for c in weights(h + 1, 1 - slot):
                c.start()

        @pl.when(m == 0)
        def _():
            z_acc[...] = jnp.zeros_like(z_acc)
            dx_acc[...] = jnp.zeros_like(dx_acc)
            dg_acc[...] = jnp.zeros_like(dg_acc)

        gu = dot(taken[g], wg_buf[slot])
        a, b = gu[:, :half], gu[:, half:]
        gate = slot_gate[g][:, :1]
        sig = 1.0 / (1.0 + jnp.exp(-a))
        s = a * sig
        act = s * b
        actg = (act * gate).astype(BF16)
        dp = dot(cots[g], wd_buf[slot], 1, 1)
        dg_acc[...] += jnp.broadcast_to(
            jnp.sum(act * dp, axis=1, keepdims=True), dg_acc.shape
        )
        dact = dp * gate
        da = dact * b * sig * (1.0 + a * (1.0 - sig))
        db = dact * s
        du = jnp.concatenate([da, db], axis=1).astype(BF16)
        z_acc[...] += dot(actg, wd_buf[slot])
        dx_acc[...] += dot(du, wg_buf[slot], 1, 1)
        for i in range(3):
            n = MODEL_WIDTH // 3
            gg[slot, i * n : (i + 1) * n, :] = dot(
                taken[g, :, i * n : (i + 1) * n], du, 0, 0
            ).astype(BF16)
        gd[slot] = dot(actg, cots[g], 0, 0).astype(BF16)

        @pl.when(h >= 2)
        def _():
            pl.semaphore_wait(free, 1)

        for c in to_core(h, slot):
            c.start()

        @pl.when(h > 0)
        def _():
            add(h - 1, 1 - slot)

        @pl.when(m == pairing - 1)
        def _():
            taken[g] = z_acc[...].astype(BF16)
            cots[g] = dx_acc[...].astype(BF16)
            slot_gate[g] = dg_acc[...]

        return carry

    lax.fori_loop(0, held, step, 0)
    add(held - 1, (held - 1) % 2)

    rows.finish()
    cotg.finish()

    home = (col == e_row).astype(F32).astype(BF16)
    home_low = (col == e_row + experts).astype(F32).astype(BF16)

    def make_back(k):
        to = pl.ds(k * CAP, CAP)
        dx = jnp.concatenate([cots[g, to, :] for g in range(groups)], axis=0)
        dg = jnp.concatenate([slot_gate[g, to, :] for g in range(groups)], axis=0)
        high = dg.astype(BF16)
        low = (dg - high.astype(F32)).astype(BF16)
        dgm = high * home + low * home_low
        pt = place[k]
        rows_all[k, :, :MODEL_WIDTH] = dot(pt, dx).astype(BF16)
        rows_all[k, :, MODEL_WIDTH:] = dot(pt, dgm).astype(BF16)

    def make_comb(k):
        to = pl.ds(k * CAP, CAP)
        y = jnp.concatenate([taken[g, to, :] for g in range(groups)], axis=0)
        cot_all[k] = dot(place[k], y).astype(BF16)

    back = LineScatter(at, rows_all, side1, line1, back_out, (s1, s2, s3, s4))
    comb = LineScatter(at, cot_all, side2, line2, own2, (t1, t2, t3, t4))
    back.begin(make_back)
    comb.begin(make_comb)
    back.sum()
    comb.sum()
    comb_out[...] = own2[...]
    back.finish()
    comb.finish()
    for h in range(held - 2, held):
        for c in own_copy(h, h % 2):
            c.wait()

    def drain(h, carry):
        for c in to_chips(h):
            c.wait()
        return carry

    lax.fori_loop(0, held, drain, 0)


def moe(sizes, sent, cot, wgu, wd):
    shards, owners, tokens, experts, held, pairing = sizes
    groups = held // pairing
    slots, rows = groups * CAP, owners * CAP
    hidden, half = wgu.shape[2], wd.shape[1]
    rg, rd = MODEL_WIDTH // shards, half // shards
    chips = shards // 2
    line = 4 if owners % 4 == 0 else 1
    side = owners // line
    width = MODEL_WIDTH + 128
    vm, dma = pltpu.VMEM, pltpu.SemaphoreType.DMA
    any_, vmem = pl.BlockSpec(memory_space=pl.ANY), pl.BlockSpec(memory_space=pltpu.VMEM)

    def pair(lead, dtype=BF16):
        return (vm((*lead, rg, hidden), dtype), vm((*lead, rd, MODEL_WIDTH), dtype))

    def outs(lead):
        return (
            jax.ShapeDtypeStruct((*lead, rg, hidden), BF16),
            jax.ShapeDtypeStruct((*lead, rd, MODEL_WIDTH), BF16),
        )

    def scatter_sems():
        return [dma((line, side)), dma((line, side)), dma((line,)), dma((line + 1,))]

    return pl.pallas_call(
        functools.partial(moe_kernel, sizes),
        name="moe",
        out_shape=(
            jax.ShapeDtypeStruct((tokens, MODEL_WIDTH), F32),
            jax.ShapeDtypeStruct((tokens, width), F32),
            outs((held,)),
            outs((chips - 1, held)),
        ),
        in_specs=[any_] * 4,
        out_specs=(vmem, vmem, (any_, any_), (any_, any_)),
        scratch_shapes=[
            vm((owners, tokens, width), BF16),
            vm((owners, tokens, MODEL_WIDTH), BF16),
            vm((groups, rows, MODEL_WIDTH), BF16),
            vm((groups, rows, MODEL_WIDTH), BF16),
            vm((groups, rows, 128), F32),
            vm((owners, tokens, slots), BF16),
            vm((2, MODEL_WIDTH, hidden), BF16),
            vm((2, half, MODEL_WIDTH), BF16),
            vm((2, MODEL_WIDTH, hidden), BF16),
            vm((2, half, MODEL_WIDTH), BF16),
            pair((2, chips)),
            pair((held, chips - 1)),
            pair((2,)),
            vm((rows, MODEL_WIDTH), F32),
            vm((rows, MODEL_WIDTH), F32),
            vm((rows, 128), F32),
            vm((line, side - 1, tokens, width), BF16),
            vm((line + 1, tokens, width), BF16),
            vm((line, side - 1, tokens, MODEL_WIDTH), BF16),
            vm((line + 1, tokens, MODEL_WIDTH), BF16),
            vm((tokens, MODEL_WIDTH), F32),
            dma((side + 1, owners)),
            dma((owners,)),
            dma((side + 1, owners)),
            dma((owners,)),
            dma((2, 2)),
            dma((2, 2, chips)),
            dma((2, 2, chips)),
            dma((2, chips - 1, held)),
            dma((2, chips - 1, held)),
            dma((2, 2)),
            pltpu.SemaphoreType.REGULAR,
            *scatter_sems(),
            *scatter_sems(),
        ],
        compiler_params=pltpu.CompilerParams(
            collective_id=1, has_side_effects=True, vmem_limit_bytes=63 * 2**20
        ),
    )(sent, cot, wgu, wd)


def plain_local(
    hidden_in,
    doc_ids,
    routes,
    gain_attn,
    w_query,
    key_matrix,
    value_matrix,
    w_output,
    gain_ffn,
    w_router,
    w_gateup,
    w_down,
    cotangent,
):
    tokens = hidden_in.shape[0]
    experts = w_router.shape[1]
    shards = lax.axis_size("fsdp")
    owners = lax.axis_size("expert")
    held = w_gateup.shape[0]
    half = w_down.shape[1]
    hidden_units = w_gateup.shape[2]
    pairing = 2 if held % 2 == 0 else 1
    groups = held // pairing
    slots = groups * CAP
    mine = lax.axis_index("expert")
    f32, bf16 = jnp.float32, jnp.bfloat16

    first = lax.all_gather(
        jnp.concatenate([w_query, key_matrix, value_matrix, w_router], axis=1),
        "fsdp",
        axis=0,
        tiled=True,
    )
    full_query, full_key, full_value, full_router = jnp.split(first, (1536, 2048, 2560), axis=1)
    full_output = lax.all_gather(w_output, "fsdp", axis=0, tiled=True)
    cot_all = lax.all_gather(cotangent, "expert", axis=0)
    weights_attn = (gain_attn, full_query, full_key, full_value, full_output, gain_ffn, full_router)
    state = forward_local(hidden_in, doc_ids[0], routes, *weights_attn)
    resid, ffn_in, probs = state[11], state[12], state[15]

    chosen = jnp.any(
        routes[:, :, None] == jnp.arange(experts, dtype=jnp.int32)[None, None, :], axis=1
    )
    below = jnp.tril(jnp.ones((tokens, tokens), bf16), -1)
    rank = jnp.dot(below, chosen.astype(bf16), preferred_element_type=f32)
    rank = jnp.where(chosen, rank, -1.0)
    gate = jnp.where(chosen, probs, 0.0)
    gate_high = gate.astype(bf16)
    gate_low = (gate - gate_high.astype(f32)).astype(bf16)
    meta = jnp.concatenate([rank.astype(bf16), gate_high, gate_low], axis=1)
    sent = jnp.concatenate(
        [ffn_in, meta, jnp.zeros((tokens, 128 - 3 * experts), bf16)], axis=1
    )
    got = lax.all_gather(sent, "expert", axis=0)
    rows_all = got[:, :, :MODEL_WIDTH]
    meta_all = got[:, :, MODEL_WIDTH:]
    lane = jnp.arange(slots, dtype=jnp.int32)
    slot_expert = (mine * held + (lane // CAP) * pairing) // 2
    spread = (jnp.arange(experts, dtype=jnp.int32)[:, None] == slot_expert[None, :]).astype(bf16)
    rank_at = jnp.dot(meta_all[:, :, :experts], spread, preferred_element_type=f32)
    gate_at = jnp.dot(
        meta_all[:, :, experts : 2 * experts], spread, preferred_element_type=f32
    ) + jnp.dot(meta_all[:, :, 2 * experts : 3 * experts], spread, preferred_element_type=f32)
    place = rank_at == (lane % CAP).astype(f32)[None, None, :]
    onehot = place.astype(bf16)
    gated = jnp.where(place, gate_at, 0.0)
    slot_gate = jnp.sum(gated, axis=1)

    def dispatch(rows):
        out = jnp.einsum("stj,std->sjd", onehot, rows, preferred_element_type=f32)
        return out.reshape(owners, groups, CAP, MODEL_WIDTH)

    taken = dispatch(rows_all).astype(bf16)
    cot_rows = dispatch(cot_all)
    slot_gate_4 = slot_gate.reshape(owners, groups, CAP, 1)
    grads_in = (cot_rows * slot_gate_4).astype(bf16)
    w_pairs = w_gateup.reshape(groups, pairing, MODEL_WIDTH, hidden_units)
    down_pairs = w_down.reshape(groups, pairing, half, MODEL_WIDTH)
    gate_up = jnp.einsum("secd,emdf->emscf", taken, w_pairs, preferred_element_type=f32)
    a, b = gate_up[..., :half], gate_up[..., half:]
    sigma = jax.nn.sigmoid(a)
    acted = (a * sigma * b).astype(bf16)
    made = jnp.einsum("emscf,emfd->secd", acted, down_pairs, preferred_element_type=f32)
    made = made.astype(bf16)
    grad_slot = jnp.sum(made.astype(f32) * cot_rows, axis=-1).reshape(owners, slots)
    grad_gate_back = jnp.where(place, grad_slot[:, None, :], 0.0).reshape(
        owners, tokens, groups, CAP
    )
    grad_gate_back = jnp.sum(grad_gate_back, axis=-1)
    onto = (
        (mine * held + jnp.arange(groups) * pairing)[:, None] // 2
        == jnp.arange(128, dtype=jnp.int32)[None, :]
    ).astype(bf16)
    grad_gate_back = jnp.dot(
        grad_gate_back.astype(bf16), onto, preferred_element_type=f32
    ).astype(bf16)
    weighted = (made.astype(f32) * slot_gate_4).astype(bf16).reshape(owners, slots, MODEL_WIDTH)
    combined = jnp.einsum("stj,sjd->std", onehot, weighted, preferred_element_type=f32)
    grad_acted = jnp.einsum("secd,emfd->emscf", grads_in, down_pairs, preferred_element_type=f32)
    grad_down = jnp.einsum("emscf,secd->emfd", acted, grads_in, preferred_element_type=f32)
    grad_a = grad_acted * b * sigma * (1.0 + a * (1.0 - sigma))
    grad_b = grad_acted * a * sigma
    joined = jnp.concatenate([grad_a, grad_b], axis=-1).astype(bf16)
    grad_gateup = jnp.einsum("secd,emscf->emdf", taken, joined, preferred_element_type=f32)
    grad_rows = jnp.einsum("emscf,emdf->secd", joined, w_pairs, preferred_element_type=f32)
    grad_rows = grad_rows.astype(bf16).reshape(owners, slots, MODEL_WIDTH)
    grad_ffn = jnp.einsum("stj,sjd->std", onehot, grad_rows, preferred_element_type=f32)
    back = jnp.concatenate([grad_ffn.astype(bf16), grad_gate_back], axis=-1)
    back = lax.psum_scatter(
        back.reshape(owners * tokens, -1), "expert", scatter_dimension=0, tiled=True
    ).astype(f32)
    grad_ffn, grad_gate_dense = back[:, :MODEL_WIDTH], back[:, MODEL_WIDTH : MODEL_WIDTH + experts]
    combined = lax.psum_scatter(
        combined.astype(bf16).reshape(owners * tokens, -1),
        "expert",
        scatter_dimension=0,
        tiled=True,
    )
    block_out = (resid + combined.astype(f32)).astype(bf16)
    grad_gateup, grad_down = (
        lax.psum_scatter(
            grad_gateup.reshape(held, MODEL_WIDTH, hidden_units).astype(bf16),
            "fsdp",
            scatter_dimension=1,
            tiled=True,
        ).astype(f32),
        lax.psum_scatter(
            grad_down.reshape(held, half, MODEL_WIDTH).astype(bf16),
            "fsdp",
            scatter_dimension=1,
            tiled=True,
        ).astype(f32),
    )
    grad_input, grads = backward_local(
        state, chosen, cotangent, grad_ffn, grad_gate_dense, *weights_attn
    )
    widths = [g.shape[1] if g.ndim == 2 else 1 for g in grads]
    flat = jnp.concatenate([g if g.ndim == 2 else g[:, None] for g in grads], axis=1)
    share = lax.psum_scatter(flat.astype(bf16), "fsdp", scatter_dimension=0, tiled=True)
    total = lax.psum(share, "expert").astype(f32)
    pieces = jnp.split(total, [sum(widths[: i + 1]) for i in range(len(widths) - 1)], axis=1)
    pieces = [p if g.ndim == 2 else p[:, 0] for p, g in zip(pieces, grads)]
    return (block_out, grad_input, *pieces, grad_gateup, grad_down)


def kernel_local(
    hidden_in,
    doc_ids,
    routes,
    gain_attn,
    w_query,
    key_matrix,
    value_matrix,
    w_output,
    gain_ffn,
    w_router,
    w_gateup,
    w_down,
    cotangent,
):
    tokens = hidden_in.shape[0]
    experts = w_router.shape[1]
    shards = lax.axis_size("fsdp")
    owners = lax.axis_size("expert")
    held = w_gateup.shape[0]
    pairing = 2 if held % 2 == 0 else 1
    f32, bf16 = jnp.float32, jnp.bfloat16

    first = lax.all_gather(
        jnp.concatenate([w_query, key_matrix, value_matrix, w_router], axis=1),
        "fsdp",
        axis=0,
        tiled=True,
    )
    full_query, full_key, full_value, full_router = jnp.split(first, (1536, 2048, 2560), axis=1)
    full_output = lax.all_gather(w_output, "fsdp", axis=0, tiled=True)
    weights_attn = (gain_attn, full_query, full_key, full_value, full_output, gain_ffn, full_router)
    state = forward_local(hidden_in, doc_ids[0], routes, *weights_attn)
    resid, ffn_in, probs = state[11], state[12], state[15]

    chosen = jnp.any(
        routes[:, :, None] == jnp.arange(experts, dtype=jnp.int32)[None, None, :], axis=1
    )
    below = jnp.tril(jnp.ones((tokens, tokens), bf16), -1)
    rank = jnp.dot(below, chosen.astype(bf16), preferred_element_type=f32)
    rank = jnp.where(chosen, rank, -1.0)
    gate = jnp.where(chosen, probs, 0.0)
    gate_high = gate.astype(bf16)
    gate_low = (gate - gate_high.astype(f32)).astype(bf16)
    meta = jnp.concatenate([rank.astype(bf16), gate_high, gate_low], axis=1)
    sent = jnp.concatenate(
        [ffn_in, meta, jnp.zeros((tokens, 128 - 3 * experts), bf16)], axis=1
    )
    sizes = (shards, owners, tokens, experts, held, pairing)
    combined, back, sums, far = moe(sizes, sent, cotangent, w_gateup, w_down)
    block_out = (resid + combined).astype(bf16)
    grad_ffn = back[:, :MODEL_WIDTH]
    grad_gate_dense = (
        back[:, MODEL_WIDTH : MODEL_WIDTH + experts]
        + back[:, MODEL_WIDTH + experts : MODEL_WIDTH + 2 * experts]
    )
    grad_gateup, grad_down = (
        s.astype(f32) + jnp.sum(r.astype(f32), axis=0) for s, r in zip(sums, far)
    )
    grad_input, grads = backward_local(
        state, chosen, cotangent, grad_ffn, grad_gate_dense, *weights_attn
    )
    widths = [g.shape[1] if g.ndim == 2 else 1 for g in grads]
    flat = jnp.concatenate([g if g.ndim == 2 else g[:, None] for g in grads], axis=1)
    share = lax.psum_scatter(flat.astype(bf16), "fsdp", scatter_dimension=0, tiled=True)
    total = lax.psum(share, "expert").astype(f32)
    pieces = jnp.split(total, [sum(widths[: i + 1]) for i in range(len(widths) - 1)], axis=1)
    pieces = [p if g.ndim == 2 else p[:, 0] for p, g in zip(pieces, grads)]
    return (block_out, grad_input, *pieces, grad_gateup, grad_down)


def local(*args):
    owners, held = lax.axis_size("expert"), args[10].shape[0]
    groups = held // (2 if held % 2 == 0 else 1)
    if owners * groups * CAP <= 2048 and owners % 4 == 0:
        return kernel_local(*args)
    return plain_local(*args)


def solution(mesh):
    in_specs = (
        P(("fsdp", "expert"), None),
        P(("fsdp", "expert"), None),
        P(("fsdp", "expert"), None),
        P(),
        P("fsdp", None),
        P("fsdp", None),
        P("fsdp", None),
        P("fsdp", None),
        P(),
        P("fsdp", None),
        P("expert", None, None),
        P("expert", None, None),
        P(("fsdp", "expert"), None),
    )
    out_specs = (
        P(("fsdp", "expert"), None),
        P(("fsdp", "expert"), None),
        P("fsdp", None),
        P("fsdp", None),
        P("fsdp", None),
        P("fsdp", None),
        P("fsdp", None),
        P("fsdp"),
        P("fsdp"),
        P("expert", "fsdp", None),
        P("expert", "fsdp", None),
    )
    return jax.shard_map(local, mesh=mesh, in_specs=in_specs, out_specs=out_specs, check_vma=False)
```

```python
import functools
import math

import jax
import jax.numpy as jnp
from jax import lax
from jax.experimental import pallas as pl
from jax.experimental.pallas import tpu as pltpu
from jax.sharding import PartitionSpec as P

MODEL_WIDTH = 1536
QUERY_HEADS = 24
KEY_VALUE_HEADS = 8
HEAD_SIZE = 64
TOP = 8
CAP = 48


EPS = 1e-05
BASE = 10000.0
SCORE_SCALE = 0.015625
MASKED = -1e30


def rope_tables(doc_row):
    document_length = doc_row.shape[0]
    places = jnp.arange(document_length, dtype=jnp.int32)
    same_doc = doc_row[:, None] == doc_row[None, :]
    starts = jnp.min(jnp.where(same_doc, places[None, :], document_length), axis=1)
    position = (places - starts).astype(jnp.float32)
    half_width = HEAD_SIZE // 2
    inverse = jnp.exp(
        -math.log(BASE) * (2.0 * jnp.arange(half_width, dtype=jnp.float32) / HEAD_SIZE)
    )
    angle = position[:, None] * inverse[None, :]
    allowed = same_doc & (places[None, :] <= places[:, None])
    return (jnp.cos(angle), jnp.sin(angle), allowed)


def rotate(tensor, cosine_table, sine_table):
    half_width = HEAD_SIZE // 2
    first_half = tensor[..., :half_width]
    second = tensor[..., half_width:]
    cos_part = cosine_table[:, None, :]
    sin_part = sine_table[:, None, :]
    return jnp.concatenate(
        [first_half * cos_part - second * sin_part, second * cos_part + first_half * sin_part],
        axis=-1,
    )


def inverse_rotation(tensor, cosine_table, sine_table):
    half_width = HEAD_SIZE // 2
    first_half = tensor[..., :half_width]
    second = tensor[..., half_width:]
    cos_part = cosine_table[:, None, :]
    sin_part = sine_table[:, None, :]
    return jnp.concatenate(
        [first_half * cos_part + second * sin_part, second * cos_part - first_half * sin_part],
        axis=-1,
    )


def norm_forward(value_rows, gain):
    scale_inv = lax.rsqrt(jnp.mean(value_rows * value_rows, axis=-1, keepdims=True) + EPS)
    normed = value_rows * scale_inv
    return ((normed * gain).astype(jnp.bfloat16), normed, scale_inv)


def norm_backward(grad_out, normed, scale_inv, gain):
    grad_normed = grad_out * gain
    grad_gain = jnp.sum(grad_out * normed, axis=0)
    value_gradients = scale_inv * (
        grad_normed - normed * jnp.mean(grad_normed * normed, axis=-1, keepdims=True)
    )
    return (value_gradients, grad_gain)


def scores_of(query_rows, key_rows, allowed):
    document_length = query_rows.shape[0]
    group_rows = query_rows.reshape(
        document_length, KEY_VALUE_HEADS, QUERY_HEADS // KEY_VALUE_HEADS, HEAD_SIZE
    )
    scores = (
        jnp.einsum("qgrd,kgd->grqk", group_rows, key_rows, preferred_element_type=jnp.float32)
        * SCORE_SCALE
    )
    return jnp.where(allowed[None, None], scores, MASKED)


def forward_local(
    hidden_rows,
    doc_row,
    route_rows,
    gain_attn,
    w_query,
    key_matrix,
    value_matrix,
    w_output,
    gain_ffn,
    w_router,
):
    document_length = hidden_rows.shape[0]
    hidden_f = hidden_rows.astype(jnp.float32)
    attention_input, normed_attn, scale_attn = norm_forward(hidden_f, gain_attn)
    cosine_table, sine_table, allowed = rope_tables(doc_row)
    query_rows = jnp.dot(attention_input, w_query, preferred_element_type=jnp.float32).reshape(
        document_length, QUERY_HEADS, HEAD_SIZE
    )
    key_rows = jnp.dot(attention_input, key_matrix, preferred_element_type=jnp.float32).reshape(
        document_length, KEY_VALUE_HEADS, HEAD_SIZE
    )
    value_rows = (
        jnp.dot(attention_input, value_matrix, preferred_element_type=jnp.float32)
        .astype(jnp.bfloat16)
        .reshape(document_length, KEY_VALUE_HEADS, HEAD_SIZE)
    )
    query_rows = rotate(query_rows, cosine_table, sine_table).astype(jnp.bfloat16)
    key_rows = rotate(key_rows, cosine_table, sine_table).astype(jnp.bfloat16)
    scores = scores_of(query_rows, key_rows, allowed)
    top_score = jnp.max(scores, axis=-1, keepdims=True)
    log_total = top_score + jnp.log(jnp.sum(jnp.exp(scores - top_score), axis=-1, keepdims=True))
    weights = jnp.exp(scores - log_total).astype(jnp.bfloat16)
    attention_mixed = jnp.einsum(
        "grqk,kgd->qgrd", weights, value_rows, preferred_element_type=jnp.float32
    )
    attention_mixed = attention_mixed.reshape(document_length, QUERY_HEADS * HEAD_SIZE).astype(
        jnp.bfloat16
    )
    resid = hidden_f + jnp.dot(attention_mixed, w_output, preferred_element_type=jnp.float32)
    ffn_in, normed_ffn, scale_ffn = norm_forward(resid, gain_ffn)
    logits = jnp.dot(ffn_in, w_router, preferred_element_type=jnp.float32)
    probs = jax.nn.softmax(logits, axis=-1)
    picks = route_rows[:, :, None] == jnp.arange(probs.shape[1], dtype=jnp.int32)[None, None, :]
    gates = jnp.sum(jnp.where(picks, probs[:, None, :], 0.0), axis=-1)
    return (
        normed_attn,
        scale_attn,
        attention_input,
        cosine_table,
        sine_table,
        allowed,
        query_rows,
        key_rows,
        value_rows,
        attention_mixed,
        log_total,
        resid,
        ffn_in,
        normed_ffn,
        scale_ffn,
        probs,
        gates,
    )


def backward_local(
    state,
    route_rows,
    cot_rows,
    grad_ffn_in,
    grad_gates,
    gain_attn,
    w_query,
    key_matrix,
    value_matrix,
    w_output,
    gain_ffn,
    w_router,
):
    (
        normed_attn,
        scale_attn,
        attention_input,
        cosine_table,
        sine_table,
        allowed,
        query_rows,
        key_rows,
        value_rows,
        attention_mixed,
        log_total,
        resid,
        ffn_in,
        normed_ffn,
        scale_ffn,
        probs,
        gates,
    ) = state
    document_length = attention_input.shape[0]
    query_group = QUERY_HEADS // KEY_VALUE_HEADS
    grad_probs = jnp.where(route_rows, grad_gates, 0.0)
    grad_logits = (
        probs * (grad_probs - jnp.sum(probs * grad_probs, axis=-1, keepdims=True))
    ).astype(jnp.bfloat16)
    grad_router = jnp.dot(ffn_in.T, grad_logits, preferred_element_type=jnp.float32)
    grad_ffn_in = grad_ffn_in + jnp.dot(grad_logits, w_router.T, preferred_element_type=jnp.float32)
    grad_resid_part, grad_gain_ffn = norm_backward(grad_ffn_in, normed_ffn, scale_ffn, gain_ffn)
    grad_resid = cot_rows.astype(jnp.float32) + grad_resid_part
    grad_attn = grad_resid.astype(jnp.bfloat16)
    grad_output = jnp.dot(attention_mixed.T, grad_attn, preferred_element_type=jnp.float32)
    mixed_gradient = jnp.dot(grad_attn, w_output.T, preferred_element_type=jnp.float32).astype(
        jnp.bfloat16
    )
    scores = scores_of(query_rows, key_rows, allowed)
    weights = jnp.exp(scores - log_total)
    weights_low = weights.astype(jnp.bfloat16)
    gradient_by_group = mixed_gradient.reshape(
        document_length, KEY_VALUE_HEADS, query_group, HEAD_SIZE
    )
    mixed_by_group = attention_mixed.reshape(
        document_length, KEY_VALUE_HEADS, query_group, HEAD_SIZE
    )
    value_gradients = jnp.einsum(
        "grqk,qgrd->kgd", weights_low, gradient_by_group, preferred_element_type=jnp.float32
    )
    grad_weights = jnp.einsum(
        "qgrd,kgd->grqk", gradient_by_group, value_rows, preferred_element_type=jnp.float32
    )
    delta = jnp.transpose(
        jnp.sum(
            gradient_by_group.astype(jnp.float32) * mixed_by_group.astype(jnp.float32), axis=-1
        ),
        (1, 2, 0),
    )
    grad_scores = (weights * (grad_weights - delta[..., None]) * SCORE_SCALE).astype(jnp.bfloat16)
    query_by_group = query_rows.reshape(document_length, KEY_VALUE_HEADS, query_group, HEAD_SIZE)
    grad_query_rows = jnp.einsum(
        "grqk,kgd->qgrd", grad_scores, key_rows, preferred_element_type=jnp.float32
    ).reshape(document_length, QUERY_HEADS, HEAD_SIZE)
    key_row_gradient = jnp.einsum(
        "grqk,qgrd->kgd", grad_scores, query_by_group, preferred_element_type=jnp.float32
    )
    grad_query_rows = (
        inverse_rotation(grad_query_rows, cosine_table, sine_table)
        .reshape(document_length, QUERY_HEADS * HEAD_SIZE)
        .astype(jnp.bfloat16)
    )
    key_row_gradient = (
        inverse_rotation(key_row_gradient, cosine_table, sine_table)
        .reshape(document_length, KEY_VALUE_HEADS * HEAD_SIZE)
        .astype(jnp.bfloat16)
    )
    value_row_gradient = value_gradients.reshape(
        document_length, KEY_VALUE_HEADS * HEAD_SIZE
    ).astype(jnp.bfloat16)
    grad_query = jnp.dot(attention_input.T, grad_query_rows, preferred_element_type=jnp.float32)
    grad_key = jnp.dot(attention_input.T, key_row_gradient, preferred_element_type=jnp.float32)
    grad_value = jnp.dot(attention_input.T, value_row_gradient, preferred_element_type=jnp.float32)
    grad_attn_in = jnp.dot(grad_query_rows, w_query.T, preferred_element_type=jnp.float32)
    grad_attn_in = grad_attn_in + jnp.dot(
        key_row_gradient, key_matrix.T, preferred_element_type=jnp.float32
    )
    grad_attn_in = grad_attn_in + jnp.dot(
        value_row_gradient, value_matrix.T, preferred_element_type=jnp.float32
    )
    grad_hidden_part, grad_gain_attn = norm_backward(
        grad_attn_in, normed_attn, scale_attn, gain_attn
    )
    grad_in = grad_resid + grad_hidden_part
    return (
        grad_in,
        (grad_query, grad_key, grad_value, grad_output, grad_router, grad_gain_attn, grad_gain_ffn),
    )


MESH = pl.DeviceIdType.MESH
F32, BF16 = jnp.float32, jnp.bfloat16


def dot(a, b, da=1, db=0):
    return lax.dot_general(a, b, (((da,), (db,)), ((), ())), preferred_element_type=F32)


class Place:
    def __init__(self, shards, owners):
        self.shards, self.owners = shards, owners
        self.line = 4 if owners % 4 == 0 else 1
        self.side = owners // self.line
        self.chips = shards // 2
        self.f = lax.axis_index("fsdp")
        self.e = lax.axis_index("expert")
        self.a, self.b = self.e // self.side, self.e % self.side
        self.x, self.c = self.f // 2, self.f % 2

    def others(self, all_fsdp):
        out = [((self.f, self.e + self.side), self.a < self.line - 1)]
        out.append(((self.f, self.e - self.side), self.a > 0))
        for i in range(1, self.side):
            out.append(((self.f, self.a * self.side + (self.b + i) % self.side), None))
        if all_fsdp:
            out += [(((self.f + i) % self.shards, self.e), None) for i in range(1, self.shards)]
            return out
        out.append(((self.x * 2 + 1 - self.c, self.e), None))
        for i in range(1, self.chips):
            out.append((((self.x + i) % self.chips * 2 + self.c, self.e), None))
        return out

    def meet(self, all_fsdp=False):
        bar = pltpu.get_barrier_semaphore()
        others = self.others(all_fsdp)
        for dev, cond in others:

            def signal(dev=dev):
                pl.semaphore_signal(bar, inc=1, device_id=dev, device_id_type=MESH)

            if cond is None:
                signal()
            else:
                pl.when(cond)(signal)
        pl.semaphore_wait(
            bar,
            len(others)
            - 2
            + jnp.where(self.a < self.line - 1, 1, 0)
            + jnp.where(self.a > 0, 1, 0),
        )


def remote(src, dst, send, recv, dev):
    return pltpu.make_async_remote_copy(
        src_ref=src, dst_ref=dst, send_sem=send, recv_sem=recv, device_id=dev, device_id_type=MESH
    )


class LineGather:
    def __init__(self, at, buf, send, recv):
        self.at, self.buf, self.send, self.recv = at, buf, send, recv

    def up(self, k):
        at = self.at
        return remote(
            self.buf.at[k], self.buf.at[k], self.send.at[0, k], self.recv.at[k], (at.f, at.e + at.side)
        )

    def down(self, k):
        at = self.at
        return remote(
            self.buf.at[k], self.buf.at[k], self.send.at[1, k], self.recv.at[k], (at.f, at.e - at.side)
        )

    def across(self, k, i):
        at = self.at
        dev = (at.f, at.a * at.side + (at.b + i) % at.side)
        return remote(
            self.buf.at[k], self.buf.at[k], self.send.at[1 + i, k], self.recv.at[k], dev
        )

    def begin(self):
        at = self.at

        @pl.when(at.a < at.line - 1)
        def _():
            self.up(at.e).start()

        @pl.when(at.a > 0)
        def _():
            self.down(at.e).start()

        for i in range(1, at.side):
            self.across(at.e, i).start()

    def relay(self):
        for s in range(1, self.at.line):
            self.relay_step(s)

    def relay_step(self, s):
        at = self.at

        @pl.when(at.a - s >= 0)
        def _():
            k = at.e - s * at.side
            self.down(k).wait_recv()

            @pl.when(at.a < at.line - 1)
            def _():
                self.up(k).start()

            for i in range(1, at.side):
                self.across(k, i).start()

        @pl.when(at.a + s < at.line)
        def _():
            k = at.e + s * at.side
            self.up(k).wait_recv()

            @pl.when(at.a > 0)
            def _():
                self.down(k).start()

            for i in range(1, at.side):
                self.across(k, i).start()

    def each(self, use):
        at = self.at

        def step(i, carry):
            k = (at.a + i) % at.line * at.side + (at.b + i // at.line) % at.side

            @pl.when(i >= at.line)
            def _():
                self.across(k, 1).wait_recv()

            use(k)
            return carry

        lax.fori_loop(0, at.owners, step, 0)

    def finish(self):
        at = self.at
        for s in range(at.line):
            k = s * at.side + at.b

            @pl.when((at.a < at.line - 1) & (at.a >= s))
            def _():
                self.up(k).wait_send()

            @pl.when((at.a > 0) & (at.a <= s))
            def _():
                self.down(k).wait_send()

            for i in range(1, at.side):
                self.across(k, i).wait_send()


class LineScatter:
    def __init__(self, at, part, side_in, line_in, own, sems):
        self.at, self.part, self.side_in, self.line_in, self.own = at, part, side_in, line_in, own
        self.ssend, self.srecv, self.lsend, self.lrecv = sems

    def across(self, s, i):
        at = self.at
        b = (at.b + i) % at.side
        j = at.side - 1 - i
        return remote(
            self.part.at[s * at.side + b],
            self.side_in.at[s, j],
            self.ssend.at[s, i - 1],
            self.srecv.at[s, j],
            (at.f, at.a * at.side + b),
        )

    def along(self, s, dev, slot):
        at = self.at
        return remote(
            self.part.at[s * at.side + at.b],
            self.line_in.at[slot],
            self.lsend.at[s],
            self.lrecv.at[slot],
            (at.f, dev),
        )

    def up(self, s):
        return self.along(s, self.at.e + self.at.side, s)

    def down(self, s):
        at = self.at
        return self.along(s, at.e - at.side, jnp.where(s == at.a - 1, at.line, s))

    def place(self, i):
        at = self.at
        return jnp.where(at.a < at.line // 2, at.line - 1 - i, i)

    def begin(self, make):
        at = self.at

        def step(n, carry):
            s, i = self.place(n % at.line), n // at.line + 1
            make(s * at.side + (at.b + i) % at.side)

            @pl.when(i < at.side)
            def _():
                self.across(s, i).start()

            return carry

        lax.fori_loop(0, at.owners, step, 0)

    def sum(self):
        at = self.at

        def step(n, carry):
            s = self.place(n)
            k = s * at.side + at.b
            for i in range(1, at.side):
                self.across(s, i).wait_recv()
            total = self.part[k].astype(F32)
            for j in range(at.side - 1):
                total = total + self.side_in[s, j].astype(F32)
            self.own[...] = total

            @pl.when(((s > at.a) & (at.a > 0)) | ((s < at.a) & (at.a < at.line - 1)))
            def _():
                self.along(s, at.e, s).wait_recv()
                self.own[...] += self.line_in[s].astype(F32)

            self.part[k] = self.own[...].astype(BF16)

            @pl.when(s > at.a)
            def _():
                self.up(s).start()

            @pl.when(s < at.a)
            def _():
                self.down(s).start()

            return carry

        lax.fori_loop(0, at.line, step, 0)
        total = self.part[at.e].astype(F32)
        self.own[...] = total

        @pl.when(at.a > 0)
        def _():
            self.along(at.a, at.e, at.a).wait_recv()
            self.own[...] += self.line_in[at.a].astype(F32)

        @pl.when(at.a < at.line - 1)
        def _():
            self.along(at.a, at.e, at.line).wait_recv()
            self.own[...] += self.line_in[at.line].astype(F32)

    def finish(self):
        at = self.at
        for s in range(at.line):
            for i in range(1, at.side):
                self.across(s, i).wait_send()

            @pl.when(at.a < s)
            def _(s=s):
                self.up(s).wait_send()

            @pl.when(at.a > s)
            def _(s=s):
                self.down(s).wait_send()


def rope_of(allowed, tokens):
    lane = lax.broadcasted_iota(jnp.int32, (tokens, 128), 1)
    position = jnp.sum(allowed.astype(F32), axis=1, keepdims=True) - 1.0
    half = HEAD_SIZE // 2
    inverse = jnp.exp(-math.log(BASE) * (2.0 * (lane % half).astype(F32) / HEAD_SIZE))
    angle = position * inverse
    return jnp.cos(angle), jnp.sin(angle), lane % HEAD_SIZE < half


def turn(x, cos, sin, first):
    half = HEAD_SIZE // 2
    other = jnp.where(first, -pltpu.roll(x, 128 - half, 1), pltpu.roll(x, half, 1))
    return x * cos + other * sin


def visible(doc, tokens):
    row = lax.broadcasted_iota(jnp.int32, (tokens, tokens), 0)
    col = lax.broadcasted_iota(jnp.int32, (tokens, tokens), 1)
    key_doc = jnp.broadcast_to(doc.astype(F32), (tokens, tokens))
    own = jnp.sum(jnp.where(row == col, key_doc, 0.0), axis=1, keepdims=True)
    return (own == key_doc) & (col <= row)


def attend_kernel(sizes, hidden, doc, routes, gain_a, gain_f, *refs):
    shards, owners, tokens, experts = sizes
    shares, cot = refs[:5], refs[5]
    h1, q, k, v, mixed, lse, resid, sent, probs_out = refs[6:15]
    fulls, cot_out = refs[15:20], refs[20]
    (bufs, cot_all, acc, lsem, xs, xr, ys, yr, zs, zr, ss, sr, cs, cr) = refs[21:]
    at = Place(shards, owners)
    rg = MODEL_WIDTH // shards
    half, quarter = rg // 2, rg // 4
    f = at.f
    sib = (at.x * 2 + 1 - at.c, at.e)
    over = ((at.x + 1) % at.chips * 2 + at.c, at.e)
    far = over[0]
    mine = (at.a + at.b) % 2
    beside = (f, at.a * at.side + (at.b + 1) % at.side)
    step = jnp.where(at.a % 2 == 0, at.side, -at.side)
    along = (f, at.e + step)
    count = len(shares)

    own = [pltpu.make_async_copy(shares[n], bufs[n].at[f], lsem.at[n]) for n in range(count)]
    own.append(pltpu.make_async_copy(cot, cot_all.at[at.e], lsem.at[count]))
    for c in own:
        c.start()

    def piece(n, g, start, size, send, recv, dev):
        ref = bufs[n].at[g, pl.ds(pl.multiple_of(start, quarter), size)]
        return remote(ref, ref, send, recv, dev)

    def out_x(n):
        start = pl.multiple_of(mine * half, half)
        return remote(
            shares[n].at[pl.ds(start, half)], bufs[n].at[f, pl.ds(start, half)],
            xs.at[n], xr.at[n], over,
        )

    def in_x(n):
        return piece(n, far, mine * half, half, xs.at[n], xr.at[n], over)

    def out_y(n):
        return piece(n, far, mine * half, quarter, ys.at[n], yr.at[n], beside)

    def in_y(n):
        return piece(n, far, (1 - mine) * half, quarter, ys.at[n], yr.at[n], beside)

    def out_z(n):
        return piece(n, far, mine * half + quarter, quarter, zs.at[n], zr.at[n], along)

    def in_z(n):
        return piece(n, far, (1 - mine) * half + quarter, quarter, zs.at[n], zr.at[n], along)

    def to_sib(n, i, g):
        start = (0, mine * half, (1 - mine) * half, (1 - mine) * half + quarter)[i]
        size = (rg, half, quarter, quarter)[i]
        return piece(n, g, start, size, ss.at[n, i], sr.at[n, i], sib)

    def own_sib(n):
        return remote(shares[n], bufs[n].at[f], ss.at[n, 0], sr.at[n, 0], sib)

    at.meet()
    for n in range(count):
        out_x(n).start()
        own_sib(n).start()
    cotg = LineGather(at, cot_all, cs, cr)
    own[count].wait()
    cotg.begin()

    x = hidden[...].astype(F32)
    scale = lax.rsqrt(jnp.mean(x * x, axis=1, keepdims=True) + EPS)
    h1[...] = (x * scale * gain_a[...]).astype(BF16)
    allowed = visible(doc[...], tokens)
    cos, sin, first = rope_of(allowed, tokens)

    ends = (0, 1536, 2048, 2560)

    def project(g):
        part = h1[:, pl.ds(pl.multiple_of(g * rg, 128), rg)]
        return [dot(part, bufs[n][g]) for n in range(3)]

    for n in range(3):
        own[n].wait()
        acc[:, ends[n] : ends[n + 1]] = dot(
            h1[:, pl.ds(pl.multiple_of(f * rg, 128), rg)], bufs[n][f]
        )

    def add(g):
        for n, got in enumerate(project(g)):
            acc[:, ends[n] : ends[n + 1]] += got

    def pass_x(n):
        in_x(n).wait_recv()
        out_y(n).start()
        out_z(n).start()
        to_sib(n, 1, far).start()

    def pass_rest(n):
        in_y(n).wait_recv()
        to_sib(n, 2, far).start()
        in_z(n).wait_recv()
        to_sib(n, 3, far).start()

    def from_sib(n, first_part, g):
        for i in (0,) if first_part else (1, 2, 3):
            to_sib(n, i, g).wait_recv()

    for n in range(3):
        from_sib(n, True, sib[0])
    add(sib[0])
    for n in (1, 2):
        pass_x(n)
    cotg.relay_step(1)
    pass_x(0)
    cotg.relay_step(2)
    for n in (1, 2, 0):
        pass_rest(n)
    add(far)
    other = (at.x + 1) % at.chips * 2 + 1 - at.c
    for n in range(3):
        from_sib(n, False, other)
    add(other)
    for n in (3, 4):
        pass_x(n)

    for j in range(16):
        cols = slice(128 * j, 128 * (j + 1))
        got = turn(acc[:, cols], cos, sin, first).astype(BF16)
        if j < 12:
            q[:, cols] = got
        else:
            k[:, 128 * (j - 12) : 128 * (j - 11)] = got
    v[...] = acc[:, 2048:].astype(BF16)
    ratio = QUERY_HEADS // KEY_VALUE_HEADS
    mask = jnp.concatenate([allowed] * ratio, axis=0)

    def head(ref, h):
        return ref[:, h * HEAD_SIZE : (h + 1) * HEAD_SIZE]

    for g in range(KEY_VALUE_HEADS):
        heads = range(g * ratio, (g + 1) * ratio)
        rows = jnp.concatenate([head(q, h) for h in heads], axis=0)
        s = jnp.where(mask, dot(rows, head(k, g), 1, 1) * SCORE_SCALE, MASKED)
        top = jnp.max(s, axis=1, keepdims=True)
        e = jnp.exp(s - top)
        total = jnp.sum(e, axis=1, keepdims=True)
        o = dot((e / total).astype(BF16), head(v, g)).astype(BF16)
        log_total = top + jnp.log(total)
        for i, h in enumerate(heads):
            mixed[:, h * HEAD_SIZE : (h + 1) * HEAD_SIZE] = o[i * tokens : (i + 1) * tokens]
            lse[:, h : h + 1] = log_total[i * tokens : (i + 1) * tokens]

    cotg.relay_step(3)
    for n in (3, 4):
        pass_rest(n)
    own[3].wait()
    own[4].wait()
    for n in (3, 4):
        from_sib(n, True, sib[0])
        from_sib(n, False, other)
    total = x
    for g in range(shards):
        total = total + dot(mixed[:, g * rg : (g + 1) * rg], bufs[3][g])
    resid[...] = total
    scale = lax.rsqrt(jnp.mean(total * total, axis=1, keepdims=True) + EPS)
    h2 = (total * scale * gain_f[...]).astype(BF16)
    sent[:, :MODEL_WIDTH] = h2
    logits = dot(h2[:, :rg], bufs[4][0])
    for g in range(1, shards):
        logits = logits + dot(h2[:, g * rg : (g + 1) * rg], bufs[4][g])
    lane = lax.broadcasted_iota(jnp.int32, (tokens, 128), 1)
    live = lane < experts
    logits = jnp.where(live, logits, MASKED)
    e = jnp.where(live, jnp.exp(logits - jnp.max(logits, axis=1, keepdims=True)), 0.0)
    probs = e / jnp.sum(e, axis=1, keepdims=True)
    probs_out[...] = probs
    ids = routes[...]
    chosen = lane == ids[:, :1]
    for i in range(1, TOP):
        chosen = chosen | (lane == ids[:, i : i + 1])
    row = lax.broadcasted_iota(jnp.int32, (tokens, tokens), 0)
    col = lax.broadcasted_iota(jnp.int32, (tokens, tokens), 1)
    below = jnp.where(row > col, 1.0, 0.0).astype(BF16)
    hits = jnp.where(chosen, 1.0, 0.0)
    rank = jnp.where(chosen, dot(below, hits.astype(BF16)), jnp.where(live, -1.0, 0.0))
    gate = jnp.where(chosen, probs, 0.0)
    high = gate.astype(BF16).astype(F32)
    low = gate - high
    meta = rank + pltpu.roll(high, experts, 1) + pltpu.roll(low, 2 * experts, 1)
    sent[:, MODEL_WIDTH:] = meta.astype(BF16)

    save = [pltpu.make_async_copy(bufs[n], fulls[n], lsem.at[n]) for n in range(count)]
    for c in save:
        c.start()
    cotg.each(lambda k: None)
    cotg.finish()
    keep = pltpu.make_async_copy(cot_all, cot_out, lsem.at[count])
    keep.start()
    for n in range(count):
        out_x(n).wait_send()
        own_sib(n).wait_send()
        out_y(n).wait_send()
        out_z(n).wait_send()
        for i in (1, 2, 3):
            to_sib(n, i, far).wait_send()
    for c in save:
        c.wait()
    keep.wait()


def attend(sizes, hidden, doc, routes, gain_a, gain_f, shares, cot):
    shards, owners, tokens, experts = sizes
    rg = MODEL_WIDTH // shards
    side = owners // 4
    vm, dma = pltpu.VMEM, pltpu.SemaphoreType.DMA
    vmem, any_ = pl.BlockSpec(memory_space=pltpu.VMEM), pl.BlockSpec(memory_space=pl.ANY)
    widths = [s.shape[1] for s in shares]
    n = len(shares)

    def shape(*dims, dtype=BF16):
        return jax.ShapeDtypeStruct(dims, dtype)

    outs = pl.pallas_call(
        functools.partial(attend_kernel, sizes),
        name="attend",
        out_shape=(
            shape(tokens, MODEL_WIDTH),
            shape(tokens, MODEL_WIDTH),
            shape(tokens, KEY_VALUE_HEADS * HEAD_SIZE),
            shape(tokens, KEY_VALUE_HEADS * HEAD_SIZE),
            shape(tokens, MODEL_WIDTH),
            shape(tokens, 128, dtype=F32),
            shape(tokens, MODEL_WIDTH, dtype=F32),
            shape(tokens, MODEL_WIDTH + 128),
            shape(tokens, 128, dtype=F32),
            *[shape(shards, rg, w) for w in widths],
            shape(owners, tokens, MODEL_WIDTH),
        ),
        in_specs=[vmem] * 5 + [any_] * (n + 1),
        out_specs=[vmem] * 9 + [any_] * (n + 1),
        scratch_shapes=[
            tuple(vm((shards, rg, w), BF16) for w in widths),
            vm((owners, tokens, MODEL_WIDTH), BF16),
            vm((tokens, 2560), F32),
            dma((n + 1,)),
            dma((n,)),
            dma((n,)),
            dma((n,)),
            dma((n,)),
            dma((n,)),
            dma((n,)),
            dma((n, 4)),
            dma((n, 4)),
            dma((side + 1, owners)),
            dma((owners,)),
        ],
        compiler_params=pltpu.CompilerParams(
            collective_id=0, has_side_effects=True, vmem_limit_bytes=60 * 2**20
        ),
    )(hidden, doc, routes, gain_a[None], gain_f[None], *shares, cot)
    return outs[:9], outs[9 : 9 + n], outs[9 + n]


def moe_kernel(sizes, sent, cot, wgu, wd, comb_out, back_out, sums, far, *scratch):
    shards, owners, tokens, experts, held, pairing = sizes
    (rows_all, cot_all, taken, cots, slot_gate, place, wg_buf, wd_buf, gg, gd, from_core, to_far,
     own_sum, z_acc, dx_acc, dg_acc, side1, line1, side2, line2, own2,
     rs, rr, wsem, coresend, corerecv, farsend, farrecv, osem, free, s1, s2, s3, s4, t1, t2, t3, t4,
     ) = scratch
    at = Place(shards, owners)
    groups = held // pairing
    slots = groups * CAP
    half = wd.shape[1]
    rg, rd = MODEL_WIDTH // shards, half // shards
    width = MODEL_WIDTH + 128

    def weights(h, slot):
        return (
            pltpu.make_async_copy(wgu.at[h], wg_buf.at[slot], wsem.at[0, slot]),
            pltpu.make_async_copy(wd.at[h], wd_buf.at[slot], wsem.at[1, slot]),
        )

    for c in weights(0, 0):
        c.start()
    at.meet()
    rows = LineGather(at, rows_all, rs, rr)
    c1 = pltpu.make_async_copy(sent, rows_all.at[at.e], osem.at[0, 0])
    c2 = pltpu.make_async_copy(cot, cot_all, osem.at[0, 1])
    c1.start()
    c2.start()
    c1.wait()
    rows.begin()
    rows.relay()
    c2.wait()

    lane = lax.broadcasted_iota(jnp.int32, (128, slots), 1)
    row = lax.broadcasted_iota(jnp.int32, (128, slots), 0)

    def expert_of(j):
        return (at.e * held + j // CAP * pairing) // 2

    e_lane = expert_of(lane)
    find_rank = (row == e_lane).astype(F32).astype(BF16)
    slot_rank = (lane % CAP).astype(F32)
    e_row = expert_of(lax.broadcasted_iota(jnp.int32, (slots, 128), 0))
    col = lax.broadcasted_iota(jnp.int32, (slots, 128), 1)
    pick_gate = (col == e_row + experts) | (col == e_row + 2 * experts)

    def dispatch_rows(k):
        rank_at = dot(rows_all[k, :, MODEL_WIDTH:], find_rank)
        pt = jnp.where(rank_at == slot_rank, 1.0, 0.0).astype(BF16)
        place[k] = pt
        got = dot(pt, rows_all[k], 0, 0)
        gate = jnp.sum(jnp.where(pick_gate, got[:, MODEL_WIDTH:], 0.0), axis=1, keepdims=True)
        gate = jnp.broadcast_to(gate, (slots, 128))
        to = pl.ds(k * CAP, CAP)
        for g in range(groups):
            taken[g, to, :] = got[g * CAP : (g + 1) * CAP, :MODEL_WIDTH].astype(BF16)
            slot_gate[g, to, :] = gate[g * CAP : (g + 1) * CAP]

    def dispatch_cot(k):
        got = dot(place[k], cot_all[k], 0, 0).astype(BF16)
        to = pl.ds(k * CAP, CAP)
        for g in range(groups):
            cots[g, to, :] = got[g * CAP : (g + 1) * CAP]

    rows.each(dispatch_rows)

    def dispatch_all(k, carry):
        dispatch_cot(k)
        return carry

    lax.fori_loop(0, owners, dispatch_all, 0)

    def to_core(h, slot):
        out = []
        for i in range(at.chips):
            f = 2 * i + 1 - at.c
            for n, (buf, r, o) in enumerate(((gg, rg, 0), (gd, rd, 1))):
                out.append(
                    remote(
                        buf.at[slot, pl.ds(pl.multiple_of(f * r, r), r)],
                        from_core[o].at[slot, i],
                        coresend.at[slot, n, i],
                        corerecv.at[slot, n, i],
                        (at.x * 2 + 1 - at.c, at.e),
                    )
                )
        return out

    def to_chips(h):
        out = []
        for i in range(1, at.chips):
            j = at.chips - 1 - i
            dev = ((at.x + i) % at.chips * 2 + at.c, at.e)
            for n in range(2):
                out.append(
                    remote(
                        to_far[n].at[h, i - 1],
                        far[n].at[j, h],
                        farsend.at[n, i - 1, h],
                        farrecv.at[n, j, h],
                        dev,
                    )
                )
        return out

    def own_copy(h, slot):
        return [
            pltpu.make_async_copy(own_sum[n].at[slot], sums[n].at[h], osem.at[n, slot])
            for n in range(2)
        ]

    def add(h, slot):
        for c in to_core(h, slot):
            c.wait()

        @pl.when(h >= 2)
        def _():
            for c in own_copy(h, slot):
                c.wait()

        for i in range(at.chips):
            x = (at.x + i) % at.chips
            f = 2 * x + at.c
            for n, (buf, r) in enumerate(((gg, rg), (gd, rd))):
                mine = buf[slot, pl.ds(pl.multiple_of(f * r, r), r)].astype(F32)
                total = (mine + from_core[n][slot, x].astype(F32)).astype(BF16)
                if i == 0:
                    own_sum[n][slot] = total
                else:
                    to_far[n][h, i - 1] = total
        for c in to_chips(h):
            c.start()
        for c in own_copy(h, slot):
            c.start()

        @pl.when(h < held - 2)
        def _():
            pl.semaphore_signal(
                free, inc=1, device_id=(at.x * 2 + 1 - at.c, at.e), device_id_type=MESH
            )

    def step(h, carry):
        slot = h % 2
        g, m = h // pairing, h % pairing
        for c in weights(h, slot):
            c.wait()

        @pl.when(h + 1 < held)
        def _():
            for c in weights(h + 1, 1 - slot):
                c.start()

        @pl.when(m == 0)
        def _():
            z_acc[...] = jnp.zeros_like(z_acc)
            dx_acc[...] = jnp.zeros_like(dx_acc)
            dg_acc[...] = jnp.zeros_like(dg_acc)

        gu = dot(taken[g], wg_buf[slot])
        a, b = gu[:, :half], gu[:, half:]
        gate = slot_gate[g][:, :1]
        sig = 1.0 / (1.0 + jnp.exp(-a))
        s = a * sig
        act = s * b
        actg = (act * gate).astype(BF16)
        dp = dot(cots[g], wd_buf[slot], 1, 1)
        dg_acc[...] += jnp.broadcast_to(
            jnp.sum(act * dp, axis=1, keepdims=True), dg_acc.shape
        )
        dact = dp * gate
        da = dact * b * sig * (1.0 + a * (1.0 - sig))
        db = dact * s
        du = jnp.concatenate([da, db], axis=1).astype(BF16)
        z_acc[...] += dot(actg, wd_buf[slot])
        dx_acc[...] += dot(du, wg_buf[slot], 1, 1)
        for i in range(3):
            n = MODEL_WIDTH // 3
            gg[slot, i * n : (i + 1) * n, :] = dot(
                taken[g, :, i * n : (i + 1) * n], du, 0, 0
            ).astype(BF16)
        gd[slot] = dot(actg, cots[g], 0, 0).astype(BF16)

        @pl.when(h >= 2)
        def _():
            pl.semaphore_wait(free, 1)

        for c in to_core(h, slot):
            c.start()

        @pl.when(h > 0)
        def _():
            add(h - 1, 1 - slot)

        @pl.when(m == pairing - 1)
        def _():
            taken[g] = z_acc[...].astype(BF16)
            cots[g] = dx_acc[...].astype(BF16)
            slot_gate[g] = dg_acc[...]

        return carry

    lax.fori_loop(0, held, step, 0)
    add(held - 1, (held - 1) % 2)

    rows.finish()

    home = (col == e_row).astype(F32).astype(BF16)
    home_low = (col == e_row + experts).astype(F32).astype(BF16)

    def make_back(k):
        to = pl.ds(k * CAP, CAP)
        dx = jnp.concatenate([cots[g, to, :] for g in range(groups)], axis=0)
        dg = jnp.concatenate([slot_gate[g, to, :] for g in range(groups)], axis=0)
        high = dg.astype(BF16)
        low = (dg - high.astype(F32)).astype(BF16)
        dgm = high * home + low * home_low
        pt = place[k]
        rows_all[k, :, :MODEL_WIDTH] = dot(pt, dx).astype(BF16)
        rows_all[k, :, MODEL_WIDTH:] = dot(pt, dgm).astype(BF16)

    def make_comb(k):
        to = pl.ds(k * CAP, CAP)
        y = jnp.concatenate([taken[g, to, :] for g in range(groups)], axis=0)
        cot_all[k] = dot(place[k], y).astype(BF16)

    back = LineScatter(at, rows_all, side1, line1, back_out, (s1, s2, s3, s4))
    comb = LineScatter(at, cot_all, side2, line2, own2, (t1, t2, t3, t4))
    back.begin(make_back)
    comb.begin(make_comb)
    back.sum()
    comb.sum()
    comb_out[...] = own2[...]
    back.finish()
    comb.finish()
    for h in range(held - 2, held):
        for c in own_copy(h, h % 2):
            c.wait()

    def drain(h, carry):
        for c in to_chips(h):
            c.wait()
        return carry

    lax.fori_loop(0, held, drain, 0)


def moe(sizes, sent, cot, wgu, wd):
    shards, owners, tokens, experts, held, pairing = sizes
    groups = held // pairing
    slots, rows = groups * CAP, owners * CAP
    hidden, half = wgu.shape[2], wd.shape[1]
    rg, rd = MODEL_WIDTH // shards, half // shards
    chips = shards // 2
    line = 4 if owners % 4 == 0 else 1
    side = owners // line
    width = MODEL_WIDTH + 128
    vm, dma = pltpu.VMEM, pltpu.SemaphoreType.DMA
    any_, vmem = pl.BlockSpec(memory_space=pl.ANY), pl.BlockSpec(memory_space=pltpu.VMEM)

    def pair(lead, dtype=BF16):
        return (vm((*lead, rg, hidden), dtype), vm((*lead, rd, MODEL_WIDTH), dtype))

    def outs(lead):
        return (
            jax.ShapeDtypeStruct((*lead, rg, hidden), BF16),
            jax.ShapeDtypeStruct((*lead, rd, MODEL_WIDTH), BF16),
        )

    def scatter_sems():
        return [dma((line, side)), dma((line, side)), dma((line,)), dma((line + 1,))]

    return pl.pallas_call(
        functools.partial(moe_kernel, sizes),
        name="moe",
        out_shape=(
            jax.ShapeDtypeStruct((tokens, MODEL_WIDTH), F32),
            jax.ShapeDtypeStruct((tokens, width), F32),
            outs((held,)),
            outs((chips - 1, held)),
        ),
        in_specs=[any_] * 4,
        out_specs=(vmem, vmem, (any_, any_), (any_, any_)),
        scratch_shapes=[
            vm((owners, tokens, width), BF16),
            vm((owners, tokens, MODEL_WIDTH), BF16),
            vm((groups, rows, MODEL_WIDTH), BF16),
            vm((groups, rows, MODEL_WIDTH), BF16),
            vm((groups, rows, 128), F32),
            vm((owners, tokens, slots), BF16),
            vm((2, MODEL_WIDTH, hidden), BF16),
            vm((2, half, MODEL_WIDTH), BF16),
            vm((2, MODEL_WIDTH, hidden), BF16),
            vm((2, half, MODEL_WIDTH), BF16),
            pair((2, chips)),
            pair((held, chips - 1)),
            pair((2,)),
            vm((rows, MODEL_WIDTH), F32),
            vm((rows, MODEL_WIDTH), F32),
            vm((rows, 128), F32),
            vm((line, side - 1, tokens, width), BF16),
            vm((line + 1, tokens, width), BF16),
            vm((line, side - 1, tokens, MODEL_WIDTH), BF16),
            vm((line + 1, tokens, MODEL_WIDTH), BF16),
            vm((tokens, MODEL_WIDTH), F32),
            dma((side + 1, owners)),
            dma((owners,)),
            dma((2, 2)),
            dma((2, 2, chips)),
            dma((2, 2, chips)),
            dma((2, chips - 1, held)),
            dma((2, chips - 1, held)),
            dma((2, 2)),
            pltpu.SemaphoreType.REGULAR,
            *scatter_sems(),
            *scatter_sems(),
        ],
        compiler_params=pltpu.CompilerParams(
            collective_id=1, has_side_effects=True, vmem_limit_bytes=63 * 2**20
        ),
    )(sent, cot, wgu, wd)


def grads_kernel(sizes, h1, mixed, right, aux, out, *scratch):
    shards, owners, tokens = sizes
    (left, rights, aux_in, turned, part, side_in, line_in, own, total,
     lsem, rsem, asem, lsend, lrecv, rsend, rrecv, asend, arecv, s1, s2, s3, s4, gs, gr) = scratch
    at = Place(shards, owners)
    rg = MODEL_WIDTH // shards
    piece = rg // owners
    wide = right.shape[1]
    split = wide - MODEL_WIDTH
    f = at.f
    sibling = (at.x * 2 + 1 - at.c, at.e)

    def rows(i):
        return pl.ds(pl.multiple_of(i * tokens, tokens), tokens)

    def cols(i):
        return pl.ds(pl.multiple_of(i * rg, rg), rg)

    own_rights = pltpu.make_async_copy(right, rights.at[rows(f)], rsem)
    own_rights.start()
    local = [
        pltpu.make_async_copy(h1.at[:, cols(f)], left.at[rows(f), pl.ds(0, rg)], lsem.at[0]),
        pltpu.make_async_copy(mixed.at[:, cols(f)], left.at[rows(f), pl.ds(rg, rg)], lsem.at[1]),
        pltpu.make_async_copy(aux.at[:, cols(f)], aux_in.at[0], asem),
    ]
    for c in local:
        c.start()
    at.meet(all_fsdp=True)

    def block(g, send, dev):
        return remote(rights.at[rows(g)], rights.at[rows(g)], rsend.at[send], rrecv.at[g], dev)

    def lefts(i):
        g = (f + i) % shards
        dev = (g, at.e)
        return (
            remote(h1.at[:, cols(g)], left.at[rows(f), pl.ds(0, rg)],
                   lsend.at[0, i - 1], lrecv.at[0, i - 1], dev),
            remote(mixed.at[:, cols(g)], left.at[rows(f), pl.ds(rg, rg)],
                   lsend.at[1, i - 1], lrecv.at[1, i - 1], dev),
            remote(aux.at[:, cols(g)], aux_in.at[i], asend.at[i - 1], arecv.at[i - 1], dev),
        )

    own_rights.wait()
    away = [(((at.x + i) % at.chips) * 2 + at.c) for i in range(1, at.chips)]
    direct = [block(f, 0, sibling)]
    direct += [block(f, 1 + n, (g, at.e)) for n, g in enumerate(away)]
    for c in direct:
        c.start()
    sent = [c for i in range(1, shards) for c in lefts(i)]
    for c in sent:
        c.start()
    passed = []
    for n, g in enumerate(away):
        block(g, 0, sibling).wait_recv()
        c = block(g, at.chips + n, sibling)
        c.start()
        passed.append(c)
    for c in local:
        c.wait()
    for c in sent:
        c.wait_recv()
    turned[...] = left[...].T
    extra = aux_in[0]
    for i in range(1, shards):
        extra = extra + aux_in[i]
    extra = extra.T.astype(BF16)
    block(at.x * 2 + 1 - at.c, 0, sibling).wait_recv()
    for n in range(1, at.chips):
        block(((at.x + n) % at.chips) * 2 + 1 - at.c, 0, sibling).wait_recv()
    step = 512
    for n in range(wide // step):
        lhs = turned[:rg] if n * step < split else turned[rg:]
        got = dot(lhs, rights[:, n * step : (n + 1) * step]).astype(BF16)
        for k in range(owners):
            part[k, :, n * step : (n + 1) * step] = got[k * piece : (k + 1) * piece]
    for k in range(owners):
        part[k, :, wide : wide + aux.shape[0]] = extra[k * piece : (k + 1) * piece]
    scatter = LineScatter(at, part, side_in, line_in, own, (s1, s2, s3, s4))
    scatter.begin(lambda k: None)
    scatter.sum()
    gather = LineGather(at, total, gs, gr)
    total[at.e] = own[...].astype(BF16)
    gather.begin()
    gather.relay()
    gather.each(lambda k: None)
    out[...] = total[...]
    for c in direct + sent + passed:
        c.wait_send()
    scatter.finish()
    gather.finish()


def sum_grads(sizes, h1, mixed, right, aux):
    shards, owners, tokens = sizes
    rg = MODEL_WIDTH // shards
    piece = rg // owners
    chips = shards // 2
    wide, extra = right.shape[1], aux.shape[0]
    full = wide + 128
    line = 4
    side = owners // line
    vm, dma = pltpu.VMEM, pltpu.SemaphoreType.DMA
    vmem = pl.BlockSpec(memory_space=pltpu.VMEM)
    return pl.pallas_call(
        functools.partial(grads_kernel, sizes),
        name="grads",
        out_shape=jax.ShapeDtypeStruct((owners, piece, full), BF16),
        in_specs=[vmem] * 4,
        out_specs=vmem,
        scratch_shapes=[
            vm((shards * tokens, 2 * rg), BF16),
            vm((shards * tokens, wide), BF16),
            vm((shards, extra, rg), F32),
            vm((2 * rg, shards * tokens), BF16),
            vm((owners, piece, full), BF16),
            vm((line, side - 1, piece, full), BF16),
            vm((line + 1, piece, full), BF16),
            vm((piece, full), F32),
            vm((owners, piece, full), BF16),
            dma((2,)),
            dma,
            dma,
            dma((2, shards - 1)),
            dma((2, shards - 1)),
            dma((2 * chips,)),
            dma((shards,)),
            dma((shards - 1,)),
            dma((shards - 1,)),
            dma((line, side)),
            dma((line, side)),
            dma((line,)),
            dma((line + 1,)),
            dma((side + 1, owners)),
            dma((owners,)),
        ],
        compiler_params=pltpu.CompilerParams(
            collective_id=2, has_side_effects=True, vmem_limit_bytes=60 * 2**20
        ),
    )(h1, mixed, right, aux)


def backward_rows(
    state,
    route_rows,
    cot_rows,
    grad_ffn_in,
    grad_gates,
    gain_attn,
    w_query,
    key_matrix,
    value_matrix,
    w_output,
    gain_ffn,
    w_router,
):
    (
        normed_attn,
        scale_attn,
        attention_input,
        cosine_table,
        sine_table,
        allowed,
        query_rows,
        key_rows,
        value_rows,
        attention_mixed,
        log_total,
        resid,
        ffn_in,
        normed_ffn,
        scale_ffn,
        probs,
        gates,
    ) = state
    document_length = attention_input.shape[0]
    query_group = QUERY_HEADS // KEY_VALUE_HEADS
    grad_probs = jnp.where(route_rows, grad_gates, 0.0)
    grad_logits = (
        probs * (grad_probs - jnp.sum(probs * grad_probs, axis=-1, keepdims=True))
    ).astype(jnp.bfloat16)
    grad_router = jnp.dot(grad_logits.T, ffn_in, preferred_element_type=jnp.float32)
    grad_ffn_in = grad_ffn_in + jnp.dot(grad_logits, w_router.T, preferred_element_type=jnp.float32)
    grad_resid_part, grad_gain_ffn = norm_backward(grad_ffn_in, normed_ffn, scale_ffn, gain_ffn)
    grad_resid = cot_rows.astype(jnp.float32) + grad_resid_part
    grad_attn = grad_resid.astype(jnp.bfloat16)
    mixed_gradient = jnp.dot(grad_attn, w_output.T, preferred_element_type=jnp.float32).astype(
        jnp.bfloat16
    )
    scores = scores_of(query_rows, key_rows, allowed)
    weights = jnp.exp(scores - log_total)
    weights_low = weights.astype(jnp.bfloat16)
    gradient_by_group = mixed_gradient.reshape(
        document_length, KEY_VALUE_HEADS, query_group, HEAD_SIZE
    )
    mixed_by_group = attention_mixed.reshape(
        document_length, KEY_VALUE_HEADS, query_group, HEAD_SIZE
    )
    value_gradients = jnp.einsum(
        "grqk,qgrd->kgd", weights_low, gradient_by_group, preferred_element_type=jnp.float32
    )
    grad_weights = jnp.einsum(
        "qgrd,kgd->grqk", gradient_by_group, value_rows, preferred_element_type=jnp.float32
    )
    delta = jnp.transpose(
        jnp.sum(
            gradient_by_group.astype(jnp.float32) * mixed_by_group.astype(jnp.float32), axis=-1
        ),
        (1, 2, 0),
    )
    grad_scores = (weights * (grad_weights - delta[..., None]) * SCORE_SCALE).astype(jnp.bfloat16)
    query_by_group = query_rows.reshape(document_length, KEY_VALUE_HEADS, query_group, HEAD_SIZE)
    grad_query_rows = jnp.einsum(
        "grqk,kgd->qgrd", grad_scores, key_rows, preferred_element_type=jnp.float32
    ).reshape(document_length, QUERY_HEADS, HEAD_SIZE)
    key_row_gradient = jnp.einsum(
        "grqk,qgrd->kgd", grad_scores, query_by_group, preferred_element_type=jnp.float32
    )
    grad_query_rows = (
        inverse_rotation(grad_query_rows, cosine_table, sine_table)
        .reshape(document_length, QUERY_HEADS * HEAD_SIZE)
        .astype(jnp.bfloat16)
    )
    key_row_gradient = (
        inverse_rotation(key_row_gradient, cosine_table, sine_table)
        .reshape(document_length, KEY_VALUE_HEADS * HEAD_SIZE)
        .astype(jnp.bfloat16)
    )
    value_row_gradient = value_gradients.reshape(
        document_length, KEY_VALUE_HEADS * HEAD_SIZE
    ).astype(jnp.bfloat16)
    grad_attn_in = jnp.dot(grad_query_rows, w_query.T, preferred_element_type=jnp.float32)
    grad_attn_in = grad_attn_in + jnp.dot(
        key_row_gradient, key_matrix.T, preferred_element_type=jnp.float32
    )
    grad_attn_in = grad_attn_in + jnp.dot(
        value_row_gradient, value_matrix.T, preferred_element_type=jnp.float32
    )
    grad_hidden_part, grad_gain_attn = norm_backward(
        grad_attn_in, normed_attn, scale_attn, gain_attn
    )
    grad_in = grad_resid + grad_hidden_part
    right = jnp.concatenate(
        [grad_query_rows, key_row_gradient, value_row_gradient, grad_attn], axis=1
    )
    aux = jnp.concatenate(
        [
            grad_router,
            grad_gain_attn[None],
            grad_gain_ffn[None],
            jnp.zeros((128 - 2 - grad_router.shape[0], MODEL_WIDTH), jnp.float32),
        ],
        axis=0,
    )
    return grad_in, right, aux


def plain_local(
    hidden_in,
    doc_ids,
    routes,
    gain_attn,
    w_query,
    key_matrix,
    value_matrix,
    w_output,
    gain_ffn,
    w_router,
    w_gateup,
    w_down,
    cotangent,
):
    tokens = hidden_in.shape[0]
    experts = w_router.shape[1]
    shards = lax.axis_size("fsdp")
    owners = lax.axis_size("expert")
    held = w_gateup.shape[0]
    half = w_down.shape[1]
    hidden_units = w_gateup.shape[2]
    pairing = 2 if held % 2 == 0 else 1
    groups = held // pairing
    slots = groups * CAP
    mine = lax.axis_index("expert")
    f32, bf16 = jnp.float32, jnp.bfloat16

    first = lax.all_gather(
        jnp.concatenate([w_query, key_matrix, value_matrix, w_router], axis=1),
        "fsdp",
        axis=0,
        tiled=True,
    )
    full_query, full_key, full_value, full_router = jnp.split(first, (1536, 2048, 2560), axis=1)
    full_output = lax.all_gather(w_output, "fsdp", axis=0, tiled=True)
    cot_all = lax.all_gather(cotangent, "expert", axis=0)
    weights_attn = (gain_attn, full_query, full_key, full_value, full_output, gain_ffn, full_router)
    state = forward_local(hidden_in, doc_ids[0], routes, *weights_attn)
    resid, ffn_in, probs = state[11], state[12], state[15]

    chosen = jnp.any(
        routes[:, :, None] == jnp.arange(experts, dtype=jnp.int32)[None, None, :], axis=1
    )
    below = jnp.tril(jnp.ones((tokens, tokens), bf16), -1)
    rank = jnp.dot(below, chosen.astype(bf16), preferred_element_type=f32)
    rank = jnp.where(chosen, rank, -1.0)
    gate = jnp.where(chosen, probs, 0.0)
    gate_high = gate.astype(bf16)
    gate_low = (gate - gate_high.astype(f32)).astype(bf16)
    meta = jnp.concatenate([rank.astype(bf16), gate_high, gate_low], axis=1)
    sent = jnp.concatenate(
        [ffn_in, meta, jnp.zeros((tokens, 128 - 3 * experts), bf16)], axis=1
    )
    got = lax.all_gather(sent, "expert", axis=0)
    rows_all = got[:, :, :MODEL_WIDTH]
    meta_all = got[:, :, MODEL_WIDTH:]
    lane = jnp.arange(slots, dtype=jnp.int32)
    slot_expert = (mine * held + (lane // CAP) * pairing) // 2
    spread = (jnp.arange(experts, dtype=jnp.int32)[:, None] == slot_expert[None, :]).astype(bf16)
    rank_at = jnp.dot(meta_all[:, :, :experts], spread, preferred_element_type=f32)
    gate_at = jnp.dot(
        meta_all[:, :, experts : 2 * experts], spread, preferred_element_type=f32
    ) + jnp.dot(meta_all[:, :, 2 * experts : 3 * experts], spread, preferred_element_type=f32)
    place = rank_at == (lane % CAP).astype(f32)[None, None, :]
    onehot = place.astype(bf16)
    gated = jnp.where(place, gate_at, 0.0)
    slot_gate = jnp.sum(gated, axis=1)

    def dispatch(rows):
        out = jnp.einsum("stj,std->sjd", onehot, rows, preferred_element_type=f32)
        return out.reshape(owners, groups, CAP, MODEL_WIDTH)

    taken = dispatch(rows_all).astype(bf16)
    cot_rows = dispatch(cot_all)
    slot_gate_4 = slot_gate.reshape(owners, groups, CAP, 1)
    grads_in = (cot_rows * slot_gate_4).astype(bf16)
    w_pairs = w_gateup.reshape(groups, pairing, MODEL_WIDTH, hidden_units)
    down_pairs = w_down.reshape(groups, pairing, half, MODEL_WIDTH)
    gate_up = jnp.einsum("secd,emdf->emscf", taken, w_pairs, preferred_element_type=f32)
    a, b = gate_up[..., :half], gate_up[..., half:]
    sigma = jax.nn.sigmoid(a)
    acted = (a * sigma * b).astype(bf16)
    made = jnp.einsum("emscf,emfd->secd", acted, down_pairs, preferred_element_type=f32)
    made = made.astype(bf16)
    grad_slot = jnp.sum(made.astype(f32) * cot_rows, axis=-1).reshape(owners, slots)
    grad_gate_back = jnp.where(place, grad_slot[:, None, :], 0.0).reshape(
        owners, tokens, groups, CAP
    )
    grad_gate_back = jnp.sum(grad_gate_back, axis=-1)
    onto = (
        (mine * held + jnp.arange(groups) * pairing)[:, None] // 2
        == jnp.arange(128, dtype=jnp.int32)[None, :]
    ).astype(bf16)
    grad_gate_back = jnp.dot(
        grad_gate_back.astype(bf16), onto, preferred_element_type=f32
    ).astype(bf16)
    weighted = (made.astype(f32) * slot_gate_4).astype(bf16).reshape(owners, slots, MODEL_WIDTH)
    combined = jnp.einsum("stj,sjd->std", onehot, weighted, preferred_element_type=f32)
    grad_acted = jnp.einsum("secd,emfd->emscf", grads_in, down_pairs, preferred_element_type=f32)
    grad_down = jnp.einsum("emscf,secd->emfd", acted, grads_in, preferred_element_type=f32)
    grad_a = grad_acted * b * sigma * (1.0 + a * (1.0 - sigma))
    grad_b = grad_acted * a * sigma
    joined = jnp.concatenate([grad_a, grad_b], axis=-1).astype(bf16)
    grad_gateup = jnp.einsum("secd,emscf->emdf", taken, joined, preferred_element_type=f32)
    grad_rows = jnp.einsum("emscf,emdf->secd", joined, w_pairs, preferred_element_type=f32)
    grad_rows = grad_rows.astype(bf16).reshape(owners, slots, MODEL_WIDTH)
    grad_ffn = jnp.einsum("stj,sjd->std", onehot, grad_rows, preferred_element_type=f32)
    back = jnp.concatenate([grad_ffn.astype(bf16), grad_gate_back], axis=-1)
    back = lax.psum_scatter(
        back.reshape(owners * tokens, -1), "expert", scatter_dimension=0, tiled=True
    ).astype(f32)
    grad_ffn, grad_gate_dense = back[:, :MODEL_WIDTH], back[:, MODEL_WIDTH : MODEL_WIDTH + experts]
    combined = lax.psum_scatter(
        combined.astype(bf16).reshape(owners * tokens, -1),
        "expert",
        scatter_dimension=0,
        tiled=True,
    )
    block_out = (resid + combined.astype(f32)).astype(bf16)
    grad_gateup, grad_down = (
        lax.psum_scatter(
            grad_gateup.reshape(held, MODEL_WIDTH, hidden_units).astype(bf16),
            "fsdp",
            scatter_dimension=1,
            tiled=True,
        ).astype(f32),
        lax.psum_scatter(
            grad_down.reshape(held, half, MODEL_WIDTH).astype(bf16),
            "fsdp",
            scatter_dimension=1,
            tiled=True,
        ).astype(f32),
    )
    grad_input, grads = backward_local(
        state, chosen, cotangent, grad_ffn, grad_gate_dense, *weights_attn
    )
    widths = [g.shape[1] if g.ndim == 2 else 1 for g in grads]
    flat = jnp.concatenate([g if g.ndim == 2 else g[:, None] for g in grads], axis=1)
    share = lax.psum_scatter(flat.astype(bf16), "fsdp", scatter_dimension=0, tiled=True)
    total = lax.psum(share, "expert").astype(f32)
    pieces = jnp.split(total, [sum(widths[: i + 1]) for i in range(len(widths) - 1)], axis=1)
    pieces = [p if g.ndim == 2 else p[:, 0] for p, g in zip(pieces, grads)]
    return (block_out, grad_input, *pieces, grad_gateup, grad_down)


def kernel_local(
    hidden_in,
    doc_ids,
    routes,
    gain_attn,
    w_query,
    key_matrix,
    value_matrix,
    w_output,
    gain_ffn,
    w_router,
    w_gateup,
    w_down,
    cotangent,
):
    tokens = hidden_in.shape[0]
    experts = w_router.shape[1]
    shards = lax.axis_size("fsdp")
    owners = lax.axis_size("expert")
    held = w_gateup.shape[0]
    pairing = 2 if held % 2 == 0 else 1
    f32, bf16 = jnp.float32, jnp.bfloat16

    router = jnp.concatenate(
        [w_router, jnp.zeros((w_router.shape[0], 128 - experts), bf16)], axis=1
    )
    shares = (w_query, key_matrix, value_matrix, w_output, router)
    made, fulls, cot_all = attend(
        (shards, owners, tokens, experts), hidden_in, doc_ids, routes, gain_attn, gain_ffn, shares,
        cotangent,
    )
    h1, q, k, v, mixed, lse, resid, sent, probs = made
    full_query, full_key, full_value, full_output, full_router = (
        w.reshape(MODEL_WIDTH, -1) for w in fulls
    )
    full_router = full_router[:, :experts]
    probs = probs[:, :experts]
    weights_attn = (gain_attn, full_query, full_key, full_value, full_output, gain_ffn, full_router)
    chosen = jnp.any(
        routes[:, :, None] == jnp.arange(experts, dtype=jnp.int32)[None, None, :], axis=1
    )
    ffn_in = sent[:, :MODEL_WIDTH]
    _, normed_attn, scale_attn = norm_forward(hidden_in.astype(f32), gain_attn)
    _, normed_ffn, scale_ffn = norm_forward(resid, gain_ffn)
    cosine, sine, allowed = rope_tables(doc_ids[0])
    ratio = QUERY_HEADS // KEY_VALUE_HEADS
    state = (
        normed_attn,
        scale_attn,
        h1,
        cosine,
        sine,
        allowed,
        q.reshape(tokens, QUERY_HEADS, HEAD_SIZE),
        k.reshape(tokens, KEY_VALUE_HEADS, HEAD_SIZE),
        v.reshape(tokens, KEY_VALUE_HEADS, HEAD_SIZE),
        mixed,
        lse[:, :QUERY_HEADS].T.reshape(KEY_VALUE_HEADS, ratio, tokens, 1),
        resid,
        ffn_in,
        normed_ffn,
        scale_ffn,
        probs,
        None,
    )
    sizes = (shards, owners, tokens, experts, held, pairing)
    combined, back, sums, far = moe(sizes, sent, cot_all, w_gateup, w_down)
    block_out = (resid + combined).astype(bf16)
    grad_ffn = back[:, :MODEL_WIDTH]
    grad_gate_dense = (
        back[:, MODEL_WIDTH : MODEL_WIDTH + experts]
        + back[:, MODEL_WIDTH + experts : MODEL_WIDTH + 2 * experts]
    )
    grad_gateup, grad_down = (
        s.astype(f32) + jnp.sum(r.astype(f32), axis=0) for s, r in zip(sums, far)
    )
    grad_input, right, aux = backward_rows(
        state, chosen, cotangent, grad_ffn, grad_gate_dense, *weights_attn
    )
    total = sum_grads((shards, owners, tokens), state[2], state[9], right, aux)
    total = total.reshape(MODEL_WIDTH // shards, -1).astype(f32)
    ends = (1536, 2048, 2560, 4096, 4096 + experts)
    grad_query, grad_key, grad_value, grad_output, grad_router, rest = jnp.split(total, ends, axis=1)
    return (
        block_out,
        grad_input,
        grad_query,
        grad_key,
        grad_value,
        grad_output,
        grad_router,
        rest[:, 0],
        rest[:, 1],
        grad_gateup,
        grad_down,
    )


def local(*args):
    owners, held = lax.axis_size("expert"), args[10].shape[0]
    groups = held // (2 if held % 2 == 0 else 1)
    if lax.axis_size("fsdp") == 4 and owners == 8 and owners * groups * CAP <= 2048:
        return kernel_local(*args)
    return plain_local(*args)


def solution(mesh):
    in_specs = (
        P(("fsdp", "expert"), None),
        P(("fsdp", "expert"), None),
        P(("fsdp", "expert"), None),
        P(),
        P("fsdp", None),
        P("fsdp", None),
        P("fsdp", None),
        P("fsdp", None),
        P(),
        P("fsdp", None),
        P("expert", None, None),
        P("expert", None, None),
        P(("fsdp", "expert"), None),
    )
    out_specs = (
        P(("fsdp", "expert"), None),
        P(("fsdp", "expert"), None),
        P("fsdp", None),
        P("fsdp", None),
        P("fsdp", None),
        P("fsdp", None),
        P("fsdp", None),
        P("fsdp"),
        P("fsdp"),
        P("expert", "fsdp", None),
        P("expert", "fsdp", None),
    )
    return jax.shard_map(local, mesh=mesh, in_specs=in_specs, out_specs=out_specs, check_vma=False)
```

```python
import functools
import math

import jax
import jax.numpy as jnp
from jax import lax
from jax.experimental import pallas as pl
from jax.experimental.pallas import tpu as pltpu
from jax.sharding import PartitionSpec as P

MODEL_WIDTH = 1536
QUERY_HEADS = 24
KEY_VALUE_HEADS = 8
HEAD_SIZE = 64
TOP = 8
CAP = 48


EPS = 1e-05
BASE = 10000.0
SCORE_SCALE = 0.015625
MASKED = -1e30


def rope_tables(doc_row):
    document_length = doc_row.shape[0]
    places = jnp.arange(document_length, dtype=jnp.int32)
    same_doc = doc_row[:, None] == doc_row[None, :]
    starts = jnp.min(jnp.where(same_doc, places[None, :], document_length), axis=1)
    position = (places - starts).astype(jnp.float32)
    half_width = HEAD_SIZE // 2
    inverse = jnp.exp(
        -math.log(BASE) * (2.0 * jnp.arange(half_width, dtype=jnp.float32) / HEAD_SIZE)
    )
    angle = position[:, None] * inverse[None, :]
    allowed = same_doc & (places[None, :] <= places[:, None])
    return (jnp.cos(angle), jnp.sin(angle), allowed)


def rotate(tensor, cosine_table, sine_table):
    half_width = HEAD_SIZE // 2
    first_half = tensor[..., :half_width]
    second = tensor[..., half_width:]
    cos_part = cosine_table[:, None, :]
    sin_part = sine_table[:, None, :]
    return jnp.concatenate(
        [first_half * cos_part - second * sin_part, second * cos_part + first_half * sin_part],
        axis=-1,
    )


def inverse_rotation(tensor, cosine_table, sine_table):
    half_width = HEAD_SIZE // 2
    first_half = tensor[..., :half_width]
    second = tensor[..., half_width:]
    cos_part = cosine_table[:, None, :]
    sin_part = sine_table[:, None, :]
    return jnp.concatenate(
        [first_half * cos_part + second * sin_part, second * cos_part - first_half * sin_part],
        axis=-1,
    )


def norm_forward(value_rows, gain):
    scale_inv = lax.rsqrt(jnp.mean(value_rows * value_rows, axis=-1, keepdims=True) + EPS)
    normed = value_rows * scale_inv
    return ((normed * gain).astype(jnp.bfloat16), normed, scale_inv)


def norm_backward(grad_out, normed, scale_inv, gain):
    grad_normed = grad_out * gain
    grad_gain = jnp.sum(grad_out * normed, axis=0)
    value_gradients = scale_inv * (
        grad_normed - normed * jnp.mean(grad_normed * normed, axis=-1, keepdims=True)
    )
    return (value_gradients, grad_gain)


def scores_of(query_rows, key_rows, allowed):
    document_length = query_rows.shape[0]
    group_rows = query_rows.reshape(
        document_length, KEY_VALUE_HEADS, QUERY_HEADS // KEY_VALUE_HEADS, HEAD_SIZE
    )
    scores = (
        jnp.einsum("qgrd,kgd->grqk", group_rows, key_rows, preferred_element_type=jnp.float32)
        * SCORE_SCALE
    )
    return jnp.where(allowed[None, None], scores, MASKED)


def forward_local(
    hidden_rows,
    doc_row,
    route_rows,
    gain_attn,
    w_query,
    key_matrix,
    value_matrix,
    w_output,
    gain_ffn,
    w_router,
):
    document_length = hidden_rows.shape[0]
    hidden_f = hidden_rows.astype(jnp.float32)
    attention_input, normed_attn, scale_attn = norm_forward(hidden_f, gain_attn)
    cosine_table, sine_table, allowed = rope_tables(doc_row)
    query_rows = jnp.dot(attention_input, w_query, preferred_element_type=jnp.float32).reshape(
        document_length, QUERY_HEADS, HEAD_SIZE
    )
    key_rows = jnp.dot(attention_input, key_matrix, preferred_element_type=jnp.float32).reshape(
        document_length, KEY_VALUE_HEADS, HEAD_SIZE
    )
    value_rows = (
        jnp.dot(attention_input, value_matrix, preferred_element_type=jnp.float32)
        .astype(jnp.bfloat16)
        .reshape(document_length, KEY_VALUE_HEADS, HEAD_SIZE)
    )
    query_rows = rotate(query_rows, cosine_table, sine_table).astype(jnp.bfloat16)
    key_rows = rotate(key_rows, cosine_table, sine_table).astype(jnp.bfloat16)
    scores = scores_of(query_rows, key_rows, allowed)
    top_score = jnp.max(scores, axis=-1, keepdims=True)
    log_total = top_score + jnp.log(jnp.sum(jnp.exp(scores - top_score), axis=-1, keepdims=True))
    weights = jnp.exp(scores - log_total).astype(jnp.bfloat16)
    attention_mixed = jnp.einsum(
        "grqk,kgd->qgrd", weights, value_rows, preferred_element_type=jnp.float32
    )
    attention_mixed = attention_mixed.reshape(document_length, QUERY_HEADS * HEAD_SIZE).astype(
        jnp.bfloat16
    )
    resid = hidden_f + jnp.dot(attention_mixed, w_output, preferred_element_type=jnp.float32)
    ffn_in, normed_ffn, scale_ffn = norm_forward(resid, gain_ffn)
    logits = jnp.dot(ffn_in, w_router, preferred_element_type=jnp.float32)
    probs = jax.nn.softmax(logits, axis=-1)
    picks = route_rows[:, :, None] == jnp.arange(probs.shape[1], dtype=jnp.int32)[None, None, :]
    gates = jnp.sum(jnp.where(picks, probs[:, None, :], 0.0), axis=-1)
    return (
        normed_attn,
        scale_attn,
        attention_input,
        cosine_table,
        sine_table,
        allowed,
        query_rows,
        key_rows,
        value_rows,
        attention_mixed,
        log_total,
        resid,
        ffn_in,
        normed_ffn,
        scale_ffn,
        probs,
        gates,
    )


def backward_local(
    state,
    route_rows,
    cot_rows,
    grad_ffn_in,
    grad_gates,
    gain_attn,
    w_query,
    key_matrix,
    value_matrix,
    w_output,
    gain_ffn,
    w_router,
):
    (
        normed_attn,
        scale_attn,
        attention_input,
        cosine_table,
        sine_table,
        allowed,
        query_rows,
        key_rows,
        value_rows,
        attention_mixed,
        log_total,
        resid,
        ffn_in,
        normed_ffn,
        scale_ffn,
        probs,
        gates,
    ) = state
    document_length = attention_input.shape[0]
    query_group = QUERY_HEADS // KEY_VALUE_HEADS
    grad_probs = jnp.where(route_rows, grad_gates, 0.0)
    grad_logits = (
        probs * (grad_probs - jnp.sum(probs * grad_probs, axis=-1, keepdims=True))
    ).astype(jnp.bfloat16)
    grad_router = jnp.dot(ffn_in.T, grad_logits, preferred_element_type=jnp.float32)
    grad_ffn_in = grad_ffn_in + jnp.dot(grad_logits, w_router.T, preferred_element_type=jnp.float32)
    grad_resid_part, grad_gain_ffn = norm_backward(grad_ffn_in, normed_ffn, scale_ffn, gain_ffn)
    grad_resid = cot_rows.astype(jnp.float32) + grad_resid_part
    grad_attn = grad_resid.astype(jnp.bfloat16)
    grad_output = jnp.dot(attention_mixed.T, grad_attn, preferred_element_type=jnp.float32)
    mixed_gradient = jnp.dot(grad_attn, w_output.T, preferred_element_type=jnp.float32).astype(
        jnp.bfloat16
    )
    scores = scores_of(query_rows, key_rows, allowed)
    weights = jnp.exp(scores - log_total)
    weights_low = weights.astype(jnp.bfloat16)
    gradient_by_group = mixed_gradient.reshape(
        document_length, KEY_VALUE_HEADS, query_group, HEAD_SIZE
    )
    mixed_by_group = attention_mixed.reshape(
        document_length, KEY_VALUE_HEADS, query_group, HEAD_SIZE
    )
    value_gradients = jnp.einsum(
        "grqk,qgrd->kgd", weights_low, gradient_by_group, preferred_element_type=jnp.float32
    )
    grad_weights = jnp.einsum(
        "qgrd,kgd->grqk", gradient_by_group, value_rows, preferred_element_type=jnp.float32
    )
    delta = jnp.transpose(
        jnp.sum(
            gradient_by_group.astype(jnp.float32) * mixed_by_group.astype(jnp.float32), axis=-1
        ),
        (1, 2, 0),
    )
    grad_scores = (weights * (grad_weights - delta[..., None]) * SCORE_SCALE).astype(jnp.bfloat16)
    query_by_group = query_rows.reshape(document_length, KEY_VALUE_HEADS, query_group, HEAD_SIZE)
    grad_query_rows = jnp.einsum(
        "grqk,kgd->qgrd", grad_scores, key_rows, preferred_element_type=jnp.float32
    ).reshape(document_length, QUERY_HEADS, HEAD_SIZE)
    key_row_gradient = jnp.einsum(
        "grqk,qgrd->kgd", grad_scores, query_by_group, preferred_element_type=jnp.float32
    )
    grad_query_rows = (
        inverse_rotation(grad_query_rows, cosine_table, sine_table)
        .reshape(document_length, QUERY_HEADS * HEAD_SIZE)
        .astype(jnp.bfloat16)
    )
    key_row_gradient = (
        inverse_rotation(key_row_gradient, cosine_table, sine_table)
        .reshape(document_length, KEY_VALUE_HEADS * HEAD_SIZE)
        .astype(jnp.bfloat16)
    )
    value_row_gradient = value_gradients.reshape(
        document_length, KEY_VALUE_HEADS * HEAD_SIZE
    ).astype(jnp.bfloat16)
    grad_query = jnp.dot(attention_input.T, grad_query_rows, preferred_element_type=jnp.float32)
    grad_key = jnp.dot(attention_input.T, key_row_gradient, preferred_element_type=jnp.float32)
    grad_value = jnp.dot(attention_input.T, value_row_gradient, preferred_element_type=jnp.float32)
    grad_attn_in = jnp.dot(grad_query_rows, w_query.T, preferred_element_type=jnp.float32)
    grad_attn_in = grad_attn_in + jnp.dot(
        key_row_gradient, key_matrix.T, preferred_element_type=jnp.float32
    )
    grad_attn_in = grad_attn_in + jnp.dot(
        value_row_gradient, value_matrix.T, preferred_element_type=jnp.float32
    )
    grad_hidden_part, grad_gain_attn = norm_backward(
        grad_attn_in, normed_attn, scale_attn, gain_attn
    )
    grad_in = grad_resid + grad_hidden_part
    return (
        grad_in,
        (grad_query, grad_key, grad_value, grad_output, grad_router, grad_gain_attn, grad_gain_ffn),
    )


MESH = pl.DeviceIdType.MESH
F32, BF16 = jnp.float32, jnp.bfloat16


def dot(a, b, da=1, db=0):
    return lax.dot_general(a, b, (((da,), (db,)), ((), ())), preferred_element_type=F32)


class Place:
    def __init__(self, shards, owners):
        self.shards, self.owners = shards, owners
        self.line = 4 if owners % 4 == 0 else 1
        self.side = owners // self.line
        self.chips = shards // 2
        self.f = lax.axis_index("fsdp")
        self.e = lax.axis_index("expert")
        self.a, self.b = self.e // self.side, self.e % self.side
        self.x, self.c = self.f // 2, self.f % 2

    def others(self, all_fsdp):
        out = [((self.f, self.e + self.side), self.a < self.line - 1)]
        out.append(((self.f, self.e - self.side), self.a > 0))
        for i in range(1, self.side):
            out.append(((self.f, self.a * self.side + (self.b + i) % self.side), None))
        if all_fsdp:
            out += [(((self.f + i) % self.shards, self.e), None) for i in range(1, self.shards)]
            return out
        out.append(((self.x * 2 + 1 - self.c, self.e), None))
        for i in range(1, self.chips):
            out.append((((self.x + i) % self.chips * 2 + self.c, self.e), None))
        return out

    def meet(self, all_fsdp=False):
        bar = pltpu.get_barrier_semaphore()
        others = self.others(all_fsdp)
        for dev, cond in others:

            def signal(dev=dev):
                pl.semaphore_signal(bar, inc=1, device_id=dev, device_id_type=MESH)

            if cond is None:
                signal()
            else:
                pl.when(cond)(signal)
        pl.semaphore_wait(
            bar,
            len(others)
            - 2
            + jnp.where(self.a < self.line - 1, 1, 0)
            + jnp.where(self.a > 0, 1, 0),
        )


def remote(src, dst, send, recv, dev):
    return pltpu.make_async_remote_copy(
        src_ref=src, dst_ref=dst, send_sem=send, recv_sem=recv, device_id=dev, device_id_type=MESH
    )


class LineGather:
    def __init__(self, at, buf, send, recv):
        self.at, self.buf, self.send, self.recv = at, buf, send, recv
        width, count = buf.shape[2], recv.shape[0]
        cut = [width * p // count // 128 * 128 for p in range(count)] + [width]
        self.parts = [pl.ds(lo, hi - lo) for lo, hi in zip(cut, cut[1:])]

    def copy(self, k, p, way, dev):
        ref = self.buf.at[k, :, self.parts[p]]
        return remote(ref, ref, self.send.at[p, way, k], self.recv.at[p, k], (self.at.f, dev))

    def up(self, k, p):
        return self.copy(k, p, 0, self.at.e + self.at.side)

    def down(self, k, p):
        return self.copy(k, p, 1, self.at.e - self.at.side)

    def across(self, k, i, p):
        at = self.at
        return self.copy(k, p, 1 + i, at.a * at.side + (at.b + i) % at.side)

    def spread(self, k, p, up, down):
        at = self.at
        if up:

            @pl.when(at.a < at.line - 1)
            def _():
                self.up(k, p).start()

        if down:

            @pl.when(at.a > 0)
            def _():
                self.down(k, p).start()

        for i in range(1, at.side):
            self.across(k, i, p).start()

    def begin(self):
        for p in range(len(self.parts)):
            self.spread(self.at.e, p, True, True)

    def relay_step(self, s):
        at = self.at
        for p in range(len(self.parts)):

            @pl.when(at.a - s >= 0)
            def _(p=p):
                k = at.e - s * at.side
                self.down(k, p).wait_recv()
                self.spread(k, p, True, False)

            @pl.when(at.a + s < at.line)
            def _(p=p):
                k = at.e + s * at.side
                self.up(k, p).wait_recv()
                self.spread(k, p, False, True)

    def relay(self):
        for s in range(1, self.at.line):
            self.relay_step(s)

    def each(self, use):
        at = self.at

        def near(s, carry):
            pl.when(s > 0)(lambda: self.relay_step(s))
            pl.when(at.a - s >= 0)(lambda: use(at.e - s * at.side))
            pl.when((s > 0) & (at.a + s < at.line))(lambda: use(at.e + s * at.side))
            return carry

        lax.fori_loop(0, at.line, near, 0)
        self.rest(use)

    def rest(self, use=None):
        at = self.at

        def take(n, carry):
            s, sign = n // 2, 1 - n % 2 * 2
            a = at.a + sign * s

            @pl.when((a >= 0) & (a < at.line) & (n != 1))
            def _():
                for i in range(1, at.side):
                    k = a * at.side + (at.b + i) % at.side
                    for p in range(len(self.parts)):
                        self.across(k, i, p).wait_recv()
                    if use is not None:
                        use(k)

            return carry

        lax.fori_loop(0, 2 * at.line, take, 0)

    def finish(self):
        at = self.at
        for s in range(at.line):
            k = s * at.side + at.b
            for p in range(len(self.parts)):

                @pl.when((at.a < at.line - 1) & (at.a >= s))
                def _(k=k, p=p):
                    self.up(k, p).wait_send()

                @pl.when((at.a > 0) & (at.a <= s))
                def _(k=k, p=p):
                    self.down(k, p).wait_send()

                for i in range(1, at.side):
                    self.across(k, i, p).wait_send()


class LineScatter:
    def __init__(self, at, part, side_in, line_in, own, sems):
        self.at, self.part, self.side_in, self.line_in, self.own = at, part, side_in, line_in, own
        self.ssend, self.srecv, self.lsend, self.lrecv = sems

    def across(self, s, i):
        at = self.at
        b = (at.b + i) % at.side
        j = at.side - 1 - i
        return remote(
            self.part.at[s * at.side + b],
            self.side_in.at[s, j],
            self.ssend.at[s, i - 1],
            self.srecv.at[s, j],
            (at.f, at.a * at.side + b),
        )

    def along(self, s, dev, slot):
        at = self.at
        return remote(
            self.part.at[s * at.side + at.b],
            self.line_in.at[slot],
            self.lsend.at[s],
            self.lrecv.at[slot],
            (at.f, dev),
        )

    def up(self, s):
        return self.along(s, self.at.e + self.at.side, s)

    def down(self, s):
        at = self.at
        return self.along(s, at.e - at.side, jnp.where(s == at.a - 1, at.line, s))

    def place(self, i):
        at = self.at
        return jnp.where(at.a < at.line // 2, at.line - 1 - i, i)

    def begin(self, make):
        at = self.at

        def step(n, carry):
            s, i = self.place(n % at.line), n // at.line + 1
            make(s * at.side + (at.b + i) % at.side)

            @pl.when(i < at.side)
            def _():
                self.across(s, i).start()

            return carry

        lax.fori_loop(0, at.owners, step, 0)

    def sum_step(self, n):
        at = self.at
        s = self.place(n)
        k = s * at.side + at.b
        for i in range(1, at.side):
            self.across(s, i).wait_recv()
        total = self.part[k].astype(F32)
        for j in range(at.side - 1):
            total = total + self.side_in[s, j].astype(F32)
        self.own[...] = total

        @pl.when(((s > at.a) & (at.a > 0)) | ((s < at.a) & (at.a < at.line - 1)))
        def _():
            self.along(s, at.e, s).wait_recv()
            self.own[...] += self.line_in[s].astype(F32)

        self.part[k] = self.own[...].astype(BF16)

        @pl.when(s > at.a)
        def _():
            self.up(s).start()

        @pl.when(s < at.a)
        def _():
            self.down(s).start()

    def sum_last(self):
        at = self.at
        self.own[...] = self.part[at.e].astype(F32)

        @pl.when(at.a > 0)
        def _():
            self.along(at.a, at.e, at.a).wait_recv()
            self.own[...] += self.line_in[at.a].astype(F32)

        @pl.when(at.a < at.line - 1)
        def _():
            self.along(at.a, at.e, at.line).wait_recv()
            self.own[...] += self.line_in[at.line].astype(F32)

    def finish(self):
        at = self.at
        for s in range(at.line):
            for i in range(1, at.side):
                self.across(s, i).wait_send()

            @pl.when(at.a < s)
            def _(s=s):
                self.up(s).wait_send()

            @pl.when(at.a > s)
            def _(s=s):
                self.down(s).wait_send()


def rope_of(allowed, tokens):
    lane = lax.broadcasted_iota(jnp.int32, (tokens, 128), 1)
    position = jnp.sum(allowed.astype(F32), axis=1, keepdims=True) - 1.0
    half = HEAD_SIZE // 2
    inverse = jnp.exp(-math.log(BASE) * (2.0 * (lane % half).astype(F32) / HEAD_SIZE))
    angle = position * inverse
    return jnp.cos(angle), jnp.sin(angle), lane % HEAD_SIZE < half


def turn(x, cos, sin, first):
    half = HEAD_SIZE // 2
    other = jnp.where(first, -pltpu.roll(x, 128 - half, 1), pltpu.roll(x, half, 1))
    return x * cos + other * sin


def visible(doc, tokens):
    row = lax.broadcasted_iota(jnp.int32, (tokens, tokens), 0)
    col = lax.broadcasted_iota(jnp.int32, (tokens, tokens), 1)
    key_doc = jnp.broadcast_to(doc.astype(F32), (tokens, tokens))
    own = jnp.sum(jnp.where(row == col, key_doc, 0.0), axis=1, keepdims=True)
    return (own == key_doc) & (col <= row)


def picked(routes, lane):
    ids = routes[...].astype(F32).T
    lane = lane.astype(F32)
    chosen = lane == ids[:, :1]
    for i in range(1, TOP):
        chosen = chosen | (lane == ids[:, i : i + 1])
    return chosen


def attend_kernel(sizes, hidden, doc, routes, gain_a, gain_f, *refs):
    shards, owners, tokens, experts = sizes
    shares, cot = refs[:5], refs[5]
    h1, q, k, v, mixed, lse, resid, sent, probs_out = refs[6:15]
    fulls, cot_out, left = refs[15:20], refs[20], refs[21]
    (bufs, cot_all, acc, lsem, xs, xr, ys, yr, ss, sr, cs, cr, ls, lr, own_left) = refs[22:]
    at = Place(shards, owners)
    rg = MODEL_WIDTH // shards
    half, quarter = rg // 2, rg // 4
    f = at.f
    sib = (at.x * 2 + 1 - at.c, at.e)
    over = ((at.x + 1) % at.chips * 2 + at.c, at.e)
    far = over[0]
    other = (at.x + 1) % at.chips * 2 + 1 - at.c
    mine = (at.a + at.b) % 2
    beside = (f, at.a * at.side + (at.b + 1) % at.side)
    step = jnp.where(at.a % 2 == 0, at.side, -at.side)
    along = (f, at.e + step)
    count = len(shares)

    own = [pltpu.make_async_copy(shares[n], bufs[n].at[f], lsem.at[n]) for n in range(count)]
    own.append(pltpu.make_async_copy(cot, cot_all.at[at.e], lsem.at[count]))
    for c in own:
        c.start()

    def piece(n, g, start, size, send, recv, dev):
        ref = bufs[n].at[g, pl.ds(pl.multiple_of(start, quarter), size)]
        return remote(ref, ref, send, recv, dev)

    def begins(i):
        return (mine * half, mine * half + quarter, (1 - mine) * half, (1 - mine) * half + quarter)[i]

    def out_x(n, i):
        start = pl.ds(pl.multiple_of(begins(i), quarter), quarter)
        return remote(
            shares[n].at[start], bufs[n].at[f, start], xs.at[n, i], xr.at[n, i], over
        )

    def in_x(n, i):
        return piece(n, far, begins(i), quarter, xs.at[n, i], xr.at[n, i], over)

    def out_yz(n, i):
        return piece(n, far, begins(i), quarter, ys.at[n, i], yr.at[n, i], (beside, along)[i])

    def in_yz(n, i):
        return piece(n, far, begins(2 + i), quarter, ys.at[n, i], yr.at[n, i], (beside, along)[i])

    def to_sib(n, i, g):
        return piece(n, g, begins(i), quarter, ss.at[n, i], sr.at[n, i], sib)

    def own_sib(n):
        return remote(shares[n], bufs[n].at[f], ss.at[n, 4], sr.at[n, 4], sib)

    def small_x():
        return remote(shares[4], bufs[4].at[f], xs.at[4, 0], xr.at[4, 0], over)

    def small_sib():
        return remote(bufs[4].at[far], bufs[4].at[far], ss.at[4, 0], sr.at[4, 0], sib)

    def pass_x(n, i):
        in_x(n, i).wait_recv()
        out_yz(n, i).start()
        to_sib(n, i, far).start()

    def pass_rest(n):
        for i in range(2):
            in_yz(n, i).wait_recv()
            to_sib(n, 2 + i, far).start()

    def from_sib(n):
        for i in range(4):
            to_sib(n, i, other).wait_recv()

    def lefts(n, i):
        g = (f + i) % shards
        return remote(
            (h1, mixed)[n].at[:, pl.ds(pl.multiple_of(g * rg, 128), rg)],
            left.at[pl.ds(f * tokens, tokens), pl.ds(n * rg, rg)],
            ls.at[n, i - 1], lr.at[n, i - 1], (g, at.e),
        )

    def left_own(n):
        return pltpu.make_async_copy(
            (h1, mixed)[n].at[:, pl.ds(pl.multiple_of(f * rg, 128), rg)],
            left.at[pl.ds(f * tokens, tokens), pl.ds(n * rg, rg)],
            own_left.at[n],
        )

    def send_left(n):
        left_own(n).start()
        for i in range(1, shards):
            lefts(n, i).start()

    at.meet(all_fsdp=True)
    order = (1, 2, 0, 3)
    for n in order[:3]:
        for i in range(2):
            out_x(n, i).start()
        own_sib(n).start()
    small_x().start()
    own_sib(4).start()
    for i in range(2):
        out_x(3, i).start()
    own_sib(3).start()
    cotg = LineGather(at, cot_all, cs, cr)
    own[count].wait()
    cotg.begin()

    x = hidden[...].astype(F32)
    scale = lax.rsqrt(jnp.mean(x * x, axis=1, keepdims=True) + EPS)
    h1[...] = (x * scale * gain_a[...].reshape(1, -1)).astype(BF16)
    allowed = visible(doc[...], tokens)
    cos, sin, first = rope_of(allowed, tokens)

    ends = (0, 1536, 2048, 2560)

    def project(g):
        part = h1[:, pl.ds(pl.multiple_of(g * rg, 128), rg)]
        return [dot(part, bufs[n][g]) for n in range(3)]

    for n in range(3):
        own[n].wait()
        acc[:, ends[n] : ends[n + 1]] = dot(
            h1[:, pl.ds(pl.multiple_of(f * rg, 128), rg)], bufs[n][f]
        )

    def add(g):
        for n, got in enumerate(project(g)):
            acc[:, ends[n] : ends[n + 1]] += got

    for n in range(3):
        own_sib(n).wait_recv()
    add(sib[0])
    for n in (1, 2):
        for i in range(2):
            pass_x(n, i)
    cotg.relay_step(1)
    pass_x(0, 0)
    cotg.relay_step(2)
    pass_x(0, 1)
    for n in (1, 2, 0):
        pass_rest(n)
    cotg.relay_step(3)
    pass_x(3, 0)
    add(far)
    for n in range(3):
        from_sib(n)
    add(other)
    small_x().wait_recv()
    small_sib().start()
    pass_x(3, 1)

    for j in range(16):
        cols = slice(128 * j, 128 * (j + 1))
        got = turn(acc[:, cols], cos, sin, first).astype(BF16)
        if j < 12:
            q[:, cols] = got
        else:
            k[:, 128 * (j - 12) : 128 * (j - 11)] = got
    v[...] = acc[:, 2048:].astype(BF16)
    ratio = QUERY_HEADS // KEY_VALUE_HEADS
    mask = jnp.concatenate([allowed] * ratio, axis=0)

    def head(ref, h):
        return ref[:, h * HEAD_SIZE : (h + 1) * HEAD_SIZE]

    for g in range(KEY_VALUE_HEADS):
        heads = range(g * ratio, (g + 1) * ratio)
        rows = jnp.concatenate([head(q, h) for h in heads], axis=0)
        s = jnp.where(mask, dot(rows, head(k, g), 1, 1) * SCORE_SCALE, MASKED)
        top = jnp.max(s, axis=1, keepdims=True)
        e = jnp.exp(s - top)
        total = jnp.sum(e, axis=1, keepdims=True)
        o = dot((e / total).astype(BF16), head(v, g)).astype(BF16)
        log_total = top + jnp.log(total)
        for i, h in enumerate(heads):
            mixed[:, h * HEAD_SIZE : (h + 1) * HEAD_SIZE] = o[i * tokens : (i + 1) * tokens]
            lse[:, h : h + 1] = log_total[i * tokens : (i + 1) * tokens]

    send_left(0)
    send_left(1)
    pass_rest(3)
    for n in (3, 4):
        own[n].wait()
        own_sib(n).wait_recv()
    small_sib().wait_recv()
    from_sib(3)
    total = x
    for g in range(shards):
        total = total + dot(mixed[:, g * rg : (g + 1) * rg], bufs[3][g])
    resid[...] = total
    scale = lax.rsqrt(jnp.mean(total * total, axis=1, keepdims=True) + EPS)
    h2 = (total * scale * gain_f[...].reshape(1, -1)).astype(BF16)
    sent[:, :MODEL_WIDTH] = h2
    logits = dot(h2[:, :rg], bufs[4][0], 1, 1)
    for g in range(1, shards):
        logits = logits + dot(h2[:, g * rg : (g + 1) * rg], bufs[4][g], 1, 1)
    logits = jnp.concatenate([logits, jnp.zeros((tokens, 128 - experts), F32)], axis=1)
    lane = lax.broadcasted_iota(jnp.int32, (tokens, 128), 1)
    live = lane < experts
    logits = jnp.where(live, logits, MASKED)
    e = jnp.where(live, jnp.exp(logits - jnp.max(logits, axis=1, keepdims=True)), 0.0)
    probs = e / jnp.sum(e, axis=1, keepdims=True)
    probs_out[...] = probs
    chosen = picked(routes, lane)
    row = lax.broadcasted_iota(jnp.int32, (tokens, tokens), 0)
    col = lax.broadcasted_iota(jnp.int32, (tokens, tokens), 1)
    below = jnp.where(row > col, 1.0, 0.0).astype(BF16)
    hits = jnp.where(chosen, 1.0, 0.0)
    rank = jnp.where(chosen, dot(below, hits.astype(BF16)), jnp.where(live, -1.0, 0.0))
    gate = jnp.where(chosen, probs, 0.0)
    high = gate.astype(BF16).astype(F32)
    low = gate - high
    meta = rank + pltpu.roll(high, experts, 1) + pltpu.roll(low, 2 * experts, 1)
    sent[:, MODEL_WIDTH:] = meta.astype(BF16)

    save = [pltpu.make_async_copy(bufs[n], fulls[n], lsem.at[n]) for n in range(count)]
    for c in save:
        c.start()
    cotg.rest()
    cotg.finish()
    keep = pltpu.make_async_copy(cot_all, cot_out, lsem.at[count])
    keep.start()
    for n in range(count):
        own_sib(n).wait_send()
    small_x().wait_send()
    small_sib().wait_send()
    for n in order:
        for i in range(2):
            out_x(n, i).wait_send()
            out_yz(n, i).wait_send()
        for i in range(4):
            to_sib(n, i, far).wait_send()
    for n in range(2):
        left_own(n).wait()
        for i in range(1, shards):
            lefts(n, i).wait()
    for c in save:
        c.wait()
    keep.wait()


def attend(sizes, hidden, doc, routes, gain_a, gain_f, shares, cot):
    shards, owners, tokens, experts = sizes
    rg = MODEL_WIDTH // shards
    side = owners // 4
    vm, dma = pltpu.VMEM, pltpu.SemaphoreType.DMA
    vmem, any_ = pl.BlockSpec(memory_space=pltpu.VMEM), pl.BlockSpec(memory_space=pl.ANY)
    n = len(shares)

    def shape(*dims, dtype=BF16):
        return jax.ShapeDtypeStruct(dims, dtype)

    outs = pl.pallas_call(
        functools.partial(attend_kernel, sizes),
        name="attend",
        out_shape=(
            shape(tokens, MODEL_WIDTH),
            shape(tokens, MODEL_WIDTH),
            shape(tokens, KEY_VALUE_HEADS * HEAD_SIZE),
            shape(tokens, KEY_VALUE_HEADS * HEAD_SIZE),
            shape(tokens, MODEL_WIDTH),
            shape(tokens, 128, dtype=F32),
            shape(tokens, MODEL_WIDTH, dtype=F32),
            shape(tokens, MODEL_WIDTH + 128),
            shape(tokens, 128, dtype=F32),
            *[shape(shards, *s.shape) for s in shares],
            shape(owners, tokens, MODEL_WIDTH),
            shape(shards * tokens, 2 * rg),
        ),
        in_specs=[vmem] * 5 + [any_] * (n + 1),
        out_specs=[vmem] * 9 + [any_] * (n + 2),
        scratch_shapes=[
            tuple(vm((shards, *s.shape), BF16) for s in shares),
            vm((owners, tokens, MODEL_WIDTH), BF16),
            vm((tokens, 2560), F32),
            dma((n + 1,)),
            dma((n, 2)),
            dma((n, 2)),
            dma((n, 2)),
            dma((n, 2)),
            dma((n, 5)),
            dma((n, 5)),
            dma((2, side + 1, owners)),
            dma((2, owners)),
            dma((2, shards - 1)),
            dma((2, shards - 1)),
            dma((2,)),
        ],
        compiler_params=pltpu.CompilerParams(
            collective_id=0, has_side_effects=True, vmem_limit_bytes=60 * 2**20
        ),
    )(hidden, doc, routes, gain_a, gain_f, *shares, cot)
    return outs[:9], outs[9 : 9 + n], outs[9 + n], outs[10 + n]


EARLY = 4


def moe_kernel(sizes, sent, cot, wgu, wd, back_out, comb_out, sums, far, away, *scratch):
    shards, owners, tokens, experts, held, pairing = sizes
    (rows_all, cot_buf, taken, cots, made, grads, slot_gate, slot_grad, place, wg_buf, wd_buf,
     acts, dus, gg, gd, from_core, stage, side1, line1,
     rs, rr, wsem, csem, coresend, corerecv, farsend, farrecv, osem, free, s1, s2, s3, s4,
     ) = scratch
    at = Place(shards, owners)
    groups = held // pairing
    slots = groups * CAP
    half = wd.shape[1]
    rg, rd = MODEL_WIDTH // shards, half // shards
    sibling = (at.x * 2 + 1 - at.c, at.e)

    def weights(g):
        out = []
        for m in range(pairing):
            h, slot = g * pairing + m, g % 2 * pairing + m
            out.append(pltpu.make_async_copy(wgu.at[h], wg_buf.at[slot], wsem.at[0, slot]))
            out.append(pltpu.make_async_copy(wd.at[h], wd_buf.at[slot], wsem.at[1, slot]))
        return out

    mine = pltpu.make_async_copy(sent, rows_all.at[at.e], osem.at[0, 0])
    mine.start()
    for c in weights(0):
        c.start()
    at.meet()
    rows = LineGather(at, rows_all, rs, rr)
    mine.wait()
    rows.begin()

    lane = lax.broadcasted_iota(jnp.int32, (128, slots), 1)
    row = lax.broadcasted_iota(jnp.int32, (128, slots), 0)

    def expert_of(j):
        return (at.e * held + j // CAP * pairing) // 2

    e_lane = expert_of(lane)
    find_rank = (row == e_lane).astype(F32).astype(BF16)
    slot_rank = (lane % CAP).astype(F32)
    e_row = expert_of(lax.broadcasted_iota(jnp.int32, (slots, 128), 0))
    col = lax.broadcasted_iota(jnp.int32, (slots, 128), 1)
    pick_gate = (col == e_row + experts) | (col == e_row + 2 * experts)

    def dispatch(k):
        rank_at = dot(rows_all[k, :, MODEL_WIDTH:], find_rank)
        pt = jnp.where(rank_at == slot_rank, 1.0, 0.0).astype(BF16)
        place[k] = pt
        got = dot(pt, rows_all[k], 0, 0)
        gate = jnp.sum(jnp.where(pick_gate, got[:, MODEL_WIDTH:], 0.0), axis=1, keepdims=True)
        gate = jnp.broadcast_to(gate, (slots, 128))
        to = pl.ds(k * CAP, CAP)
        for g in range(groups):
            taken[g, to, :] = got[g * CAP : (g + 1) * CAP, :MODEL_WIDTH].astype(BF16)
            slot_gate[g, to, :] = gate[g * CAP : (g + 1) * CAP]

    def dispatch_both(k):
        pull = pltpu.make_async_copy(cot.at[k], cot_buf.at[0], csem.at[0])
        pull.start()
        dispatch(k)
        pull.wait()
        got = dot(place[k], cot_buf[0], 0, 0).astype(BF16)
        to = pl.ds(k * CAP, CAP)
        for g in range(groups):
            cots[g, to, :] = got[g * CAP : (g + 1) * CAP]

    rows.each(dispatch_both)
    rows.finish()

    def through(g):
        for c in weights(g):
            c.wait()

        @pl.when(g + 1 < groups)
        def _():
            for c in weights(g + 1):
                c.start()

        gate = slot_gate[g][:, :1]
        total = jnp.zeros((owners * CAP, 1), F32)
        for m in range(pairing):
            h, slot = g * pairing + m, g % 2 * pairing + m
            gu = dot(taken[g], wg_buf[slot])
            a, b = gu[:, :half], gu[:, half:]
            sig = 1.0 / (1.0 + jnp.exp(-a))
            s = a * sig
            act = s * b
            acts[h] = (act * gate).astype(BF16)
            dp = dot(cots[g], wd_buf[slot], 1, 1)
            total = total + jnp.sum(act * dp, axis=1, keepdims=True)
            dact = dp * gate
            dus[h, :, :half] = (dact * b * sig * (1.0 + a * (1.0 - sig))).astype(BF16)
            dus[h, :, half:] = (dact * s).astype(BF16)
        slot_grad[g] = jnp.broadcast_to(total, (owners * CAP, 128))
        n = MODEL_WIDTH // 3
        for i in range(3):
            cols = slice(i * n, (i + 1) * n)
            y = 0.0
            dx = 0.0
            for m in range(pairing):
                h, slot = g * pairing + m, g % 2 * pairing + m
                y = y + dot(acts[h], wd_buf[slot, :, cols])
                dx = dx + dot(dus[h], wg_buf[slot, cols, :], 1, 1)
            made[g, :, cols] = y.astype(BF16)
            grads[g, :, cols] = dx.astype(BF16)

    def to_core(h):
        slot = h % 2
        out = []
        for i in range(at.chips):
            f = 2 * i + 1 - at.c
            for n, (buf, r) in enumerate(((gg, rg), (gd, rd))):
                out.append(
                    remote(
                        buf.at[slot, pl.ds(pl.multiple_of(f * r, r), r)],
                        from_core[n].at[slot, i],
                        coresend.at[slot, n, i],
                        corerecv.at[slot, n, i],
                        sibling,
                    )
                )
        return out

    def to_chips(h):
        return chip_copies(at, h, away, h, far, farsend, farrecv)

    def keep(h):
        slot = h % 2
        out = []
        for n in range(2):
            out.append(pltpu.make_async_copy(stage[n].at[slot, 0], sums[n].at[h], osem.at[n, slot]))
            for i in range(1, at.chips):
                out.append(
                    pltpu.make_async_copy(
                        stage[n].at[slot, i], away[n].at[h, i - 1], osem.at[2 * i + n, slot]
                    )
                )
        return out

    def add(h):
        slot = h % 2
        for c in to_core(h):
            c.wait()

        @pl.when(h >= 2)
        def _():
            leave(h - 2)

        for i in range(at.chips):
            x = (at.x + i) % at.chips
            f = 2 * x + at.c
            for n, (buf, r) in enumerate(((gg, rg), (gd, rd))):
                own = buf[slot, pl.ds(pl.multiple_of(f * r, r), r)].astype(F32)
                stage[n][slot, i] = (own + from_core[n][slot, x].astype(F32)).astype(BF16)
        for c in keep(h):
            c.start()

        @pl.when(h < held - 2)
        def _():
            pl.semaphore_signal(free, inc=1, device_id=sibling, device_id_type=MESH)

    def leave(h):
        for c in keep(h):
            c.wait()

        @pl.when(h < EARLY)
        def _():
            for c in to_chips(h):
                c.start()

    def weigh(h):
        g, slot = h // pairing, h % 2
        n = MODEL_WIDTH // 3
        for i in range(3):
            gg[slot, i * n : (i + 1) * n, :] = dot(
                taken[g, :, i * n : (i + 1) * n], dus[h], 0, 0
            ).astype(BF16)
        gd[slot] = dot(acts[h], cots[g], 0, 0).astype(BF16)

        @pl.when(h >= 2)
        def _():
            pl.semaphore_wait(free, 1)

        for c in to_core(h):
            c.start()

        @pl.when(h > 0)
        def _():
            add(h - 1)

    home = (col == e_row).astype(F32).astype(BF16)
    home_low = (col == e_row + experts).astype(F32).astype(BF16)
    parts = ((0, 512), (512, 1024), (1024, 1536))

    def make_back(k):
        to = pl.ds(k * CAP, CAP)
        dg = jnp.concatenate([slot_grad[g, to, :] for g in range(groups)], axis=0)
        high = dg.astype(BF16)
        low = (dg - high.astype(F32)).astype(BF16)
        pt = place[k]
        for lo, hi in parts:
            dx = jnp.concatenate([grads[g, to, lo:hi] for g in range(groups)], axis=0)
            rows_all[k, :, lo:hi] = dot(pt, dx).astype(BF16)
        rows_all[k, :, MODEL_WIDTH:] = dot(pt, high * home + low * home_low).astype(BF16)

    back = LineScatter(at, rows_all, side1, line1, back_out, (s1, s2, s3, s4))

    def step(i, carry):
        @pl.when(i < groups)
        def _():
            through(i)

        @pl.when(i == groups)
        def _():
            back.begin(make_back)

        @pl.when(i >= 1)
        def _():
            weigh(i - 1)

        @pl.when(i == held - 1)
        def _():
            back.sum_step(0)

        return carry

    lax.fori_loop(0, held + 1, step, 0)
    add(held - 1)
    back.sum_step(1)

    def combine(k, carry):
        to = pl.ds(k * CAP, CAP)
        slot = k % 2

        def put(j):
            return pltpu.make_async_copy(cot_buf.at[j % 2], comb_out.at[j], csem.at[j % 2])

        @pl.when(k >= 2)
        def _():
            put(k - 2).wait()

        for lo, hi in parts:
            y = jnp.concatenate([made[g, to, lo:hi] for g in range(groups)], axis=0)
            cot_buf[slot, :, lo:hi] = dot(place[k], y).astype(BF16)
        put(k).start()

        @pl.when(k == owners - 1)
        def _():
            put(k - 1).wait()
            put(k).wait()

        return carry

    lax.fori_loop(0, owners, combine, 0)
    for h in range(held - 2, held):
        leave(h)
    back.sum_step(2)
    back.sum_step(3)
    back.sum_last()
    back.finish()

    def drain(h, carry):
        for c in to_chips(h):
            c.wait()
        return carry

    lax.fori_loop(0, EARLY, drain, 0)


def chip_copies(at, h, away, j, far, send, recv):
    out = []
    for i in range(1, at.chips):
        back = at.chips - 1 - i
        dev = ((at.x + i) % at.chips * 2 + at.c, at.e)
        for n in range(2):
            out.append(
                remote(
                    away[n].at[h, i - 1], far[n].at[back, j], send.at[n, i - 1, j],
                    recv.at[n, back, j], dev,
                )
            )
    return out


def moe(sizes, sent, cot, wgu, wd):
    shards, owners, tokens, experts, held, pairing = sizes
    groups = held // pairing
    slots, rows = groups * CAP, owners * CAP
    hidden, half = wgu.shape[2], wd.shape[1]
    rg, rd = MODEL_WIDTH // shards, half // shards
    chips = shards // 2
    line = 4
    side = owners // line
    width = MODEL_WIDTH + 128
    vm, dma = pltpu.VMEM, pltpu.SemaphoreType.DMA
    any_, vmem = pl.BlockSpec(memory_space=pl.ANY), pl.BlockSpec(memory_space=pltpu.VMEM)

    def pair(lead):
        return (vm((*lead, rg, hidden), BF16), vm((*lead, rd, MODEL_WIDTH), BF16))

    def outs(lead):
        return (
            jax.ShapeDtypeStruct((*lead, rg, hidden), BF16),
            jax.ShapeDtypeStruct((*lead, rd, MODEL_WIDTH), BF16),
        )

    return pl.pallas_call(
        functools.partial(moe_kernel, sizes),
        name="moe",
        out_shape=(
            jax.ShapeDtypeStruct((tokens, width), F32),
            jax.ShapeDtypeStruct((owners, tokens, MODEL_WIDTH), BF16),
            outs((held,)),
            outs((chips - 1, EARLY)),
            outs((held, chips - 1)),
        ),
        in_specs=[any_] * 4,
        out_specs=(vmem, any_, (any_, any_), (any_, any_), (any_, any_)),
        scratch_shapes=[
            vm((owners, tokens, width), BF16),
            vm((2, tokens, MODEL_WIDTH), BF16),
            vm((groups, rows, MODEL_WIDTH), BF16),
            vm((groups, rows, MODEL_WIDTH), BF16),
            vm((groups, rows, MODEL_WIDTH), BF16),
            vm((groups, rows, MODEL_WIDTH), BF16),
            vm((groups, rows, 128), F32),
            vm((groups, rows, 128), F32),
            vm((owners, tokens, slots), BF16),
            vm((2 * pairing, MODEL_WIDTH, hidden), BF16),
            vm((2 * pairing, half, MODEL_WIDTH), BF16),
            vm((held, rows, half), BF16),
            vm((held, rows, hidden), BF16),
            vm((2, MODEL_WIDTH, hidden), BF16),
            vm((2, half, MODEL_WIDTH), BF16),
            pair((2, chips)),
            pair((2, chips)),
            vm((line, side - 1, tokens, width), BF16),
            vm((line + 1, tokens, width), BF16),
            dma((2, side + 1, owners)),
            dma((2, owners)),
            dma((2, 2 * pairing)),
            dma((2,)),
            dma((2, 2, chips)),
            dma((2, 2, chips)),
            dma((2, chips - 1, EARLY)),
            dma((2, chips - 1, EARLY)),
            dma((2 * chips, 2)),
            pltpu.SemaphoreType.REGULAR,
            dma((line, side)),
            dma((line, side)),
            dma((line,)),
            dma((line + 1,)),
        ],
        compiler_params=pltpu.CompilerParams(
            collective_id=1, has_side_effects=True, vmem_limit_bytes=63 * 2**20
        ),
    )(sent, cot, wgu, wd)


def reverse_kernel(sizes, hidden, doc, routes, gain_a, gain_f, cot, q, k, v, mixed, lse, resid, sent,
                   probs, back, wo, wr, wq, wk, wv, comb, left_in, away0, away1, *refs):
    shards, owners, tokens, experts, held = sizes
    block_out, grad_in, total_o, total_q, far = refs[:5]
    (w_bufs, left, turned, rights, dgrad, dattn_f, dqkv, aux, aux_in, comb_part, comb_side, comb_line,
     comb_own, part_o, side_o, line_o, own_o, part_q, side_q, line_q, own_q,
     wsem, rsend, rrecv, asend, arecv, farsend, farrecv, *sems) = refs[5:]
    at = Place(shards, owners)
    away = (away0, away1)
    rg = MODEL_WIDTH // shards
    piece = rg // owners
    split = dqkv.shape[1]
    f = at.f
    sibling = (at.x * 2 + 1 - at.c, at.e)
    over = ((at.x + 1) % at.chips * 2 + at.c, at.e)
    ratio = QUERY_HEADS // KEY_VALUE_HEADS

    fulls = (wo, wr, wq, wk, wv)
    loads = [pltpu.make_async_copy(comb, comb_part, wsem.at[0])]
    loads += [pltpu.make_async_copy(w, b, wsem.at[1 + i]) for i, (w, b) in enumerate(zip(fulls, w_bufs))]
    loads.append(pltpu.make_async_copy(left_in, left, wsem.at[6]))
    for c in loads:
        c.start()
    at.meet(all_fsdp=True)

    combine = LineScatter(at, comb_part, comb_side, comb_line, comb_own, sems[:4])
    outer = LineScatter(at, part_o, side_o, line_o, own_o, sems[4:8])
    inner = LineScatter(at, part_q, side_q, line_q, own_q, sems[8:12])
    outer_all = LineGather(at, total_o, sems[12], sems[13])
    inner_all = LineGather(at, total_q, sems[14], sems[15])
    loads[0].wait()
    combine.begin(lambda k: None)

    def rows(i):
        return pl.ds(pl.multiple_of(i * tokens, tokens), tokens)

    def block(chunk, g, send, dev):
        cols = (pl.ds(split, MODEL_WIDTH), pl.ds(0, split))[chunk]
        ref = rights.at[rows(g), cols]
        return remote(ref, ref, rsend.at[chunk, send], rrecv.at[chunk, g], dev)

    def send_rights(chunk):
        block(chunk, f, 0, sibling).start()
        block(chunk, f, 1, over).start()

    def pass_rights(chunk):
        block(chunk, over[0], 0, sibling).wait_recv()
        block(chunk, over[0], 2, sibling).start()

    def take_rights(chunk):
        block(chunk, sibling[0], 0, sibling).wait_recv()
        block(chunk, (at.x + 1) % at.chips * 2 + 1 - at.c, 0, sibling).wait_recv()

    def late(h):
        return chip_copies(at, h, away, h - EARLY, far, farsend, farrecv)

    h2 = sent[:, :MODEL_WIDTH]
    lane = lax.broadcasted_iota(jnp.int32, (tokens, 128), 1)
    chosen = picked(routes, lane)
    meta = back[:, MODEL_WIDTH:]
    dprobs = jnp.where(chosen, meta + pltpu.roll(meta, 128 - experts, 1), 0.0)
    p = probs[...]
    dlogits = (p * (dprobs - jnp.sum(p * dprobs, axis=1, keepdims=True))).astype(BF16)
    loads[1].wait()
    loads[2].wait()
    aux[...] = dot(dlogits, h2, 0, 0)[: aux.shape[0]]

    def full(i):
        return w_bufs[i][...].reshape(MODEL_WIDTH, -1)

    dh = back[:, :MODEL_WIDTH] + jnp.concatenate(
        [dot(dlogits[:, :experts], w_bufs[1][g]) for g in range(shards)], axis=1
    )
    x = resid[...]
    scale = lax.rsqrt(jnp.mean(x * x, axis=1, keepdims=True) + EPS)
    n = x * scale
    aux[experts + 1 : experts + 2, :] = jnp.sum(dh * n, axis=0, keepdims=True)
    dn = dh * gain_f[...].reshape(1, -1)
    dres = cot[...].astype(F32) + scale * (dn - n * jnp.mean(dn * n, axis=1, keepdims=True))
    dgrad[...] = dres
    dattn = dres.astype(BF16)
    rights[rows(f), split:] = dattn
    send_rights(0)
    for c in late(EARLY):
        c.start()
    dattn_f[...] = dot(dattn, full(0), 1, 1).astype(BF16)

    allowed = visible(doc[...], tokens)
    cos, sin, first = rope_of(allowed, tokens)
    mask = jnp.concatenate([allowed] * ratio, axis=0)

    def stack(ref, heads):
        return jnp.concatenate(
            [ref[:, h * HEAD_SIZE : (h + 1) * HEAD_SIZE] for h in heads], axis=0
        )

    kept = QUERY_HEADS * HEAD_SIZE
    span = KEY_VALUE_HEADS * HEAD_SIZE
    for g in range(KEY_VALUE_HEADS):
        heads = range(g * ratio, (g + 1) * ratio)
        one = slice(g * HEAD_SIZE, (g + 1) * HEAD_SIZE)
        qs, ks, vs = stack(q, heads), k[:, one], v[:, one]
        dos, os = stack(dattn_f, heads), stack(mixed, heads)
        logs = jnp.concatenate([lse[:, h : h + 1] for h in heads], axis=0)
        s = jnp.where(mask, dot(qs, ks, 1, 1) * SCORE_SCALE, MASKED)
        w = jnp.exp(s - logs)
        low = w.astype(BF16)
        delta = jnp.sum(dos.astype(F32) * os.astype(F32), axis=1, keepdims=True)
        ds = (w * (dot(dos, vs, 1, 1) - delta) * SCORE_SCALE).astype(BF16)
        dq = dot(ds, ks)
        for i, h in enumerate(heads):
            dqkv[:, h * HEAD_SIZE : (h + 1) * HEAD_SIZE] = dq[i * tokens : (i + 1) * tokens]
        dqkv[:, kept + g * HEAD_SIZE : kept + (g + 1) * HEAD_SIZE] = dot(ds, qs, 0, 0)
        at_v = kept + span + g * HEAD_SIZE
        dqkv[:, at_v : at_v + HEAD_SIZE] = dot(low, dos, 0, 0)
        if g == 2:
            combine.sum_step(0)
        if g == 5:
            pass_rights(0)

    for j in range((kept + span) // 128):
        cols = slice(128 * j, 128 * (j + 1))
        rights[rows(f), cols] = turn(dqkv[:, cols], cos, -sin, first).astype(BF16)
    rights[rows(f), kept + span : split] = dqkv[:, kept + span :].astype(BF16)
    send_rights(1)
    combine.sum_step(1)
    for i in range(3, 6):
        loads[i].wait()
    mine = rights[rows(f), :split]
    dh = dot(mine[:, :kept], full(2), 1, 1)
    dh = dh + dot(mine[:, kept : kept + span], full(3), 1, 1)
    dh = dh + dot(mine[:, kept + span :], full(4), 1, 1)
    x = hidden[...].astype(F32)
    scale = lax.rsqrt(jnp.mean(x * x, axis=1, keepdims=True) + EPS)
    n = x * scale
    aux[experts : experts + 1, :] = jnp.sum(dh * n, axis=0, keepdims=True)
    dn = dh * gain_a[...].reshape(1, -1)
    grad_in[...] = dgrad[...] + scale * (dn - n * jnp.mean(dn * n, axis=1, keepdims=True))

    def cols(g):
        return pl.ds(pl.multiple_of(g * rg, 128), rg)

    def auxes(i):
        g = (f + i) % shards
        return remote(
            aux.at[:, cols(g)], aux_in.at[i], asend.at[i - 1], arecv.at[i - 1], (g, at.e)
        )

    for i in range(1, shards):
        auxes(i).start()
    for h in range(EARLY + 1, held):
        for c in late(h):
            c.start()
    aux_in[0] = aux[:, cols(f)]

    loads[6].wait()
    turned[...] = left[...].T
    take_rights(0)
    step = 512

    def product(part, half, lo, hi):
        for a in range(lo, hi, step):
            got = dot(turned[half * rg : (half + 1) * rg], rights[:, a : a + step]).astype(BF16)
            for i in range(owners):
                part[i, :, a - lo : a - lo + step] = got[i * piece : (i + 1) * piece]

    product(part_o, 1, split, split + MODEL_WIDTH)
    outer.begin(lambda k: None)
    combine.sum_step(2)
    pass_rights(1)
    combine.sum_step(3)
    outer.sum_step(0)
    combine.sum_last()
    block_out[...] = (resid[...] + comb_own[...]).astype(BF16)
    take_rights(1)
    extra = aux_in[0]
    for i in range(1, shards):
        auxes(i).wait_recv()
        extra = extra + aux_in[i]
    extra = jnp.concatenate([extra, jnp.zeros((128 - extra.shape[0], rg), F32)], axis=0)
    extra = extra.T.astype(BF16)
    product(part_q, 0, 0, split)
    for i in range(owners):
        part_q[i, :, split:] = extra[i * piece : (i + 1) * piece]
    inner.begin(lambda k: None)
    for i in range(1, 4):
        outer.sum_step(i)
    outer.sum_last()
    total_o[at.e] = own_o[...].astype(BF16)
    outer_all.begin()
    inner.sum_step(0)
    inner.sum_step(1)
    outer_all.relay_step(1)
    inner.sum_step(2)
    outer_all.relay_step(2)
    inner.sum_step(3)
    outer_all.relay_step(3)
    inner.sum_last()
    total_q[at.e] = own_q[...].astype(BF16)
    inner_all.begin()
    inner_all.relay()
    outer_all.rest()
    inner_all.rest()
    for chunk in range(2):
        for i in range(3):
            block(chunk, f, i, sibling).wait_send()
    for i in range(1, shards):
        auxes(i).wait_send()
    for t in (combine, outer, inner, outer_all, inner_all):
        t.finish()
    for h in range(EARLY, held):
        for c in late(h):
            c.wait()


def reverse(sizes, vmem_args, fulls, comb, left, away):
    shards, owners, tokens, experts, held = sizes
    rg = MODEL_WIDTH // shards
    piece = rg // owners
    chips = shards // 2
    line = 4
    side = owners // line
    split = MODEL_WIDTH + 2 * KEY_VALUE_HEADS * HEAD_SIZE
    wide = split + 128
    extra = 48
    vm, dma = pltpu.VMEM, pltpu.SemaphoreType.DMA
    vmem, any_ = pl.BlockSpec(memory_space=pltpu.VMEM), pl.BlockSpec(memory_space=pl.ANY)

    def scatter(rows, width):
        return [
            vm((owners, rows, width), BF16),
            vm((line, side - 1, rows, width), BF16),
            vm((line + 1, rows, width), BF16),
            vm((rows, width), F32),
        ]

    shape = jax.ShapeDtypeStruct
    return pl.pallas_call(
        functools.partial(reverse_kernel, sizes),
        name="reverse",
        out_shape=(
            shape((tokens, MODEL_WIDTH), BF16),
            shape((tokens, MODEL_WIDTH), F32),
            shape((owners, piece, MODEL_WIDTH), BF16),
            shape((owners, piece, wide), BF16),
            tuple(shape((chips - 1, held - EARLY, *a.shape[2:]), BF16) for a in away),
        ),
        in_specs=[vmem] * len(vmem_args) + [any_] * 9,
        out_specs=(vmem, vmem, vmem, vmem, (any_, any_)),
        scratch_shapes=[
            tuple(vm(w.shape, BF16) for w in fulls),
            vm((shards * tokens, 2 * rg), BF16),
            vm((2 * rg, shards * tokens), BF16),
            vm((shards * tokens, split + MODEL_WIDTH), BF16),
            vm((tokens, MODEL_WIDTH), F32),
            vm((tokens, MODEL_WIDTH), BF16),
            vm((tokens, split), F32),
            vm((extra, MODEL_WIDTH), F32),
            vm((shards, extra, rg), F32),
            *scatter(tokens, MODEL_WIDTH),
            *scatter(piece, MODEL_WIDTH),
            *scatter(piece, wide),
            dma((7,)),
            dma((2, 3)),
            dma((2, shards)),
            dma((shards - 1,)),
            dma((shards - 1,)),
            dma((2, chips - 1, held - EARLY)),
            dma((2, chips - 1, held - EARLY)),
            *([dma((line, side)), dma((line, side)), dma((line,)), dma((line + 1,))] * 3),
            *([dma((1, side + 1, owners)), dma((1, owners))] * 2),
        ],
        compiler_params=pltpu.CompilerParams(
            collective_id=2, has_side_effects=True, vmem_limit_bytes=63 * 2**20
        ),
    )(*vmem_args, *fulls, comb, left, *away)


def plain_local(
    hidden_in,
    doc_ids,
    routes,
    gain_attn,
    w_query,
    key_matrix,
    value_matrix,
    w_output,
    gain_ffn,
    w_router,
    w_gateup,
    w_down,
    cotangent,
):
    tokens = hidden_in.shape[0]
    experts = w_router.shape[1]
    shards = lax.axis_size("fsdp")
    owners = lax.axis_size("expert")
    held = w_gateup.shape[0]
    half = w_down.shape[1]
    hidden_units = w_gateup.shape[2]
    pairing = 2 if held % 2 == 0 else 1
    groups = held // pairing
    slots = groups * CAP
    mine = lax.axis_index("expert")
    f32, bf16 = jnp.float32, jnp.bfloat16

    first = lax.all_gather(
        jnp.concatenate([w_query, key_matrix, value_matrix, w_router], axis=1),
        "fsdp",
        axis=0,
        tiled=True,
    )
    full_query, full_key, full_value, full_router = jnp.split(first, (1536, 2048, 2560), axis=1)
    full_output = lax.all_gather(w_output, "fsdp", axis=0, tiled=True)
    cot_all = lax.all_gather(cotangent, "expert", axis=0)
    weights_attn = (gain_attn, full_query, full_key, full_value, full_output, gain_ffn, full_router)
    state = forward_local(hidden_in, doc_ids[0], routes, *weights_attn)
    resid, ffn_in, probs = state[11], state[12], state[15]

    chosen = jnp.any(
        routes[:, :, None] == jnp.arange(experts, dtype=jnp.int32)[None, None, :], axis=1
    )
    below = jnp.tril(jnp.ones((tokens, tokens), bf16), -1)
    rank = jnp.dot(below, chosen.astype(bf16), preferred_element_type=f32)
    rank = jnp.where(chosen, rank, -1.0)
    gate = jnp.where(chosen, probs, 0.0)
    gate_high = gate.astype(bf16)
    gate_low = (gate - gate_high.astype(f32)).astype(bf16)
    meta = jnp.concatenate([rank.astype(bf16), gate_high, gate_low], axis=1)
    sent = jnp.concatenate(
        [ffn_in, meta, jnp.zeros((tokens, 128 - 3 * experts), bf16)], axis=1
    )
    got = lax.all_gather(sent, "expert", axis=0)
    rows_all = got[:, :, :MODEL_WIDTH]
    meta_all = got[:, :, MODEL_WIDTH:]
    lane = jnp.arange(slots, dtype=jnp.int32)
    slot_expert = (mine * held + (lane // CAP) * pairing) // 2
    spread = (jnp.arange(experts, dtype=jnp.int32)[:, None] == slot_expert[None, :]).astype(bf16)
    rank_at = jnp.dot(meta_all[:, :, :experts], spread, preferred_element_type=f32)
    gate_at = jnp.dot(
        meta_all[:, :, experts : 2 * experts], spread, preferred_element_type=f32
    ) + jnp.dot(meta_all[:, :, 2 * experts : 3 * experts], spread, preferred_element_type=f32)
    place = rank_at == (lane % CAP).astype(f32)[None, None, :]
    onehot = place.astype(bf16)
    gated = jnp.where(place, gate_at, 0.0)
    slot_gate = jnp.sum(gated, axis=1)

    def dispatch(rows):
        out = jnp.einsum("stj,std->sjd", onehot, rows, preferred_element_type=f32)
        return out.reshape(owners, groups, CAP, MODEL_WIDTH)

    taken = dispatch(rows_all).astype(bf16)
    cot_rows = dispatch(cot_all)
    slot_gate_4 = slot_gate.reshape(owners, groups, CAP, 1)
    grads_in = (cot_rows * slot_gate_4).astype(bf16)
    w_pairs = w_gateup.reshape(groups, pairing, MODEL_WIDTH, hidden_units)
    down_pairs = w_down.reshape(groups, pairing, half, MODEL_WIDTH)
    gate_up = jnp.einsum("secd,emdf->emscf", taken, w_pairs, preferred_element_type=f32)
    a, b = gate_up[..., :half], gate_up[..., half:]
    sigma = jax.nn.sigmoid(a)
    acted = (a * sigma * b).astype(bf16)
    made = jnp.einsum("emscf,emfd->secd", acted, down_pairs, preferred_element_type=f32)
    made = made.astype(bf16)
    grad_slot = jnp.sum(made.astype(f32) * cot_rows, axis=-1).reshape(owners, slots)
    grad_gate_back = jnp.where(place, grad_slot[:, None, :], 0.0).reshape(
        owners, tokens, groups, CAP
    )
    grad_gate_back = jnp.sum(grad_gate_back, axis=-1)
    onto = (
        (mine * held + jnp.arange(groups) * pairing)[:, None] // 2
        == jnp.arange(128, dtype=jnp.int32)[None, :]
    ).astype(bf16)
    grad_gate_back = jnp.dot(
        grad_gate_back.astype(bf16), onto, preferred_element_type=f32
    ).astype(bf16)
    weighted = (made.astype(f32) * slot_gate_4).astype(bf16).reshape(owners, slots, MODEL_WIDTH)
    combined = jnp.einsum("stj,sjd->std", onehot, weighted, preferred_element_type=f32)
    grad_acted = jnp.einsum("secd,emfd->emscf", grads_in, down_pairs, preferred_element_type=f32)
    grad_down = jnp.einsum("emscf,secd->emfd", acted, grads_in, preferred_element_type=f32)
    grad_a = grad_acted * b * sigma * (1.0 + a * (1.0 - sigma))
    grad_b = grad_acted * a * sigma
    joined = jnp.concatenate([grad_a, grad_b], axis=-1).astype(bf16)
    grad_gateup = jnp.einsum("secd,emscf->emdf", taken, joined, preferred_element_type=f32)
    grad_rows = jnp.einsum("emscf,emdf->secd", joined, w_pairs, preferred_element_type=f32)
    grad_rows = grad_rows.astype(bf16).reshape(owners, slots, MODEL_WIDTH)
    grad_ffn = jnp.einsum("stj,sjd->std", onehot, grad_rows, preferred_element_type=f32)
    back = jnp.concatenate([grad_ffn.astype(bf16), grad_gate_back], axis=-1)
    back = lax.psum_scatter(
        back.reshape(owners * tokens, -1), "expert", scatter_dimension=0, tiled=True
    ).astype(f32)
    grad_ffn, grad_gate_dense = back[:, :MODEL_WIDTH], back[:, MODEL_WIDTH : MODEL_WIDTH + experts]
    combined = lax.psum_scatter(
        combined.astype(bf16).reshape(owners * tokens, -1),
        "expert",
        scatter_dimension=0,
        tiled=True,
    )
    block_out = (resid + combined.astype(f32)).astype(bf16)
    grad_gateup, grad_down = (
        lax.psum_scatter(
            grad_gateup.reshape(held, MODEL_WIDTH, hidden_units).astype(bf16),
            "fsdp",
            scatter_dimension=1,
            tiled=True,
        ).astype(f32),
        lax.psum_scatter(
            grad_down.reshape(held, half, MODEL_WIDTH).astype(bf16),
            "fsdp",
            scatter_dimension=1,
            tiled=True,
        ).astype(f32),
    )
    grad_input, grads = backward_local(
        state, chosen, cotangent, grad_ffn, grad_gate_dense, *weights_attn
    )
    widths = [g.shape[1] if g.ndim == 2 else 1 for g in grads]
    flat = jnp.concatenate([g if g.ndim == 2 else g[:, None] for g in grads], axis=1)
    share = lax.psum_scatter(flat.astype(bf16), "fsdp", scatter_dimension=0, tiled=True)
    total = lax.psum(share, "expert").astype(f32)
    pieces = jnp.split(total, [sum(widths[: i + 1]) for i in range(len(widths) - 1)], axis=1)
    pieces = [p if g.ndim == 2 else p[:, 0] for p, g in zip(pieces, grads)]
    return (block_out, grad_input, *pieces, grad_gateup, grad_down)


def kernel_local(
    hidden_in,
    doc_ids,
    routes,
    gain_attn,
    w_query,
    key_matrix,
    value_matrix,
    w_output,
    gain_ffn,
    w_router,
    w_gateup,
    w_down,
    cotangent,
):
    tokens = hidden_in.shape[0]
    experts = w_router.shape[1]
    shards = lax.axis_size("fsdp")
    owners = lax.axis_size("expert")
    held = w_gateup.shape[0]
    pairing = 2 if held % 2 == 0 else 1
    f32, bf16 = jnp.float32, jnp.bfloat16

    shares = (w_query, key_matrix, value_matrix, w_output, w_router.T)
    made, fulls, cot_all, left = attend(
        (shards, owners, tokens, experts), hidden_in, doc_ids, routes.T, gain_attn, gain_ffn, shares,
        cotangent,
    )
    h1, q, k, v, mixed, lse, resid, sent, probs = made
    sizes = (shards, owners, tokens, experts, held, pairing)
    back, comb, sums, far, away = moe(sizes, sent, cot_all, w_gateup, w_down)
    wq, wk, wv, wo, wr = fulls
    block_out, grad_input, total_o, total_q, far_late = reverse(
        (shards, owners, tokens, experts, held),
        (hidden_in, doc_ids, routes.T, gain_attn, gain_ffn, cotangent, q, k, v, mixed,
         lse, resid, sent, probs, back),
        (wo, wr, wq, wk, wv),
        comb,
        left,
        away,
    )
    grad_gateup, grad_down = (
        s.astype(f32)
        + jnp.sum(jnp.concatenate([r, t], axis=1).astype(f32), axis=0)
        for s, r, t in zip(sums, far, far_late)
    )
    grad_output = total_o.reshape(-1, MODEL_WIDTH).astype(f32)
    rest = total_q.reshape(-1, total_q.shape[2]).astype(f32)
    return (
        block_out,
        grad_input,
        rest[:, :1536],
        rest[:, 1536:2048],
        rest[:, 2048:2560],
        grad_output,
        rest[:, 2560 : 2560 + experts],
        rest[:, 2560 + experts],
        rest[:, 2561 + experts],
        grad_gateup,
        grad_down,
    )


def local(*args):
    owners, held = lax.axis_size("expert"), args[10].shape[0]
    groups = held // (2 if held % 2 == 0 else 1)
    if lax.axis_size("fsdp") == 4 and owners == 8 and owners * groups * CAP <= 2048:
        return kernel_local(*args)
    return plain_local(*args)


def solution(mesh):
    in_specs = (
        P(("fsdp", "expert"), None),
        P(("fsdp", "expert"), None),
        P(("fsdp", "expert"), None),
        P(),
        P("fsdp", None),
        P("fsdp", None),
        P("fsdp", None),
        P("fsdp", None),
        P(),
        P("fsdp", None),
        P("expert", None, None),
        P("expert", None, None),
        P(("fsdp", "expert"), None),
    )
    out_specs = (
        P(("fsdp", "expert"), None),
        P(("fsdp", "expert"), None),
        P("fsdp", None),
        P("fsdp", None),
        P("fsdp", None),
        P("fsdp", None),
        P("fsdp", None),
        P("fsdp"),
        P("fsdp"),
        P("expert", "fsdp", None),
        P("expert", "fsdp", None),
    )
    return jax.shard_map(local, mesh=mesh, in_specs=in_specs, out_specs=out_specs, check_vma=False)
```

```python
import functools
import math

import jax
import jax.numpy as jnp
from jax import lax
from jax.experimental import pallas as pl
from jax.experimental.pallas import tpu as pltpu
from jax.sharding import PartitionSpec as P

MODEL_WIDTH = 1536
QUERY_HEADS = 24
KEY_VALUE_HEADS = 8
HEAD_SIZE = 64
TOP = 8
CAP = 48


EPS = 1e-05
BASE = 10000.0
SCORE_SCALE = 0.015625
MASKED = -1e30


def rope_tables(doc_row):
    document_length = doc_row.shape[0]
    places = jnp.arange(document_length, dtype=jnp.int32)
    same_doc = doc_row[:, None] == doc_row[None, :]
    starts = jnp.min(jnp.where(same_doc, places[None, :], document_length), axis=1)
    position = (places - starts).astype(jnp.float32)
    half_width = HEAD_SIZE // 2
    inverse = jnp.exp(
        -math.log(BASE) * (2.0 * jnp.arange(half_width, dtype=jnp.float32) / HEAD_SIZE)
    )
    angle = position[:, None] * inverse[None, :]
    allowed = same_doc & (places[None, :] <= places[:, None])
    return (jnp.cos(angle), jnp.sin(angle), allowed)


def rotate(tensor, cosine_table, sine_table):
    half_width = HEAD_SIZE // 2
    first_half = tensor[..., :half_width]
    second = tensor[..., half_width:]
    cos_part = cosine_table[:, None, :]
    sin_part = sine_table[:, None, :]
    return jnp.concatenate(
        [first_half * cos_part - second * sin_part, second * cos_part + first_half * sin_part],
        axis=-1,
    )


def inverse_rotation(tensor, cosine_table, sine_table):
    half_width = HEAD_SIZE // 2
    first_half = tensor[..., :half_width]
    second = tensor[..., half_width:]
    cos_part = cosine_table[:, None, :]
    sin_part = sine_table[:, None, :]
    return jnp.concatenate(
        [first_half * cos_part + second * sin_part, second * cos_part - first_half * sin_part],
        axis=-1,
    )


def norm_forward(value_rows, gain):
    scale_inv = lax.rsqrt(jnp.mean(value_rows * value_rows, axis=-1, keepdims=True) + EPS)
    normed = value_rows * scale_inv
    return ((normed * gain).astype(jnp.bfloat16), normed, scale_inv)


def norm_backward(grad_out, normed, scale_inv, gain):
    grad_normed = grad_out * gain
    grad_gain = jnp.sum(grad_out * normed, axis=0)
    value_gradients = scale_inv * (
        grad_normed - normed * jnp.mean(grad_normed * normed, axis=-1, keepdims=True)
    )
    return (value_gradients, grad_gain)


def scores_of(query_rows, key_rows, allowed):
    document_length = query_rows.shape[0]
    group_rows = query_rows.reshape(
        document_length, KEY_VALUE_HEADS, QUERY_HEADS // KEY_VALUE_HEADS, HEAD_SIZE
    )
    scores = (
        jnp.einsum("qgrd,kgd->grqk", group_rows, key_rows, preferred_element_type=jnp.float32)
        * SCORE_SCALE
    )
    return jnp.where(allowed[None, None], scores, MASKED)


def forward_local(
    hidden_rows,
    doc_row,
    route_rows,
    gain_attn,
    w_query,
    key_matrix,
    value_matrix,
    w_output,
    gain_ffn,
    w_router,
):
    document_length = hidden_rows.shape[0]
    hidden_f = hidden_rows.astype(jnp.float32)
    attention_input, normed_attn, scale_attn = norm_forward(hidden_f, gain_attn)
    cosine_table, sine_table, allowed = rope_tables(doc_row)
    query_rows = jnp.dot(attention_input, w_query, preferred_element_type=jnp.float32).reshape(
        document_length, QUERY_HEADS, HEAD_SIZE
    )
    key_rows = jnp.dot(attention_input, key_matrix, preferred_element_type=jnp.float32).reshape(
        document_length, KEY_VALUE_HEADS, HEAD_SIZE
    )
    value_rows = (
        jnp.dot(attention_input, value_matrix, preferred_element_type=jnp.float32)
        .astype(jnp.bfloat16)
        .reshape(document_length, KEY_VALUE_HEADS, HEAD_SIZE)
    )
    query_rows = rotate(query_rows, cosine_table, sine_table).astype(jnp.bfloat16)
    key_rows = rotate(key_rows, cosine_table, sine_table).astype(jnp.bfloat16)
    scores = scores_of(query_rows, key_rows, allowed)
    top_score = jnp.max(scores, axis=-1, keepdims=True)
    log_total = top_score + jnp.log(jnp.sum(jnp.exp(scores - top_score), axis=-1, keepdims=True))
    weights = jnp.exp(scores - log_total).astype(jnp.bfloat16)
    attention_mixed = jnp.einsum(
        "grqk,kgd->qgrd", weights, value_rows, preferred_element_type=jnp.float32
    )
    attention_mixed = attention_mixed.reshape(document_length, QUERY_HEADS * HEAD_SIZE).astype(
        jnp.bfloat16
    )
    resid = hidden_f + jnp.dot(attention_mixed, w_output, preferred_element_type=jnp.float32)
    ffn_in, normed_ffn, scale_ffn = norm_forward(resid, gain_ffn)
    logits = jnp.dot(ffn_in, w_router, preferred_element_type=jnp.float32)
    probs = jax.nn.softmax(logits, axis=-1)
    picks = route_rows[:, :, None] == jnp.arange(probs.shape[1], dtype=jnp.int32)[None, None, :]
    gates = jnp.sum(jnp.where(picks, probs[:, None, :], 0.0), axis=-1)
    return (
        normed_attn,
        scale_attn,
        attention_input,
        cosine_table,
        sine_table,
        allowed,
        query_rows,
        key_rows,
        value_rows,
        attention_mixed,
        log_total,
        resid,
        ffn_in,
        normed_ffn,
        scale_ffn,
        probs,
        gates,
    )


def backward_local(
    state,
    route_rows,
    cot_rows,
    grad_ffn_in,
    grad_gates,
    gain_attn,
    w_query,
    key_matrix,
    value_matrix,
    w_output,
    gain_ffn,
    w_router,
):
    (
        normed_attn,
        scale_attn,
        attention_input,
        cosine_table,
        sine_table,
        allowed,
        query_rows,
        key_rows,
        value_rows,
        attention_mixed,
        log_total,
        resid,
        ffn_in,
        normed_ffn,
        scale_ffn,
        probs,
        gates,
    ) = state
    document_length = attention_input.shape[0]
    query_group = QUERY_HEADS // KEY_VALUE_HEADS
    grad_probs = jnp.where(route_rows, grad_gates, 0.0)
    grad_logits = (
        probs * (grad_probs - jnp.sum(probs * grad_probs, axis=-1, keepdims=True))
    ).astype(jnp.bfloat16)
    grad_router = jnp.dot(ffn_in.T, grad_logits, preferred_element_type=jnp.float32)
    grad_ffn_in = grad_ffn_in + jnp.dot(grad_logits, w_router.T, preferred_element_type=jnp.float32)
    grad_resid_part, grad_gain_ffn = norm_backward(grad_ffn_in, normed_ffn, scale_ffn, gain_ffn)
    grad_resid = cot_rows.astype(jnp.float32) + grad_resid_part
    grad_attn = grad_resid.astype(jnp.bfloat16)
    grad_output = jnp.dot(attention_mixed.T, grad_attn, preferred_element_type=jnp.float32)
    mixed_gradient = jnp.dot(grad_attn, w_output.T, preferred_element_type=jnp.float32).astype(
        jnp.bfloat16
    )
    scores = scores_of(query_rows, key_rows, allowed)
    weights = jnp.exp(scores - log_total)
    weights_low = weights.astype(jnp.bfloat16)
    gradient_by_group = mixed_gradient.reshape(
        document_length, KEY_VALUE_HEADS, query_group, HEAD_SIZE
    )
    mixed_by_group = attention_mixed.reshape(
        document_length, KEY_VALUE_HEADS, query_group, HEAD_SIZE
    )
    value_gradients = jnp.einsum(
        "grqk,qgrd->kgd", weights_low, gradient_by_group, preferred_element_type=jnp.float32
    )
    grad_weights = jnp.einsum(
        "qgrd,kgd->grqk", gradient_by_group, value_rows, preferred_element_type=jnp.float32
    )
    delta = jnp.transpose(
        jnp.sum(
            gradient_by_group.astype(jnp.float32) * mixed_by_group.astype(jnp.float32), axis=-1
        ),
        (1, 2, 0),
    )
    grad_scores = (weights * (grad_weights - delta[..., None]) * SCORE_SCALE).astype(jnp.bfloat16)
    query_by_group = query_rows.reshape(document_length, KEY_VALUE_HEADS, query_group, HEAD_SIZE)
    grad_query_rows = jnp.einsum(
        "grqk,kgd->qgrd", grad_scores, key_rows, preferred_element_type=jnp.float32
    ).reshape(document_length, QUERY_HEADS, HEAD_SIZE)
    key_row_gradient = jnp.einsum(
        "grqk,qgrd->kgd", grad_scores, query_by_group, preferred_element_type=jnp.float32
    )
    grad_query_rows = (
        inverse_rotation(grad_query_rows, cosine_table, sine_table)
        .reshape(document_length, QUERY_HEADS * HEAD_SIZE)
        .astype(jnp.bfloat16)
    )
    key_row_gradient = (
        inverse_rotation(key_row_gradient, cosine_table, sine_table)
        .reshape(document_length, KEY_VALUE_HEADS * HEAD_SIZE)
        .astype(jnp.bfloat16)
    )
    value_row_gradient = value_gradients.reshape(
        document_length, KEY_VALUE_HEADS * HEAD_SIZE
    ).astype(jnp.bfloat16)
    grad_query = jnp.dot(attention_input.T, grad_query_rows, preferred_element_type=jnp.float32)
    grad_key = jnp.dot(attention_input.T, key_row_gradient, preferred_element_type=jnp.float32)
    grad_value = jnp.dot(attention_input.T, value_row_gradient, preferred_element_type=jnp.float32)
    grad_attn_in = jnp.dot(grad_query_rows, w_query.T, preferred_element_type=jnp.float32)
    grad_attn_in = grad_attn_in + jnp.dot(
        key_row_gradient, key_matrix.T, preferred_element_type=jnp.float32
    )
    grad_attn_in = grad_attn_in + jnp.dot(
        value_row_gradient, value_matrix.T, preferred_element_type=jnp.float32
    )
    grad_hidden_part, grad_gain_attn = norm_backward(
        grad_attn_in, normed_attn, scale_attn, gain_attn
    )
    grad_in = grad_resid + grad_hidden_part
    return (
        grad_in,
        (grad_query, grad_key, grad_value, grad_output, grad_router, grad_gain_attn, grad_gain_ffn),
    )


MESH = pl.DeviceIdType.MESH
F32, BF16 = jnp.float32, jnp.bfloat16


def dot(a, b, da=1, db=0):
    return lax.dot_general(a, b, (((da,), (db,)), ((), ())), preferred_element_type=F32)


class Place:
    def __init__(self, shards, owners):
        self.shards, self.owners = shards, owners
        self.line = 4 if owners % 4 == 0 else 1
        self.side = owners // self.line
        self.chips = shards // 2
        self.f = lax.axis_index("fsdp")
        self.e = lax.axis_index("expert")
        self.a, self.b = self.e // self.side, self.e % self.side
        self.x, self.c = self.f // 2, self.f % 2

    def detour(self):
        end = self.line - 1
        got = jnp.where(self.a % 2 == 0, end, 0)
        return got, end - got, self.e + jnp.where(self.a % 2 == 0, self.side, -self.side)

    def others(self, all_fsdp):
        out = [((self.f, self.e + self.side), self.a < self.line - 1)]
        out.append(((self.f, self.e - self.side), self.a > 0))
        for i in range(1, self.side):
            out.append(((self.f, self.a * self.side + (self.b + i) % self.side), None))
        if all_fsdp:
            out += [(((self.f + i) % self.shards, self.e), None) for i in range(1, self.shards)]
            return out
        out.append(((self.x * 2 + 1 - self.c, self.e), None))
        for i in range(1, self.chips):
            out.append((((self.x + i) % self.chips * 2 + self.c, self.e), None))
        return out

    def meet(self, all_fsdp=False):
        bar = pltpu.get_barrier_semaphore()
        others = self.others(all_fsdp)
        for dev, cond in others:

            def signal(dev=dev):
                pl.semaphore_signal(bar, inc=1, device_id=dev, device_id_type=MESH)

            if cond is None:
                signal()
            else:
                pl.when(cond)(signal)
        pl.semaphore_wait(
            bar,
            len(others)
            - 2
            + jnp.where(self.a < self.line - 1, 1, 0)
            + jnp.where(self.a > 0, 1, 0),
        )


def remote(src, dst, send, recv, dev):
    return pltpu.make_async_remote_copy(
        src_ref=src, dst_ref=dst, send_sem=send, recv_sem=recv, device_id=dev, device_id_type=MESH
    )


class LineGather:
    def __init__(self, at, buf, send, recv, balance=False):
        self.at, self.buf, self.send, self.recv = at, buf, send, recv
        self.balance = balance
        width, count = buf.shape[2], recv.shape[0]
        cut = [width * p // count // 128 * 128 for p in range(count)] + [width]
        self.parts = [pl.ds(lo, hi - lo) for lo, hi in zip(cut, cut[1:])]

    def copy(self, k, p, way, dev):
        ref = self.buf.at[k, :, self.parts[p]]
        return remote(ref, ref, self.send.at[p, way, k], self.recv.at[p, k], (self.at.f, dev))

    def up(self, k, p):
        return self.copy(k, p, 0, self.at.e + self.at.side)

    def down(self, k, p):
        return self.copy(k, p, 1, self.at.e - self.at.side)

    def across(self, k, i, p):
        at = self.at
        return self.copy(k, p, 1 + i, at.a * at.side + (at.b + i) % at.side)

    def spread(self, k, p, up, down, across=True):
        at = self.at
        if up:

            @pl.when(at.a < at.line - 1)
            def _():
                self.up(k, p).start()

        if down:

            @pl.when(at.a > 0)
            def _():
                self.down(k, p).start()

        if across and (p < len(self.parts) - 1 or not self.balance):
            self.across(k, 1, p).start()
        elif across:
            pl.when(k // at.side != at.detour()[0])(lambda: self.across(k, 1, p).start())

    def detour(self):
        at = self.at
        k = at.detour()[1] * at.side + 1 - at.b
        return self.copy(k, len(self.parts) - 1, 3, at.detour()[2])

    def begin(self):
        for p in range(len(self.parts)):
            self.spread(self.at.e, p, True, True)

    def relay_step(self, s, across=True):
        at = self.at
        for p in range(len(self.parts)):

            @pl.when(at.a - s >= 0)
            def _(p=p):
                k = at.e - s * at.side
                self.down(k, p).wait_recv()
                self.spread(k, p, True, False, across)

            @pl.when(at.a + s < at.line)
            def _(p=p):
                k = at.e + s * at.side
                self.up(k, p).wait_recv()
                self.spread(k, p, False, True, across)

    def cross(self, n):
        at = self.at
        a = (
            jnp.where(at.a > 0, at.a - 1, at.a + 1),
            jnp.where(at.a == 0, 2, jnp.where(at.a == at.line - 1, at.a - 2, at.a + 1)),
            jnp.where(at.a < at.line // 2, at.line - 1, 0),
        )[n - 1]
        for p in range(len(self.parts)):
            self.spread(a * at.side + at.b, p, False, False)

    def relay(self):
        for s in range(1, self.at.line):
            self.relay_step(s)

    def each(self, use):
        at = self.at

        def near(s, carry):
            pl.when(s > 0)(lambda: self.relay_step(s))
            pl.when(at.a - s >= 0)(lambda: use(at.e - s * at.side))
            pl.when((s > 0) & (at.a + s < at.line))(lambda: use(at.e + s * at.side))
            return carry

        lax.fori_loop(0, at.line, near, 0)
        self.rest(use)

    def rest(self, use=None):
        at = self.at

        def take(n, carry):
            s, sign = n // 2, 1 - n % 2 * 2
            a = at.a + sign * s

            @pl.when((a >= 0) & (a < at.line) & (n != 1))
            def _():
                k = a * at.side + 1 - at.b
                for p in range(len(self.parts)):
                    self.across(k, 1, p).wait_recv()
                if self.balance:
                    pl.when(a == at.detour()[1])(lambda: self.detour().start())
                if use is not None:
                    use(k)

            return carry

        lax.fori_loop(0, 2 * at.line, take, 0)

    def finish(self):
        at = self.at
        for s in range(at.line):
            k = s * at.side + at.b
            for p in range(len(self.parts)):

                @pl.when((at.a < at.line - 1) & (at.a >= s))
                def _(k=k, p=p):
                    self.up(k, p).wait_send()

                @pl.when((at.a > 0) & (at.a <= s))
                def _(k=k, p=p):
                    self.down(k, p).wait_send()

                if p < len(self.parts) - 1 or not self.balance:
                    self.across(k, 1, p).wait_send()
                else:
                    pl.when(s != at.detour()[0])(
                        lambda k=k, p=p: self.across(k, 1, p).wait_send()
                    )
        if self.balance:
            self.detour().wait_send()


class LineScatter:
    def __init__(self, at, part, side_in, line_in, own, extra, sems, balance=False):
        self.balance = balance
        self.at, self.part, self.side_in, self.line_in, self.own = at, part, side_in, line_in, own
        self.extra = extra
        self.ssend, self.srecv, self.lsend, self.lrecv, self.esem = sems
        width = part.shape[2]
        self.cut = width // 256 * 128
        self.parts = (pl.ds(0, self.cut), pl.ds(self.cut, width - self.cut))

    def across(self, s, p):
        at = self.at
        return remote(
            self.part.at[s * at.side + 1 - at.b, :, self.parts[p]],
            self.side_in.at[s, :, self.parts[p]],
            self.ssend.at[s, p],
            self.srecv.at[s, p],
            (at.f, at.a * at.side + 1 - at.b),
        )

    def detour(self):
        at = self.at
        k = at.detour()[0] * at.side + 1 - at.b
        return remote(
            self.part.at[k, :, self.parts[1]], self.extra, self.esem.at[0], self.esem.at[1],
            (at.f, at.detour()[2]),
        )

    def join(self):
        at = self.at
        s = at.detour()[1]
        k = s * at.side + 1 - at.b
        self.detour().wait_recv()
        mine = self.part[k, :, self.cut :].astype(F32)
        self.part[k, :, self.cut :] = (mine + self.extra[...].astype(F32)).astype(BF16)
        self.across(s, 1).start()

    def along(self, s, dev, slot):
        at = self.at
        return remote(
            self.part.at[s * at.side + at.b],
            self.line_in.at[slot],
            self.lsend.at[s],
            self.lrecv.at[slot],
            (at.f, dev),
        )

    def up(self, s):
        return self.along(s, self.at.e + self.at.side, s)

    def down(self, s):
        at = self.at
        return self.along(s, at.e - at.side, jnp.where(s == at.a - 1, at.line, s))

    def place(self, i):
        at = self.at
        return jnp.where(at.a < at.line // 2, at.line - 1 - i, i)

    def middle(self):
        at = self.at
        return (at.a > 0) & (at.a < at.line - 1)

    def launch(self, make, lo, hi):
        at = self.at
        got, passed, _ = at.detour()

        def step(n, carry):
            s = self.place(n)
            make(s * at.side + 1 - at.b)
            self.across(s, 0).start()
            if self.balance:
                pl.when(s == got)(lambda: self.detour().start())
                pl.when((s != got) & (s != passed))(lambda: self.across(s, 1).start())
            else:
                self.across(s, 1).start()
            return carry

        lax.fori_loop(lo, hi, step, 0)

    def begin(self, make):
        self.launch(make, 0, 2)

    def more(self, make):
        at = self.at
        if self.balance:
            pl.when(self.middle())(self.join)
        self.launch(make, 2, at.line)

        def step(n, carry):
            make(n * at.side + at.b)
            return carry

        lax.fori_loop(0, at.line, step, 0)

    def sum_step(self, n):
        at = self.at
        if n == 1 and self.balance:
            pl.when(jnp.logical_not(self.middle()))(self.join)
        s = self.place(n)
        k = s * at.side + at.b
        got = at.detour()[0]
        self.own[...] = self.part[k].astype(F32)
        self.across(s, 0).wait_recv()
        self.own[:, : self.cut] += self.side_in[s, :, : self.cut].astype(F32)

        @pl.when((s != got) | (not self.balance))
        def _():
            self.across(s, 1).wait_recv()
            self.own[:, self.cut :] += self.side_in[s, :, self.cut :].astype(F32)

        @pl.when(((s > at.a) & (at.a > 0)) | ((s < at.a) & (at.a < at.line - 1)))
        def _():
            self.along(s, at.e, s).wait_recv()
            self.own[...] += self.line_in[s].astype(F32)

        self.part[k] = self.own[...].astype(BF16)

        @pl.when(s > at.a)
        def _():
            self.up(s).start()

        @pl.when(s < at.a)
        def _():
            self.down(s).start()

    def sum_last(self):
        at = self.at
        self.own[...] = self.part[at.e].astype(F32)

        @pl.when(at.a > 0)
        def _():
            self.along(at.a, at.e, at.a).wait_recv()
            self.own[...] += self.line_in[at.a].astype(F32)

        @pl.when(at.a < at.line - 1)
        def _():
            self.along(at.a, at.e, at.line).wait_recv()
            self.own[...] += self.line_in[at.line].astype(F32)

    def finish(self):
        at = self.at
        if self.balance:
            self.detour().wait_send()
        for s in range(at.line):
            self.across(s, 0).wait_send()
            pl.when((s != at.detour()[0]) | (not self.balance))(
                lambda s=s: self.across(s, 1).wait_send()
            )

            @pl.when(at.a < s)
            def _(s=s):
                self.up(s).wait_send()

            @pl.when(at.a > s)
            def _(s=s):
                self.down(s).wait_send()


def rope_of(allowed, tokens):
    lane = lax.broadcasted_iota(jnp.int32, (tokens, 128), 1)
    position = jnp.sum(allowed.astype(F32), axis=1, keepdims=True) - 1.0
    half = HEAD_SIZE // 2
    inverse = jnp.exp(-math.log(BASE) * (2.0 * (lane % half).astype(F32) / HEAD_SIZE))
    angle = position * inverse
    return jnp.cos(angle), jnp.sin(angle), lane % HEAD_SIZE < half


def turn(x, cos, sin, first):
    half = HEAD_SIZE // 2
    other = jnp.where(first, -pltpu.roll(x, 128 - half, 1), pltpu.roll(x, half, 1))
    return x * cos + other * sin


def visible(doc, tokens):
    row = lax.broadcasted_iota(jnp.int32, (tokens, tokens), 0)
    col = lax.broadcasted_iota(jnp.int32, (tokens, tokens), 1)
    key_doc = jnp.broadcast_to(doc.astype(F32), (tokens, tokens))
    own = jnp.sum(jnp.where(row == col, key_doc, 0.0), axis=1, keepdims=True)
    return (own == key_doc) & (col <= row)


def picked(routes, lane):
    ids = routes[...].astype(F32).T
    lane = lane.astype(F32)
    chosen = lane == ids[:, :1]
    for i in range(1, TOP):
        chosen = chosen | (lane == ids[:, i : i + 1])
    return chosen


def attend_kernel(sizes, hidden, doc, routes, gain_a, gain_f, *refs):
    shards, owners, tokens, experts = sizes
    shares, cot = refs[:5], refs[5]
    h1, q, k, v, mixed, lse, resid, sent, probs_out = refs[6:15]
    fulls, cot_out, left = refs[15:20], refs[20], refs[21]
    (bufs, cot_all, acc, lsem, xs, xr, ys, yr, ss, sr, cs, cr, ls, lr, own_left) = refs[22:]
    at = Place(shards, owners)
    rg = MODEL_WIDTH // shards
    half, quarter = rg // 2, rg // 4
    f = at.f
    sib = (at.x * 2 + 1 - at.c, at.e)
    over = ((at.x + 1) % at.chips * 2 + at.c, at.e)
    far = over[0]
    other = (at.x + 1) % at.chips * 2 + 1 - at.c
    mine = (at.a + at.b) % 2
    beside = (f, at.a * at.side + (at.b + 1) % at.side)
    step = jnp.where(at.a % 2 == 0, at.side, -at.side)
    along = (f, at.e + step)
    count = len(shares)

    own = [pltpu.make_async_copy(shares[n], bufs[n].at[f], lsem.at[n]) for n in range(count)]
    own.append(pltpu.make_async_copy(cot, cot_all.at[at.e], lsem.at[count]))
    for c in own:
        c.start()

    def piece(n, g, start, size, send, recv, dev):
        ref = bufs[n].at[g, pl.ds(pl.multiple_of(start, quarter), size)]
        return remote(ref, ref, send, recv, dev)

    def begins(i):
        return (mine * half, mine * half + quarter, (1 - mine) * half, (1 - mine) * half + quarter)[i]

    def out_x(n, i):
        start = pl.ds(pl.multiple_of(begins(i), quarter), quarter)
        return remote(
            shares[n].at[start], bufs[n].at[f, start], xs.at[n, i], xr.at[n, i], over
        )

    def in_x(n, i):
        return piece(n, far, begins(i), quarter, xs.at[n, i], xr.at[n, i], over)

    def out_yz(n, i):
        return piece(n, far, begins(i), quarter, ys.at[n, i], yr.at[n, i], (beside, along)[i])

    def in_yz(n, i):
        return piece(n, far, begins(2 + i), quarter, ys.at[n, i], yr.at[n, i], (beside, along)[i])

    def to_sib(n, i, g):
        return piece(n, g, begins(i), quarter, ss.at[n, i], sr.at[n, i], sib)

    def own_sib(n):
        return remote(shares[n], bufs[n].at[f], ss.at[n, 4], sr.at[n, 4], sib)

    def small_x():
        return remote(shares[4], bufs[4].at[f], xs.at[4, 0], xr.at[4, 0], over)

    def small_sib():
        return remote(bufs[4].at[far], bufs[4].at[far], ss.at[4, 0], sr.at[4, 0], sib)

    def pass_x(n, i):
        in_x(n, i).wait_recv()
        out_yz(n, i).start()
        to_sib(n, i, far).start()

    def pass_rest(n):
        for i in range(2):
            in_yz(n, i).wait_recv()
            to_sib(n, 2 + i, far).start()

    def from_sib(n):
        for i in range(4):
            to_sib(n, i, other).wait_recv()

    def lefts(n, i):
        g = (f + i) % shards
        return remote(
            (h1, mixed)[n].at[:, pl.ds(pl.multiple_of(g * rg, 128), rg)],
            left.at[pl.ds(f * tokens, tokens), pl.ds(n * rg, rg)],
            ls.at[n, i - 1], lr.at[n, i - 1], (g, at.e),
        )

    def left_own(n):
        return pltpu.make_async_copy(
            (h1, mixed)[n].at[:, pl.ds(pl.multiple_of(f * rg, 128), rg)],
            left.at[pl.ds(f * tokens, tokens), pl.ds(n * rg, rg)],
            own_left.at[n],
        )

    def send_left(n):
        left_own(n).start()
        for i in range(1, shards):
            lefts(n, i).start()

    at.meet(all_fsdp=True)
    order = (1, 2, 0, 3)
    for n in order[:3]:
        for i in range(2):
            out_x(n, i).start()
        own_sib(n).start()
    small_x().start()
    own_sib(4).start()
    for i in range(2):
        out_x(3, i).start()
    own_sib(3).start()
    cotg = LineGather(at, cot_all, cs, cr)
    own[count].wait()
    cotg.begin()

    x = hidden[...].astype(F32)
    scale = lax.rsqrt(jnp.mean(x * x, axis=1, keepdims=True) + EPS)
    h1[...] = (x * scale * gain_a[...].reshape(1, -1)).astype(BF16)
    allowed = visible(doc[...], tokens)
    cos, sin, first = rope_of(allowed, tokens)

    ends = (0, 1536, 2048, 2560)

    def project(g):
        part = h1[:, pl.ds(pl.multiple_of(g * rg, 128), rg)]
        return [dot(part, bufs[n][g]) for n in range(3)]

    for n in range(3):
        own[n].wait()
        acc[:, ends[n] : ends[n + 1]] = dot(
            h1[:, pl.ds(pl.multiple_of(f * rg, 128), rg)], bufs[n][f]
        )

    def add(g):
        for n, got in enumerate(project(g)):
            acc[:, ends[n] : ends[n + 1]] += got

    for n in range(3):
        own_sib(n).wait_recv()
    add(sib[0])
    for n in (1, 2):
        for i in range(2):
            pass_x(n, i)
    cotg.relay_step(1, False)
    cotg.cross(1)
    pass_x(0, 0)
    cotg.relay_step(2, False)
    pass_x(0, 1)
    cotg.cross(2)
    for n in (1, 2, 0):
        pass_rest(n)
    pass_x(3, 0)
    cotg.relay_step(3, False)
    cotg.cross(3)
    add(far)
    for n in range(3):
        from_sib(n)
    add(other)
    small_x().wait_recv()
    small_sib().start()
    pass_x(3, 1)
    save = [pltpu.make_async_copy(bufs[n], fulls[n], lsem.at[n]) for n in range(count)]
    for c in save[:3]:
        c.start()

    for j in range(16):
        cols = slice(128 * j, 128 * (j + 1))
        got = turn(acc[:, cols], cos, sin, first).astype(BF16)
        if j < 12:
            q[:, cols] = got
        else:
            k[:, 128 * (j - 12) : 128 * (j - 11)] = got
    v[...] = acc[:, 2048:].astype(BF16)
    ratio = QUERY_HEADS // KEY_VALUE_HEADS
    mask = jnp.concatenate([allowed] * ratio, axis=0)

    def head(ref, h):
        return ref[:, h * HEAD_SIZE : (h + 1) * HEAD_SIZE]

    for g in range(KEY_VALUE_HEADS):
        heads = range(g * ratio, (g + 1) * ratio)
        rows = jnp.concatenate([head(q, h) for h in heads], axis=0)
        s = jnp.where(mask, dot(rows, head(k, g), 1, 1) * SCORE_SCALE, MASKED)
        top = jnp.max(s, axis=1, keepdims=True)
        e = jnp.exp(s - top)
        total = jnp.sum(e, axis=1, keepdims=True)
        o = dot((e / total).astype(BF16), head(v, g)).astype(BF16)
        log_total = top + jnp.log(total)
        for i, h in enumerate(heads):
            mixed[:, h * HEAD_SIZE : (h + 1) * HEAD_SIZE] = o[i * tokens : (i + 1) * tokens]
            lse[:, h : h + 1] = log_total[i * tokens : (i + 1) * tokens]

    send_left(0)
    send_left(1)
    pass_rest(3)
    for n in (3, 4):
        own[n].wait()
        own_sib(n).wait_recv()
    small_sib().wait_recv()
    from_sib(3)
    total = x
    for g in range(shards):
        total = total + dot(mixed[:, g * rg : (g + 1) * rg], bufs[3][g])
    resid[...] = total
    scale = lax.rsqrt(jnp.mean(total * total, axis=1, keepdims=True) + EPS)
    h2 = (total * scale * gain_f[...].reshape(1, -1)).astype(BF16)
    sent[:, :MODEL_WIDTH] = h2
    logits = dot(h2[:, :rg], bufs[4][0], 1, 1)
    for g in range(1, shards):
        logits = logits + dot(h2[:, g * rg : (g + 1) * rg], bufs[4][g], 1, 1)
    logits = jnp.concatenate([logits, jnp.zeros((tokens, 128 - experts), F32)], axis=1)
    lane = lax.broadcasted_iota(jnp.int32, (tokens, 128), 1)
    live = lane < experts
    logits = jnp.where(live, logits, MASKED)
    e = jnp.where(live, jnp.exp(logits - jnp.max(logits, axis=1, keepdims=True)), 0.0)
    probs = e / jnp.sum(e, axis=1, keepdims=True)
    probs_out[...] = probs
    chosen = picked(routes, lane)
    row = lax.broadcasted_iota(jnp.int32, (tokens, tokens), 0)
    col = lax.broadcasted_iota(jnp.int32, (tokens, tokens), 1)
    below = jnp.where(row > col, 1.0, 0.0).astype(BF16)
    hits = jnp.where(chosen, 1.0, 0.0)
    rank = jnp.where(chosen, dot(below, hits.astype(BF16)), jnp.where(live, -1.0, 0.0))
    gate = jnp.where(chosen, probs, 0.0)
    high = gate.astype(BF16).astype(F32)
    low = gate - high
    meta = rank + pltpu.roll(high, experts, 1) + pltpu.roll(low, 2 * experts, 1)
    sent[:, MODEL_WIDTH:] = meta.astype(BF16)

    for c in save[3:]:
        c.start()
    cotg.rest()
    cotg.finish()
    keep = pltpu.make_async_copy(cot_all, cot_out, lsem.at[count])
    keep.start()
    for n in range(count):
        own_sib(n).wait_send()
    small_x().wait_send()
    small_sib().wait_send()
    for n in order:
        for i in range(2):
            out_x(n, i).wait_send()
            out_yz(n, i).wait_send()
        for i in range(4):
            to_sib(n, i, far).wait_send()
    for n in range(2):
        left_own(n).wait()
        for i in range(1, shards):
            lefts(n, i).wait()
    for c in save:
        c.wait()
    keep.wait()


def attend(sizes, hidden, doc, routes, gain_a, gain_f, shares, cot):
    shards, owners, tokens, experts = sizes
    rg = MODEL_WIDTH // shards
    side = owners // 4
    vm, dma = pltpu.VMEM, pltpu.SemaphoreType.DMA
    vmem, any_ = pl.BlockSpec(memory_space=pltpu.VMEM), pl.BlockSpec(memory_space=pl.ANY)
    n = len(shares)

    def shape(*dims, dtype=BF16):
        return jax.ShapeDtypeStruct(dims, dtype)

    outs = pl.pallas_call(
        functools.partial(attend_kernel, sizes),
        name="attend",
        out_shape=(
            shape(tokens, MODEL_WIDTH),
            shape(tokens, MODEL_WIDTH),
            shape(tokens, KEY_VALUE_HEADS * HEAD_SIZE),
            shape(tokens, KEY_VALUE_HEADS * HEAD_SIZE),
            shape(tokens, MODEL_WIDTH),
            shape(tokens, 128, dtype=F32),
            shape(tokens, MODEL_WIDTH, dtype=F32),
            shape(tokens, MODEL_WIDTH + 128),
            shape(tokens, 128, dtype=F32),
            *[shape(shards, *s.shape) for s in shares],
            shape(owners, tokens, MODEL_WIDTH),
            shape(shards * tokens, 2 * rg),
        ),
        in_specs=[vmem] * 5 + [any_] * (n + 1),
        out_specs=[vmem] * 9 + [any_] * (n + 2),
        scratch_shapes=[
            tuple(vm((shards, *s.shape), BF16) for s in shares),
            vm((owners, tokens, MODEL_WIDTH), BF16),
            vm((tokens, 2560), F32),
            dma((n + 1,)),
            dma((n, 2)),
            dma((n, 2)),
            dma((n, 2)),
            dma((n, 2)),
            dma((n, 5)),
            dma((n, 5)),
            dma((2, side + 2, owners)),
            dma((2, owners)),
            dma((2, shards - 1)),
            dma((2, shards - 1)),
            dma((2,)),
        ],
        compiler_params=pltpu.CompilerParams(
            collective_id=0, has_side_effects=True, vmem_limit_bytes=60 * 2**20
        ),
    )(hidden, doc, routes, gain_a, gain_f, *shares, cot)
    return outs[:9], outs[9 : 9 + n], outs[9 + n], outs[10 + n]


EARLY = 4
AHEAD = 2


def moe_kernel(sizes, sent, cot, wgu, wd, back_out, comb_out, sums, far, away, *scratch):
    shards, owners, tokens, experts, held, pairing = sizes
    (rows_all, cot_buf, taken, cots, made, grads, slot_gate, slot_grad, place, wg_buf, wd_buf,
     acts, dus, gg, gd, from_core, stage, side1, line1, extra1,
     rs, rr, wsem, csem, coresend, corerecv, farsend, farrecv, osem, free, s1, s2, s3, s4, s5,
     ) = scratch
    at = Place(shards, owners)
    groups = held // pairing
    slots = groups * CAP
    half = wd.shape[1]
    rg, rd = MODEL_WIDTH // shards, half // shards
    sibling = (at.x * 2 + 1 - at.c, at.e)

    def weights(g):
        out = []
        for m in range(pairing):
            h, slot = g * pairing + m, g % 2 * pairing + m
            out.append(pltpu.make_async_copy(wgu.at[h], wg_buf.at[slot], wsem.at[0, slot]))
            out.append(pltpu.make_async_copy(wd.at[h], wd_buf.at[slot], wsem.at[1, slot]))
        return out

    mine = pltpu.make_async_copy(sent, rows_all.at[at.e], osem.at[0, 0])
    mine.start()
    for c in weights(0):
        c.start()
    at.meet()
    rows = LineGather(at, rows_all, rs, rr)
    mine.wait()
    rows.begin()

    lane = lax.broadcasted_iota(jnp.int32, (128, slots), 1)
    row = lax.broadcasted_iota(jnp.int32, (128, slots), 0)

    def expert_of(j):
        return (at.e * held + j // CAP * pairing) // 2

    e_lane = expert_of(lane)
    find_rank = (row == e_lane).astype(F32).astype(BF16)
    slot_rank = (lane % CAP).astype(F32)
    e_row = expert_of(lax.broadcasted_iota(jnp.int32, (slots, 128), 0))
    col = lax.broadcasted_iota(jnp.int32, (slots, 128), 1)
    pick_gate = (col == e_row + experts) | (col == e_row + 2 * experts)

    def dispatch(k):
        rank_at = dot(rows_all[k, :, MODEL_WIDTH:], find_rank)
        pt = jnp.where(rank_at == slot_rank, 1.0, 0.0).astype(BF16)
        place[k] = pt
        got = dot(pt, rows_all[k], 0, 0)
        gate = jnp.sum(jnp.where(pick_gate, got[:, MODEL_WIDTH:], 0.0), axis=1, keepdims=True)
        gate = jnp.broadcast_to(gate, (slots, 128))
        to = pl.ds(k * CAP, CAP)
        for g in range(groups):
            taken[g, to, :] = got[g * CAP : (g + 1) * CAP, :MODEL_WIDTH].astype(BF16)
            slot_gate[g, to, :] = gate[g * CAP : (g + 1) * CAP]

    def dispatch_both(k):
        pull = pltpu.make_async_copy(cot.at[k], cot_buf.at[0], csem.at[0])
        pull.start()
        dispatch(k)
        pull.wait()
        got = dot(place[k], cot_buf[0], 0, 0).astype(BF16)
        to = pl.ds(k * CAP, CAP)
        for g in range(groups):
            cots[g, to, :] = got[g * CAP : (g + 1) * CAP]

    rows.each(dispatch_both)
    rows.finish()

    def through(g):
        for c in weights(g):
            c.wait()

        @pl.when(g + 1 < groups)
        def _():
            for c in weights(g + 1):
                c.start()

        gate = slot_gate[g][:, :1]
        total = jnp.zeros((owners * CAP, 1), F32)
        for m in range(pairing):
            h, slot = g * pairing + m, g % 2 * pairing + m
            gu = dot(taken[g], wg_buf[slot])
            a, b = gu[:, :half], gu[:, half:]
            sig = 1.0 / (1.0 + jnp.exp(-a))
            s = a * sig
            act = s * b
            acts[h] = (act * gate).astype(BF16)
            dp = dot(cots[g], wd_buf[slot], 1, 1)
            total = total + jnp.sum(act * dp, axis=1, keepdims=True)
            dact = dp * gate
            dus[h, :, :half] = (dact * b * sig * (1.0 + a * (1.0 - sig))).astype(BF16)
            dus[h, :, half:] = (dact * s).astype(BF16)
        slot_grad[g] = jnp.broadcast_to(total, (owners * CAP, 128))
        n = MODEL_WIDTH // 3
        for i in range(3):
            cols = slice(i * n, (i + 1) * n)
            y = 0.0
            dx = 0.0
            for m in range(pairing):
                h, slot = g * pairing + m, g % 2 * pairing + m
                y = y + dot(acts[h], wd_buf[slot, :, cols])
                dx = dx + dot(dus[h], wg_buf[slot, cols, :], 1, 1)
            made[g, :, cols] = y.astype(BF16)
            grads[g, :, cols] = dx.astype(BF16)

    def to_core(h):
        slot = h % 2
        out = []
        for i in range(at.chips):
            f = 2 * i + 1 - at.c
            for n, (buf, r) in enumerate(((gg, rg), (gd, rd))):
                out.append(
                    remote(
                        buf.at[slot, pl.ds(pl.multiple_of(f * r, r), r)],
                        from_core[n].at[slot, i],
                        coresend.at[slot, n, i],
                        corerecv.at[slot, n, i],
                        sibling,
                    )
                )
        return out

    def to_chips(h):
        return chip_copies(at, h, away, h, far, farsend, farrecv)

    def keep(h):
        slot = h % 2
        out = []
        for n in range(2):
            out.append(pltpu.make_async_copy(stage[n].at[slot, 0], sums[n].at[h], osem.at[n, slot]))
            for i in range(1, at.chips):
                out.append(
                    pltpu.make_async_copy(
                        stage[n].at[slot, i], away[n].at[h, i - 1], osem.at[2 * i + n, slot]
                    )
                )
        return out

    def add(h):
        slot = h % 2
        for c in to_core(h):
            c.wait()

        for i in range(at.chips):
            x = (at.x + i) % at.chips
            f = 2 * x + at.c
            for n, (buf, r) in enumerate(((gg, rg), (gd, rd))):
                own = buf[slot, pl.ds(pl.multiple_of(f * r, r), r)].astype(F32)
                stage[n][slot, i] = (own + from_core[n][slot, x].astype(F32)).astype(BF16)
        for c in keep(h):
            c.start()

        @pl.when(h < held - 2)
        def _():
            pl.semaphore_signal(free, inc=1, device_id=sibling, device_id_type=MESH)

    def leave(h):
        for c in keep(h):
            c.wait()

        @pl.when(h < EARLY)
        def _():
            for c in to_chips(h):
                c.start()

    def weigh(h):
        g, slot = h // pairing, h % 2
        n = MODEL_WIDTH // 3
        for i in range(3):
            gg[slot, i * n : (i + 1) * n, :] = dot(
                taken[g, :, i * n : (i + 1) * n], dus[h], 0, 0
            ).astype(BF16)
        gd[slot] = dot(acts[h], cots[g], 0, 0).astype(BF16)

        @pl.when(h >= 2)
        def _():
            pl.semaphore_wait(free, 1)

        for c in to_core(h):
            c.start()

    home = (col == e_row).astype(F32).astype(BF16)
    home_low = (col == e_row + experts).astype(F32).astype(BF16)
    parts = ((0, 512), (512, 1024), (1024, 1536))

    def make_back(k):
        to = pl.ds(k * CAP, CAP)
        dg = jnp.concatenate([slot_grad[g, to, :] for g in range(groups)], axis=0)
        high = dg.astype(BF16)
        low = (dg - high.astype(F32)).astype(BF16)
        pt = place[k]
        for lo, hi in parts:
            dx = jnp.concatenate([grads[g, to, lo:hi] for g in range(groups)], axis=0)
            rows_all[k, :, lo:hi] = dot(pt, dx).astype(BF16)
        rows_all[k, :, MODEL_WIDTH:] = dot(pt, high * home + low * home_low).astype(BF16)

    back = LineScatter(at, rows_all, side1, line1, back_out, extra1, (s1, s2, s3, s4, s5), True)

    def step(i, carry):
        @pl.when(i < groups)
        def _():
            through(i)

        @pl.when(i == groups)
        def _():
            back.begin(make_back)
            back.more(make_back)

        def staged(back, act):
            h = jnp.where(i < groups, i, i - gap) - back
            early = (i >= back) & (i < AHEAD + back)
            pl.when(early | (i >= groups + back))(lambda: act(h))

        staged(2, leave)
        staged(0, weigh)
        staged(1, add)

        for n in range(2):

            @pl.when(i == groups + 3 + 4 * n)
            def _(n=n):
                back.sum_step(n)

        return carry

    gap = groups - AHEAD
    lax.fori_loop(0, held + gap, step, 0)
    leave(held - 2)
    add(held - 1)
    back.sum_step(2)

    def combine(k, carry):
        to = pl.ds(k * CAP, CAP)
        slot = k % 2

        def put(j):
            return pltpu.make_async_copy(cot_buf.at[j % 2], comb_out.at[j], csem.at[j % 2])

        @pl.when(k >= 2)
        def _():
            put(k - 2).wait()

        for lo, hi in parts:
            y = jnp.concatenate([made[g, to, lo:hi] for g in range(groups)], axis=0)
            cot_buf[slot, :, lo:hi] = dot(place[k], y).astype(BF16)
        put(k).start()

        @pl.when(k == owners - 1)
        def _():
            put(k - 1).wait()
            put(k).wait()

        return carry

    lax.fori_loop(0, owners, combine, 0)
    leave(held - 1)
    back.sum_step(3)
    back.sum_last()
    back.finish()

    def drain(h, carry):
        for c in to_chips(h):
            c.wait()
        return carry

    lax.fori_loop(0, EARLY, drain, 0)


def chip_copies(at, h, away, j, far, send, recv):
    out = []
    for i in range(1, at.chips):
        back = at.chips - 1 - i
        dev = ((at.x + i) % at.chips * 2 + at.c, at.e)
        for n in range(2):
            out.append(
                remote(
                    away[n].at[h, i - 1], far[n].at[back, h], send.at[n, i - 1, j],
                    recv.at[n, back, j], dev,
                )
            )
    return out


def moe(sizes, sent, cot, wgu, wd):
    shards, owners, tokens, experts, held, pairing = sizes
    groups = held // pairing
    slots, rows = groups * CAP, owners * CAP
    hidden, half = wgu.shape[2], wd.shape[1]
    rg, rd = MODEL_WIDTH // shards, half // shards
    chips = shards // 2
    line = 4
    side = owners // line
    width = MODEL_WIDTH + 128
    vm, dma = pltpu.VMEM, pltpu.SemaphoreType.DMA
    any_, vmem = pl.BlockSpec(memory_space=pl.ANY), pl.BlockSpec(memory_space=pltpu.VMEM)

    def pair(lead):
        return (vm((*lead, rg, hidden), BF16), vm((*lead, rd, MODEL_WIDTH), BF16))

    def outs(lead):
        return (
            jax.ShapeDtypeStruct((*lead, rg, hidden), BF16),
            jax.ShapeDtypeStruct((*lead, rd, MODEL_WIDTH), BF16),
        )

    return pl.pallas_call(
        functools.partial(moe_kernel, sizes),
        name="moe",
        out_shape=(
            jax.ShapeDtypeStruct((tokens, width), F32),
            jax.ShapeDtypeStruct((owners, tokens, MODEL_WIDTH), BF16),
            outs((held,)),
            outs((chips - 1, held)),
            outs((held, chips - 1)),
        ),
        in_specs=[any_] * 4,
        out_specs=(vmem, any_, (any_, any_), (any_, any_), (any_, any_)),
        scratch_shapes=[
            vm((owners, tokens, width), BF16),
            vm((2, tokens, MODEL_WIDTH), BF16),
            vm((groups, rows, MODEL_WIDTH), BF16),
            vm((groups, rows, MODEL_WIDTH), BF16),
            vm((groups, rows, MODEL_WIDTH), BF16),
            vm((groups, rows, MODEL_WIDTH), BF16),
            vm((groups, rows, 128), F32),
            vm((groups, rows, 128), F32),
            vm((owners, tokens, slots), BF16),
            vm((2 * pairing, MODEL_WIDTH, hidden), BF16),
            vm((2 * pairing, half, MODEL_WIDTH), BF16),
            vm((held, rows, half), BF16),
            vm((held, rows, hidden), BF16),
            vm((2, MODEL_WIDTH, hidden), BF16),
            vm((2, half, MODEL_WIDTH), BF16),
            pair((2, chips)),
            pair((2, chips)),
            vm((line, tokens, width), BF16),
            vm((line + 1, tokens, width), BF16),
            vm((tokens, width - width // 256 * 128), BF16),
            dma((2, side + 2, owners)),
            dma((2, owners)),
            dma((2, 2 * pairing)),
            dma((2,)),
            dma((2, 2, chips)),
            dma((2, 2, chips)),
            dma((2, chips - 1, EARLY)),
            dma((2, chips - 1, EARLY)),
            dma((2 * chips, 2)),
            pltpu.SemaphoreType.REGULAR,
            dma((line, 2)),
            dma((line, 2)),
            dma((line,)),
            dma((line + 1,)),
            dma((2,)),
        ],
        compiler_params=pltpu.CompilerParams(
            collective_id=1, has_side_effects=True, vmem_limit_bytes=63 * 2**20
        ),
    )(sent, cot, wgu, wd)


def reverse_kernel(sizes, hidden, doc, routes, gain_a, gain_f, cot, q, k, v, mixed, lse, resid, sent,
                   probs, back, wo, wr, wq, wk, wv, comb, left_in, away0, away1, far0, far1, *refs):
    shards, owners, tokens, experts, held = sizes
    block_out, grad_in, out_o, out_q, out_k, out_v, out_r, far = refs[:8]
    (w_bufs, left, turned, rights, dgrad, dattn_f, dqkv, aux, aux_in, comb_part, comb_side, comb_line,
     comb_own, comb_x, part_o, side_o, line_o, own_o, extra_o, part_q, side_q, line_q, own_q, extra_q,
     total_o, total_q, wsem, rsend, rrecv, asend, arecv, farsend, farrecv, *sems) = refs[8:]
    at = Place(shards, owners)
    away = (away0, away1)
    rg = MODEL_WIDTH // shards
    piece = rg // owners
    split = dqkv.shape[1]
    f = at.f
    sibling = (at.x * 2 + 1 - at.c, at.e)
    over = ((at.x + 1) % at.chips * 2 + at.c, at.e)
    ratio = QUERY_HEADS // KEY_VALUE_HEADS

    fulls = (wo, wr, wq, wk, wv)
    loads = [pltpu.make_async_copy(comb, comb_part, wsem.at[0])]
    loads += [pltpu.make_async_copy(w, b, wsem.at[1 + i]) for i, (w, b) in enumerate(zip(fulls, w_bufs))]
    loads.append(pltpu.make_async_copy(left_in, left, wsem.at[6]))
    for c in loads:
        c.start()
    at.meet(all_fsdp=True)

    combine = LineScatter(at, comb_part, comb_side, comb_line, comb_own, comb_x, sems[:5], True)
    outer = LineScatter(at, part_o, side_o, line_o, own_o, extra_o, sems[5:10], True)
    inner = LineScatter(at, part_q, side_q, line_q, own_q, extra_q, sems[10:15], True)
    outer_all = LineGather(at, total_o, sems[15], sems[16])
    inner_all = LineGather(at, total_q, sems[17], sems[18])
    loads[0].wait()
    nothing = lambda k: None
    combine.begin(nothing)

    def rows(i):
        return pl.ds(pl.multiple_of(i * tokens, tokens), tokens)

    def block(chunk, g, send, dev):
        cols = (pl.ds(split, MODEL_WIDTH), pl.ds(0, split))[chunk]
        ref = rights.at[rows(g), cols]
        return remote(ref, ref, rsend.at[chunk, send], rrecv.at[chunk, g], dev)

    def send_rights(chunk):
        block(chunk, f, 0, sibling).start()
        block(chunk, f, 1, over).start()

    def pass_rights(chunk):
        block(chunk, over[0], 0, sibling).wait_recv()
        block(chunk, over[0], 2, sibling).start()

    def take_rights(chunk):
        block(chunk, sibling[0], 0, sibling).wait_recv()
        block(chunk, (at.x + 1) % at.chips * 2 + 1 - at.c, 0, sibling).wait_recv()

    def late(h):
        return chip_copies(at, h, away, h - EARLY, far, farsend, farrecv)

    h2 = sent[:, :MODEL_WIDTH]
    lane = lax.broadcasted_iota(jnp.int32, (tokens, 128), 1)
    chosen = picked(routes, lane)
    meta = back[:, MODEL_WIDTH:]
    dprobs = jnp.where(chosen, meta + pltpu.roll(meta, 128 - experts, 1), 0.0)
    p = probs[...]
    dlogits = (p * (dprobs - jnp.sum(p * dprobs, axis=1, keepdims=True))).astype(BF16)
    loads[1].wait()
    loads[2].wait()
    aux[...] = dot(dlogits, h2, 0, 0)[: aux.shape[0]]

    def full(i):
        return w_bufs[i][...].reshape(MODEL_WIDTH, -1)

    dh = back[:, :MODEL_WIDTH] + jnp.concatenate(
        [dot(dlogits[:, :experts], w_bufs[1][g]) for g in range(shards)], axis=1
    )
    x = resid[...]
    scale = lax.rsqrt(jnp.mean(x * x, axis=1, keepdims=True) + EPS)
    n = x * scale
    aux[experts + 1 : experts + 2, :] = jnp.sum(dh * n, axis=0, keepdims=True)
    dn = dh * gain_f[...].reshape(1, -1)
    dres = cot[...].astype(F32) + scale * (dn - n * jnp.mean(dn * n, axis=1, keepdims=True))
    dgrad[...] = dres
    dattn = dres.astype(BF16)
    rights[rows(f), split:] = dattn
    send_rights(0)
    for c in late(EARLY):
        c.start()
    dattn_f[...] = dot(dattn, full(0), 1, 1).astype(BF16)
    combine.more(nothing)

    allowed = visible(doc[...], tokens)
    cos, sin, first = rope_of(allowed, tokens)
    mask = jnp.concatenate([allowed] * ratio, axis=0)

    def stack(ref, heads):
        return jnp.concatenate(
            [ref[:, h * HEAD_SIZE : (h + 1) * HEAD_SIZE] for h in heads], axis=0
        )

    kept = QUERY_HEADS * HEAD_SIZE
    span = KEY_VALUE_HEADS * HEAD_SIZE
    for g in range(KEY_VALUE_HEADS):
        heads = range(g * ratio, (g + 1) * ratio)
        one = slice(g * HEAD_SIZE, (g + 1) * HEAD_SIZE)
        qs, ks, vs = stack(q, heads), k[:, one], v[:, one]
        dos, os = stack(dattn_f, heads), stack(mixed, heads)
        logs = jnp.concatenate([lse[:, h : h + 1] for h in heads], axis=0)
        s = jnp.where(mask, dot(qs, ks, 1, 1) * SCORE_SCALE, MASKED)
        w = jnp.exp(s - logs)
        low = w.astype(BF16)
        delta = jnp.sum(dos.astype(F32) * os.astype(F32), axis=1, keepdims=True)
        ds = (w * (dot(dos, vs, 1, 1) - delta) * SCORE_SCALE).astype(BF16)
        dq = dot(ds, ks)
        for i, h in enumerate(heads):
            dqkv[:, h * HEAD_SIZE : (h + 1) * HEAD_SIZE] = dq[i * tokens : (i + 1) * tokens]
        dqkv[:, kept + g * HEAD_SIZE : kept + (g + 1) * HEAD_SIZE] = dot(ds, qs, 0, 0)
        at_v = kept + span + g * HEAD_SIZE
        dqkv[:, at_v : at_v + HEAD_SIZE] = dot(low, dos, 0, 0)
        if g == 3:
            combine.sum_step(0)

    for j in range((kept + span) // 128):
        cols = slice(128 * j, 128 * (j + 1))
        rights[rows(f), cols] = turn(dqkv[:, cols], cos, -sin, first).astype(BF16)
    rights[rows(f), kept + span : split] = dqkv[:, kept + span :].astype(BF16)
    send_rights(1)
    pass_rights(0)
    loads[6].wait()
    turned[...] = left[...].T
    take_rights(0)
    step = 512

    def product(part, half, lo, hi):
        for a in range(lo, hi, step):
            got = dot(turned[half * rg : (half + 1) * rg], rights[:, a : a + step]).astype(BF16)
            for i in range(owners):
                part[i, :, a - lo : a - lo + step] = got[i * piece : (i + 1) * piece]

    product(part_o, 1, split, split + MODEL_WIDTH)
    outer.begin(nothing)
    combine.sum_step(1)
    for i in range(3, 6):
        loads[i].wait()
    mine = rights[rows(f), :split]
    dh = dot(mine[:, :kept], full(2), 1, 1)
    dh = dh + dot(mine[:, kept : kept + span], full(3), 1, 1)
    dh = dh + dot(mine[:, kept + span :], full(4), 1, 1)
    x = hidden[...].astype(F32)
    scale = lax.rsqrt(jnp.mean(x * x, axis=1, keepdims=True) + EPS)
    n = x * scale
    aux[experts : experts + 1, :] = jnp.sum(dh * n, axis=0, keepdims=True)
    dn = dh * gain_a[...].reshape(1, -1)
    grad_in[...] = dgrad[...] + scale * (dn - n * jnp.mean(dn * n, axis=1, keepdims=True))

    def cols(g):
        return pl.ds(pl.multiple_of(g * rg, 128), rg)

    def auxes(i):
        g = (f + i) % shards
        return remote(
            aux.at[:, cols(g)], aux_in.at[i], asend.at[i - 1], arecv.at[i - 1], (g, at.e)
        )

    for i in range(1, shards):
        auxes(i).start()
    for h in range(EARLY + 1, held):
        for c in late(h):
            c.start()
    aux_in[0] = aux[:, cols(f)]

    outer.more(nothing)
    combine.sum_step(2)
    combine.sum_step(3)
    pass_rights(1)
    outer.sum_step(0)
    combine.sum_last()
    block_out[...] = (resid[...] + comb_own[...]).astype(BF16)
    take_rights(1)
    extra = aux_in[0]
    for i in range(1, shards):
        auxes(i).wait_recv()
        extra = extra + aux_in[i]
    extra = jnp.concatenate([extra, jnp.zeros((128 - extra.shape[0], rg), F32)], axis=0)
    extra = extra.T.astype(BF16)
    product(part_q, 0, 0, split)
    for i in range(owners):
        part_q[i, :, split:] = extra[i * piece : (i + 1) * piece]
    inner.begin(nothing)
    for i in range(1, 4):
        outer.sum_step(i)
    outer.sum_last()
    inner.more(nothing)
    total_o[at.e] = own_o[...].astype(BF16)
    outer_all.begin()
    inner.sum_step(0)
    outer_all.relay_step(1)
    inner.sum_step(1)
    inner.sum_step(2)
    outer_all.relay_step(2)
    inner.sum_step(3)
    inner.sum_last()
    total_q[at.e] = own_q[...].astype(BF16)
    inner_all.begin()
    outer_all.relay_step(3)
    inner_all.relay()
    outer_all.rest()

    def shown(k, carry):
        to = pl.ds(pl.multiple_of(k * piece, piece), piece)
        out_o[to, :] = total_o[k]
        return carry

    lax.fori_loop(0, owners, shown, 0)
    inner_all.rest()

    def shown_too(k, carry):
        to = pl.ds(pl.multiple_of(k * piece, piece), piece)
        out_q[to, :] = total_q[k, :, :kept]
        out_k[to, :] = total_q[k, :, kept : kept + span]
        out_v[to, :] = total_q[k, :, kept + span : split]
        out_r[to, :] = total_q[k, :, split:]
        return carry

    lax.fori_loop(0, owners, shown_too, 0)
    for chunk in range(2):
        for i in range(3):
            block(chunk, f, i, sibling).wait_send()
    for i in range(1, shards):
        auxes(i).wait_send()
    for t in (combine, outer, inner, outer_all, inner_all):
        t.finish()
    for h in range(EARLY, held):
        for c in late(h):
            c.wait()


def reverse(sizes, vmem_args, fulls, comb, left, away, far):
    shards, owners, tokens, experts, held = sizes
    rg = MODEL_WIDTH // shards
    piece = rg // owners
    chips = shards // 2
    line = 4
    side = owners // line
    split = MODEL_WIDTH + 2 * KEY_VALUE_HEADS * HEAD_SIZE
    wide = split + 128
    extra = 48
    vm, dma = pltpu.VMEM, pltpu.SemaphoreType.DMA
    vmem, any_ = pl.BlockSpec(memory_space=pltpu.VMEM), pl.BlockSpec(memory_space=pl.ANY)

    def scatter(rows, width):
        return [
            vm((owners, rows, width), BF16),
            vm((line, rows, width), BF16),
            vm((line + 1, rows, width), BF16),
            vm((rows, width), F32),
            vm((rows, width - width // 256 * 128), BF16),
        ]

    shape = jax.ShapeDtypeStruct
    return pl.pallas_call(
        functools.partial(reverse_kernel, sizes),
        name="reverse",
        out_shape=(
            shape((tokens, MODEL_WIDTH), BF16),
            shape((tokens, MODEL_WIDTH), F32),
            shape((rg, MODEL_WIDTH), BF16),
            shape((rg, MODEL_WIDTH), BF16),
            shape((rg, KEY_VALUE_HEADS * HEAD_SIZE), BF16),
            shape((rg, KEY_VALUE_HEADS * HEAD_SIZE), BF16),
            shape((rg, 128), BF16),
            tuple(shape(r.shape, BF16) for r in far),
        ),
        in_specs=[vmem] * len(vmem_args) + [any_] * 11,
        out_specs=(*[vmem] * 7, (any_, any_)),
        input_output_aliases={len(vmem_args) + 9: 7, len(vmem_args) + 10: 8},
        scratch_shapes=[
            tuple(vm(w.shape, BF16) for w in fulls),
            vm((shards * tokens, 2 * rg), BF16),
            vm((2 * rg, shards * tokens), BF16),
            vm((shards * tokens, split + MODEL_WIDTH), BF16),
            vm((tokens, MODEL_WIDTH), F32),
            vm((tokens, MODEL_WIDTH), BF16),
            vm((tokens, split), F32),
            vm((extra, MODEL_WIDTH), F32),
            vm((shards, extra, rg), F32),
            *scatter(tokens, MODEL_WIDTH),
            *scatter(piece, MODEL_WIDTH),
            *scatter(piece, wide),
            vm((owners, piece, MODEL_WIDTH), BF16),
            vm((owners, piece, wide), BF16),
            dma((7,)),
            dma((2, 3)),
            dma((2, shards)),
            dma((shards - 1,)),
            dma((shards - 1,)),
            dma((2, chips - 1, held - EARLY)),
            dma((2, chips - 1, held - EARLY)),
            *([dma((line, 2)), dma((line, 2)), dma((line,)), dma((line + 1,)), dma((2,))] * 3),
            *([dma((2, side + 2, owners)), dma((2, owners))] * 2),
        ],
        compiler_params=pltpu.CompilerParams(
            collective_id=2, has_side_effects=True, vmem_limit_bytes=63 * 2**20
        ),
    )(*vmem_args, *fulls, comb, left, *away, *far)


def finish_kernel(experts, *refs):
    (s0, r0, s1, r1, q, k, v, o, extra, rows, gradient), outs = refs[:11], refs[11:]
    o0, o1, oq, ok, ov, oo, orouter, oga, ogf, orows, ograd = outs
    for a, b, c in ((s0, r0, o0), (s1, r1, o1)):
        total = a[...].astype(F32)
        for i in range(b.shape[0]):
            total = total + b[i].astype(F32)
        c[...] = total
    for a, b in ((q, oq), (k, ok), (v, ov), (o, oo)):
        b[...] = a[...].astype(F32)
    orows[...] = rows[...]
    ograd[...] = gradient[...]

    @pl.when(pl.program_id(0) == 0)
    def _():
        turned = extra[...].astype(F32).T
        orouter[...] = turned[:experts]
        oga[...] = turned[experts]
        ogf[...] = turned[experts + 1]


def finish(experts, sums, far, grads, extra, rows, gradient):
    steps = 8
    rg = sums[0].shape[1]
    two = [s.reshape(-1, s.shape[2]) for s in sums]
    away = [r.reshape(r.shape[0], -1, r.shape[3]) for r in far]

    def rows_of(a):
        return pl.BlockSpec((a.shape[0] // steps, a.shape[1]), lambda i: (i, 0))

    def deep(a):
        return pl.BlockSpec((a.shape[0], a.shape[1] // steps, a.shape[2]), lambda i: (0, i, 0))

    def whole(shape):
        return pl.BlockSpec(shape, lambda i: (0,) * len(shape))

    shape = jax.ShapeDtypeStruct
    small = [(experts, rg), (rg,), (rg,)]
    out = pl.pallas_call(
        functools.partial(finish_kernel, experts),
        name="finish",
        grid=(steps,),
        out_shape=(
            *[shape(a.shape, F32) for a in two],
            *[shape(a.shape, F32) for a in grads],
            *[shape(a, F32) for a in small],
            shape(rows.shape, rows.dtype),
            shape(gradient.shape, F32),
        ),
        in_specs=[
            rows_of(two[0]), deep(away[0]), rows_of(two[1]), deep(away[1]),
            *[rows_of(a) for a in grads], whole(extra.shape), rows_of(rows), rows_of(gradient),
        ],
        out_specs=(
            *[rows_of(a) for a in two], *[rows_of(a) for a in grads], *[whole(a) for a in small],
            rows_of(rows), rows_of(gradient),
        ),
    )(two[0], away[0], two[1], away[1], *grads, extra, rows, gradient)
    return out[0].reshape(sums[0].shape), out[1].reshape(sums[1].shape), *out[2:]


def plain_local(
    hidden_in,
    doc_ids,
    routes,
    gain_attn,
    w_query,
    key_matrix,
    value_matrix,
    w_output,
    gain_ffn,
    w_router,
    w_gateup,
    w_down,
    cotangent,
):
    tokens = hidden_in.shape[0]
    experts = w_router.shape[1]
    shards = lax.axis_size("fsdp")
    owners = lax.axis_size("expert")
    held = w_gateup.shape[0]
    half = w_down.shape[1]
    hidden_units = w_gateup.shape[2]
    pairing = 2 if held % 2 == 0 else 1
    groups = held // pairing
    slots = groups * CAP
    mine = lax.axis_index("expert")
    f32, bf16 = jnp.float32, jnp.bfloat16

    first = lax.all_gather(
        jnp.concatenate([w_query, key_matrix, value_matrix, w_router], axis=1),
        "fsdp",
        axis=0,
        tiled=True,
    )
    full_query, full_key, full_value, full_router = jnp.split(first, (1536, 2048, 2560), axis=1)
    full_output = lax.all_gather(w_output, "fsdp", axis=0, tiled=True)
    cot_all = lax.all_gather(cotangent, "expert", axis=0)
    weights_attn = (gain_attn, full_query, full_key, full_value, full_output, gain_ffn, full_router)
    state = forward_local(hidden_in, doc_ids[0], routes, *weights_attn)
    resid, ffn_in, probs = state[11], state[12], state[15]

    chosen = jnp.any(
        routes[:, :, None] == jnp.arange(experts, dtype=jnp.int32)[None, None, :], axis=1
    )
    below = jnp.tril(jnp.ones((tokens, tokens), bf16), -1)
    rank = jnp.dot(below, chosen.astype(bf16), preferred_element_type=f32)
    rank = jnp.where(chosen, rank, -1.0)
    gate = jnp.where(chosen, probs, 0.0)
    gate_high = gate.astype(bf16)
    gate_low = (gate - gate_high.astype(f32)).astype(bf16)
    meta = jnp.concatenate([rank.astype(bf16), gate_high, gate_low], axis=1)
    sent = jnp.concatenate(
        [ffn_in, meta, jnp.zeros((tokens, 128 - 3 * experts), bf16)], axis=1
    )
    got = lax.all_gather(sent, "expert", axis=0)
    rows_all = got[:, :, :MODEL_WIDTH]
    meta_all = got[:, :, MODEL_WIDTH:]
    lane = jnp.arange(slots, dtype=jnp.int32)
    slot_expert = (mine * held + (lane // CAP) * pairing) // 2
    spread = (jnp.arange(experts, dtype=jnp.int32)[:, None] == slot_expert[None, :]).astype(bf16)
    rank_at = jnp.dot(meta_all[:, :, :experts], spread, preferred_element_type=f32)
    gate_at = jnp.dot(
        meta_all[:, :, experts : 2 * experts], spread, preferred_element_type=f32
    ) + jnp.dot(meta_all[:, :, 2 * experts : 3 * experts], spread, preferred_element_type=f32)
    place = rank_at == (lane % CAP).astype(f32)[None, None, :]
    onehot = place.astype(bf16)
    gated = jnp.where(place, gate_at, 0.0)
    slot_gate = jnp.sum(gated, axis=1)

    def dispatch(rows):
        out = jnp.einsum("stj,std->sjd", onehot, rows, preferred_element_type=f32)
        return out.reshape(owners, groups, CAP, MODEL_WIDTH)

    taken = dispatch(rows_all).astype(bf16)
    cot_rows = dispatch(cot_all)
    slot_gate_4 = slot_gate.reshape(owners, groups, CAP, 1)
    grads_in = (cot_rows * slot_gate_4).astype(bf16)
    w_pairs = w_gateup.reshape(groups, pairing, MODEL_WIDTH, hidden_units)
    down_pairs = w_down.reshape(groups, pairing, half, MODEL_WIDTH)
    gate_up = jnp.einsum("secd,emdf->emscf", taken, w_pairs, preferred_element_type=f32)
    a, b = gate_up[..., :half], gate_up[..., half:]
    sigma = jax.nn.sigmoid(a)
    acted = (a * sigma * b).astype(bf16)
    made = jnp.einsum("emscf,emfd->secd", acted, down_pairs, preferred_element_type=f32)
    made = made.astype(bf16)
    grad_slot = jnp.sum(made.astype(f32) * cot_rows, axis=-1).reshape(owners, slots)
    grad_gate_back = jnp.where(place, grad_slot[:, None, :], 0.0).reshape(
        owners, tokens, groups, CAP
    )
    grad_gate_back = jnp.sum(grad_gate_back, axis=-1)
    onto = (
        (mine * held + jnp.arange(groups) * pairing)[:, None] // 2
        == jnp.arange(128, dtype=jnp.int32)[None, :]
    ).astype(bf16)
    grad_gate_back = jnp.dot(
        grad_gate_back.astype(bf16), onto, preferred_element_type=f32
    ).astype(bf16)
    weighted = (made.astype(f32) * slot_gate_4).astype(bf16).reshape(owners, slots, MODEL_WIDTH)
    combined = jnp.einsum("stj,sjd->std", onehot, weighted, preferred_element_type=f32)
    grad_acted = jnp.einsum("secd,emfd->emscf", grads_in, down_pairs, preferred_element_type=f32)
    grad_down = jnp.einsum("emscf,secd->emfd", acted, grads_in, preferred_element_type=f32)
    grad_a = grad_acted * b * sigma * (1.0 + a * (1.0 - sigma))
    grad_b = grad_acted * a * sigma
    joined = jnp.concatenate([grad_a, grad_b], axis=-1).astype(bf16)
    grad_gateup = jnp.einsum("secd,emscf->emdf", taken, joined, preferred_element_type=f32)
    grad_rows = jnp.einsum("emscf,emdf->secd", joined, w_pairs, preferred_element_type=f32)
    grad_rows = grad_rows.astype(bf16).reshape(owners, slots, MODEL_WIDTH)
    grad_ffn = jnp.einsum("stj,sjd->std", onehot, grad_rows, preferred_element_type=f32)
    back = jnp.concatenate([grad_ffn.astype(bf16), grad_gate_back], axis=-1)
    back = lax.psum_scatter(
        back.reshape(owners * tokens, -1), "expert", scatter_dimension=0, tiled=True
    ).astype(f32)
    grad_ffn, grad_gate_dense = back[:, :MODEL_WIDTH], back[:, MODEL_WIDTH : MODEL_WIDTH + experts]
    combined = lax.psum_scatter(
        combined.astype(bf16).reshape(owners * tokens, -1),
        "expert",
        scatter_dimension=0,
        tiled=True,
    )
    block_out = (resid + combined.astype(f32)).astype(bf16)
    grad_gateup, grad_down = (
        lax.psum_scatter(
            grad_gateup.reshape(held, MODEL_WIDTH, hidden_units).astype(bf16),
            "fsdp",
            scatter_dimension=1,
            tiled=True,
        ).astype(f32),
        lax.psum_scatter(
            grad_down.reshape(held, half, MODEL_WIDTH).astype(bf16),
            "fsdp",
            scatter_dimension=1,
            tiled=True,
        ).astype(f32),
    )
    grad_input, grads = backward_local(
        state, chosen, cotangent, grad_ffn, grad_gate_dense, *weights_attn
    )
    widths = [g.shape[1] if g.ndim == 2 else 1 for g in grads]
    flat = jnp.concatenate([g if g.ndim == 2 else g[:, None] for g in grads], axis=1)
    share = lax.psum_scatter(flat.astype(bf16), "fsdp", scatter_dimension=0, tiled=True)
    total = lax.psum(share, "expert").astype(f32)
    pieces = jnp.split(total, [sum(widths[: i + 1]) for i in range(len(widths) - 1)], axis=1)
    pieces = [p if g.ndim == 2 else p[:, 0] for p, g in zip(pieces, grads)]
    return (block_out, grad_input, *pieces, grad_gateup, grad_down)


def kernel_local(
    hidden_in,
    doc_ids,
    routes,
    gain_attn,
    w_query,
    key_matrix,
    value_matrix,
    w_output,
    gain_ffn,
    w_router,
    w_gateup,
    w_down,
    cotangent,
):
    tokens = hidden_in.shape[0]
    experts = w_router.shape[1]
    shards = lax.axis_size("fsdp")
    owners = lax.axis_size("expert")
    held = w_gateup.shape[0]
    pairing = 2 if held % 2 == 0 else 1
    f32, bf16 = jnp.float32, jnp.bfloat16

    shares = (w_query, key_matrix, value_matrix, w_output, w_router.T)
    made, fulls, cot_all, left = attend(
        (shards, owners, tokens, experts), hidden_in, doc_ids, routes.T, gain_attn, gain_ffn, shares,
        cotangent,
    )
    h1, q, k, v, mixed, lse, resid, sent, probs = made
    sizes = (shards, owners, tokens, experts, held, pairing)
    back, comb, sums, far, away = moe(sizes, sent, cot_all, w_gateup, w_down)
    wq, wk, wv, wo, wr = fulls
    block_out, grad_input, total_o, total_q, total_k, total_v, total_r, far = reverse(
        (shards, owners, tokens, experts, held),
        (hidden_in, doc_ids, routes.T, gain_attn, gain_ffn, cotangent, q, k, v, mixed,
         lse, resid, sent, probs, back),
        (wo, wr, wq, wk, wv),
        comb,
        left,
        away,
        far,
    )
    out = finish(
        experts, sums, far, (total_q, total_k, total_v, total_o), total_r, block_out, grad_input
    )
    grad_gateup, grad_down, grad_q, grad_k, grad_v, grad_o, grad_r, ga, gf, block, gradient = out
    return (
        block,
        gradient,
        grad_q,
        grad_k,
        grad_v,
        grad_o,
        grad_r.T,
        ga,
        gf,
        grad_gateup,
        grad_down,
    )


def local(*args):
    owners, held = lax.axis_size("expert"), args[10].shape[0]
    groups = held // (2 if held % 2 == 0 else 1)
    if lax.axis_size("fsdp") == 4 and owners == 8 and owners * groups * CAP <= 2048:
        return kernel_local(*args)
    return plain_local(*args)


def solution(mesh):
    in_specs = (
        P(("fsdp", "expert"), None),
        P(("fsdp", "expert"), None),
        P(("fsdp", "expert"), None),
        P(),
        P("fsdp", None),
        P("fsdp", None),
        P("fsdp", None),
        P("fsdp", None),
        P(),
        P("fsdp", None),
        P("expert", None, None),
        P("expert", None, None),
        P(("fsdp", "expert"), None),
    )
    out_specs = (
        P(("fsdp", "expert"), None),
        P(("fsdp", "expert"), None),
        P("fsdp", None),
        P("fsdp", None),
        P("fsdp", None),
        P("fsdp", None),
        P("fsdp", None),
        P("fsdp"),
        P("fsdp"),
        P("expert", "fsdp", None),
        P("expert", "fsdp", None),
    )
    return jax.shard_map(local, mesh=mesh, in_specs=in_specs, out_specs=out_specs, check_vma=False)
```

```python
import functools
import math

import jax
import jax.numpy as jnp
from jax import lax
from jax.experimental import pallas as pl
from jax.experimental.pallas import tpu as pltpu
from jax.sharding import PartitionSpec as P

MODEL_WIDTH = 1536
QUERY_HEADS = 24
KEY_VALUE_HEADS = 8
HEAD_SIZE = 64
TOP = 8
CAP = 48


EPS = 1e-05
BASE = 10000.0
SCORE_SCALE = 0.015625
MASKED = -1e30


def rope_tables(doc_row):
    document_length = doc_row.shape[0]
    places = jnp.arange(document_length, dtype=jnp.int32)
    same_doc = doc_row[:, None] == doc_row[None, :]
    starts = jnp.min(jnp.where(same_doc, places[None, :], document_length), axis=1)
    position = (places - starts).astype(jnp.float32)
    half_width = HEAD_SIZE // 2
    inverse = jnp.exp(
        -math.log(BASE) * (2.0 * jnp.arange(half_width, dtype=jnp.float32) / HEAD_SIZE)
    )
    angle = position[:, None] * inverse[None, :]
    allowed = same_doc & (places[None, :] <= places[:, None])
    return (jnp.cos(angle), jnp.sin(angle), allowed)


def rotate(tensor, cosine_table, sine_table):
    half_width = HEAD_SIZE // 2
    first_half = tensor[..., :half_width]
    second = tensor[..., half_width:]
    cos_part = cosine_table[:, None, :]
    sin_part = sine_table[:, None, :]
    return jnp.concatenate(
        [first_half * cos_part - second * sin_part, second * cos_part + first_half * sin_part],
        axis=-1,
    )


def inverse_rotation(tensor, cosine_table, sine_table):
    half_width = HEAD_SIZE // 2
    first_half = tensor[..., :half_width]
    second = tensor[..., half_width:]
    cos_part = cosine_table[:, None, :]
    sin_part = sine_table[:, None, :]
    return jnp.concatenate(
        [first_half * cos_part + second * sin_part, second * cos_part - first_half * sin_part],
        axis=-1,
    )


def norm_forward(value_rows, gain):
    scale_inv = lax.rsqrt(jnp.mean(value_rows * value_rows, axis=-1, keepdims=True) + EPS)
    normed = value_rows * scale_inv
    return ((normed * gain).astype(jnp.bfloat16), normed, scale_inv)


def norm_backward(grad_out, normed, scale_inv, gain):
    grad_normed = grad_out * gain
    grad_gain = jnp.sum(grad_out * normed, axis=0)
    value_gradients = scale_inv * (
        grad_normed - normed * jnp.mean(grad_normed * normed, axis=-1, keepdims=True)
    )
    return (value_gradients, grad_gain)


def scores_of(query_rows, key_rows, allowed):
    document_length = query_rows.shape[0]
    group_rows = query_rows.reshape(
        document_length, KEY_VALUE_HEADS, QUERY_HEADS // KEY_VALUE_HEADS, HEAD_SIZE
    )
    scores = (
        jnp.einsum("qgrd,kgd->grqk", group_rows, key_rows, preferred_element_type=jnp.float32)
        * SCORE_SCALE
    )
    return jnp.where(allowed[None, None], scores, MASKED)


def forward_local(
    hidden_rows,
    doc_row,
    route_rows,
    gain_attn,
    w_query,
    key_matrix,
    value_matrix,
    w_output,
    gain_ffn,
    w_router,
):
    document_length = hidden_rows.shape[0]
    hidden_f = hidden_rows.astype(jnp.float32)
    attention_input, normed_attn, scale_attn = norm_forward(hidden_f, gain_attn)
    cosine_table, sine_table, allowed = rope_tables(doc_row)
    query_rows = jnp.dot(attention_input, w_query, preferred_element_type=jnp.float32).reshape(
        document_length, QUERY_HEADS, HEAD_SIZE
    )
    key_rows = jnp.dot(attention_input, key_matrix, preferred_element_type=jnp.float32).reshape(
        document_length, KEY_VALUE_HEADS, HEAD_SIZE
    )
    value_rows = (
        jnp.dot(attention_input, value_matrix, preferred_element_type=jnp.float32)
        .astype(jnp.bfloat16)
        .reshape(document_length, KEY_VALUE_HEADS, HEAD_SIZE)
    )
    query_rows = rotate(query_rows, cosine_table, sine_table).astype(jnp.bfloat16)
    key_rows = rotate(key_rows, cosine_table, sine_table).astype(jnp.bfloat16)
    scores = scores_of(query_rows, key_rows, allowed)
    top_score = jnp.max(scores, axis=-1, keepdims=True)
    log_total = top_score + jnp.log(jnp.sum(jnp.exp(scores - top_score), axis=-1, keepdims=True))
    weights = jnp.exp(scores - log_total).astype(jnp.bfloat16)
    attention_mixed = jnp.einsum(
        "grqk,kgd->qgrd", weights, value_rows, preferred_element_type=jnp.float32
    )
    attention_mixed = attention_mixed.reshape(document_length, QUERY_HEADS * HEAD_SIZE).astype(
        jnp.bfloat16
    )
    resid = hidden_f + jnp.dot(attention_mixed, w_output, preferred_element_type=jnp.float32)
    ffn_in, normed_ffn, scale_ffn = norm_forward(resid, gain_ffn)
    logits = jnp.dot(ffn_in, w_router, preferred_element_type=jnp.float32)
    probs = jax.nn.softmax(logits, axis=-1)
    picks = route_rows[:, :, None] == jnp.arange(probs.shape[1], dtype=jnp.int32)[None, None, :]
    gates = jnp.sum(jnp.where(picks, probs[:, None, :], 0.0), axis=-1)
    return (
        normed_attn,
        scale_attn,
        attention_input,
        cosine_table,
        sine_table,
        allowed,
        query_rows,
        key_rows,
        value_rows,
        attention_mixed,
        log_total,
        resid,
        ffn_in,
        normed_ffn,
        scale_ffn,
        probs,
        gates,
    )


def backward_local(
    state,
    route_rows,
    cot_rows,
    grad_ffn_in,
    grad_gates,
    gain_attn,
    w_query,
    key_matrix,
    value_matrix,
    w_output,
    gain_ffn,
    w_router,
):
    (
        normed_attn,
        scale_attn,
        attention_input,
        cosine_table,
        sine_table,
        allowed,
        query_rows,
        key_rows,
        value_rows,
        attention_mixed,
        log_total,
        resid,
        ffn_in,
        normed_ffn,
        scale_ffn,
        probs,
        gates,
    ) = state
    document_length = attention_input.shape[0]
    query_group = QUERY_HEADS // KEY_VALUE_HEADS
    grad_probs = jnp.where(route_rows, grad_gates, 0.0)
    grad_logits = (
        probs * (grad_probs - jnp.sum(probs * grad_probs, axis=-1, keepdims=True))
    ).astype(jnp.bfloat16)
    grad_router = jnp.dot(ffn_in.T, grad_logits, preferred_element_type=jnp.float32)
    grad_ffn_in = grad_ffn_in + jnp.dot(grad_logits, w_router.T, preferred_element_type=jnp.float32)
    grad_resid_part, grad_gain_ffn = norm_backward(grad_ffn_in, normed_ffn, scale_ffn, gain_ffn)
    grad_resid = cot_rows.astype(jnp.float32) + grad_resid_part
    grad_attn = grad_resid.astype(jnp.bfloat16)
    grad_output = jnp.dot(attention_mixed.T, grad_attn, preferred_element_type=jnp.float32)
    mixed_gradient = jnp.dot(grad_attn, w_output.T, preferred_element_type=jnp.float32).astype(
        jnp.bfloat16
    )
    scores = scores_of(query_rows, key_rows, allowed)
    weights = jnp.exp(scores - log_total)
    weights_low = weights.astype(jnp.bfloat16)
    gradient_by_group = mixed_gradient.reshape(
        document_length, KEY_VALUE_HEADS, query_group, HEAD_SIZE
    )
    mixed_by_group = attention_mixed.reshape(
        document_length, KEY_VALUE_HEADS, query_group, HEAD_SIZE
    )
    value_gradients = jnp.einsum(
        "grqk,qgrd->kgd", weights_low, gradient_by_group, preferred_element_type=jnp.float32
    )
    grad_weights = jnp.einsum(
        "qgrd,kgd->grqk", gradient_by_group, value_rows, preferred_element_type=jnp.float32
    )
    delta = jnp.transpose(
        jnp.sum(
            gradient_by_group.astype(jnp.float32) * mixed_by_group.astype(jnp.float32), axis=-1
        ),
        (1, 2, 0),
    )
    grad_scores = (weights * (grad_weights - delta[..., None]) * SCORE_SCALE).astype(jnp.bfloat16)
    query_by_group = query_rows.reshape(document_length, KEY_VALUE_HEADS, query_group, HEAD_SIZE)
    grad_query_rows = jnp.einsum(
        "grqk,kgd->qgrd", grad_scores, key_rows, preferred_element_type=jnp.float32
    ).reshape(document_length, QUERY_HEADS, HEAD_SIZE)
    key_row_gradient = jnp.einsum(
        "grqk,qgrd->kgd", grad_scores, query_by_group, preferred_element_type=jnp.float32
    )
    grad_query_rows = (
        inverse_rotation(grad_query_rows, cosine_table, sine_table)
        .reshape(document_length, QUERY_HEADS * HEAD_SIZE)
        .astype(jnp.bfloat16)
    )
    key_row_gradient = (
        inverse_rotation(key_row_gradient, cosine_table, sine_table)
        .reshape(document_length, KEY_VALUE_HEADS * HEAD_SIZE)
        .astype(jnp.bfloat16)
    )
    value_row_gradient = value_gradients.reshape(
        document_length, KEY_VALUE_HEADS * HEAD_SIZE
    ).astype(jnp.bfloat16)
    grad_query = jnp.dot(attention_input.T, grad_query_rows, preferred_element_type=jnp.float32)
    grad_key = jnp.dot(attention_input.T, key_row_gradient, preferred_element_type=jnp.float32)
    grad_value = jnp.dot(attention_input.T, value_row_gradient, preferred_element_type=jnp.float32)
    grad_attn_in = jnp.dot(grad_query_rows, w_query.T, preferred_element_type=jnp.float32)
    grad_attn_in = grad_attn_in + jnp.dot(
        key_row_gradient, key_matrix.T, preferred_element_type=jnp.float32
    )
    grad_attn_in = grad_attn_in + jnp.dot(
        value_row_gradient, value_matrix.T, preferred_element_type=jnp.float32
    )
    grad_hidden_part, grad_gain_attn = norm_backward(
        grad_attn_in, normed_attn, scale_attn, gain_attn
    )
    grad_in = grad_resid + grad_hidden_part
    return (
        grad_in,
        (grad_query, grad_key, grad_value, grad_output, grad_router, grad_gain_attn, grad_gain_ffn),
    )


MESH = pl.DeviceIdType.MESH
F32, BF16 = jnp.float32, jnp.bfloat16


def dot(a, b, da=1, db=0):
    return lax.dot_general(a, b, (((da,), (db,)), ((), ())), preferred_element_type=F32)


class Place:
    def __init__(self, shards, owners):
        self.shards, self.owners = shards, owners
        self.line = 4 if owners % 4 == 0 else 1
        self.side = owners // self.line
        self.chips = shards // 2
        self.f = lax.axis_index("fsdp")
        self.e = lax.axis_index("expert")
        self.a, self.b = self.e // self.side, self.e % self.side
        self.x, self.c = self.f // 2, self.f % 2

    def detour(self):
        end = self.line - 1
        got = jnp.where(self.a % 2 == 0, end, 0)
        return got, end - got, self.e + jnp.where(self.a % 2 == 0, self.side, -self.side)

    def others(self, all_fsdp):
        out = [((self.f, self.e + self.side), self.a < self.line - 1)]
        out.append(((self.f, self.e - self.side), self.a > 0))
        for i in range(1, self.side):
            out.append(((self.f, self.a * self.side + (self.b + i) % self.side), None))
        if all_fsdp:
            out += [(((self.f + i) % self.shards, self.e), None) for i in range(1, self.shards)]
            return out
        out.append(((self.x * 2 + 1 - self.c, self.e), None))
        for i in range(1, self.chips):
            out.append((((self.x + i) % self.chips * 2 + self.c, self.e), None))
        return out

    def meet(self, all_fsdp=False):
        bar = pltpu.get_barrier_semaphore()
        others = self.others(all_fsdp)
        for dev, cond in others:

            def signal(dev=dev):
                pl.semaphore_signal(bar, inc=1, device_id=dev, device_id_type=MESH)

            if cond is None:
                signal()
            else:
                pl.when(cond)(signal)
        pl.semaphore_wait(
            bar,
            len(others)
            - 2
            + jnp.where(self.a < self.line - 1, 1, 0)
            + jnp.where(self.a > 0, 1, 0),
        )


def remote(src, dst, send, recv, dev):
    return pltpu.make_async_remote_copy(
        src_ref=src, dst_ref=dst, send_sem=send, recv_sem=recv, device_id=dev, device_id_type=MESH
    )


class LineGather:
    def __init__(self, at, buf, send, recv, balance=False):
        self.at, self.buf, self.send, self.recv = at, buf, send, recv
        self.balance = balance
        width, count = buf.shape[2], recv.shape[0]
        cut = [width * p // count // 128 * 128 for p in range(count)] + [width]
        self.parts = [pl.ds(lo, hi - lo) for lo, hi in zip(cut, cut[1:])]

    def copy(self, k, p, way, dev):
        ref = self.buf.at[k, :, self.parts[p]]
        return remote(ref, ref, self.send.at[p, way, k], self.recv.at[p, k], (self.at.f, dev))

    def up(self, k, p):
        return self.copy(k, p, 0, self.at.e + self.at.side)

    def down(self, k, p):
        return self.copy(k, p, 1, self.at.e - self.at.side)

    def across(self, k, i, p):
        at = self.at
        return self.copy(k, p, 1 + i, at.a * at.side + (at.b + i) % at.side)

    def spread(self, k, p, up, down, across=True):
        at = self.at
        if up:

            @pl.when(at.a < at.line - 1)
            def _():
                self.up(k, p).start()

        if down:

            @pl.when(at.a > 0)
            def _():
                self.down(k, p).start()

        if across and (p < len(self.parts) - 1 or not self.balance):
            self.across(k, 1, p).start()
        elif across:
            pl.when(k // at.side != at.detour()[0])(lambda: self.across(k, 1, p).start())

    def detour(self):
        at = self.at
        k = at.detour()[1] * at.side + 1 - at.b
        return self.copy(k, len(self.parts) - 1, 3, at.detour()[2])

    def begin(self):
        for p in range(len(self.parts)):
            self.spread(self.at.e, p, True, True)

    def relay_step(self, s, across=True):
        at = self.at
        for p in range(len(self.parts)):

            @pl.when(at.a - s >= 0)
            def _(p=p):
                k = at.e - s * at.side
                self.down(k, p).wait_recv()
                self.spread(k, p, True, False, across)

            @pl.when(at.a + s < at.line)
            def _(p=p):
                k = at.e + s * at.side
                self.up(k, p).wait_recv()
                self.spread(k, p, False, True, across)

    def cross(self, n):
        at = self.at
        a = (
            jnp.where(at.a > 0, at.a - 1, at.a + 1),
            jnp.where(at.a == 0, 2, jnp.where(at.a == at.line - 1, at.a - 2, at.a + 1)),
            jnp.where(at.a < at.line // 2, at.line - 1, 0),
        )[n - 1]
        for p in range(len(self.parts)):
            self.spread(a * at.side + at.b, p, False, False)

    def relay(self):
        for s in range(1, self.at.line):
            self.relay_step(s)

    def each(self, use):
        at = self.at

        def near(s, carry):
            pl.when(s > 0)(lambda: self.relay_step(s))
            pl.when(at.a - s >= 0)(lambda: use(at.e - s * at.side))
            pl.when((s > 0) & (at.a + s < at.line))(lambda: use(at.e + s * at.side))
            return carry

        lax.fori_loop(0, at.line, near, 0)
        self.rest(use)

    def rest(self, use=None):
        at = self.at

        def take(n, carry):
            s, sign = n // 2, 1 - n % 2 * 2
            a = at.a + sign * s

            @pl.when((a >= 0) & (a < at.line) & (n != 1))
            def _():
                k = a * at.side + 1 - at.b
                for p in range(len(self.parts)):
                    self.across(k, 1, p).wait_recv()
                if self.balance:
                    pl.when(a == at.detour()[1])(lambda: self.detour().start())
                if use is not None:
                    use(k)

            return carry

        lax.fori_loop(0, 2 * at.line, take, 0)

    def finish(self):
        at = self.at
        for s in range(at.line):
            k = s * at.side + at.b
            for p in range(len(self.parts)):

                @pl.when((at.a < at.line - 1) & (at.a >= s))
                def _(k=k, p=p):
                    self.up(k, p).wait_send()

                @pl.when((at.a > 0) & (at.a <= s))
                def _(k=k, p=p):
                    self.down(k, p).wait_send()

                if p < len(self.parts) - 1 or not self.balance:
                    self.across(k, 1, p).wait_send()
                else:
                    pl.when(s != at.detour()[0])(
                        lambda k=k, p=p: self.across(k, 1, p).wait_send()
                    )
        if self.balance:
            self.detour().wait_send()


class LineScatter:
    def __init__(self, at, part, side_in, line_in, own, extra, sems, balance=False):
        self.balance = balance
        self.at, self.part, self.side_in, self.line_in, self.own = at, part, side_in, line_in, own
        self.extra = extra
        self.ssend, self.srecv, self.lsend, self.lrecv, self.esem = sems
        width = part.shape[2]
        self.cut = width // 256 * 128
        self.parts = (pl.ds(0, self.cut), pl.ds(self.cut, width - self.cut))

    def across(self, s, p):
        at = self.at
        return remote(
            self.part.at[s * at.side + 1 - at.b, :, self.parts[p]],
            self.side_in.at[s, :, self.parts[p]],
            self.ssend.at[s, p],
            self.srecv.at[s, p],
            (at.f, at.a * at.side + 1 - at.b),
        )

    def detour(self):
        at = self.at
        k = at.detour()[0] * at.side + 1 - at.b
        return remote(
            self.part.at[k, :, self.parts[1]], self.extra, self.esem.at[0], self.esem.at[1],
            (at.f, at.detour()[2]),
        )

    def join(self):
        at = self.at
        s = at.detour()[1]
        k = s * at.side + 1 - at.b
        self.detour().wait_recv()
        mine = self.part[k, :, self.cut :].astype(F32)
        self.part[k, :, self.cut :] = (mine + self.extra[...].astype(F32)).astype(BF16)
        self.across(s, 1).start()

    def along(self, s, dev, slot):
        at = self.at
        return remote(
            self.part.at[s * at.side + at.b],
            self.line_in.at[slot],
            self.lsend.at[s],
            self.lrecv.at[slot],
            (at.f, dev),
        )

    def up(self, s):
        return self.along(s, self.at.e + self.at.side, s)

    def down(self, s):
        at = self.at
        return self.along(s, at.e - at.side, jnp.where(s == at.a - 1, at.line, s))

    def place(self, i):
        at = self.at
        return jnp.where(at.a < at.line // 2, at.line - 1 - i, i)

    def middle(self):
        at = self.at
        return (at.a > 0) & (at.a < at.line - 1)

    def launch(self, make, lo, hi):
        at = self.at
        got, passed, _ = at.detour()

        def step(n, carry):
            s = self.place(n)
            make(s * at.side + 1 - at.b)
            self.across(s, 0).start()
            if self.balance:
                pl.when(s == got)(lambda: self.detour().start())
                pl.when((s != got) & (s != passed))(lambda: self.across(s, 1).start())
            else:
                self.across(s, 1).start()
            return carry

        lax.fori_loop(lo, hi, step, 0)

    def begin(self, make):
        self.launch(make, 0, 2)

    def more(self, make):
        at = self.at
        if self.balance:
            pl.when(self.middle())(self.join)
        self.launch(make, 2, at.line)

        def step(n, carry):
            make(n * at.side + at.b)
            return carry

        lax.fori_loop(0, at.line, step, 0)

    def sum_step(self, n):
        at = self.at
        if n == 1 and self.balance:
            pl.when(jnp.logical_not(self.middle()))(self.join)
        s = self.place(n)
        k = s * at.side + at.b
        got = at.detour()[0]
        self.own[...] = self.part[k].astype(F32)
        self.across(s, 0).wait_recv()
        self.own[:, : self.cut] += self.side_in[s, :, : self.cut].astype(F32)

        @pl.when((s != got) | (not self.balance))
        def _():
            self.across(s, 1).wait_recv()
            self.own[:, self.cut :] += self.side_in[s, :, self.cut :].astype(F32)

        @pl.when(((s > at.a) & (at.a > 0)) | ((s < at.a) & (at.a < at.line - 1)))
        def _():
            self.along(s, at.e, s).wait_recv()
            self.own[...] += self.line_in[s].astype(F32)

        self.part[k] = self.own[...].astype(BF16)

        @pl.when(s > at.a)
        def _():
            self.up(s).start()

        @pl.when(s < at.a)
        def _():
            self.down(s).start()

    def sum_last(self):
        at = self.at
        self.own[...] = self.part[at.e].astype(F32)

        @pl.when(at.a > 0)
        def _():
            self.along(at.a, at.e, at.a).wait_recv()
            self.own[...] += self.line_in[at.a].astype(F32)

        @pl.when(at.a < at.line - 1)
        def _():
            self.along(at.a, at.e, at.line).wait_recv()
            self.own[...] += self.line_in[at.line].astype(F32)

    def finish(self):
        at = self.at
        if self.balance:
            self.detour().wait_send()
        for s in range(at.line):
            self.across(s, 0).wait_send()
            pl.when((s != at.detour()[0]) | (not self.balance))(
                lambda s=s: self.across(s, 1).wait_send()
            )

            @pl.when(at.a < s)
            def _(s=s):
                self.up(s).wait_send()

            @pl.when(at.a > s)
            def _(s=s):
                self.down(s).wait_send()


def rope_of(allowed, tokens):
    lane = lax.broadcasted_iota(jnp.int32, (tokens, 128), 1)
    position = jnp.sum(allowed.astype(F32), axis=1, keepdims=True) - 1.0
    half = HEAD_SIZE // 2
    inverse = jnp.exp(-math.log(BASE) * (2.0 * (lane % half).astype(F32) / HEAD_SIZE))
    angle = position * inverse
    return jnp.cos(angle), jnp.sin(angle), lane % HEAD_SIZE < half


def turn(x, cos, sin, first):
    half = HEAD_SIZE // 2
    other = jnp.where(first, -pltpu.roll(x, 128 - half, 1), pltpu.roll(x, half, 1))
    return x * cos + other * sin


def visible(doc, tokens):
    row = lax.broadcasted_iota(jnp.int32, (tokens, tokens), 0)
    col = lax.broadcasted_iota(jnp.int32, (tokens, tokens), 1)
    key_doc = jnp.broadcast_to(doc.astype(F32), (tokens, tokens))
    own = jnp.sum(jnp.where(row == col, key_doc, 0.0), axis=1, keepdims=True)
    return (own == key_doc) & (col <= row)


def picked(routes, lane):
    ids = routes[...].astype(F32).T
    lane = lane.astype(F32)
    chosen = lane == ids[:, :1]
    for i in range(1, TOP):
        chosen = chosen | (lane == ids[:, i : i + 1])
    return chosen


def attend_kernel(sizes, hidden, doc, routes, gain_a, gain_f, *refs):
    shards, owners, tokens, experts = sizes
    shares, cot = refs[:5], refs[5]
    h1, q, k, v, mixed, lse, resid, sent, probs_out = refs[6:15]
    fulls, cot_out, left = refs[15:20], refs[20], refs[21]
    (bufs, cot_all, acc, lsem, xs, xr, ys, yr, ss, sr, cs, cr, ls, lr, own_left) = refs[22:]
    at = Place(shards, owners)
    rg = MODEL_WIDTH // shards
    half, quarter = rg // 2, rg // 4
    f = at.f
    sib = (at.x * 2 + 1 - at.c, at.e)
    over = ((at.x + 1) % at.chips * 2 + at.c, at.e)
    far = over[0]
    other = (at.x + 1) % at.chips * 2 + 1 - at.c
    mine = (at.a + at.b) % 2
    beside = (f, at.a * at.side + (at.b + 1) % at.side)
    step = jnp.where(at.a % 2 == 0, at.side, -at.side)
    along = (f, at.e + step)
    count = len(shares)

    own = [pltpu.make_async_copy(shares[n], bufs[n].at[f], lsem.at[n]) for n in range(count)]
    own.append(pltpu.make_async_copy(cot, cot_all.at[at.e], lsem.at[count]))
    for c in own:
        c.start()

    def piece(n, g, start, size, send, recv, dev):
        ref = bufs[n].at[g, pl.ds(pl.multiple_of(start, quarter), size)]
        return remote(ref, ref, send, recv, dev)

    def begins(i):
        return (mine * half, mine * half + quarter, (1 - mine) * half, (1 - mine) * half + quarter)[i]

    def out_x(n, i):
        start = pl.ds(pl.multiple_of(begins(i), quarter), quarter)
        return remote(
            shares[n].at[start], bufs[n].at[f, start], xs.at[n, i], xr.at[n, i], over
        )

    def in_x(n, i):
        return piece(n, far, begins(i), quarter, xs.at[n, i], xr.at[n, i], over)

    def out_yz(n, i):
        return piece(n, far, begins(i), quarter, ys.at[n, i], yr.at[n, i], (beside, along)[i])

    def in_yz(n, i):
        return piece(n, far, begins(2 + i), quarter, ys.at[n, i], yr.at[n, i], (beside, along)[i])

    def to_sib(n, i, g):
        return piece(n, g, begins(i), quarter, ss.at[n, i], sr.at[n, i], sib)

    def own_sib(n):
        return remote(shares[n], bufs[n].at[f], ss.at[n, 4], sr.at[n, 4], sib)

    def small_x():
        return remote(shares[4], bufs[4].at[f], xs.at[4, 0], xr.at[4, 0], over)

    def small_sib():
        return remote(bufs[4].at[far], bufs[4].at[far], ss.at[4, 0], sr.at[4, 0], sib)

    def pass_x(n, i):
        in_x(n, i).wait_recv()
        out_yz(n, i).start()
        to_sib(n, i, far).start()

    def pass_rest(n):
        for i in range(2):
            in_yz(n, i).wait_recv()
            to_sib(n, 2 + i, far).start()

    def from_sib(n):
        for i in range(4):
            to_sib(n, i, other).wait_recv()

    def lefts(n, i):
        g = (f + i) % shards
        return remote(
            (h1, mixed)[n].at[:, pl.ds(pl.multiple_of(g * rg, 128), rg)],
            left.at[pl.ds(f * tokens, tokens), pl.ds(n * rg, rg)],
            ls.at[n, i - 1], lr.at[n, i - 1], (g, at.e),
        )

    def left_own(n):
        return pltpu.make_async_copy(
            (h1, mixed)[n].at[:, pl.ds(pl.multiple_of(f * rg, 128), rg)],
            left.at[pl.ds(f * tokens, tokens), pl.ds(n * rg, rg)],
            own_left.at[n],
        )

    def send_left(n):
        left_own(n).start()
        for i in range(1, shards):
            lefts(n, i).start()

    at.meet(all_fsdp=True)
    order = (0, 1, 2, 3)
    for n in order[:3]:
        for i in range(2):
            out_x(n, i).start()
        own_sib(n).start()
    small_x().start()
    own_sib(4).start()
    for i in range(2):
        out_x(3, i).start()
    own_sib(3).start()
    cotg = LineGather(at, cot_all, cs, cr)
    own[count].wait()
    cotg.begin()

    x = hidden[...].astype(F32)
    scale = lax.rsqrt(jnp.mean(x * x, axis=1, keepdims=True) + EPS)
    h1[...] = (x * scale * gain_a[...].reshape(1, -1)).astype(BF16)
    allowed = visible(doc[...], tokens)
    cos, sin, first = rope_of(allowed, tokens)

    ends = (0, 1536, 2048, 2560)

    def project(g):
        part = h1[:, pl.ds(pl.multiple_of(g * rg, 128), rg)]
        return [dot(part, bufs[n][g]) for n in range(3)]

    for n in range(3):
        own[n].wait()
        acc[:, ends[n] : ends[n + 1]] = dot(
            h1[:, pl.ds(pl.multiple_of(f * rg, 128), rg)], bufs[n][f]
        )

    def add(g):
        for n, got in enumerate(project(g)):
            acc[:, ends[n] : ends[n + 1]] += got

    for n in range(3):
        own_sib(n).wait_recv()
    add(sib[0])
    pass_x(0, 0)
    cotg.relay_step(1, False)
    cotg.cross(1)
    pass_x(0, 1)
    cotg.relay_step(2, False)
    for n in (1, 2):
        for i in range(2):
            pass_x(n, i)
    cotg.cross(2)
    for n in range(3):
        pass_rest(n)
    pass_x(3, 0)
    cotg.relay_step(3, False)
    cotg.cross(3)
    add(far)
    for n in range(3):
        from_sib(n)
    add(other)
    small_x().wait_recv()
    small_sib().start()
    pass_x(3, 1)
    save = [pltpu.make_async_copy(bufs[n], fulls[n], lsem.at[n]) for n in range(count)]
    for c in save[:3]:
        c.start()

    for j in range(16):
        cols = slice(128 * j, 128 * (j + 1))
        got = turn(acc[:, cols], cos, sin, first).astype(BF16)
        if j < 12:
            q[:, cols] = got
        else:
            k[:, 128 * (j - 12) : 128 * (j - 11)] = got
    v[...] = acc[:, 2048:].astype(BF16)
    ratio = QUERY_HEADS // KEY_VALUE_HEADS
    mask = jnp.concatenate([allowed] * ratio, axis=0)

    def head(ref, h):
        return ref[:, h * HEAD_SIZE : (h + 1) * HEAD_SIZE]

    for g in range(KEY_VALUE_HEADS):
        heads = range(g * ratio, (g + 1) * ratio)
        rows = jnp.concatenate([head(q, h) for h in heads], axis=0)
        s = jnp.where(mask, dot(rows, head(k, g), 1, 1) * SCORE_SCALE, MASKED)
        top = jnp.max(s, axis=1, keepdims=True)
        e = jnp.exp(s - top)
        total = jnp.sum(e, axis=1, keepdims=True)
        o = dot((e / total).astype(BF16), head(v, g)).astype(BF16)
        log_total = top + jnp.log(total)
        for i, h in enumerate(heads):
            mixed[:, h * HEAD_SIZE : (h + 1) * HEAD_SIZE] = o[i * tokens : (i + 1) * tokens]
            lse[:, h : h + 1] = log_total[i * tokens : (i + 1) * tokens]

    send_left(0)
    send_left(1)

    def output(g):
        return dot(mixed[:, pl.ds(pl.multiple_of(g * rg, 128), rg)], bufs[3][g])

    for n in (3, 4):
        own[n].wait()
        own_sib(n).wait_recv()
    resid[...] = x + output(f) + output(sib[0])
    pass_rest(3)
    resid[...] += output(far)
    small_sib().wait_recv()
    from_sib(3)
    total = resid[...] + output(other)
    resid[...] = total
    scale = lax.rsqrt(jnp.mean(total * total, axis=1, keepdims=True) + EPS)
    h2 = (total * scale * gain_f[...].reshape(1, -1)).astype(BF16)
    sent[:, :MODEL_WIDTH] = h2
    logits = dot(h2[:, :rg], bufs[4][0], 1, 1)
    for g in range(1, shards):
        logits = logits + dot(h2[:, g * rg : (g + 1) * rg], bufs[4][g], 1, 1)
    logits = jnp.concatenate([logits, jnp.zeros((tokens, 128 - experts), F32)], axis=1)
    lane = lax.broadcasted_iota(jnp.int32, (tokens, 128), 1)
    live = lane < experts
    logits = jnp.where(live, logits, MASKED)
    e = jnp.where(live, jnp.exp(logits - jnp.max(logits, axis=1, keepdims=True)), 0.0)
    probs = e / jnp.sum(e, axis=1, keepdims=True)
    probs_out[...] = probs
    chosen = picked(routes, lane)
    row = lax.broadcasted_iota(jnp.int32, (tokens, tokens), 0)
    col = lax.broadcasted_iota(jnp.int32, (tokens, tokens), 1)
    below = jnp.where(row > col, 1.0, 0.0).astype(BF16)
    hits = jnp.where(chosen, 1.0, 0.0)
    rank = jnp.where(chosen, dot(below, hits.astype(BF16)), jnp.where(live, -1.0, 0.0))
    gate = jnp.where(chosen, probs, 0.0)
    high = gate.astype(BF16).astype(F32)
    low = gate - high
    meta = rank + pltpu.roll(high, experts, 1) + pltpu.roll(low, 2 * experts, 1)
    sent[:, MODEL_WIDTH:] = meta.astype(BF16)

    for c in save[3:]:
        c.start()
    cotg.rest()
    cotg.finish()
    keep = pltpu.make_async_copy(cot_all, cot_out, lsem.at[count])
    keep.start()
    for n in range(count):
        own_sib(n).wait_send()
    small_x().wait_send()
    small_sib().wait_send()
    for n in order:
        for i in range(2):
            out_x(n, i).wait_send()
            out_yz(n, i).wait_send()
        for i in range(4):
            to_sib(n, i, far).wait_send()
    for n in range(2):
        left_own(n).wait()
        for i in range(1, shards):
            lefts(n, i).wait()
    for c in save:
        c.wait()
    keep.wait()


def attend(sizes, hidden, doc, routes, gain_a, gain_f, shares, cot):
    shards, owners, tokens, experts = sizes
    rg = MODEL_WIDTH // shards
    side = owners // 4
    vm, dma = pltpu.VMEM, pltpu.SemaphoreType.DMA
    vmem, any_ = pl.BlockSpec(memory_space=pltpu.VMEM), pl.BlockSpec(memory_space=pl.ANY)
    n = len(shares)

    def shape(*dims, dtype=BF16):
        return jax.ShapeDtypeStruct(dims, dtype)

    outs = pl.pallas_call(
        functools.partial(attend_kernel, sizes),
        name="attend",
        out_shape=(
            shape(tokens, MODEL_WIDTH),
            shape(tokens, MODEL_WIDTH),
            shape(tokens, KEY_VALUE_HEADS * HEAD_SIZE),
            shape(tokens, KEY_VALUE_HEADS * HEAD_SIZE),
            shape(tokens, MODEL_WIDTH),
            shape(tokens, 128, dtype=F32),
            shape(tokens, MODEL_WIDTH, dtype=F32),
            shape(tokens, MODEL_WIDTH + 128),
            shape(tokens, 128, dtype=F32),
            *[shape(shards, *s.shape) for s in shares],
            shape(owners, tokens, MODEL_WIDTH),
            shape(shards * tokens, 2 * rg),
        ),
        in_specs=[vmem] * 5 + [any_] * (n + 1),
        out_specs=[vmem] * 9 + [any_] * (n + 2),
        scratch_shapes=[
            tuple(vm((shards, *s.shape), BF16) for s in shares),
            vm((owners, tokens, MODEL_WIDTH), BF16),
            vm((tokens, 2560), F32),
            dma((n + 1,)),
            dma((n, 2)),
            dma((n, 2)),
            dma((n, 2)),
            dma((n, 2)),
            dma((n, 5)),
            dma((n, 5)),
            dma((2, side + 2, owners)),
            dma((2, owners)),
            dma((2, shards - 1)),
            dma((2, shards - 1)),
            dma((2,)),
        ],
        compiler_params=pltpu.CompilerParams(
            collective_id=0, has_side_effects=True, vmem_limit_bytes=60 * 2**20
        ),
    )(hidden, doc, routes, gain_a, gain_f, *shares, cot)
    return outs[:9], outs[9 : 9 + n], outs[9 + n], outs[10 + n]


EARLY = 4
AHEAD = 2


def moe_kernel(sizes, sent, cot, wgu, wd, back_out, comb_out, sums, far, away, *scratch):
    shards, owners, tokens, experts, held, pairing = sizes
    (rows_all, cot_buf, taken, cots, made, grads, slot_gate, slot_grad, place, wg_buf, wd_buf,
     acts, dus, gg, gd, turned, from_core, stage, side1, line1, extra1,
     rs, rr, wsem, csem, coresend, corerecv, farsend, farrecv, osem, free, s1, s2, s3, s4, s5,
     ) = scratch
    at = Place(shards, owners)
    groups = held // pairing
    slots = groups * CAP
    half = wd.shape[1]
    rg, rd = MODEL_WIDTH // shards, half // shards
    sibling = (at.x * 2 + 1 - at.c, at.e)

    def weights(g):
        out = []
        for m in range(pairing):
            h, slot = g * pairing + m, g % 2 * pairing + m
            out.append(pltpu.make_async_copy(wgu.at[h], wg_buf.at[slot], wsem.at[0, slot]))
            out.append(pltpu.make_async_copy(wd.at[h], wd_buf.at[slot], wsem.at[1, slot]))
        return out

    mine = pltpu.make_async_copy(sent, rows_all.at[at.e], osem.at[0, 0])
    mine.start()
    for c in weights(0):
        c.start()
    at.meet()
    rows = LineGather(at, rows_all, rs, rr)
    mine.wait()
    rows.begin()

    lane = lax.broadcasted_iota(jnp.int32, (128, slots), 1)
    row = lax.broadcasted_iota(jnp.int32, (128, slots), 0)

    def expert_of(j):
        return (at.e * held + j // CAP * pairing) // 2

    e_lane = expert_of(lane)
    find_rank = (row == e_lane).astype(F32).astype(BF16)
    slot_rank = (lane % CAP).astype(F32)
    e_row = expert_of(lax.broadcasted_iota(jnp.int32, (slots, 128), 0))
    col = lax.broadcasted_iota(jnp.int32, (slots, 128), 1)
    pick_gate = (col == e_row + experts) | (col == e_row + 2 * experts)

    def dispatch(k):
        rank_at = dot(rows_all[k, :, MODEL_WIDTH:], find_rank)
        pt = jnp.where(rank_at == slot_rank, 1.0, 0.0).astype(BF16)
        place[k] = pt
        got = dot(pt, rows_all[k], 0, 0)
        gate = jnp.sum(jnp.where(pick_gate, got[:, MODEL_WIDTH:], 0.0), axis=1, keepdims=True)
        gate = jnp.broadcast_to(gate, (slots, 128))
        to = pl.ds(k * CAP, CAP)
        for g in range(groups):
            taken[g, to, :] = got[g * CAP : (g + 1) * CAP, :MODEL_WIDTH].astype(BF16)
            slot_gate[g, to, :] = gate[g * CAP : (g + 1) * CAP]

    def dispatch_both(k):
        pull = pltpu.make_async_copy(cot.at[k], cot_buf.at[0], csem.at[0])
        pull.start()
        dispatch(k)
        pull.wait()
        got = dot(place[k], cot_buf[0], 0, 0).astype(BF16)
        to = pl.ds(k * CAP, CAP)
        for g in range(groups):
            cots[g, to, :] = got[g * CAP : (g + 1) * CAP]

    rows.each(dispatch_both)
    rows.finish()

    def through(g):
        for c in weights(g):
            c.wait()

        @pl.when(g + 1 < groups)
        def _():
            for c in weights(g + 1):
                c.start()

        gate = slot_gate[g][:, :1]
        total = jnp.zeros((owners * CAP, 1), F32)
        for m in range(pairing):
            h, slot = g * pairing + m, g % 2 * pairing + m
            gu = dot(taken[g], wg_buf[slot])
            a, b = gu[:, :half], gu[:, half:]
            sig = 1.0 / (1.0 + jnp.exp(-a))
            s = a * sig
            act = s * b
            acts[h] = (act * gate).astype(BF16)
            dp = dot(cots[g], wd_buf[slot], 1, 1)
            total = total + jnp.sum(act * dp, axis=1, keepdims=True)
            dact = dp * gate
            dus[h, :, :half] = (dact * b * sig * (1.0 + a * (1.0 - sig))).astype(BF16)
            dus[h, :, half:] = (dact * s).astype(BF16)
        slot_grad[g] = jnp.broadcast_to(total, (owners * CAP, 128))
        n = MODEL_WIDTH // 3
        for i in range(3):
            cols = slice(i * n, (i + 1) * n)
            y = 0.0
            dx = 0.0
            for m in range(pairing):
                h, slot = g * pairing + m, g % 2 * pairing + m
                y = y + dot(acts[h], wd_buf[slot, :, cols])
                dx = dx + dot(dus[h], wg_buf[slot, cols, :], 1, 1)
            made[g, :, cols] = y.astype(BF16)
            grads[g, :, cols] = dx.astype(BF16)

    def to_core(h):
        slot = h % 2
        out = []
        for i in range(at.chips):
            f = 2 * i + 1 - at.c
            for n, (buf, r) in enumerate(((gg, rg), (gd, rd))):
                out.append(
                    remote(
                        buf.at[slot, pl.ds(pl.multiple_of(f * r, r), r)],
                        from_core[n].at[slot, i],
                        coresend.at[slot, n, i],
                        corerecv.at[slot, n, i],
                        sibling,
                    )
                )
        return out

    def to_chips(h):
        return chip_copies(at, h, away, h, far, farsend, farrecv)

    def keep(h):
        slot = h % 2
        out = []
        for n in range(2):
            out.append(pltpu.make_async_copy(stage[n].at[slot, 0], sums[n].at[h], osem.at[n, slot]))
            for i in range(1, at.chips):
                out.append(
                    pltpu.make_async_copy(
                        stage[n].at[slot, i], away[n].at[h, i - 1], osem.at[2 * i + n, slot]
                    )
                )
        return out

    def add(h):
        slot = h % 2
        for c in to_core(h):
            c.wait()

        for i in range(at.chips):
            x = (at.x + i) % at.chips
            f = 2 * x + at.c
            for n, (buf, r) in enumerate(((gg, rg), (gd, rd))):
                own = buf[slot, pl.ds(pl.multiple_of(f * r, r), r)]
                stage[n][slot, i] = own + from_core[n][slot, x]
        for c in keep(h):
            c.start()

        @pl.when(h < held - 2)
        def _():
            pl.semaphore_signal(free, inc=1, device_id=sibling, device_id_type=MESH)

    def leave(h):
        for c in keep(h):
            c.wait()

        @pl.when(h < EARLY)
        def _():
            for c in to_chips(h):
                c.start()

    def weigh(h):
        g, slot = h // pairing, h % 2
        n = MODEL_WIDTH // 3

        @pl.when(h % pairing == 0)
        def _():
            turned[...] = taken[g].T

        for i in range(3):
            gg[slot, i * n : (i + 1) * n, :] = dot(
                turned[i * n : (i + 1) * n], dus[h]
            ).astype(BF16)
        gd[slot] = dot(acts[h], cots[g], 0, 0).astype(BF16)

        @pl.when(h >= 2)
        def _():
            pl.semaphore_wait(free, 1)

        for c in to_core(h):
            c.start()

    home = (col == e_row).astype(F32).astype(BF16)
    home_low = (col == e_row + experts).astype(F32).astype(BF16)
    parts = ((0, 512), (512, 1024), (1024, 1536))

    def make_back(k):
        to = pl.ds(k * CAP, CAP)
        dg = jnp.concatenate([slot_grad[g, to, :] for g in range(groups)], axis=0)
        high = dg.astype(BF16)
        low = (dg - high.astype(F32)).astype(BF16)
        pt = place[k]
        for lo, hi in parts:
            dx = jnp.concatenate([grads[g, to, lo:hi] for g in range(groups)], axis=0)
            rows_all[k, :, lo:hi] = dot(pt, dx).astype(BF16)
        rows_all[k, :, MODEL_WIDTH:] = dot(pt, high * home + low * home_low).astype(BF16)

    back = LineScatter(at, rows_all, side1, line1, back_out, extra1, (s1, s2, s3, s4, s5), True)

    def step(i, carry):
        @pl.when(i < groups)
        def _():
            through(i)

        @pl.when(i == groups)
        def _():
            back.begin(make_back)
            back.more(make_back)

        def staged(back, act):
            h = jnp.where(i < groups, i, i - gap) - back
            early = (i >= back) & (i < AHEAD + back)
            pl.when(early | (i >= groups + back))(lambda: act(h))

        staged(2, leave)
        staged(0, weigh)
        staged(1, add)

        for n in range(2):

            @pl.when(i == groups + 3 + 3 * n)
            def _(n=n):
                back.sum_step(n)

        return carry

    gap = groups - AHEAD
    lax.fori_loop(0, held + gap, step, 0)
    back.sum_step(2)

    def combine(k, carry):
        to = pl.ds(k * CAP, CAP)
        slot = k % 2

        def put(j):
            return pltpu.make_async_copy(cot_buf.at[j % 2], comb_out.at[j], csem.at[j % 2])

        @pl.when(k >= 2)
        def _():
            put(k - 2).wait()

        for lo, hi in parts:
            y = jnp.concatenate([made[g, to, lo:hi] for g in range(groups)], axis=0)
            cot_buf[slot, :, lo:hi] = dot(place[k], y).astype(BF16)
        put(k).start()

        @pl.when(k == owners - 1)
        def _():
            put(k - 1).wait()
            put(k).wait()

        return carry

    back.sum_step(3)
    leave(held - 2)
    add(held - 1)
    lax.fori_loop(0, owners, combine, 0)
    leave(held - 1)
    back.sum_last()
    back.finish()

    def drain(h, carry):
        for c in to_chips(h):
            c.wait()
        return carry

    lax.fori_loop(0, EARLY, drain, 0)


def chip_copies(at, h, away, j, far, send, recv):
    out = []
    for i in range(1, at.chips):
        back = at.chips - 1 - i
        dev = ((at.x + i) % at.chips * 2 + at.c, at.e)
        for n in range(2):
            out.append(
                remote(
                    away[n].at[h, i - 1], far[n].at[back, h], send.at[n, i - 1, j],
                    recv.at[n, back, j], dev,
                )
            )
    return out


def moe(sizes, sent, cot, wgu, wd):
    shards, owners, tokens, experts, held, pairing = sizes
    groups = held // pairing
    slots, rows = groups * CAP, owners * CAP
    hidden, half = wgu.shape[2], wd.shape[1]
    rg, rd = MODEL_WIDTH // shards, half // shards
    chips = shards // 2
    line = 4
    side = owners // line
    width = MODEL_WIDTH + 128
    vm, dma = pltpu.VMEM, pltpu.SemaphoreType.DMA
    any_, vmem = pl.BlockSpec(memory_space=pl.ANY), pl.BlockSpec(memory_space=pltpu.VMEM)

    def pair(lead):
        return (vm((*lead, rg, hidden), BF16), vm((*lead, rd, MODEL_WIDTH), BF16))

    def outs(lead):
        return (
            jax.ShapeDtypeStruct((*lead, rg, hidden), BF16),
            jax.ShapeDtypeStruct((*lead, rd, MODEL_WIDTH), BF16),
        )

    return pl.pallas_call(
        functools.partial(moe_kernel, sizes),
        name="moe",
        out_shape=(
            jax.ShapeDtypeStruct((tokens, width), F32),
            jax.ShapeDtypeStruct((owners, tokens, MODEL_WIDTH), BF16),
            outs((held,)),
            outs((chips - 1, held)),
            outs((held, chips - 1)),
        ),
        in_specs=[any_] * 4,
        out_specs=(vmem, any_, (any_, any_), (any_, any_), (any_, any_)),
        scratch_shapes=[
            vm((owners, tokens, width), BF16),
            vm((2, tokens, MODEL_WIDTH), BF16),
            vm((groups, rows, MODEL_WIDTH), BF16),
            vm((groups, rows, MODEL_WIDTH), BF16),
            vm((groups, rows, MODEL_WIDTH), BF16),
            vm((groups, rows, MODEL_WIDTH), BF16),
            vm((groups, rows, 128), F32),
            vm((groups, rows, 128), F32),
            vm((owners, tokens, slots), BF16),
            vm((2 * pairing, MODEL_WIDTH, hidden), BF16),
            vm((2 * pairing, half, MODEL_WIDTH), BF16),
            vm((held, rows, half), BF16),
            vm((held, rows, hidden), BF16),
            vm((2, MODEL_WIDTH, hidden), BF16),
            vm((2, half, MODEL_WIDTH), BF16),
            vm((MODEL_WIDTH, rows), BF16),
            pair((2, chips)),
            pair((2, chips)),
            vm((line, tokens, width), BF16),
            vm((line + 1, tokens, width), BF16),
            vm((tokens, width - width // 256 * 128), BF16),
            dma((2, side + 2, owners)),
            dma((2, owners)),
            dma((2, 2 * pairing)),
            dma((2,)),
            dma((2, 2, chips)),
            dma((2, 2, chips)),
            dma((2, chips - 1, EARLY)),
            dma((2, chips - 1, EARLY)),
            dma((2 * chips, 2)),
            pltpu.SemaphoreType.REGULAR,
            dma((line, 2)),
            dma((line, 2)),
            dma((line,)),
            dma((line + 1,)),
            dma((2,)),
        ],
        compiler_params=pltpu.CompilerParams(
            collective_id=1, has_side_effects=True, vmem_limit_bytes=63 * 2**20
        ),
    )(sent, cot, wgu, wd)


def reverse_kernel(sizes, hidden, doc, routes, gain_a, gain_f, cot, q, k, v, mixed, lse, resid, sent,
                   probs, back, wo, wr, wq, wk, wv, comb, left_in, away0, away1, far0, far1, *refs):
    shards, owners, tokens, experts, held = sizes
    block_out, grad_in, out_o, out_q, out_k, out_v, out_r, far = refs[:8]
    (w_bufs, left, turned, rights, dgrad, dattn_f, dqkv, aux, aux_in, comb_part, comb_side, comb_line,
     comb_own, comb_x, part_o, side_o, line_o, own_o, extra_o, part_q, side_q, line_q, own_q, extra_q,
     total_o, total_q, wsem, rsend, rrecv, asend, arecv, farsend, farrecv, *sems) = refs[8:]
    at = Place(shards, owners)
    away = (away0, away1)
    rg = MODEL_WIDTH // shards
    piece = rg // owners
    split = dqkv.shape[1]
    f = at.f
    sibling = (at.x * 2 + 1 - at.c, at.e)
    over = ((at.x + 1) % at.chips * 2 + at.c, at.e)
    ratio = QUERY_HEADS // KEY_VALUE_HEADS

    fulls = (wo, wr, wq, wk, wv)
    loads = [pltpu.make_async_copy(comb, comb_part, wsem.at[0])]
    loads += [pltpu.make_async_copy(w, b, wsem.at[1 + i]) for i, (w, b) in enumerate(zip(fulls, w_bufs))]
    loads.append(pltpu.make_async_copy(left_in, left, wsem.at[6]))
    for c in loads:
        c.start()
    at.meet(all_fsdp=True)

    combine = LineScatter(at, comb_part, comb_side, comb_line, comb_own, comb_x, sems[:5], True)
    outer = LineScatter(at, part_o, side_o, line_o, own_o, extra_o, sems[5:10], True)
    inner = LineScatter(at, part_q, side_q, line_q, own_q, extra_q, sems[10:15], True)
    outer_all = LineGather(at, total_o, sems[15], sems[16])
    inner_all = LineGather(at, total_q, sems[17], sems[18])
    loads[0].wait()
    nothing = lambda k: None
    combine.begin(nothing)

    def rows(i):
        return pl.ds(pl.multiple_of(i * tokens, tokens), tokens)

    def block(chunk, g, send, dev):
        cols = (pl.ds(split, MODEL_WIDTH), pl.ds(0, split))[chunk]
        ref = rights.at[rows(g), cols]
        return remote(ref, ref, rsend.at[chunk, send], rrecv.at[chunk, g], dev)

    def send_rights(chunk):
        block(chunk, f, 0, sibling).start()
        block(chunk, f, 1, over).start()

    def pass_rights(chunk):
        block(chunk, over[0], 0, sibling).wait_recv()
        block(chunk, over[0], 2, sibling).start()

    def take_rights(chunk):
        block(chunk, sibling[0], 0, sibling).wait_recv()
        block(chunk, (at.x + 1) % at.chips * 2 + 1 - at.c, 0, sibling).wait_recv()

    def late(h):
        return chip_copies(at, h, away, h - EARLY, far, farsend, farrecv)

    h2 = sent[:, :MODEL_WIDTH]
    lane = lax.broadcasted_iota(jnp.int32, (tokens, 128), 1)
    chosen = picked(routes, lane)
    meta = back[:, MODEL_WIDTH:]
    dprobs = jnp.where(chosen, meta + pltpu.roll(meta, 128 - experts, 1), 0.0)
    p = probs[...]
    dlogits = (p * (dprobs - jnp.sum(p * dprobs, axis=1, keepdims=True))).astype(BF16)
    loads[1].wait()
    loads[2].wait()
    aux[...] = dot(dlogits, h2, 0, 0)[: aux.shape[0]]

    def full(i):
        return w_bufs[i][...].reshape(MODEL_WIDTH, -1)

    dh = back[:, :MODEL_WIDTH] + jnp.concatenate(
        [dot(dlogits[:, :experts], w_bufs[1][g]) for g in range(shards)], axis=1
    )
    x = resid[...]
    scale = lax.rsqrt(jnp.mean(x * x, axis=1, keepdims=True) + EPS)
    n = x * scale
    aux[experts + 1 : experts + 2, :] = jnp.sum(dh * n, axis=0, keepdims=True)
    dn = dh * gain_f[...].reshape(1, -1)
    dres = cot[...].astype(F32) + scale * (dn - n * jnp.mean(dn * n, axis=1, keepdims=True))
    dgrad[...] = dres
    dattn = dres.astype(BF16)
    rights[rows(f), split:] = dattn
    send_rights(0)
    for c in late(EARLY):
        c.start()
    dattn_f[...] = dot(dattn, full(0), 1, 1).astype(BF16)
    combine.more(nothing)

    allowed = visible(doc[...], tokens)
    cos, sin, first = rope_of(allowed, tokens)
    mask = jnp.concatenate([allowed] * ratio, axis=0)

    def stack(ref, heads):
        return jnp.concatenate(
            [ref[:, h * HEAD_SIZE : (h + 1) * HEAD_SIZE] for h in heads], axis=0
        )

    kept = QUERY_HEADS * HEAD_SIZE
    span = KEY_VALUE_HEADS * HEAD_SIZE
    for g in range(KEY_VALUE_HEADS):
        heads = range(g * ratio, (g + 1) * ratio)
        one = slice(g * HEAD_SIZE, (g + 1) * HEAD_SIZE)
        qs, ks, vs = stack(q, heads), k[:, one], v[:, one]
        dos, os = stack(dattn_f, heads), stack(mixed, heads)
        logs = jnp.concatenate([lse[:, h : h + 1] for h in heads], axis=0)
        s = jnp.where(mask, dot(qs, ks, 1, 1) * SCORE_SCALE, MASKED)
        w = jnp.exp(s - logs)
        low = w.astype(BF16)
        delta = jnp.sum(dos.astype(F32) * os.astype(F32), axis=1, keepdims=True)
        ds = (w * (dot(dos, vs, 1, 1) - delta) * SCORE_SCALE).astype(BF16)
        dq = dot(ds, ks)
        for i, h in enumerate(heads):
            dqkv[:, h * HEAD_SIZE : (h + 1) * HEAD_SIZE] = dq[i * tokens : (i + 1) * tokens]
        dqkv[:, kept + g * HEAD_SIZE : kept + (g + 1) * HEAD_SIZE] = dot(ds, qs, 0, 0)
        at_v = kept + span + g * HEAD_SIZE
        dqkv[:, at_v : at_v + HEAD_SIZE] = dot(low, dos, 0, 0)
        if g == 3:
            combine.sum_step(0)

    for j in range((kept + span) // 128):
        cols = slice(128 * j, 128 * (j + 1))
        rights[rows(f), cols] = turn(dqkv[:, cols], cos, -sin, first).astype(BF16)
    rights[rows(f), kept + span : split] = dqkv[:, kept + span :].astype(BF16)
    send_rights(1)
    pass_rights(0)
    loads[6].wait()
    turned[...] = left[...].T
    take_rights(0)
    step = 512

    def product(part, half, lo, hi):
        for a in range(lo, hi, step):
            got = dot(turned[half * rg : (half + 1) * rg], rights[:, a : a + step]).astype(BF16)
            for i in range(owners):
                part[i, :, a - lo : a - lo + step] = got[i * piece : (i + 1) * piece]

    product(part_o, 1, split, split + MODEL_WIDTH)
    outer.begin(nothing)
    combine.sum_step(1)
    for i in range(3, 6):
        loads[i].wait()
    mine = rights[rows(f), :split]
    dh = dot(mine[:, :kept], full(2), 1, 1)
    dh = dh + dot(mine[:, kept : kept + span], full(3), 1, 1)
    dh = dh + dot(mine[:, kept + span :], full(4), 1, 1)
    x = hidden[...].astype(F32)
    scale = lax.rsqrt(jnp.mean(x * x, axis=1, keepdims=True) + EPS)
    n = x * scale
    aux[experts : experts + 1, :] = jnp.sum(dh * n, axis=0, keepdims=True)
    dn = dh * gain_a[...].reshape(1, -1)
    grad_in[...] = dgrad[...] + scale * (dn - n * jnp.mean(dn * n, axis=1, keepdims=True))

    def cols(g):
        return pl.ds(pl.multiple_of(g * rg, 128), rg)

    def auxes(i):
        g = (f + i) % shards
        return remote(
            aux.at[:, cols(g)], aux_in.at[i], asend.at[i - 1], arecv.at[i - 1], (g, at.e)
        )

    for i in range(1, shards):
        auxes(i).start()
    for h in range(EARLY + 1, held):
        for c in late(h):
            c.start()
    aux_in[0] = aux[:, cols(f)]

    outer.more(nothing)
    combine.sum_step(2)
    combine.sum_step(3)
    pass_rights(1)
    outer.sum_step(0)
    combine.sum_last()
    block_out[...] = (resid[...] + comb_own[...]).astype(BF16)
    take_rights(1)
    extra = aux_in[0]
    for i in range(1, shards):
        auxes(i).wait_recv()
        extra = extra + aux_in[i]
    extra = jnp.concatenate([extra, jnp.zeros((128 - extra.shape[0], rg), F32)], axis=0)
    extra = extra.T.astype(BF16)
    product(part_q, 0, 0, split)
    for i in range(owners):
        part_q[i, :, split:] = extra[i * piece : (i + 1) * piece]
    inner.begin(nothing)
    for i in range(1, 4):
        outer.sum_step(i)
    outer.sum_last()
    inner.more(nothing)
    total_o[at.e] = own_o[...].astype(BF16)
    outer_all.begin()
    inner.sum_step(0)
    outer_all.relay_step(1)
    inner.sum_step(1)
    inner.sum_step(2)
    outer_all.relay_step(2)
    inner.sum_step(3)
    inner.sum_last()
    total_q[at.e] = own_q[...].astype(BF16)
    inner_all.begin()
    outer_all.relay_step(3)
    inner_all.relay()
    outer_all.rest()

    def shown(k, carry):
        to = pl.ds(pl.multiple_of(k * piece, piece), piece)
        out_o[to, :] = total_o[k]
        return carry

    lax.fori_loop(0, owners, shown, 0)
    inner_all.rest()

    def shown_too(k, carry):
        to = pl.ds(pl.multiple_of(k * piece, piece), piece)
        out_q[to, :] = total_q[k, :, :kept]
        out_k[to, :] = total_q[k, :, kept : kept + span]
        out_v[to, :] = total_q[k, :, kept + span : split]
        out_r[to, :] = total_q[k, :, split:]
        return carry

    lax.fori_loop(0, owners, shown_too, 0)
    for chunk in range(2):
        for i in range(3):
            block(chunk, f, i, sibling).wait_send()
    for i in range(1, shards):
        auxes(i).wait_send()
    for t in (combine, outer, inner, outer_all, inner_all):
        t.finish()
    for h in range(EARLY, held):
        for c in late(h):
            c.wait()


def reverse(sizes, vmem_args, fulls, comb, left, away, far):
    shards, owners, tokens, experts, held = sizes
    rg = MODEL_WIDTH // shards
    piece = rg // owners
    chips = shards // 2
    line = 4
    side = owners // line
    split = MODEL_WIDTH + 2 * KEY_VALUE_HEADS * HEAD_SIZE
    wide = split + 128
    extra = 48
    vm, dma = pltpu.VMEM, pltpu.SemaphoreType.DMA
    vmem, any_ = pl.BlockSpec(memory_space=pltpu.VMEM), pl.BlockSpec(memory_space=pl.ANY)

    def scatter(rows, width):
        return [
            vm((owners, rows, width), BF16),
            vm((line, rows, width), BF16),
            vm((line + 1, rows, width), BF16),
            vm((rows, width), F32),
            vm((rows, width - width // 256 * 128), BF16),
        ]

    shape = jax.ShapeDtypeStruct
    return pl.pallas_call(
        functools.partial(reverse_kernel, sizes),
        name="reverse",
        out_shape=(
            shape((tokens, MODEL_WIDTH), BF16),
            shape((tokens, MODEL_WIDTH), F32),
            shape((rg, MODEL_WIDTH), BF16),
            shape((rg, MODEL_WIDTH), BF16),
            shape((rg, KEY_VALUE_HEADS * HEAD_SIZE), BF16),
            shape((rg, KEY_VALUE_HEADS * HEAD_SIZE), BF16),
            shape((rg, 128), BF16),
            tuple(shape(r.shape, BF16) for r in far),
        ),
        in_specs=[vmem] * len(vmem_args) + [any_] * 11,
        out_specs=(*[vmem] * 7, (any_, any_)),
        input_output_aliases={len(vmem_args) + 9: 7, len(vmem_args) + 10: 8},
        scratch_shapes=[
            tuple(vm(w.shape, BF16) for w in fulls),
            vm((shards * tokens, 2 * rg), BF16),
            vm((2 * rg, shards * tokens), BF16),
            vm((shards * tokens, split + MODEL_WIDTH), BF16),
            vm((tokens, MODEL_WIDTH), F32),
            vm((tokens, MODEL_WIDTH), BF16),
            vm((tokens, split), F32),
            vm((extra, MODEL_WIDTH), F32),
            vm((shards, extra, rg), F32),
            *scatter(tokens, MODEL_WIDTH),
            *scatter(piece, MODEL_WIDTH),
            *scatter(piece, wide),
            vm((owners, piece, MODEL_WIDTH), BF16),
            vm((owners, piece, wide), BF16),
            dma((7,)),
            dma((2, 3)),
            dma((2, shards)),
            dma((shards - 1,)),
            dma((shards - 1,)),
            dma((2, chips - 1, held - EARLY)),
            dma((2, chips - 1, held - EARLY)),
            *([dma((line, 2)), dma((line, 2)), dma((line,)), dma((line + 1,)), dma((2,))] * 3),
            *([dma((2, side + 2, owners)), dma((2, owners))] * 2),
        ],
        compiler_params=pltpu.CompilerParams(
            collective_id=2, has_side_effects=True, vmem_limit_bytes=63 * 2**20
        ),
    )(*vmem_args, *fulls, comb, left, *away, *far)


def finish_kernel(experts, *refs):
    (s0, r0, s1, r1, q, k, v, o, extra, rows, gradient), outs = refs[:11], refs[11:]
    o0, o1, oq, ok, ov, oo, orouter, oga, ogf, orows, ograd = outs
    for a, b, c in ((s0, r0, o0), (s1, r1, o1)):
        total = a[...].astype(F32)
        for i in range(b.shape[0]):
            total = total + b[i].astype(F32)
        c[...] = total
    for a, b in ((q, oq), (k, ok), (v, ov), (o, oo)):
        b[...] = a[...].astype(F32)
    orows[...] = rows[...]
    ograd[...] = gradient[...]

    @pl.when(pl.program_id(0) == 0)
    def _():
        turned = extra[...].astype(F32).T
        orouter[...] = turned[:experts]
        oga[...] = turned[experts]
        ogf[...] = turned[experts + 1]


def finish(experts, sums, far, grads, extra, rows, gradient):
    steps = 2
    rg = sums[0].shape[1]
    two = [s.reshape(-1, s.shape[2]) for s in sums]
    away = [r.reshape(r.shape[0], -1, r.shape[3]) for r in far]

    def rows_of(a):
        return pl.BlockSpec((a.shape[0] // steps, a.shape[1]), lambda i: (i, 0))

    def deep(a):
        return pl.BlockSpec((a.shape[0], a.shape[1] // steps, a.shape[2]), lambda i: (0, i, 0))

    def whole(shape):
        return pl.BlockSpec(shape, lambda i: (0,) * len(shape))

    shape = jax.ShapeDtypeStruct
    small = [(experts, rg), (rg,), (rg,)]
    out = pl.pallas_call(
        functools.partial(finish_kernel, experts),
        name="finish",
        grid=(steps,),
        out_shape=(
            *[shape(a.shape, F32) for a in two],
            *[shape(a.shape, F32) for a in grads],
            *[shape(a, F32) for a in small],
            shape(rows.shape, rows.dtype),
            shape(gradient.shape, F32),
        ),
        in_specs=[
            rows_of(two[0]), deep(away[0]), rows_of(two[1]), deep(away[1]),
            *[rows_of(a) for a in grads], whole(extra.shape), rows_of(rows), rows_of(gradient),
        ],
        out_specs=(
            *[rows_of(a) for a in two], *[rows_of(a) for a in grads], *[whole(a) for a in small],
            rows_of(rows), rows_of(gradient),
        ),
    )(two[0], away[0], two[1], away[1], *grads, extra, rows, gradient)
    return out[0].reshape(sums[0].shape), out[1].reshape(sums[1].shape), *out[2:]


def plain_local(
    hidden_in,
    doc_ids,
    routes,
    gain_attn,
    w_query,
    key_matrix,
    value_matrix,
    w_output,
    gain_ffn,
    w_router,
    w_gateup,
    w_down,
    cotangent,
):
    tokens = hidden_in.shape[0]
    experts = w_router.shape[1]
    shards = lax.axis_size("fsdp")
    owners = lax.axis_size("expert")
    held = w_gateup.shape[0]
    half = w_down.shape[1]
    hidden_units = w_gateup.shape[2]
    pairing = 2 if held % 2 == 0 else 1
    groups = held // pairing
    slots = groups * CAP
    mine = lax.axis_index("expert")
    f32, bf16 = jnp.float32, jnp.bfloat16

    first = lax.all_gather(
        jnp.concatenate([w_query, key_matrix, value_matrix, w_router], axis=1),
        "fsdp",
        axis=0,
        tiled=True,
    )
    full_query, full_key, full_value, full_router = jnp.split(first, (1536, 2048, 2560), axis=1)
    full_output = lax.all_gather(w_output, "fsdp", axis=0, tiled=True)
    cot_all = lax.all_gather(cotangent, "expert", axis=0)
    weights_attn = (gain_attn, full_query, full_key, full_value, full_output, gain_ffn, full_router)
    state = forward_local(hidden_in, doc_ids[0], routes, *weights_attn)
    resid, ffn_in, probs = state[11], state[12], state[15]

    chosen = jnp.any(
        routes[:, :, None] == jnp.arange(experts, dtype=jnp.int32)[None, None, :], axis=1
    )
    below = jnp.tril(jnp.ones((tokens, tokens), bf16), -1)
    rank = jnp.dot(below, chosen.astype(bf16), preferred_element_type=f32)
    rank = jnp.where(chosen, rank, -1.0)
    gate = jnp.where(chosen, probs, 0.0)
    gate_high = gate.astype(bf16)
    gate_low = (gate - gate_high.astype(f32)).astype(bf16)
    meta = jnp.concatenate([rank.astype(bf16), gate_high, gate_low], axis=1)
    sent = jnp.concatenate(
        [ffn_in, meta, jnp.zeros((tokens, 128 - 3 * experts), bf16)], axis=1
    )
    got = lax.all_gather(sent, "expert", axis=0)
    rows_all = got[:, :, :MODEL_WIDTH]
    meta_all = got[:, :, MODEL_WIDTH:]
    lane = jnp.arange(slots, dtype=jnp.int32)
    slot_expert = (mine * held + (lane // CAP) * pairing) // 2
    spread = (jnp.arange(experts, dtype=jnp.int32)[:, None] == slot_expert[None, :]).astype(bf16)
    rank_at = jnp.dot(meta_all[:, :, :experts], spread, preferred_element_type=f32)
    gate_at = jnp.dot(
        meta_all[:, :, experts : 2 * experts], spread, preferred_element_type=f32
    ) + jnp.dot(meta_all[:, :, 2 * experts : 3 * experts], spread, preferred_element_type=f32)
    place = rank_at == (lane % CAP).astype(f32)[None, None, :]
    onehot = place.astype(bf16)
    gated = jnp.where(place, gate_at, 0.0)
    slot_gate = jnp.sum(gated, axis=1)

    def dispatch(rows):
        out = jnp.einsum("stj,std->sjd", onehot, rows, preferred_element_type=f32)
        return out.reshape(owners, groups, CAP, MODEL_WIDTH)

    taken = dispatch(rows_all).astype(bf16)
    cot_rows = dispatch(cot_all)
    slot_gate_4 = slot_gate.reshape(owners, groups, CAP, 1)
    grads_in = (cot_rows * slot_gate_4).astype(bf16)
    w_pairs = w_gateup.reshape(groups, pairing, MODEL_WIDTH, hidden_units)
    down_pairs = w_down.reshape(groups, pairing, half, MODEL_WIDTH)
    gate_up = jnp.einsum("secd,emdf->emscf", taken, w_pairs, preferred_element_type=f32)
    a, b = gate_up[..., :half], gate_up[..., half:]
    sigma = jax.nn.sigmoid(a)
    acted = (a * sigma * b).astype(bf16)
    made = jnp.einsum("emscf,emfd->secd", acted, down_pairs, preferred_element_type=f32)
    made = made.astype(bf16)
    grad_slot = jnp.sum(made.astype(f32) * cot_rows, axis=-1).reshape(owners, slots)
    grad_gate_back = jnp.where(place, grad_slot[:, None, :], 0.0).reshape(
        owners, tokens, groups, CAP
    )
    grad_gate_back = jnp.sum(grad_gate_back, axis=-1)
    onto = (
        (mine * held + jnp.arange(groups) * pairing)[:, None] // 2
        == jnp.arange(128, dtype=jnp.int32)[None, :]
    ).astype(bf16)
    grad_gate_back = jnp.dot(
        grad_gate_back.astype(bf16), onto, preferred_element_type=f32
    ).astype(bf16)
    weighted = (made.astype(f32) * slot_gate_4).astype(bf16).reshape(owners, slots, MODEL_WIDTH)
    combined = jnp.einsum("stj,sjd->std", onehot, weighted, preferred_element_type=f32)
    grad_acted = jnp.einsum("secd,emfd->emscf", grads_in, down_pairs, preferred_element_type=f32)
    grad_down = jnp.einsum("emscf,secd->emfd", acted, grads_in, preferred_element_type=f32)
    grad_a = grad_acted * b * sigma * (1.0 + a * (1.0 - sigma))
    grad_b = grad_acted * a * sigma
    joined = jnp.concatenate([grad_a, grad_b], axis=-1).astype(bf16)
    grad_gateup = jnp.einsum("secd,emscf->emdf", taken, joined, preferred_element_type=f32)
    grad_rows = jnp.einsum("emscf,emdf->secd", joined, w_pairs, preferred_element_type=f32)
    grad_rows = grad_rows.astype(bf16).reshape(owners, slots, MODEL_WIDTH)
    grad_ffn = jnp.einsum("stj,sjd->std", onehot, grad_rows, preferred_element_type=f32)
    back = jnp.concatenate([grad_ffn.astype(bf16), grad_gate_back], axis=-1)
    back = lax.psum_scatter(
        back.reshape(owners * tokens, -1), "expert", scatter_dimension=0, tiled=True
    ).astype(f32)
    grad_ffn, grad_gate_dense = back[:, :MODEL_WIDTH], back[:, MODEL_WIDTH : MODEL_WIDTH + experts]
    combined = lax.psum_scatter(
        combined.astype(bf16).reshape(owners * tokens, -1),
        "expert",
        scatter_dimension=0,
        tiled=True,
    )
    block_out = (resid + combined.astype(f32)).astype(bf16)
    grad_gateup, grad_down = (
        lax.psum_scatter(
            grad_gateup.reshape(held, MODEL_WIDTH, hidden_units).astype(bf16),
            "fsdp",
            scatter_dimension=1,
            tiled=True,
        ).astype(f32),
        lax.psum_scatter(
            grad_down.reshape(held, half, MODEL_WIDTH).astype(bf16),
            "fsdp",
            scatter_dimension=1,
            tiled=True,
        ).astype(f32),
    )
    grad_input, grads = backward_local(
        state, chosen, cotangent, grad_ffn, grad_gate_dense, *weights_attn
    )
    widths = [g.shape[1] if g.ndim == 2 else 1 for g in grads]
    flat = jnp.concatenate([g if g.ndim == 2 else g[:, None] for g in grads], axis=1)
    share = lax.psum_scatter(flat.astype(bf16), "fsdp", scatter_dimension=0, tiled=True)
    total = lax.psum(share, "expert").astype(f32)
    pieces = jnp.split(total, [sum(widths[: i + 1]) for i in range(len(widths) - 1)], axis=1)
    pieces = [p if g.ndim == 2 else p[:, 0] for p, g in zip(pieces, grads)]
    return (block_out, grad_input, *pieces, grad_gateup, grad_down)


def kernel_local(
    hidden_in,
    doc_ids,
    routes,
    gain_attn,
    w_query,
    key_matrix,
    value_matrix,
    w_output,
    gain_ffn,
    w_router,
    w_gateup,
    w_down,
    cotangent,
):
    tokens = hidden_in.shape[0]
    experts = w_router.shape[1]
    shards = lax.axis_size("fsdp")
    owners = lax.axis_size("expert")
    held = w_gateup.shape[0]
    pairing = 2 if held % 2 == 0 else 1
    f32, bf16 = jnp.float32, jnp.bfloat16

    shares = (w_query, key_matrix, value_matrix, w_output, w_router.T)
    made, fulls, cot_all, left = attend(
        (shards, owners, tokens, experts), hidden_in, doc_ids, routes.T, gain_attn, gain_ffn, shares,
        cotangent,
    )
    h1, q, k, v, mixed, lse, resid, sent, probs = made
    sizes = (shards, owners, tokens, experts, held, pairing)
    back, comb, sums, far, away = moe(sizes, sent, cot_all, w_gateup, w_down)
    wq, wk, wv, wo, wr = fulls
    block_out, grad_input, total_o, total_q, total_k, total_v, total_r, far = reverse(
        (shards, owners, tokens, experts, held),
        (hidden_in, doc_ids, routes.T, gain_attn, gain_ffn, cotangent, q, k, v, mixed,
         lse, resid, sent, probs, back),
        (wo, wr, wq, wk, wv),
        comb,
        left,
        away,
        far,
    )
    out = finish(
        experts, sums, far, (total_q, total_k, total_v, total_o), total_r, block_out, grad_input
    )
    grad_gateup, grad_down, grad_q, grad_k, grad_v, grad_o, grad_r, ga, gf, block, gradient = out
    return (
        block,
        gradient,
        grad_q,
        grad_k,
        grad_v,
        grad_o,
        grad_r.T,
        ga,
        gf,
        grad_gateup,
        grad_down,
    )


def local(*args):
    owners, held = lax.axis_size("expert"), args[10].shape[0]
    groups = held // (2 if held % 2 == 0 else 1)
    if lax.axis_size("fsdp") == 4 and owners == 8 and owners * groups * CAP <= 2048:
        return kernel_local(*args)
    return plain_local(*args)


def solution(mesh):
    in_specs = (
        P(("fsdp", "expert"), None),
        P(("fsdp", "expert"), None),
        P(("fsdp", "expert"), None),
        P(),
        P("fsdp", None),
        P("fsdp", None),
        P("fsdp", None),
        P("fsdp", None),
        P(),
        P("fsdp", None),
        P("expert", None, None),
        P("expert", None, None),
        P(("fsdp", "expert"), None),
    )
    out_specs = (
        P(("fsdp", "expert"), None),
        P(("fsdp", "expert"), None),
        P("fsdp", None),
        P("fsdp", None),
        P("fsdp", None),
        P("fsdp", None),
        P("fsdp", None),
        P("fsdp"),
        P("fsdp"),
        P("expert", "fsdp", None),
        P("expert", "fsdp", None),
    )
    return jax.shard_map(local, mesh=mesh, in_specs=in_specs, out_specs=out_specs, check_vma=False)
```

```python
import functools
import math

import jax
import jax.numpy as jnp
from jax import lax
from jax.experimental import pallas as pl
from jax.experimental.pallas import tpu as pltpu
from jax.sharding import PartitionSpec as P

MODEL_WIDTH = 1536
QUERY_HEADS = 24
KEY_VALUE_HEADS = 8
HEAD_SIZE = 64
TOP = 8
CAP = 48


EPS = 1e-05
BASE = 10000.0
SCORE_SCALE = 0.015625
MASKED = -1e30


def rope_tables(doc_row):
    document_length = doc_row.shape[0]
    places = jnp.arange(document_length, dtype=jnp.int32)
    same_doc = doc_row[:, None] == doc_row[None, :]
    starts = jnp.min(jnp.where(same_doc, places[None, :], document_length), axis=1)
    position = (places - starts).astype(jnp.float32)
    half_width = HEAD_SIZE // 2
    inverse = jnp.exp(
        -math.log(BASE) * (2.0 * jnp.arange(half_width, dtype=jnp.float32) / HEAD_SIZE)
    )
    angle = position[:, None] * inverse[None, :]
    allowed = same_doc & (places[None, :] <= places[:, None])
    return (jnp.cos(angle), jnp.sin(angle), allowed)


def rotate(tensor, cosine_table, sine_table):
    half_width = HEAD_SIZE // 2
    first_half = tensor[..., :half_width]
    second = tensor[..., half_width:]
    cos_part = cosine_table[:, None, :]
    sin_part = sine_table[:, None, :]
    return jnp.concatenate(
        [first_half * cos_part - second * sin_part, second * cos_part + first_half * sin_part],
        axis=-1,
    )


def inverse_rotation(tensor, cosine_table, sine_table):
    half_width = HEAD_SIZE // 2
    first_half = tensor[..., :half_width]
    second = tensor[..., half_width:]
    cos_part = cosine_table[:, None, :]
    sin_part = sine_table[:, None, :]
    return jnp.concatenate(
        [first_half * cos_part + second * sin_part, second * cos_part - first_half * sin_part],
        axis=-1,
    )


def norm_forward(value_rows, gain):
    scale_inv = lax.rsqrt(jnp.mean(value_rows * value_rows, axis=-1, keepdims=True) + EPS)
    normed = value_rows * scale_inv
    return ((normed * gain).astype(jnp.bfloat16), normed, scale_inv)


def norm_backward(grad_out, normed, scale_inv, gain):
    grad_normed = grad_out * gain
    grad_gain = jnp.sum(grad_out * normed, axis=0)
    value_gradients = scale_inv * (
        grad_normed - normed * jnp.mean(grad_normed * normed, axis=-1, keepdims=True)
    )
    return (value_gradients, grad_gain)


def scores_of(query_rows, key_rows, allowed):
    document_length = query_rows.shape[0]
    group_rows = query_rows.reshape(
        document_length, KEY_VALUE_HEADS, QUERY_HEADS // KEY_VALUE_HEADS, HEAD_SIZE
    )
    scores = (
        jnp.einsum("qgrd,kgd->grqk", group_rows, key_rows, preferred_element_type=jnp.float32)
        * SCORE_SCALE
    )
    return jnp.where(allowed[None, None], scores, MASKED)


def forward_local(
    hidden_rows,
    doc_row,
    route_rows,
    gain_attn,
    w_query,
    key_matrix,
    value_matrix,
    w_output,
    gain_ffn,
    w_router,
):
    document_length = hidden_rows.shape[0]
    hidden_f = hidden_rows.astype(jnp.float32)
    attention_input, normed_attn, scale_attn = norm_forward(hidden_f, gain_attn)
    cosine_table, sine_table, allowed = rope_tables(doc_row)
    query_rows = jnp.dot(attention_input, w_query, preferred_element_type=jnp.float32).reshape(
        document_length, QUERY_HEADS, HEAD_SIZE
    )
    key_rows = jnp.dot(attention_input, key_matrix, preferred_element_type=jnp.float32).reshape(
        document_length, KEY_VALUE_HEADS, HEAD_SIZE
    )
    value_rows = (
        jnp.dot(attention_input, value_matrix, preferred_element_type=jnp.float32)
        .astype(jnp.bfloat16)
        .reshape(document_length, KEY_VALUE_HEADS, HEAD_SIZE)
    )
    query_rows = rotate(query_rows, cosine_table, sine_table).astype(jnp.bfloat16)
    key_rows = rotate(key_rows, cosine_table, sine_table).astype(jnp.bfloat16)
    scores = scores_of(query_rows, key_rows, allowed)
    top_score = jnp.max(scores, axis=-1, keepdims=True)
    log_total = top_score + jnp.log(jnp.sum(jnp.exp(scores - top_score), axis=-1, keepdims=True))
    weights = jnp.exp(scores - log_total).astype(jnp.bfloat16)
    attention_mixed = jnp.einsum(
        "grqk,kgd->qgrd", weights, value_rows, preferred_element_type=jnp.float32
    )
    attention_mixed = attention_mixed.reshape(document_length, QUERY_HEADS * HEAD_SIZE).astype(
        jnp.bfloat16
    )
    resid = hidden_f + jnp.dot(attention_mixed, w_output, preferred_element_type=jnp.float32)
    ffn_in, normed_ffn, scale_ffn = norm_forward(resid, gain_ffn)
    logits = jnp.dot(ffn_in, w_router, preferred_element_type=jnp.float32)
    probs = jax.nn.softmax(logits, axis=-1)
    picks = route_rows[:, :, None] == jnp.arange(probs.shape[1], dtype=jnp.int32)[None, None, :]
    gates = jnp.sum(jnp.where(picks, probs[:, None, :], 0.0), axis=-1)
    return (
        normed_attn,
        scale_attn,
        attention_input,
        cosine_table,
        sine_table,
        allowed,
        query_rows,
        key_rows,
        value_rows,
        attention_mixed,
        log_total,
        resid,
        ffn_in,
        normed_ffn,
        scale_ffn,
        probs,
        gates,
    )


def backward_local(
    state,
    route_rows,
    cot_rows,
    grad_ffn_in,
    grad_gates,
    gain_attn,
    w_query,
    key_matrix,
    value_matrix,
    w_output,
    gain_ffn,
    w_router,
):
    (
        normed_attn,
        scale_attn,
        attention_input,
        cosine_table,
        sine_table,
        allowed,
        query_rows,
        key_rows,
        value_rows,
        attention_mixed,
        log_total,
        resid,
        ffn_in,
        normed_ffn,
        scale_ffn,
        probs,
        gates,
    ) = state
    document_length = attention_input.shape[0]
    query_group = QUERY_HEADS // KEY_VALUE_HEADS
    grad_probs = jnp.where(route_rows, grad_gates, 0.0)
    grad_logits = (
        probs * (grad_probs - jnp.sum(probs * grad_probs, axis=-1, keepdims=True))
    ).astype(jnp.bfloat16)
    grad_router = jnp.dot(ffn_in.T, grad_logits, preferred_element_type=jnp.float32)
    grad_ffn_in = grad_ffn_in + jnp.dot(grad_logits, w_router.T, preferred_element_type=jnp.float32)
    grad_resid_part, grad_gain_ffn = norm_backward(grad_ffn_in, normed_ffn, scale_ffn, gain_ffn)
    grad_resid = cot_rows.astype(jnp.float32) + grad_resid_part
    grad_attn = grad_resid.astype(jnp.bfloat16)
    grad_output = jnp.dot(attention_mixed.T, grad_attn, preferred_element_type=jnp.float32)
    mixed_gradient = jnp.dot(grad_attn, w_output.T, preferred_element_type=jnp.float32).astype(
        jnp.bfloat16
    )
    scores = scores_of(query_rows, key_rows, allowed)
    weights = jnp.exp(scores - log_total)
    weights_low = weights.astype(jnp.bfloat16)
    gradient_by_group = mixed_gradient.reshape(
        document_length, KEY_VALUE_HEADS, query_group, HEAD_SIZE
    )
    mixed_by_group = attention_mixed.reshape(
        document_length, KEY_VALUE_HEADS, query_group, HEAD_SIZE
    )
    value_gradients = jnp.einsum(
        "grqk,qgrd->kgd", weights_low, gradient_by_group, preferred_element_type=jnp.float32
    )
    grad_weights = jnp.einsum(
        "qgrd,kgd->grqk", gradient_by_group, value_rows, preferred_element_type=jnp.float32
    )
    delta = jnp.transpose(
        jnp.sum(
            gradient_by_group.astype(jnp.float32) * mixed_by_group.astype(jnp.float32), axis=-1
        ),
        (1, 2, 0),
    )
    grad_scores = (weights * (grad_weights - delta[..., None]) * SCORE_SCALE).astype(jnp.bfloat16)
    query_by_group = query_rows.reshape(document_length, KEY_VALUE_HEADS, query_group, HEAD_SIZE)
    grad_query_rows = jnp.einsum(
        "grqk,kgd->qgrd", grad_scores, key_rows, preferred_element_type=jnp.float32
    ).reshape(document_length, QUERY_HEADS, HEAD_SIZE)
    key_row_gradient = jnp.einsum(
        "grqk,qgrd->kgd", grad_scores, query_by_group, preferred_element_type=jnp.float32
    )
    grad_query_rows = (
        inverse_rotation(grad_query_rows, cosine_table, sine_table)
        .reshape(document_length, QUERY_HEADS * HEAD_SIZE)
        .astype(jnp.bfloat16)
    )
    key_row_gradient = (
        inverse_rotation(key_row_gradient, cosine_table, sine_table)
        .reshape(document_length, KEY_VALUE_HEADS * HEAD_SIZE)
        .astype(jnp.bfloat16)
    )
    value_row_gradient = value_gradients.reshape(
        document_length, KEY_VALUE_HEADS * HEAD_SIZE
    ).astype(jnp.bfloat16)
    grad_query = jnp.dot(attention_input.T, grad_query_rows, preferred_element_type=jnp.float32)
    grad_key = jnp.dot(attention_input.T, key_row_gradient, preferred_element_type=jnp.float32)
    grad_value = jnp.dot(attention_input.T, value_row_gradient, preferred_element_type=jnp.float32)
    grad_attn_in = jnp.dot(grad_query_rows, w_query.T, preferred_element_type=jnp.float32)
    grad_attn_in = grad_attn_in + jnp.dot(
        key_row_gradient, key_matrix.T, preferred_element_type=jnp.float32
    )
    grad_attn_in = grad_attn_in + jnp.dot(
        value_row_gradient, value_matrix.T, preferred_element_type=jnp.float32
    )
    grad_hidden_part, grad_gain_attn = norm_backward(
        grad_attn_in, normed_attn, scale_attn, gain_attn
    )
    grad_in = grad_resid + grad_hidden_part
    return (
        grad_in,
        (grad_query, grad_key, grad_value, grad_output, grad_router, grad_gain_attn, grad_gain_ffn),
    )


MESH = pl.DeviceIdType.MESH
F32, BF16 = jnp.float32, jnp.bfloat16


def dot(a, b, da=1, db=0):
    return lax.dot_general(a, b, (((da,), (db,)), ((), ())), preferred_element_type=F32)


class Place:
    def __init__(self, shards, owners):
        self.shards, self.owners = shards, owners
        self.line = 4 if owners % 4 == 0 else 1
        self.side = owners // self.line
        self.chips = shards // 2
        self.f = lax.axis_index("fsdp")
        self.e = lax.axis_index("expert")
        self.a, self.b = self.e // self.side, self.e % self.side
        self.x, self.c = self.f // 2, self.f % 2

    def detour(self):
        end = self.line - 1
        got = jnp.where(self.a % 2 == 0, end, 0)
        return got, end - got, self.e + jnp.where(self.a % 2 == 0, self.side, -self.side)

    def others(self, all_fsdp):
        out = [((self.f, self.e + self.side), self.a < self.line - 1)]
        out.append(((self.f, self.e - self.side), self.a > 0))
        for i in range(1, self.side):
            out.append(((self.f, self.a * self.side + (self.b + i) % self.side), None))
        if all_fsdp:
            out += [(((self.f + i) % self.shards, self.e), None) for i in range(1, self.shards)]
            return out
        out.append(((self.x * 2 + 1 - self.c, self.e), None))
        for i in range(1, self.chips):
            out.append((((self.x + i) % self.chips * 2 + self.c, self.e), None))
        return out

    def meet(self, all_fsdp=False):
        bar = pltpu.get_barrier_semaphore()
        others = self.others(all_fsdp)
        for dev, cond in others:

            def signal(dev=dev):
                pl.semaphore_signal(bar, inc=1, device_id=dev, device_id_type=MESH)

            if cond is None:
                signal()
            else:
                pl.when(cond)(signal)
        pl.semaphore_wait(
            bar,
            len(others)
            - 2
            + jnp.where(self.a < self.line - 1, 1, 0)
            + jnp.where(self.a > 0, 1, 0),
        )


def remote(src, dst, send, recv, dev):
    return pltpu.make_async_remote_copy(
        src_ref=src, dst_ref=dst, send_sem=send, recv_sem=recv, device_id=dev, device_id_type=MESH
    )


class LineGather:
    def __init__(self, at, buf, send, recv, balance=False):
        self.at, self.buf, self.send, self.recv = at, buf, send, recv
        self.balance = balance
        width, count = buf.shape[2], recv.shape[0]
        cut = [width * p // count // 128 * 128 for p in range(count)] + [width]
        self.parts = [pl.ds(lo, hi - lo) for lo, hi in zip(cut, cut[1:])]

    def copy(self, k, p, way, dev):
        ref = self.buf.at[k, :, self.parts[p]]
        return remote(ref, ref, self.send.at[p, way, k], self.recv.at[p, k], (self.at.f, dev))

    def up(self, k, p):
        return self.copy(k, p, 0, self.at.e + self.at.side)

    def down(self, k, p):
        return self.copy(k, p, 1, self.at.e - self.at.side)

    def across(self, k, i, p):
        at = self.at
        return self.copy(k, p, 1 + i, at.a * at.side + (at.b + i) % at.side)

    def spread(self, k, p, up, down, across=True):
        at = self.at
        if up:

            @pl.when(at.a < at.line - 1)
            def _():
                self.up(k, p).start()

        if down:

            @pl.when(at.a > 0)
            def _():
                self.down(k, p).start()

        if across and (p < len(self.parts) - 1 or not self.balance):
            self.across(k, 1, p).start()
        elif across:
            pl.when(k // at.side != at.detour()[0])(lambda: self.across(k, 1, p).start())

    def detour(self):
        at = self.at
        k = at.detour()[1] * at.side + 1 - at.b
        return self.copy(k, len(self.parts) - 1, 3, at.detour()[2])

    def begin(self):
        for p in range(len(self.parts)):
            self.spread(self.at.e, p, True, True)

    def relay_step(self, s, across=True):
        at = self.at
        for p in range(len(self.parts)):

            @pl.when(at.a - s >= 0)
            def _(p=p):
                k = at.e - s * at.side
                self.down(k, p).wait_recv()
                self.spread(k, p, True, False, across)

            @pl.when(at.a + s < at.line)
            def _(p=p):
                k = at.e + s * at.side
                self.up(k, p).wait_recv()
                self.spread(k, p, False, True, across)

    def cross(self, n):
        at = self.at
        a = (
            jnp.where(at.a > 0, at.a - 1, at.a + 1),
            jnp.where(at.a == 0, 2, jnp.where(at.a == at.line - 1, at.a - 2, at.a + 1)),
            jnp.where(at.a < at.line // 2, at.line - 1, 0),
        )[n - 1]
        for p in range(len(self.parts)):
            self.spread(a * at.side + at.b, p, False, False)

    def relay(self):
        for s in range(1, self.at.line):
            self.relay_step(s)

    def each(self, use):
        at = self.at

        def near(s, carry):
            pl.when(s > 0)(lambda: self.relay_step(s))
            pl.when(at.a - s >= 0)(lambda: use(at.e - s * at.side))
            pl.when((s > 0) & (at.a + s < at.line))(lambda: use(at.e + s * at.side))
            return carry

        lax.fori_loop(0, at.line, near, 0)
        self.rest(use)

    def rest(self, use=None):
        at = self.at

        def take(n, carry):
            s, sign = n // 2, 1 - n % 2 * 2
            a = at.a + sign * s

            @pl.when((a >= 0) & (a < at.line) & (n != 1))
            def _():
                k = a * at.side + 1 - at.b
                for p in range(len(self.parts)):
                    self.across(k, 1, p).wait_recv()
                if self.balance:
                    pl.when(a == at.detour()[1])(lambda: self.detour().start())
                if use is not None:
                    use(k)

            return carry

        lax.fori_loop(0, 2 * at.line, take, 0)

    def finish(self):
        at = self.at
        for s in range(at.line):
            k = s * at.side + at.b
            for p in range(len(self.parts)):

                @pl.when((at.a < at.line - 1) & (at.a >= s))
                def _(k=k, p=p):
                    self.up(k, p).wait_send()

                @pl.when((at.a > 0) & (at.a <= s))
                def _(k=k, p=p):
                    self.down(k, p).wait_send()

                if p < len(self.parts) - 1 or not self.balance:
                    self.across(k, 1, p).wait_send()
                else:
                    pl.when(s != at.detour()[0])(
                        lambda k=k, p=p: self.across(k, 1, p).wait_send()
                    )
        if self.balance:
            self.detour().wait_send()


class LineScatter:
    def __init__(self, at, part, side_in, line_in, own, extra, sems, balance=False):
        self.balance = balance
        self.at, self.part, self.side_in, self.line_in, self.own = at, part, side_in, line_in, own
        self.extra = extra
        self.ssend, self.srecv, self.lsend, self.lrecv, self.esem = sems
        width = part.shape[2]
        self.cut = width // 256 * 128
        self.parts = (pl.ds(0, self.cut), pl.ds(self.cut, width - self.cut))

    def across(self, s, p):
        at = self.at
        return remote(
            self.part.at[s * at.side + 1 - at.b, :, self.parts[p]],
            self.side_in.at[s, :, self.parts[p]],
            self.ssend.at[s, p],
            self.srecv.at[s, p],
            (at.f, at.a * at.side + 1 - at.b),
        )

    def detour(self):
        at = self.at
        k = at.detour()[0] * at.side + 1 - at.b
        return remote(
            self.part.at[k, :, self.parts[1]], self.extra, self.esem.at[0], self.esem.at[1],
            (at.f, at.detour()[2]),
        )

    def join(self):
        at = self.at
        s = at.detour()[1]
        k = s * at.side + 1 - at.b
        self.detour().wait_recv()
        mine = self.part[k, :, self.cut :].astype(F32)
        self.part[k, :, self.cut :] = (mine + self.extra[...].astype(F32)).astype(BF16)
        self.across(s, 1).start()

    def along(self, s, dev, slot):
        at = self.at
        return remote(
            self.part.at[s * at.side + at.b],
            self.line_in.at[slot],
            self.lsend.at[s],
            self.lrecv.at[slot],
            (at.f, dev),
        )

    def up(self, s):
        return self.along(s, self.at.e + self.at.side, s)

    def down(self, s):
        at = self.at
        return self.along(s, at.e - at.side, jnp.where(s == at.a - 1, at.line, s))

    def place(self, i):
        at = self.at
        return jnp.where(at.a < at.line // 2, at.line - 1 - i, i)

    def middle(self):
        at = self.at
        return (at.a > 0) & (at.a < at.line - 1)

    def launch(self, make, lo, hi):
        at = self.at
        got, passed, _ = at.detour()

        def step(n, carry):
            s = self.place(n)
            make(s * at.side + 1 - at.b)
            self.across(s, 0).start()
            if self.balance:
                pl.when(s == got)(lambda: self.detour().start())
                pl.when((s != got) & (s != passed))(lambda: self.across(s, 1).start())
            else:
                self.across(s, 1).start()
            return carry

        lax.fori_loop(lo, hi, step, 0)

    def begin(self, make):
        self.launch(make, 0, 2)

    def more(self, make):
        at = self.at
        if self.balance:
            pl.when(self.middle())(self.join)
        self.launch(make, 2, at.line)

        def step(n, carry):
            make(n * at.side + at.b)
            return carry

        lax.fori_loop(0, at.line, step, 0)

    def sum_step(self, n):
        at = self.at
        if n == 1 and self.balance:
            pl.when(jnp.logical_not(self.middle()))(self.join)
        s = self.place(n)
        k = s * at.side + at.b
        got = at.detour()[0]
        self.own[...] = self.part[k].astype(F32)
        self.across(s, 0).wait_recv()
        self.own[:, : self.cut] += self.side_in[s, :, : self.cut].astype(F32)

        @pl.when((s != got) | (not self.balance))
        def _():
            self.across(s, 1).wait_recv()
            self.own[:, self.cut :] += self.side_in[s, :, self.cut :].astype(F32)

        @pl.when(((s > at.a) & (at.a > 0)) | ((s < at.a) & (at.a < at.line - 1)))
        def _():
            self.along(s, at.e, s).wait_recv()
            self.own[...] += self.line_in[s].astype(F32)

        self.part[k] = self.own[...].astype(BF16)

        @pl.when(s > at.a)
        def _():
            self.up(s).start()

        @pl.when(s < at.a)
        def _():
            self.down(s).start()

    def sum_last(self):
        at = self.at
        self.own[...] = self.part[at.e].astype(F32)

        @pl.when(at.a > 0)
        def _():
            self.along(at.a, at.e, at.a).wait_recv()
            self.own[...] += self.line_in[at.a].astype(F32)

        @pl.when(at.a < at.line - 1)
        def _():
            self.along(at.a, at.e, at.line).wait_recv()
            self.own[...] += self.line_in[at.line].astype(F32)

    def finish(self):
        at = self.at
        if self.balance:
            self.detour().wait_send()
        for s in range(at.line):
            self.across(s, 0).wait_send()
            pl.when((s != at.detour()[0]) | (not self.balance))(
                lambda s=s: self.across(s, 1).wait_send()
            )

            @pl.when(at.a < s)
            def _(s=s):
                self.up(s).wait_send()

            @pl.when(at.a > s)
            def _(s=s):
                self.down(s).wait_send()


def rope_of(allowed, tokens):
    lane = lax.broadcasted_iota(jnp.int32, (tokens, 128), 1)
    position = jnp.sum(allowed.astype(F32), axis=1, keepdims=True) - 1.0
    half = HEAD_SIZE // 2
    inverse = jnp.exp(-math.log(BASE) * (2.0 * (lane % half).astype(F32) / HEAD_SIZE))
    angle = position * inverse
    return jnp.cos(angle), jnp.sin(angle), lane % HEAD_SIZE < half


def turn(x, cos, sin, first):
    half = HEAD_SIZE // 2
    other = jnp.where(first, -pltpu.roll(x, 128 - half, 1), pltpu.roll(x, half, 1))
    return x * cos + other * sin


def visible(doc, tokens):
    row = lax.broadcasted_iota(jnp.int32, (tokens, tokens), 0)
    col = lax.broadcasted_iota(jnp.int32, (tokens, tokens), 1)
    key_doc = jnp.broadcast_to(doc.astype(F32), (tokens, tokens))
    own = jnp.sum(jnp.where(row == col, key_doc, 0.0), axis=1, keepdims=True)
    return (own == key_doc) & (col <= row)


def picked(routes, lane):
    ids = routes[...].astype(F32).T
    lane = lane.astype(F32)
    chosen = lane == ids[:, :1]
    for i in range(1, TOP):
        chosen = chosen | (lane == ids[:, i : i + 1])
    return chosen


def attend_kernel(sizes, hidden, doc, routes, gain_a, gain_f, *refs):
    shards, owners, tokens, experts = sizes
    shares, cot = refs[:5], refs[5]
    h1, q, k, v, mixed, lse, resid, sent, probs_out = refs[6:15]
    fulls, cot_out, left = refs[15:20], refs[20], refs[21]
    (bufs, cot_all, acc, lsem, xs, xr, ys, yr, ss, sr, cs, cr, ls, lr, own_left) = refs[22:]
    at = Place(shards, owners)
    rg = MODEL_WIDTH // shards
    half, quarter = rg // 2, rg // 4
    f = at.f
    sib = (at.x * 2 + 1 - at.c, at.e)
    over = ((at.x + 1) % at.chips * 2 + at.c, at.e)
    far = over[0]
    other = (at.x + 1) % at.chips * 2 + 1 - at.c
    mine = (at.a + at.b) % 2
    beside = (f, at.a * at.side + (at.b + 1) % at.side)
    step = jnp.where(at.a % 2 == 0, at.side, -at.side)
    along = (f, at.e + step)
    count = len(shares)

    own = [pltpu.make_async_copy(shares[n], bufs[n].at[f], lsem.at[n]) for n in range(count)]
    own.append(pltpu.make_async_copy(cot, cot_all.at[at.e], lsem.at[count]))
    for c in own:
        c.start()

    def piece(n, g, start, size, send, recv, dev):
        ref = bufs[n].at[g, pl.ds(pl.multiple_of(start, quarter), size)]
        return remote(ref, ref, send, recv, dev)

    def begins(i):
        return (mine * half, mine * half + quarter, (1 - mine) * half, (1 - mine) * half + quarter)[i]

    def out_x(n, i):
        start = pl.ds(pl.multiple_of(begins(i), quarter), quarter)
        return remote(
            shares[n].at[start], bufs[n].at[f, start], xs.at[n, i], xr.at[n, i], over
        )

    def in_x(n, i):
        return piece(n, far, begins(i), quarter, xs.at[n, i], xr.at[n, i], over)

    def out_yz(n, i):
        return piece(n, far, begins(i), quarter, ys.at[n, i], yr.at[n, i], (beside, along)[i])

    def in_yz(n, i):
        return piece(n, far, begins(2 + i), quarter, ys.at[n, i], yr.at[n, i], (beside, along)[i])

    def to_sib(n, i, g):
        return piece(n, g, begins(i), quarter, ss.at[n, i], sr.at[n, i], sib)

    def own_sib(n):
        return remote(shares[n], bufs[n].at[f], ss.at[n, 4], sr.at[n, 4], sib)

    def small_x():
        return remote(shares[4], bufs[4].at[f], xs.at[4, 0], xr.at[4, 0], over)

    def small_sib():
        return remote(bufs[4].at[far], bufs[4].at[far], ss.at[4, 0], sr.at[4, 0], sib)

    def pass_x(n, i):
        in_x(n, i).wait_recv()
        out_yz(n, i).start()
        to_sib(n, i, far).start()

    def pass_rest(n):
        for i in range(2):
            in_yz(n, i).wait_recv()
            to_sib(n, 2 + i, far).start()

    def from_sib(n):
        for i in range(4):
            to_sib(n, i, other).wait_recv()

    def lefts(n, i):
        g = (f + i) % shards
        return remote(
            (h1, mixed)[n].at[:, pl.ds(pl.multiple_of(g * rg, 128), rg)],
            left.at[pl.ds(f * tokens, tokens), pl.ds(n * rg, rg)],
            ls.at[n, i - 1], lr.at[n, i - 1], (g, at.e),
        )

    def left_own(n):
        return pltpu.make_async_copy(
            (h1, mixed)[n].at[:, pl.ds(pl.multiple_of(f * rg, 128), rg)],
            left.at[pl.ds(f * tokens, tokens), pl.ds(n * rg, rg)],
            own_left.at[n],
        )

    def send_left(n):
        left_own(n).start()
        for i in range(1, shards):
            lefts(n, i).start()

    at.meet(all_fsdp=True)
    order = (0, 1, 2, 3)
    for n in order[:3]:
        for i in range(2):
            out_x(n, i).start()
        own_sib(n).start()
    small_x().start()
    own_sib(4).start()
    for i in range(2):
        out_x(3, i).start()
    own_sib(3).start()
    cotg = LineGather(at, cot_all, cs, cr)
    own[count].wait()
    cotg.begin()

    x = hidden[...].astype(F32)
    scale = lax.rsqrt(jnp.mean(x * x, axis=1, keepdims=True) + EPS)
    h1[...] = (x * scale * gain_a[...].reshape(1, -1)).astype(BF16)
    allowed = visible(doc[...], tokens)
    cos, sin, first = rope_of(allowed, tokens)

    ends = (0, 1536, 2048, 2560)

    def project(g):
        part = h1[:, pl.ds(pl.multiple_of(g * rg, 128), rg)]
        return [dot(part, bufs[n][g]) for n in range(3)]

    for n in range(3):
        own[n].wait()
        acc[:, ends[n] : ends[n + 1]] = dot(
            h1[:, pl.ds(pl.multiple_of(f * rg, 128), rg)], bufs[n][f]
        )

    def add(g):
        for n, got in enumerate(project(g)):
            acc[:, ends[n] : ends[n + 1]] += got

    for n in range(3):
        own_sib(n).wait_recv()
    add(sib[0])
    pass_x(0, 0)
    cotg.relay_step(1, False)
    cotg.cross(1)
    pass_x(0, 1)
    cotg.relay_step(2, False)
    for n in (1, 2):
        for i in range(2):
            pass_x(n, i)
    cotg.cross(2)
    for n in range(3):
        pass_rest(n)
    pass_x(3, 0)
    cotg.relay_step(3, False)
    cotg.cross(3)
    add(far)
    for n in range(3):
        from_sib(n)
    add(other)
    small_x().wait_recv()
    small_sib().start()
    pass_x(3, 1)
    save = [pltpu.make_async_copy(bufs[n], fulls[n], lsem.at[n]) for n in range(count)]
    for c in save[:3]:
        c.start()

    for j in range(16):
        cols = slice(128 * j, 128 * (j + 1))
        got = turn(acc[:, cols], cos, sin, first).astype(BF16)
        if j < 12:
            q[:, cols] = got
        else:
            k[:, 128 * (j - 12) : 128 * (j - 11)] = got
    v[...] = acc[:, 2048:].astype(BF16)
    ratio = QUERY_HEADS // KEY_VALUE_HEADS
    mask = jnp.concatenate([allowed] * ratio, axis=0)

    def head(ref, h):
        return ref[:, h * HEAD_SIZE : (h + 1) * HEAD_SIZE]

    for g in range(KEY_VALUE_HEADS):
        heads = range(g * ratio, (g + 1) * ratio)
        rows = jnp.concatenate([head(q, h) for h in heads], axis=0)
        s = jnp.where(mask, dot(rows, head(k, g), 1, 1) * SCORE_SCALE, MASKED)
        top = jnp.max(s, axis=1, keepdims=True)
        e = jnp.exp(s - top)
        total = jnp.sum(e, axis=1, keepdims=True)
        o = dot((e / total).astype(BF16), head(v, g)).astype(BF16)
        log_total = top + jnp.log(total)
        for i, h in enumerate(heads):
            mixed[:, h * HEAD_SIZE : (h + 1) * HEAD_SIZE] = o[i * tokens : (i + 1) * tokens]
            lse[:, h : h + 1] = log_total[i * tokens : (i + 1) * tokens]

    send_left(0)
    send_left(1)

    def output(g):
        return dot(mixed[:, pl.ds(pl.multiple_of(g * rg, 128), rg)], bufs[3][g])

    for n in (3, 4):
        own[n].wait()
        own_sib(n).wait_recv()
    resid[...] = x + output(f) + output(sib[0])
    pass_rest(3)
    resid[...] += output(far)
    small_sib().wait_recv()
    from_sib(3)
    total = resid[...] + output(other)
    resid[...] = total
    scale = lax.rsqrt(jnp.mean(total * total, axis=1, keepdims=True) + EPS)
    h2 = (total * scale * gain_f[...].reshape(1, -1)).astype(BF16)
    sent[:, :MODEL_WIDTH] = h2
    logits = dot(h2[:, :rg], bufs[4][0], 1, 1)
    for g in range(1, shards):
        logits = logits + dot(h2[:, g * rg : (g + 1) * rg], bufs[4][g], 1, 1)
    logits = jnp.concatenate([logits, jnp.zeros((tokens, 128 - experts), F32)], axis=1)
    lane = lax.broadcasted_iota(jnp.int32, (tokens, 128), 1)
    live = lane < experts
    logits = jnp.where(live, logits, MASKED)
    e = jnp.where(live, jnp.exp(logits - jnp.max(logits, axis=1, keepdims=True)), 0.0)
    probs = e / jnp.sum(e, axis=1, keepdims=True)
    probs_out[...] = probs
    chosen = picked(routes, lane)
    row = lax.broadcasted_iota(jnp.int32, (tokens, tokens), 0)
    col = lax.broadcasted_iota(jnp.int32, (tokens, tokens), 1)
    below = jnp.where(row > col, 1.0, 0.0).astype(BF16)
    hits = jnp.where(chosen, 1.0, 0.0)
    rank = jnp.where(chosen, dot(below, hits.astype(BF16)), jnp.where(live, -1.0, 0.0))
    gate = jnp.where(chosen, probs, 0.0)
    high = gate.astype(BF16).astype(F32)
    low = gate - high
    meta = rank + pltpu.roll(high, experts, 1) + pltpu.roll(low, 2 * experts, 1)
    sent[:, MODEL_WIDTH:] = meta.astype(BF16)

    for c in save[3:]:
        c.start()
    cotg.rest()
    cotg.finish()
    keep = pltpu.make_async_copy(cot_all, cot_out, lsem.at[count])
    keep.start()
    for n in range(count):
        own_sib(n).wait_send()
    small_x().wait_send()
    small_sib().wait_send()
    for n in order:
        for i in range(2):
            out_x(n, i).wait_send()
            out_yz(n, i).wait_send()
        for i in range(4):
            to_sib(n, i, far).wait_send()
    for n in range(2):
        left_own(n).wait()
        for i in range(1, shards):
            lefts(n, i).wait()
    for c in save:
        c.wait()
    keep.wait()


def attend(sizes, hidden, doc, routes, gain_a, gain_f, shares, cot):
    shards, owners, tokens, experts = sizes
    rg = MODEL_WIDTH // shards
    side = owners // 4
    vm, dma = pltpu.VMEM, pltpu.SemaphoreType.DMA
    vmem, any_ = pl.BlockSpec(memory_space=pltpu.VMEM), pl.BlockSpec(memory_space=pl.ANY)
    n = len(shares)

    def shape(*dims, dtype=BF16):
        return jax.ShapeDtypeStruct(dims, dtype)

    outs = pl.pallas_call(
        functools.partial(attend_kernel, sizes),
        name="attend",
        out_shape=(
            shape(tokens, MODEL_WIDTH),
            shape(tokens, MODEL_WIDTH),
            shape(tokens, KEY_VALUE_HEADS * HEAD_SIZE),
            shape(tokens, KEY_VALUE_HEADS * HEAD_SIZE),
            shape(tokens, MODEL_WIDTH),
            shape(tokens, 128, dtype=F32),
            shape(tokens, MODEL_WIDTH, dtype=F32),
            shape(tokens, MODEL_WIDTH + 128),
            shape(tokens, 128, dtype=F32),
            *[shape(shards, *s.shape) for s in shares],
            shape(owners, tokens, MODEL_WIDTH),
            shape(shards * tokens, 2 * rg),
        ),
        in_specs=[vmem] * 5 + [any_] * (n + 1),
        out_specs=[vmem] * 9 + [any_] * (n + 2),
        scratch_shapes=[
            tuple(vm((shards, *s.shape), BF16) for s in shares),
            vm((owners, tokens, MODEL_WIDTH), BF16),
            vm((tokens, 2560), F32),
            dma((n + 1,)),
            dma((n, 2)),
            dma((n, 2)),
            dma((n, 2)),
            dma((n, 2)),
            dma((n, 5)),
            dma((n, 5)),
            dma((2, side + 2, owners)),
            dma((2, owners)),
            dma((2, shards - 1)),
            dma((2, shards - 1)),
            dma((2,)),
        ],
        compiler_params=pltpu.CompilerParams(
            collective_id=0, has_side_effects=True, vmem_limit_bytes=60 * 2**20
        ),
    )(hidden, doc, routes, gain_a, gain_f, *shares, cot)
    return outs[:9], outs[9 : 9 + n], outs[9 + n], outs[10 + n]


EARLY = 4
AHEAD = 2


def moe_kernel(sizes, sent, cot, wgu, wd, back_out, comb_out, sums, far, away, *scratch):
    shards, owners, tokens, experts, held, pairing = sizes
    (rows_all, cot_buf, taken, cots, made, grads, slot_gate, slot_grad, place, wg_buf, wd_buf,
     acts, dus, gg, gd, turned, from_core, stage, side1, line1, extra1,
     rs, rr, wsem, csem, coresend, corerecv, farsend, farrecv, osem, free, s1, s2, s3, s4, s5,
     ) = scratch
    at = Place(shards, owners)
    groups = held // pairing
    slots = groups * CAP
    half = wd.shape[1]
    rg, rd = MODEL_WIDTH // shards, half // shards
    sibling = (at.x * 2 + 1 - at.c, at.e)

    def weights(g):
        out = []
        for m in range(pairing):
            h, slot = g * pairing + m, g % 2 * pairing + m
            out.append(pltpu.make_async_copy(wgu.at[h], wg_buf.at[slot], wsem.at[0, slot]))
            out.append(pltpu.make_async_copy(wd.at[h], wd_buf.at[slot], wsem.at[1, slot]))
        return out

    mine = pltpu.make_async_copy(sent, rows_all.at[at.e], osem.at[0, 0])
    mine.start()
    for c in weights(0):
        c.start()
    at.meet()
    rows = LineGather(at, rows_all, rs, rr)
    mine.wait()
    rows.begin()

    lane = lax.broadcasted_iota(jnp.int32, (128, slots), 1)
    row = lax.broadcasted_iota(jnp.int32, (128, slots), 0)

    def expert_of(j):
        return (at.e * held + j // CAP * pairing) // 2

    e_lane = expert_of(lane)
    find_rank = (row == e_lane).astype(F32).astype(BF16)
    slot_rank = (lane % CAP).astype(F32)
    e_row = expert_of(lax.broadcasted_iota(jnp.int32, (slots, 128), 0))
    col = lax.broadcasted_iota(jnp.int32, (slots, 128), 1)
    pick_gate = (col == e_row + experts) | (col == e_row + 2 * experts)

    def dispatch(k):
        rank_at = dot(rows_all[k, :, MODEL_WIDTH:], find_rank)
        pt = jnp.where(rank_at == slot_rank, 1.0, 0.0).astype(BF16)
        place[k] = pt
        got = dot(pt, rows_all[k], 0, 0)
        gate = jnp.sum(jnp.where(pick_gate, got[:, MODEL_WIDTH:], 0.0), axis=1, keepdims=True)
        gate = jnp.broadcast_to(gate, (slots, 128))
        to = pl.ds(k * CAP, CAP)
        for g in range(groups):
            taken[g, to, :] = got[g * CAP : (g + 1) * CAP, :MODEL_WIDTH].astype(BF16)
            slot_gate[g, to, :] = gate[g * CAP : (g + 1) * CAP]

    def dispatch_both(k):
        pull = pltpu.make_async_copy(cot.at[k], cot_buf.at[0], csem.at[0])
        pull.start()
        dispatch(k)
        pull.wait()
        got = dot(place[k], cot_buf[0], 0, 0).astype(BF16)
        to = pl.ds(k * CAP, CAP)
        for g in range(groups):
            cots[g, to, :] = got[g * CAP : (g + 1) * CAP]

    rows.each(dispatch_both)
    rows.finish()

    def through(g):
        for c in weights(g):
            c.wait()

        @pl.when(g + 1 < groups)
        def _():
            for c in weights(g + 1):
                c.start()

        gate = slot_gate[g][:, :1]
        total = jnp.zeros((owners * CAP, 1), F32)
        for m in range(pairing):
            h, slot = g * pairing + m, g % 2 * pairing + m
            gu = dot(taken[g], wg_buf[slot])
            a, b = gu[:, :half], gu[:, half:]
            sig = 1.0 / (1.0 + jnp.exp(-a))
            s = a * sig
            act = s * b
            acts[h] = (act * gate).astype(BF16)
            dp = dot(cots[g], wd_buf[slot], 1, 1)
            total = total + jnp.sum(act * dp, axis=1, keepdims=True)
            dact = dp * gate
            dus[h, :, :half] = (dact * b * sig * (1.0 + a * (1.0 - sig))).astype(BF16)
            dus[h, :, half:] = (dact * s).astype(BF16)
        slot_grad[g] = jnp.broadcast_to(total, (owners * CAP, 128))
        n = MODEL_WIDTH // 3
        for i in range(3):
            cols = slice(i * n, (i + 1) * n)
            y = 0.0
            dx = 0.0
            for m in range(pairing):
                h, slot = g * pairing + m, g % 2 * pairing + m
                y = y + dot(acts[h], wd_buf[slot, :, cols])
                dx = dx + dot(dus[h], wg_buf[slot, cols, :], 1, 1)
            made[g, :, cols] = y.astype(BF16)
            grads[g, :, cols] = dx.astype(BF16)

    def to_core(h):
        slot = h % 2
        out = []
        for i in range(at.chips):
            f = 2 * i + 1 - at.c
            for n, (buf, r) in enumerate(((gg, rg), (gd, rd))):
                out.append(
                    remote(
                        buf.at[slot, pl.ds(pl.multiple_of(f * r, r), r)],
                        from_core[n].at[slot, i],
                        coresend.at[slot, n, i],
                        corerecv.at[slot, n, i],
                        sibling,
                    )
                )
        return out

    def to_chips(h):
        return chip_copies(at, h, away, h, far, farsend, farrecv)

    def keep(h):
        slot = h % 2
        out = []
        for n in range(2):
            out.append(pltpu.make_async_copy(stage[n].at[slot, 0], sums[n].at[h], osem.at[n, slot]))
            for i in range(1, at.chips):
                out.append(
                    pltpu.make_async_copy(
                        stage[n].at[slot, i], away[n].at[h, i - 1], osem.at[2 * i + n, slot]
                    )
                )
        return out

    def add(h):
        slot = h % 2
        for c in to_core(h):
            c.wait()

        for i in range(at.chips):
            x = (at.x + i) % at.chips
            f = 2 * x + at.c
            for n, (buf, r) in enumerate(((gg, rg), (gd, rd))):
                own = buf[slot, pl.ds(pl.multiple_of(f * r, r), r)]
                stage[n][slot, i] = own + from_core[n][slot, x]
        for c in keep(h):
            c.start()

        @pl.when(h < held - 2)
        def _():
            pl.semaphore_signal(free, inc=1, device_id=sibling, device_id_type=MESH)

    def leave(h):
        for c in keep(h):
            c.wait()

        @pl.when(h < EARLY)
        def _():
            for c in to_chips(h):
                c.start()

        @pl.when(h == EARLY)
        def _():
            for c in to_chips(h)[0::2]:
                c.start()

    def weigh(h):
        g, slot = h // pairing, h % 2
        n = MODEL_WIDTH // 3

        @pl.when(h % pairing == 0)
        def _():
            turned[...] = taken[g].T

        for i in range(3):
            gg[slot, i * n : (i + 1) * n, :] = dot(
                turned[i * n : (i + 1) * n], dus[h]
            ).astype(BF16)
        gd[slot] = dot(acts[h], cots[g], 0, 0).astype(BF16)

        @pl.when(h >= 2)
        def _():
            pl.semaphore_wait(free, 1)

        for c in to_core(h):
            c.start()

    home = (col == e_row).astype(F32).astype(BF16)
    home_low = (col == e_row + experts).astype(F32).astype(BF16)
    parts = ((0, 512), (512, 1024), (1024, 1536))

    def make_back(k):
        to = pl.ds(k * CAP, CAP)
        dg = jnp.concatenate([slot_grad[g, to, :] for g in range(groups)], axis=0)
        high = dg.astype(BF16)
        low = (dg - high.astype(F32)).astype(BF16)
        pt = place[k]
        for lo, hi in parts:
            dx = jnp.concatenate([grads[g, to, lo:hi] for g in range(groups)], axis=0)
            rows_all[k, :, lo:hi] = dot(pt, dx).astype(BF16)
        rows_all[k, :, MODEL_WIDTH:] = dot(pt, high * home + low * home_low).astype(BF16)

    back = LineScatter(at, rows_all, side1, line1, back_out, extra1, (s1, s2, s3, s4, s5), True)

    def step(i, carry):
        @pl.when((i >= 2) & (i < AHEAD + 2))
        def _():
            leave(i - 2)

        @pl.when(i < groups)
        def _():
            through(i)

        @pl.when(i == groups)
        def _():
            back.begin(make_back)
            back.more(make_back)

        def staged(back, act):
            h = jnp.where(i < groups, i, i - gap) - back
            early = (i >= back) & (i < AHEAD + back) & (back < 2)
            pl.when(early | (i >= groups + back))(lambda: act(h))

        staged(2, leave)
        staged(0, weigh)
        staged(1, add)

        for n in range(2):

            @pl.when(i == groups + 3 + 3 * n)
            def _(n=n):
                back.sum_step(n)

        return carry

    gap = groups - AHEAD
    lax.fori_loop(0, held + gap, step, 0)
    back.sum_step(2)

    def combine(k, carry):
        to = pl.ds(k * CAP, CAP)
        slot = k % 2

        def put(j):
            return pltpu.make_async_copy(cot_buf.at[j % 2], comb_out.at[j], csem.at[j % 2])

        @pl.when(k >= 2)
        def _():
            put(k - 2).wait()

        for lo, hi in parts:
            y = jnp.concatenate([made[g, to, lo:hi] for g in range(groups)], axis=0)
            cot_buf[slot, :, lo:hi] = dot(place[k], y).astype(BF16)
        put(k).start()

        @pl.when(k == owners - 1)
        def _():
            put(k - 1).wait()
            put(k).wait()

        return carry

    back.sum_step(3)
    leave(held - 2)
    add(held - 1)
    lax.fori_loop(0, owners, combine, 0)
    leave(held - 1)
    back.sum_last()
    back.finish()

    def drain(h, carry):
        for c in to_chips(h):
            c.wait()
        return carry

    lax.fori_loop(0, EARLY, drain, 0)
    for c in to_chips(EARLY)[0::2]:
        c.wait()


def chip_copies(at, h, away, j, far, send, recv):
    out = []
    for i in range(1, at.chips):
        back = at.chips - 1 - i
        dev = ((at.x + i) % at.chips * 2 + at.c, at.e)
        for n in range(2):
            out.append(
                remote(
                    away[n].at[h, i - 1], far[n].at[back, h], send.at[n, i - 1, j],
                    recv.at[n, back, j], dev,
                )
            )
    return out


def moe(sizes, sent, cot, wgu, wd):
    shards, owners, tokens, experts, held, pairing = sizes
    groups = held // pairing
    slots, rows = groups * CAP, owners * CAP
    hidden, half = wgu.shape[2], wd.shape[1]
    rg, rd = MODEL_WIDTH // shards, half // shards
    chips = shards // 2
    line = 4
    side = owners // line
    width = MODEL_WIDTH + 128
    vm, dma = pltpu.VMEM, pltpu.SemaphoreType.DMA
    any_, vmem = pl.BlockSpec(memory_space=pl.ANY), pl.BlockSpec(memory_space=pltpu.VMEM)

    def pair(lead):
        return (vm((*lead, rg, hidden), BF16), vm((*lead, rd, MODEL_WIDTH), BF16))

    def outs(lead):
        return (
            jax.ShapeDtypeStruct((*lead, rg, hidden), BF16),
            jax.ShapeDtypeStruct((*lead, rd, MODEL_WIDTH), BF16),
        )

    return pl.pallas_call(
        functools.partial(moe_kernel, sizes),
        name="moe",
        out_shape=(
            jax.ShapeDtypeStruct((tokens, width), F32),
            jax.ShapeDtypeStruct((owners, tokens, MODEL_WIDTH), BF16),
            outs((held,)),
            outs((chips - 1, held)),
            outs((held, chips - 1)),
        ),
        in_specs=[any_] * 4,
        out_specs=(vmem, any_, (any_, any_), (any_, any_), (any_, any_)),
        scratch_shapes=[
            vm((owners, tokens, width), BF16),
            vm((2, tokens, MODEL_WIDTH), BF16),
            vm((groups, rows, MODEL_WIDTH), BF16),
            vm((groups, rows, MODEL_WIDTH), BF16),
            vm((groups, rows, MODEL_WIDTH), BF16),
            vm((groups, rows, MODEL_WIDTH), BF16),
            vm((groups, rows, 128), F32),
            vm((groups, rows, 128), F32),
            vm((owners, tokens, slots), BF16),
            vm((2 * pairing, MODEL_WIDTH, hidden), BF16),
            vm((2 * pairing, half, MODEL_WIDTH), BF16),
            vm((held, rows, half), BF16),
            vm((held, rows, hidden), BF16),
            vm((2, MODEL_WIDTH, hidden), BF16),
            vm((2, half, MODEL_WIDTH), BF16),
            vm((MODEL_WIDTH, rows), BF16),
            pair((2, chips)),
            pair((2, chips)),
            vm((line, tokens, width), BF16),
            vm((line + 1, tokens, width), BF16),
            vm((tokens, width - width // 256 * 128), BF16),
            dma((2, side + 2, owners)),
            dma((2, owners)),
            dma((2, 2 * pairing)),
            dma((2,)),
            dma((2, 2, chips)),
            dma((2, 2, chips)),
            dma((2, chips - 1, EARLY + 1)),
            dma((2, chips - 1, EARLY + 1)),
            dma((2 * chips, 2)),
            pltpu.SemaphoreType.REGULAR,
            dma((line, 2)),
            dma((line, 2)),
            dma((line,)),
            dma((line + 1,)),
            dma((2,)),
        ],
        compiler_params=pltpu.CompilerParams(
            collective_id=1, has_side_effects=True, vmem_limit_bytes=63 * 2**20
        ),
    )(sent, cot, wgu, wd)


def reverse_kernel(sizes, hidden, doc, routes, gain_a, gain_f, cot, q, k, v, mixed, lse, resid, sent,
                   probs, back, wo, wr, wq, wk, wv, comb, left_in, away0, away1, far0, far1, *refs):
    shards, owners, tokens, experts, held = sizes
    block_out, grad_in, out_o, out_q, out_k, out_v, out_r, far = refs[:8]
    (w_bufs, left, turned, rights, dgrad, dattn_f, dqkv, aux, aux_in, comb_part, comb_side, comb_line,
     comb_own, comb_x, part_o, side_o, line_o, own_o, extra_o, part_q, side_q, line_q, own_q, extra_q,
     total_o, total_q, wsem, rsend, rrecv, asend, arecv, farsend, farrecv, *sems) = refs[8:]
    at = Place(shards, owners)
    away = (away0, away1)
    rg = MODEL_WIDTH // shards
    piece = rg // owners
    split = dqkv.shape[1]
    f = at.f
    sibling = (at.x * 2 + 1 - at.c, at.e)
    over = ((at.x + 1) % at.chips * 2 + at.c, at.e)
    ratio = QUERY_HEADS // KEY_VALUE_HEADS

    fulls = (wo, wr, wq, wk, wv)
    loads = [pltpu.make_async_copy(comb, comb_part, wsem.at[0])]
    loads += [pltpu.make_async_copy(w, b, wsem.at[1 + i]) for i, (w, b) in enumerate(zip(fulls, w_bufs))]
    loads.append(pltpu.make_async_copy(left_in, left, wsem.at[6]))
    for c in loads:
        c.start()
    at.meet(all_fsdp=True)

    combine = LineScatter(at, comb_part, comb_side, comb_line, comb_own, comb_x, sems[:5], True)
    outer = LineScatter(at, part_o, side_o, line_o, own_o, extra_o, sems[5:10], True)
    inner = LineScatter(at, part_q, side_q, line_q, own_q, extra_q, sems[10:15], True)
    outer_all = LineGather(at, total_o, sems[15], sems[16])
    inner_all = LineGather(at, total_q, sems[17], sems[18])
    loads[0].wait()
    nothing = lambda k: None
    combine.begin(nothing)

    def rows(i):
        return pl.ds(pl.multiple_of(i * tokens, tokens), tokens)

    def block(chunk, g, send, dev):
        cols = (pl.ds(split, MODEL_WIDTH), pl.ds(0, split))[chunk]
        ref = rights.at[rows(g), cols]
        return remote(ref, ref, rsend.at[chunk, send], rrecv.at[chunk, g], dev)

    def send_rights(chunk):
        block(chunk, f, 0, sibling).start()
        block(chunk, f, 1, over).start()

    def pass_rights(chunk):
        block(chunk, over[0], 0, sibling).wait_recv()
        block(chunk, over[0], 2, sibling).start()

    def take_rights(chunk):
        block(chunk, sibling[0], 0, sibling).wait_recv()
        block(chunk, (at.x + 1) % at.chips * 2 + 1 - at.c, 0, sibling).wait_recv()

    def late(h):
        return chip_copies(at, h, away, h - EARLY, far, farsend, farrecv)

    h2 = sent[:, :MODEL_WIDTH]
    lane = lax.broadcasted_iota(jnp.int32, (tokens, 128), 1)
    chosen = picked(routes, lane)
    meta = back[:, MODEL_WIDTH:]
    dprobs = jnp.where(chosen, meta + pltpu.roll(meta, 128 - experts, 1), 0.0)
    p = probs[...]
    dlogits = (p * (dprobs - jnp.sum(p * dprobs, axis=1, keepdims=True))).astype(BF16)
    loads[1].wait()
    loads[2].wait()
    aux[...] = dot(dlogits, h2, 0, 0)[: aux.shape[0]]

    def full(i):
        return w_bufs[i][...].reshape(MODEL_WIDTH, -1)

    dh = back[:, :MODEL_WIDTH] + jnp.concatenate(
        [dot(dlogits[:, :experts], w_bufs[1][g]) for g in range(shards)], axis=1
    )
    x = resid[...]
    scale = lax.rsqrt(jnp.mean(x * x, axis=1, keepdims=True) + EPS)
    n = x * scale
    aux[experts + 1 : experts + 2, :] = jnp.sum(dh * n, axis=0, keepdims=True)
    dn = dh * gain_f[...].reshape(1, -1)
    dres = cot[...].astype(F32) + scale * (dn - n * jnp.mean(dn * n, axis=1, keepdims=True))
    dgrad[...] = dres
    dattn = dres.astype(BF16)
    rights[rows(f), split:] = dattn
    send_rights(0)
    for c in late(EARLY)[1::2]:
        c.start()
    dattn_f[...] = dot(dattn, full(0), 1, 1).astype(BF16)
    combine.more(nothing)

    allowed = visible(doc[...], tokens)
    cos, sin, first = rope_of(allowed, tokens)
    mask = jnp.concatenate([allowed] * ratio, axis=0)

    def stack(ref, heads):
        return jnp.concatenate(
            [ref[:, h * HEAD_SIZE : (h + 1) * HEAD_SIZE] for h in heads], axis=0
        )

    kept = QUERY_HEADS * HEAD_SIZE
    span = KEY_VALUE_HEADS * HEAD_SIZE
    for g in range(KEY_VALUE_HEADS):
        heads = range(g * ratio, (g + 1) * ratio)
        one = slice(g * HEAD_SIZE, (g + 1) * HEAD_SIZE)
        qs, ks, vs = stack(q, heads), k[:, one], v[:, one]
        dos, os = stack(dattn_f, heads), stack(mixed, heads)
        logs = jnp.concatenate([lse[:, h : h + 1] for h in heads], axis=0)
        s = jnp.where(mask, dot(qs, ks, 1, 1) * SCORE_SCALE, MASKED)
        w = jnp.exp(s - logs)
        low = w.astype(BF16)
        delta = jnp.sum(dos.astype(F32) * os.astype(F32), axis=1, keepdims=True)
        ds = (w * (dot(dos, vs, 1, 1) - delta) * SCORE_SCALE).astype(BF16)
        dq = dot(ds, ks)
        for i, h in enumerate(heads):
            dqkv[:, h * HEAD_SIZE : (h + 1) * HEAD_SIZE] = dq[i * tokens : (i + 1) * tokens]
        dqkv[:, kept + g * HEAD_SIZE : kept + (g + 1) * HEAD_SIZE] = dot(ds, qs, 0, 0)
        at_v = kept + span + g * HEAD_SIZE
        dqkv[:, at_v : at_v + HEAD_SIZE] = dot(low, dos, 0, 0)
        if g == 3:
            combine.sum_step(0)

    for j in range((kept + span) // 128):
        cols = slice(128 * j, 128 * (j + 1))
        rights[rows(f), cols] = turn(dqkv[:, cols], cos, -sin, first).astype(BF16)
    rights[rows(f), kept + span : split] = dqkv[:, kept + span :].astype(BF16)
    send_rights(1)
    pass_rights(0)
    loads[6].wait()
    turned[...] = left[...].T
    take_rights(0)
    step = 512

    def product(part, half, lo, hi):
        for a in range(lo, hi, step):
            got = dot(turned[half * rg : (half + 1) * rg], rights[:, a : a + step]).astype(BF16)
            for i in range(owners):
                part[i, :, a - lo : a - lo + step] = got[i * piece : (i + 1) * piece]

    product(part_o, 1, split, split + MODEL_WIDTH)
    outer.begin(nothing)
    combine.sum_step(1)
    for i in range(3, 6):
        loads[i].wait()
    mine = rights[rows(f), :split]
    dh = dot(mine[:, :kept], full(2), 1, 1)
    dh = dh + dot(mine[:, kept : kept + span], full(3), 1, 1)
    dh = dh + dot(mine[:, kept + span :], full(4), 1, 1)
    x = hidden[...].astype(F32)
    scale = lax.rsqrt(jnp.mean(x * x, axis=1, keepdims=True) + EPS)
    n = x * scale
    aux[experts : experts + 1, :] = jnp.sum(dh * n, axis=0, keepdims=True)
    dn = dh * gain_a[...].reshape(1, -1)
    grad_in[...] = dgrad[...] + scale * (dn - n * jnp.mean(dn * n, axis=1, keepdims=True))

    def cols(g):
        return pl.ds(pl.multiple_of(g * rg, 128), rg)

    def auxes(i):
        g = (f + i) % shards
        return remote(
            aux.at[:, cols(g)], aux_in.at[i], asend.at[i - 1], arecv.at[i - 1], (g, at.e)
        )

    for i in range(1, shards):
        auxes(i).start()
    for h in range(EARLY + 1, held):
        for c in late(h):
            c.start()
    aux_in[0] = aux[:, cols(f)]

    outer.more(nothing)
    combine.sum_step(2)
    combine.sum_step(3)
    pass_rights(1)
    outer.sum_step(0)
    combine.sum_last()
    block_out[...] = (resid[...] + comb_own[...]).astype(BF16)
    take_rights(1)
    extra = aux_in[0]
    for i in range(1, shards):
        auxes(i).wait_recv()
        extra = extra + aux_in[i]
    extra = jnp.concatenate([extra, jnp.zeros((128 - extra.shape[0], rg), F32)], axis=0)
    extra = extra.T.astype(BF16)
    product(part_q, 0, 0, split)
    for i in range(owners):
        part_q[i, :, split:] = extra[i * piece : (i + 1) * piece]
    inner.begin(nothing)
    for i in range(1, 4):
        outer.sum_step(i)
    outer.sum_last()
    inner.more(nothing)
    total_o[at.e] = own_o[...].astype(BF16)
    outer_all.begin()
    inner.sum_step(0)
    outer_all.relay_step(1)
    inner.sum_step(1)
    inner.sum_step(2)
    outer_all.relay_step(2)
    inner.sum_step(3)
    inner.sum_last()
    total_q[at.e] = own_q[...].astype(BF16)
    inner_all.begin()
    outer_all.relay_step(3)
    inner_all.relay()
    outer_all.rest()

    def shown(k, carry):
        to = pl.ds(pl.multiple_of(k * piece, piece), piece)
        out_o[to, :] = total_o[k]
        return carry

    lax.fori_loop(0, owners, shown, 0)
    inner_all.rest()

    def shown_too(k, carry):
        to = pl.ds(pl.multiple_of(k * piece, piece), piece)
        out_q[to, :] = total_q[k, :, :kept]
        out_k[to, :] = total_q[k, :, kept : kept + span]
        out_v[to, :] = total_q[k, :, kept + span : split]
        out_r[to, :] = total_q[k, :, split:]
        return carry

    lax.fori_loop(0, owners, shown_too, 0)
    for chunk in range(2):
        for i in range(3):
            block(chunk, f, i, sibling).wait_send()
    for i in range(1, shards):
        auxes(i).wait_send()
    for t in (combine, outer, inner, outer_all, inner_all):
        t.finish()
    for h in range(EARLY, held):
        for c in late(h)[1::2] if h == EARLY else late(h):
            c.wait()


def reverse(sizes, vmem_args, fulls, comb, left, away, far):
    shards, owners, tokens, experts, held = sizes
    rg = MODEL_WIDTH // shards
    piece = rg // owners
    chips = shards // 2
    line = 4
    side = owners // line
    split = MODEL_WIDTH + 2 * KEY_VALUE_HEADS * HEAD_SIZE
    wide = split + 128
    extra = 48
    vm, dma = pltpu.VMEM, pltpu.SemaphoreType.DMA
    vmem, any_ = pl.BlockSpec(memory_space=pltpu.VMEM), pl.BlockSpec(memory_space=pl.ANY)

    def scatter(rows, width):
        return [
            vm((owners, rows, width), BF16),
            vm((line, rows, width), BF16),
            vm((line + 1, rows, width), BF16),
            vm((rows, width), F32),
            vm((rows, width - width // 256 * 128), BF16),
        ]

    shape = jax.ShapeDtypeStruct
    return pl.pallas_call(
        functools.partial(reverse_kernel, sizes),
        name="reverse",
        out_shape=(
            shape((tokens, MODEL_WIDTH), BF16),
            shape((tokens, MODEL_WIDTH), F32),
            shape((rg, MODEL_WIDTH), BF16),
            shape((rg, MODEL_WIDTH), BF16),
            shape((rg, KEY_VALUE_HEADS * HEAD_SIZE), BF16),
            shape((rg, KEY_VALUE_HEADS * HEAD_SIZE), BF16),
            shape((rg, 128), BF16),
            tuple(shape(r.shape, BF16) for r in far),
        ),
        in_specs=[vmem] * len(vmem_args) + [any_] * 11,
        out_specs=(*[vmem] * 7, (any_, any_)),
        input_output_aliases={len(vmem_args) + 9: 7, len(vmem_args) + 10: 8},
        scratch_shapes=[
            tuple(vm(w.shape, BF16) for w in fulls),
            vm((shards * tokens, 2 * rg), BF16),
            vm((2 * rg, shards * tokens), BF16),
            vm((shards * tokens, split + MODEL_WIDTH), BF16),
            vm((tokens, MODEL_WIDTH), F32),
            vm((tokens, MODEL_WIDTH), BF16),
            vm((tokens, split), F32),
            vm((extra, MODEL_WIDTH), F32),
            vm((shards, extra, rg), F32),
            *scatter(tokens, MODEL_WIDTH),
            *scatter(piece, MODEL_WIDTH),
            *scatter(piece, wide),
            vm((owners, piece, MODEL_WIDTH), BF16),
            vm((owners, piece, wide), BF16),
            dma((7,)),
            dma((2, 3)),
            dma((2, shards)),
            dma((shards - 1,)),
            dma((shards - 1,)),
            dma((2, chips - 1, held - EARLY)),
            dma((2, chips - 1, held - EARLY)),
            *([dma((line, 2)), dma((line, 2)), dma((line,)), dma((line + 1,)), dma((2,))] * 3),
            *([dma((2, side + 2, owners)), dma((2, owners))] * 2),
        ],
        compiler_params=pltpu.CompilerParams(
            collective_id=2, has_side_effects=True, vmem_limit_bytes=63 * 2**20
        ),
    )(*vmem_args, *fulls, comb, left, *away, *far)


def finish_kernel(experts, *refs):
    (s0, r0, s1, r1, q, k, v, o, extra, rows, gradient), outs = refs[:11], refs[11:]
    o0, o1, oq, ok, ov, oo, orouter, oga, ogf, orows, ograd = outs
    for a, b, c in ((s0, r0, o0), (s1, r1, o1)):
        total = a[...].astype(F32)
        for i in range(b.shape[0]):
            total = total + b[i].astype(F32)
        c[...] = total
    for a, b in ((q, oq), (k, ok), (v, ov), (o, oo)):
        b[...] = a[...].astype(F32)
    orows[...] = rows[...]
    ograd[...] = gradient[...]

    @pl.when(pl.program_id(0) == 0)
    def _():
        turned = extra[...].astype(F32).T
        orouter[...] = turned[:experts]
        oga[...] = turned[experts]
        ogf[...] = turned[experts + 1]


def finish(experts, sums, far, grads, extra, rows, gradient):
    steps = 2
    rg = sums[0].shape[1]
    two = [s.reshape(-1, s.shape[2]) for s in sums]
    away = [r.reshape(r.shape[0], -1, r.shape[3]) for r in far]

    def rows_of(a):
        return pl.BlockSpec((a.shape[0] // steps, a.shape[1]), lambda i: (i, 0))

    def deep(a):
        return pl.BlockSpec((a.shape[0], a.shape[1] // steps, a.shape[2]), lambda i: (0, i, 0))

    def whole(shape):
        return pl.BlockSpec(shape, lambda i: (0,) * len(shape))

    shape = jax.ShapeDtypeStruct
    small = [(experts, rg), (rg,), (rg,)]
    out = pl.pallas_call(
        functools.partial(finish_kernel, experts),
        name="finish",
        grid=(steps,),
        out_shape=(
            *[shape(a.shape, F32) for a in two],
            *[shape(a.shape, F32) for a in grads],
            *[shape(a, F32) for a in small],
            shape(rows.shape, rows.dtype),
            shape(gradient.shape, F32),
        ),
        in_specs=[
            rows_of(two[0]), deep(away[0]), rows_of(two[1]), deep(away[1]),
            *[rows_of(a) for a in grads], whole(extra.shape), rows_of(rows), rows_of(gradient),
        ],
        out_specs=(
            *[rows_of(a) for a in two], *[rows_of(a) for a in grads], *[whole(a) for a in small],
            rows_of(rows), rows_of(gradient),
        ),
    )(two[0], away[0], two[1], away[1], *grads, extra, rows, gradient)
    return out[0].reshape(sums[0].shape), out[1].reshape(sums[1].shape), *out[2:]


def plain_local(
    hidden_in,
    doc_ids,
    routes,
    gain_attn,
    w_query,
    key_matrix,
    value_matrix,
    w_output,
    gain_ffn,
    w_router,
    w_gateup,
    w_down,
    cotangent,
):
    tokens = hidden_in.shape[0]
    experts = w_router.shape[1]
    shards = lax.axis_size("fsdp")
    owners = lax.axis_size("expert")
    held = w_gateup.shape[0]
    half = w_down.shape[1]
    hidden_units = w_gateup.shape[2]
    pairing = 2 if held % 2 == 0 else 1
    groups = held // pairing
    slots = groups * CAP
    mine = lax.axis_index("expert")
    f32, bf16 = jnp.float32, jnp.bfloat16

    first = lax.all_gather(
        jnp.concatenate([w_query, key_matrix, value_matrix, w_router], axis=1),
        "fsdp",
        axis=0,
        tiled=True,
    )
    full_query, full_key, full_value, full_router = jnp.split(first, (1536, 2048, 2560), axis=1)
    full_output = lax.all_gather(w_output, "fsdp", axis=0, tiled=True)
    cot_all = lax.all_gather(cotangent, "expert", axis=0)
    weights_attn = (gain_attn, full_query, full_key, full_value, full_output, gain_ffn, full_router)
    state = forward_local(hidden_in, doc_ids[0], routes, *weights_attn)
    resid, ffn_in, probs = state[11], state[12], state[15]

    chosen = jnp.any(
        routes[:, :, None] == jnp.arange(experts, dtype=jnp.int32)[None, None, :], axis=1
    )
    below = jnp.tril(jnp.ones((tokens, tokens), bf16), -1)
    rank = jnp.dot(below, chosen.astype(bf16), preferred_element_type=f32)
    rank = jnp.where(chosen, rank, -1.0)
    gate = jnp.where(chosen, probs, 0.0)
    gate_high = gate.astype(bf16)
    gate_low = (gate - gate_high.astype(f32)).astype(bf16)
    meta = jnp.concatenate([rank.astype(bf16), gate_high, gate_low], axis=1)
    sent = jnp.concatenate(
        [ffn_in, meta, jnp.zeros((tokens, 128 - 3 * experts), bf16)], axis=1
    )
    got = lax.all_gather(sent, "expert", axis=0)
    rows_all = got[:, :, :MODEL_WIDTH]
    meta_all = got[:, :, MODEL_WIDTH:]
    lane = jnp.arange(slots, dtype=jnp.int32)
    slot_expert = (mine * held + (lane // CAP) * pairing) // 2
    spread = (jnp.arange(experts, dtype=jnp.int32)[:, None] == slot_expert[None, :]).astype(bf16)
    rank_at = jnp.dot(meta_all[:, :, :experts], spread, preferred_element_type=f32)
    gate_at = jnp.dot(
        meta_all[:, :, experts : 2 * experts], spread, preferred_element_type=f32
    ) + jnp.dot(meta_all[:, :, 2 * experts : 3 * experts], spread, preferred_element_type=f32)
    place = rank_at == (lane % CAP).astype(f32)[None, None, :]
    onehot = place.astype(bf16)
    gated = jnp.where(place, gate_at, 0.0)
    slot_gate = jnp.sum(gated, axis=1)

    def dispatch(rows):
        out = jnp.einsum("stj,std->sjd", onehot, rows, preferred_element_type=f32)
        return out.reshape(owners, groups, CAP, MODEL_WIDTH)

    taken = dispatch(rows_all).astype(bf16)
    cot_rows = dispatch(cot_all)
    slot_gate_4 = slot_gate.reshape(owners, groups, CAP, 1)
    grads_in = (cot_rows * slot_gate_4).astype(bf16)
    w_pairs = w_gateup.reshape(groups, pairing, MODEL_WIDTH, hidden_units)
    down_pairs = w_down.reshape(groups, pairing, half, MODEL_WIDTH)
    gate_up = jnp.einsum("secd,emdf->emscf", taken, w_pairs, preferred_element_type=f32)
    a, b = gate_up[..., :half], gate_up[..., half:]
    sigma = jax.nn.sigmoid(a)
    acted = (a * sigma * b).astype(bf16)
    made = jnp.einsum("emscf,emfd->secd", acted, down_pairs, preferred_element_type=f32)
    made = made.astype(bf16)
    grad_slot = jnp.sum(made.astype(f32) * cot_rows, axis=-1).reshape(owners, slots)
    grad_gate_back = jnp.where(place, grad_slot[:, None, :], 0.0).reshape(
        owners, tokens, groups, CAP
    )
    grad_gate_back = jnp.sum(grad_gate_back, axis=-1)
    onto = (
        (mine * held + jnp.arange(groups) * pairing)[:, None] // 2
        == jnp.arange(128, dtype=jnp.int32)[None, :]
    ).astype(bf16)
    grad_gate_back = jnp.dot(
        grad_gate_back.astype(bf16), onto, preferred_element_type=f32
    ).astype(bf16)
    weighted = (made.astype(f32) * slot_gate_4).astype(bf16).reshape(owners, slots, MODEL_WIDTH)
    combined = jnp.einsum("stj,sjd->std", onehot, weighted, preferred_element_type=f32)
    grad_acted = jnp.einsum("secd,emfd->emscf", grads_in, down_pairs, preferred_element_type=f32)
    grad_down = jnp.einsum("emscf,secd->emfd", acted, grads_in, preferred_element_type=f32)
    grad_a = grad_acted * b * sigma * (1.0 + a * (1.0 - sigma))
    grad_b = grad_acted * a * sigma
    joined = jnp.concatenate([grad_a, grad_b], axis=-1).astype(bf16)
    grad_gateup = jnp.einsum("secd,emscf->emdf", taken, joined, preferred_element_type=f32)
    grad_rows = jnp.einsum("emscf,emdf->secd", joined, w_pairs, preferred_element_type=f32)
    grad_rows = grad_rows.astype(bf16).reshape(owners, slots, MODEL_WIDTH)
    grad_ffn = jnp.einsum("stj,sjd->std", onehot, grad_rows, preferred_element_type=f32)
    back = jnp.concatenate([grad_ffn.astype(bf16), grad_gate_back], axis=-1)
    back = lax.psum_scatter(
        back.reshape(owners * tokens, -1), "expert", scatter_dimension=0, tiled=True
    ).astype(f32)
    grad_ffn, grad_gate_dense = back[:, :MODEL_WIDTH], back[:, MODEL_WIDTH : MODEL_WIDTH + experts]
    combined = lax.psum_scatter(
        combined.astype(bf16).reshape(owners * tokens, -1),
        "expert",
        scatter_dimension=0,
        tiled=True,
    )
    block_out = (resid + combined.astype(f32)).astype(bf16)
    grad_gateup, grad_down = (
        lax.psum_scatter(
            grad_gateup.reshape(held, MODEL_WIDTH, hidden_units).astype(bf16),
            "fsdp",
            scatter_dimension=1,
            tiled=True,
        ).astype(f32),
        lax.psum_scatter(
            grad_down.reshape(held, half, MODEL_WIDTH).astype(bf16),
            "fsdp",
            scatter_dimension=1,
            tiled=True,
        ).astype(f32),
    )
    grad_input, grads = backward_local(
        state, chosen, cotangent, grad_ffn, grad_gate_dense, *weights_attn
    )
    widths = [g.shape[1] if g.ndim == 2 else 1 for g in grads]
    flat = jnp.concatenate([g if g.ndim == 2 else g[:, None] for g in grads], axis=1)
    share = lax.psum_scatter(flat.astype(bf16), "fsdp", scatter_dimension=0, tiled=True)
    total = lax.psum(share, "expert").astype(f32)
    pieces = jnp.split(total, [sum(widths[: i + 1]) for i in range(len(widths) - 1)], axis=1)
    pieces = [p if g.ndim == 2 else p[:, 0] for p, g in zip(pieces, grads)]
    return (block_out, grad_input, *pieces, grad_gateup, grad_down)


def kernel_local(
    hidden_in,
    doc_ids,
    routes,
    gain_attn,
    w_query,
    key_matrix,
    value_matrix,
    w_output,
    gain_ffn,
    w_router,
    w_gateup,
    w_down,
    cotangent,
):
    tokens = hidden_in.shape[0]
    experts = w_router.shape[1]
    shards = lax.axis_size("fsdp")
    owners = lax.axis_size("expert")
    held = w_gateup.shape[0]
    pairing = 2 if held % 2 == 0 else 1
    f32, bf16 = jnp.float32, jnp.bfloat16

    shares = (w_query, key_matrix, value_matrix, w_output, w_router.T)
    made, fulls, cot_all, left = attend(
        (shards, owners, tokens, experts), hidden_in, doc_ids, routes.T, gain_attn, gain_ffn, shares,
        cotangent,
    )
    h1, q, k, v, mixed, lse, resid, sent, probs = made
    sizes = (shards, owners, tokens, experts, held, pairing)
    back, comb, sums, far, away = moe(sizes, sent, cot_all, w_gateup, w_down)
    wq, wk, wv, wo, wr = fulls
    block_out, grad_input, total_o, total_q, total_k, total_v, total_r, far = reverse(
        (shards, owners, tokens, experts, held),
        (hidden_in, doc_ids, routes.T, gain_attn, gain_ffn, cotangent, q, k, v, mixed,
         lse, resid, sent, probs, back),
        (wo, wr, wq, wk, wv),
        comb,
        left,
        away,
        far,
    )
    out = finish(
        experts, sums, far, (total_q, total_k, total_v, total_o), total_r, block_out, grad_input
    )
    grad_gateup, grad_down, grad_q, grad_k, grad_v, grad_o, grad_r, ga, gf, block, gradient = out
    return (
        block,
        gradient,
        grad_q,
        grad_k,
        grad_v,
        grad_o,
        grad_r.T,
        ga,
        gf,
        grad_gateup,
        grad_down,
    )


def local(*args):
    owners, held = lax.axis_size("expert"), args[10].shape[0]
    groups = held // (2 if held % 2 == 0 else 1)
    if lax.axis_size("fsdp") == 4 and owners == 8 and owners * groups * CAP <= 2048:
        return kernel_local(*args)
    return plain_local(*args)


def solution(mesh):
    in_specs = (
        P(("fsdp", "expert"), None),
        P(("fsdp", "expert"), None),
        P(("fsdp", "expert"), None),
        P(),
        P("fsdp", None),
        P("fsdp", None),
        P("fsdp", None),
        P("fsdp", None),
        P(),
        P("fsdp", None),
        P("expert", None, None),
        P("expert", None, None),
        P(("fsdp", "expert"), None),
    )
    out_specs = (
        P(("fsdp", "expert"), None),
        P(("fsdp", "expert"), None),
        P("fsdp", None),
        P("fsdp", None),
        P("fsdp", None),
        P("fsdp", None),
        P("fsdp", None),
        P("fsdp"),
        P("fsdp"),
        P("expert", "fsdp", None),
        P("expert", "fsdp", None),
    )
    return jax.shard_map(local, mesh=mesh, in_specs=in_specs, out_specs=out_specs, check_vma=False)
```

```python
import functools
import math

import jax
import jax.numpy as jnp
from jax import lax
from jax.experimental import pallas as pl
from jax.experimental.pallas import tpu as pltpu
from jax.sharding import PartitionSpec as P

MODEL_WIDTH = 1536
QUERY_HEADS = 24
KEY_VALUE_HEADS = 8
HEAD_SIZE = 64
TOP = 8
CAP = 48


EPS = 1e-05
BASE = 10000.0
SCORE_SCALE = 0.015625
MASKED = -1e30


def rope_tables(doc_row):
    document_length = doc_row.shape[0]
    places = jnp.arange(document_length, dtype=jnp.int32)
    same_doc = doc_row[:, None] == doc_row[None, :]
    starts = jnp.min(jnp.where(same_doc, places[None, :], document_length), axis=1)
    position = (places - starts).astype(jnp.float32)
    half_width = HEAD_SIZE // 2
    inverse = jnp.exp(
        -math.log(BASE) * (2.0 * jnp.arange(half_width, dtype=jnp.float32) / HEAD_SIZE)
    )
    angle = position[:, None] * inverse[None, :]
    allowed = same_doc & (places[None, :] <= places[:, None])
    return (jnp.cos(angle), jnp.sin(angle), allowed)


def rotate(tensor, cosine_table, sine_table):
    half_width = HEAD_SIZE // 2
    first_half = tensor[..., :half_width]
    second = tensor[..., half_width:]
    cos_part = cosine_table[:, None, :]
    sin_part = sine_table[:, None, :]
    return jnp.concatenate(
        [first_half * cos_part - second * sin_part, second * cos_part + first_half * sin_part],
        axis=-1,
    )


def inverse_rotation(tensor, cosine_table, sine_table):
    half_width = HEAD_SIZE // 2
    first_half = tensor[..., :half_width]
    second = tensor[..., half_width:]
    cos_part = cosine_table[:, None, :]
    sin_part = sine_table[:, None, :]
    return jnp.concatenate(
        [first_half * cos_part + second * sin_part, second * cos_part - first_half * sin_part],
        axis=-1,
    )


def norm_forward(value_rows, gain):
    scale_inv = lax.rsqrt(jnp.mean(value_rows * value_rows, axis=-1, keepdims=True) + EPS)
    normed = value_rows * scale_inv
    return ((normed * gain).astype(jnp.bfloat16), normed, scale_inv)


def norm_backward(grad_out, normed, scale_inv, gain):
    grad_normed = grad_out * gain
    grad_gain = jnp.sum(grad_out * normed, axis=0)
    value_gradients = scale_inv * (
        grad_normed - normed * jnp.mean(grad_normed * normed, axis=-1, keepdims=True)
    )
    return (value_gradients, grad_gain)


def scores_of(query_rows, key_rows, allowed):
    document_length = query_rows.shape[0]
    group_rows = query_rows.reshape(
        document_length, KEY_VALUE_HEADS, QUERY_HEADS // KEY_VALUE_HEADS, HEAD_SIZE
    )
    scores = (
        jnp.einsum("qgrd,kgd->grqk", group_rows, key_rows, preferred_element_type=jnp.float32)
        * SCORE_SCALE
    )
    return jnp.where(allowed[None, None], scores, MASKED)


def forward_local(
    hidden_rows,
    doc_row,
    route_rows,
    gain_attn,
    w_query,
    key_matrix,
    value_matrix,
    w_output,
    gain_ffn,
    w_router,
):
    document_length = hidden_rows.shape[0]
    hidden_f = hidden_rows.astype(jnp.float32)
    attention_input, normed_attn, scale_attn = norm_forward(hidden_f, gain_attn)
    cosine_table, sine_table, allowed = rope_tables(doc_row)
    query_rows = jnp.dot(attention_input, w_query, preferred_element_type=jnp.float32).reshape(
        document_length, QUERY_HEADS, HEAD_SIZE
    )
    key_rows = jnp.dot(attention_input, key_matrix, preferred_element_type=jnp.float32).reshape(
        document_length, KEY_VALUE_HEADS, HEAD_SIZE
    )
    value_rows = (
        jnp.dot(attention_input, value_matrix, preferred_element_type=jnp.float32)
        .astype(jnp.bfloat16)
        .reshape(document_length, KEY_VALUE_HEADS, HEAD_SIZE)
    )
    query_rows = rotate(query_rows, cosine_table, sine_table).astype(jnp.bfloat16)
    key_rows = rotate(key_rows, cosine_table, sine_table).astype(jnp.bfloat16)
    scores = scores_of(query_rows, key_rows, allowed)
    top_score = jnp.max(scores, axis=-1, keepdims=True)
    log_total = top_score + jnp.log(jnp.sum(jnp.exp(scores - top_score), axis=-1, keepdims=True))
    weights = jnp.exp(scores - log_total).astype(jnp.bfloat16)
    attention_mixed = jnp.einsum(
        "grqk,kgd->qgrd", weights, value_rows, preferred_element_type=jnp.float32
    )
    attention_mixed = attention_mixed.reshape(document_length, QUERY_HEADS * HEAD_SIZE).astype(
        jnp.bfloat16
    )
    resid = hidden_f + jnp.dot(attention_mixed, w_output, preferred_element_type=jnp.float32)
    ffn_in, normed_ffn, scale_ffn = norm_forward(resid, gain_ffn)
    logits = jnp.dot(ffn_in, w_router, preferred_element_type=jnp.float32)
    probs = jax.nn.softmax(logits, axis=-1)
    picks = route_rows[:, :, None] == jnp.arange(probs.shape[1], dtype=jnp.int32)[None, None, :]
    gates = jnp.sum(jnp.where(picks, probs[:, None, :], 0.0), axis=-1)
    return (
        normed_attn,
        scale_attn,
        attention_input,
        cosine_table,
        sine_table,
        allowed,
        query_rows,
        key_rows,
        value_rows,
        attention_mixed,
        log_total,
        resid,
        ffn_in,
        normed_ffn,
        scale_ffn,
        probs,
        gates,
    )


def backward_local(
    state,
    route_rows,
    cot_rows,
    grad_ffn_in,
    grad_gates,
    gain_attn,
    w_query,
    key_matrix,
    value_matrix,
    w_output,
    gain_ffn,
    w_router,
):
    (
        normed_attn,
        scale_attn,
        attention_input,
        cosine_table,
        sine_table,
        allowed,
        query_rows,
        key_rows,
        value_rows,
        attention_mixed,
        log_total,
        resid,
        ffn_in,
        normed_ffn,
        scale_ffn,
        probs,
        gates,
    ) = state
    document_length = attention_input.shape[0]
    query_group = QUERY_HEADS // KEY_VALUE_HEADS
    grad_probs = jnp.where(route_rows, grad_gates, 0.0)
    grad_logits = (
        probs * (grad_probs - jnp.sum(probs * grad_probs, axis=-1, keepdims=True))
    ).astype(jnp.bfloat16)
    grad_router = jnp.dot(ffn_in.T, grad_logits, preferred_element_type=jnp.float32)
    grad_ffn_in = grad_ffn_in + jnp.dot(grad_logits, w_router.T, preferred_element_type=jnp.float32)
    grad_resid_part, grad_gain_ffn = norm_backward(grad_ffn_in, normed_ffn, scale_ffn, gain_ffn)
    grad_resid = cot_rows.astype(jnp.float32) + grad_resid_part
    grad_attn = grad_resid.astype(jnp.bfloat16)
    grad_output = jnp.dot(attention_mixed.T, grad_attn, preferred_element_type=jnp.float32)
    mixed_gradient = jnp.dot(grad_attn, w_output.T, preferred_element_type=jnp.float32).astype(
        jnp.bfloat16
    )
    scores = scores_of(query_rows, key_rows, allowed)
    weights = jnp.exp(scores - log_total)
    weights_low = weights.astype(jnp.bfloat16)
    gradient_by_group = mixed_gradient.reshape(
        document_length, KEY_VALUE_HEADS, query_group, HEAD_SIZE
    )
    mixed_by_group = attention_mixed.reshape(
        document_length, KEY_VALUE_HEADS, query_group, HEAD_SIZE
    )
    value_gradients = jnp.einsum(
        "grqk,qgrd->kgd", weights_low, gradient_by_group, preferred_element_type=jnp.float32
    )
    grad_weights = jnp.einsum(
        "qgrd,kgd->grqk", gradient_by_group, value_rows, preferred_element_type=jnp.float32
    )
    delta = jnp.transpose(
        jnp.sum(
            gradient_by_group.astype(jnp.float32) * mixed_by_group.astype(jnp.float32), axis=-1
        ),
        (1, 2, 0),
    )
    grad_scores = (weights * (grad_weights - delta[..., None]) * SCORE_SCALE).astype(jnp.bfloat16)
    query_by_group = query_rows.reshape(document_length, KEY_VALUE_HEADS, query_group, HEAD_SIZE)
    grad_query_rows = jnp.einsum(
        "grqk,kgd->qgrd", grad_scores, key_rows, preferred_element_type=jnp.float32
    ).reshape(document_length, QUERY_HEADS, HEAD_SIZE)
    key_row_gradient = jnp.einsum(
        "grqk,qgrd->kgd", grad_scores, query_by_group, preferred_element_type=jnp.float32
    )
    grad_query_rows = (
        inverse_rotation(grad_query_rows, cosine_table, sine_table)
        .reshape(document_length, QUERY_HEADS * HEAD_SIZE)
        .astype(jnp.bfloat16)
    )
    key_row_gradient = (
        inverse_rotation(key_row_gradient, cosine_table, sine_table)
        .reshape(document_length, KEY_VALUE_HEADS * HEAD_SIZE)
        .astype(jnp.bfloat16)
    )
    value_row_gradient = value_gradients.reshape(
        document_length, KEY_VALUE_HEADS * HEAD_SIZE
    ).astype(jnp.bfloat16)
    grad_query = jnp.dot(attention_input.T, grad_query_rows, preferred_element_type=jnp.float32)
    grad_key = jnp.dot(attention_input.T, key_row_gradient, preferred_element_type=jnp.float32)
    grad_value = jnp.dot(attention_input.T, value_row_gradient, preferred_element_type=jnp.float32)
    grad_attn_in = jnp.dot(grad_query_rows, w_query.T, preferred_element_type=jnp.float32)
    grad_attn_in = grad_attn_in + jnp.dot(
        key_row_gradient, key_matrix.T, preferred_element_type=jnp.float32
    )
    grad_attn_in = grad_attn_in + jnp.dot(
        value_row_gradient, value_matrix.T, preferred_element_type=jnp.float32
    )
    grad_hidden_part, grad_gain_attn = norm_backward(
        grad_attn_in, normed_attn, scale_attn, gain_attn
    )
    grad_in = grad_resid + grad_hidden_part
    return (
        grad_in,
        (grad_query, grad_key, grad_value, grad_output, grad_router, grad_gain_attn, grad_gain_ffn),
    )


MESH = pl.DeviceIdType.MESH
F32, BF16 = jnp.float32, jnp.bfloat16


def dot(a, b, da=1, db=0):
    return lax.dot_general(a, b, (((da,), (db,)), ((), ())), preferred_element_type=F32)


class Place:
    def __init__(self, shards, owners):
        self.shards, self.owners = shards, owners
        self.line = 4 if owners % 4 == 0 else 1
        self.side = owners // self.line
        self.chips = shards // 2
        self.f = lax.axis_index("fsdp")
        self.e = lax.axis_index("expert")
        self.a, self.b = self.e // self.side, self.e % self.side
        self.x, self.c = self.f // 2, self.f % 2

    def detour(self):
        end = self.line - 1
        got = jnp.where(self.a % 2 == 0, end, 0)
        return got, end - got, self.e + jnp.where(self.a % 2 == 0, self.side, -self.side)

    def others(self, all_fsdp):
        out = [((self.f, self.e + self.side), self.a < self.line - 1)]
        out.append(((self.f, self.e - self.side), self.a > 0))
        for i in range(1, self.side):
            out.append(((self.f, self.a * self.side + (self.b + i) % self.side), None))
        if all_fsdp:
            out += [(((self.f + i) % self.shards, self.e), None) for i in range(1, self.shards)]
            return out
        out.append(((self.x * 2 + 1 - self.c, self.e), None))
        for i in range(1, self.chips):
            out.append((((self.x + i) % self.chips * 2 + self.c, self.e), None))
        return out

    def meet(self, all_fsdp=False):
        bar = pltpu.get_barrier_semaphore()
        others = self.others(all_fsdp)
        for dev, cond in others:

            def signal(dev=dev):
                pl.semaphore_signal(bar, inc=1, device_id=dev, device_id_type=MESH)

            if cond is None:
                signal()
            else:
                pl.when(cond)(signal)
        pl.semaphore_wait(
            bar,
            len(others)
            - 2
            + jnp.where(self.a < self.line - 1, 1, 0)
            + jnp.where(self.a > 0, 1, 0),
        )


def remote(src, dst, send, recv, dev):
    return pltpu.make_async_remote_copy(
        src_ref=src, dst_ref=dst, send_sem=send, recv_sem=recv, device_id=dev, device_id_type=MESH
    )


class LineGather:
    def __init__(self, at, buf, send, recv, balance=False):
        self.at, self.buf, self.send, self.recv = at, buf, send, recv
        self.balance = balance
        width, count = buf.shape[2], recv.shape[0]
        cut = [width * p // count // 128 * 128 for p in range(count)] + [width]
        self.parts = [pl.ds(lo, hi - lo) for lo, hi in zip(cut, cut[1:])]

    def copy(self, k, p, way, dev):
        ref = self.buf.at[k, :, self.parts[p]]
        return remote(ref, ref, self.send.at[p, way, k], self.recv.at[p, k], (self.at.f, dev))

    def up(self, k, p):
        return self.copy(k, p, 0, self.at.e + self.at.side)

    def down(self, k, p):
        return self.copy(k, p, 1, self.at.e - self.at.side)

    def across(self, k, i, p):
        at = self.at
        return self.copy(k, p, 1 + i, at.a * at.side + (at.b + i) % at.side)

    def spread(self, k, p, up, down, across=True):
        at = self.at
        if up:

            @pl.when(at.a < at.line - 1)
            def _():
                self.up(k, p).start()

        if down:

            @pl.when(at.a > 0)
            def _():
                self.down(k, p).start()

        if across and (p < len(self.parts) - 1 or not self.balance):
            self.across(k, 1, p).start()
        elif across:
            pl.when(k // at.side != at.detour()[0])(lambda: self.across(k, 1, p).start())

    def detour(self):
        at = self.at
        k = at.detour()[1] * at.side + 1 - at.b
        return self.copy(k, len(self.parts) - 1, 3, at.detour()[2])

    def begin(self):
        for p in range(len(self.parts)):
            self.spread(self.at.e, p, True, True)

    def relay_step(self, s, across=True):
        at = self.at
        for p in range(len(self.parts)):

            @pl.when(at.a - s >= 0)
            def _(p=p):
                k = at.e - s * at.side
                self.down(k, p).wait_recv()
                self.spread(k, p, True, False, across)

            @pl.when(at.a + s < at.line)
            def _(p=p):
                k = at.e + s * at.side
                self.up(k, p).wait_recv()
                self.spread(k, p, False, True, across)

    def cross(self, n):
        at = self.at
        a = (
            jnp.where(at.a > 0, at.a - 1, at.a + 1),
            jnp.where(at.a == 0, 2, jnp.where(at.a == at.line - 1, at.a - 2, at.a + 1)),
            jnp.where(at.a < at.line // 2, at.line - 1, 0),
        )[n - 1]
        for p in range(len(self.parts)):
            self.spread(a * at.side + at.b, p, False, False)

    def relay(self):
        for s in range(1, self.at.line):
            self.relay_step(s)

    def each(self, use):
        at = self.at

        def near(s, carry):
            pl.when(s > 0)(lambda: self.relay_step(s))
            pl.when(at.a - s >= 0)(lambda: use(at.e - s * at.side))
            pl.when((s > 0) & (at.a + s < at.line))(lambda: use(at.e + s * at.side))
            return carry

        lax.fori_loop(0, at.line, near, 0)
        self.rest(use)

    def rest(self, use=None):
        at = self.at

        def take(n, carry):
            s, sign = n // 2, 1 - n % 2 * 2
            a = at.a + sign * s

            @pl.when((a >= 0) & (a < at.line) & (n != 1))
            def _():
                k = a * at.side + 1 - at.b
                for p in range(len(self.parts)):
                    self.across(k, 1, p).wait_recv()
                if self.balance:
                    pl.when(a == at.detour()[1])(lambda: self.detour().start())
                if use is not None:
                    use(k)

            return carry

        lax.fori_loop(0, 2 * at.line, take, 0)

    def finish(self):
        at = self.at
        for s in range(at.line):
            k = s * at.side + at.b
            for p in range(len(self.parts)):

                @pl.when((at.a < at.line - 1) & (at.a >= s))
                def _(k=k, p=p):
                    self.up(k, p).wait_send()

                @pl.when((at.a > 0) & (at.a <= s))
                def _(k=k, p=p):
                    self.down(k, p).wait_send()

                if p < len(self.parts) - 1 or not self.balance:
                    self.across(k, 1, p).wait_send()
                else:
                    pl.when(s != at.detour()[0])(
                        lambda k=k, p=p: self.across(k, 1, p).wait_send()
                    )
        if self.balance:
            self.detour().wait_send()


class LineScatter:
    def __init__(self, at, part, side_in, line_in, own, extra, sems, balance=False):
        self.balance = balance
        self.at, self.part, self.side_in, self.line_in, self.own = at, part, side_in, line_in, own
        self.extra = extra
        self.ssend, self.srecv, self.lsend, self.lrecv, self.esem = sems
        width = part.shape[2]
        self.cut = width // 256 * 128
        self.parts = (pl.ds(0, self.cut), pl.ds(self.cut, width - self.cut))

    def across(self, s, p):
        at = self.at
        return remote(
            self.part.at[s * at.side + 1 - at.b, :, self.parts[p]],
            self.side_in.at[s, :, self.parts[p]],
            self.ssend.at[s, p],
            self.srecv.at[s, p],
            (at.f, at.a * at.side + 1 - at.b),
        )

    def detour(self):
        at = self.at
        k = at.detour()[0] * at.side + 1 - at.b
        return remote(
            self.part.at[k, :, self.parts[1]], self.extra, self.esem.at[0], self.esem.at[1],
            (at.f, at.detour()[2]),
        )

    def join(self):
        at = self.at
        s = at.detour()[1]
        k = s * at.side + 1 - at.b
        self.detour().wait_recv()
        mine = self.part[k, :, self.cut :].astype(F32)
        self.part[k, :, self.cut :] = (mine + self.extra[...].astype(F32)).astype(BF16)
        self.across(s, 1).start()

    def along(self, s, dev, slot):
        at = self.at
        return remote(
            self.part.at[s * at.side + at.b],
            self.line_in.at[slot],
            self.lsend.at[s],
            self.lrecv.at[slot],
            (at.f, dev),
        )

    def up(self, s):
        return self.along(s, self.at.e + self.at.side, s)

    def down(self, s):
        at = self.at
        return self.along(s, at.e - at.side, jnp.where(s == at.a - 1, at.line, s))

    def place(self, i):
        at = self.at
        return jnp.where(at.a < at.line // 2, at.line - 1 - i, i)

    def middle(self):
        at = self.at
        return (at.a > 0) & (at.a < at.line - 1)

    def launch(self, make, lo, hi):
        at = self.at
        got, passed, _ = at.detour()

        def step(n, carry):
            s = self.place(n)
            make(s * at.side + 1 - at.b)
            self.across(s, 0).start()
            if self.balance:
                pl.when(s == got)(lambda: self.detour().start())
                pl.when((s != got) & (s != passed))(lambda: self.across(s, 1).start())
            else:
                self.across(s, 1).start()
            return carry

        lax.fori_loop(lo, hi, step, 0)

    def begin(self, make):
        self.launch(make, 0, 2)

    def more(self, make):
        at = self.at
        if self.balance:
            pl.when(self.middle())(self.join)
        self.launch(make, 2, at.line)

        def step(n, carry):
            make(n * at.side + at.b)
            return carry

        lax.fori_loop(0, at.line, step, 0)

    def sum_step(self, n):
        at = self.at
        if n == 1 and self.balance:
            pl.when(jnp.logical_not(self.middle()))(self.join)
        s = self.place(n)
        k = s * at.side + at.b
        got = at.detour()[0]
        self.own[...] = self.part[k].astype(F32)
        self.across(s, 0).wait_recv()
        self.own[:, : self.cut] += self.side_in[s, :, : self.cut].astype(F32)

        @pl.when((s != got) | (not self.balance))
        def _():
            self.across(s, 1).wait_recv()
            self.own[:, self.cut :] += self.side_in[s, :, self.cut :].astype(F32)

        @pl.when(((s > at.a) & (at.a > 0)) | ((s < at.a) & (at.a < at.line - 1)))
        def _():
            self.along(s, at.e, s).wait_recv()
            self.own[...] += self.line_in[s].astype(F32)

        self.part[k] = self.own[...].astype(BF16)

        @pl.when(s > at.a)
        def _():
            self.up(s).start()

        @pl.when(s < at.a)
        def _():
            self.down(s).start()

    def sum_last(self):
        at = self.at
        self.own[...] = self.part[at.e].astype(F32)

        @pl.when(at.a > 0)
        def _():
            self.along(at.a, at.e, at.a).wait_recv()
            self.own[...] += self.line_in[at.a].astype(F32)

        @pl.when(at.a < at.line - 1)
        def _():
            self.along(at.a, at.e, at.line).wait_recv()
            self.own[...] += self.line_in[at.line].astype(F32)

    def finish(self):
        at = self.at
        if self.balance:
            self.detour().wait_send()
        for s in range(at.line):
            self.across(s, 0).wait_send()
            pl.when((s != at.detour()[0]) | (not self.balance))(
                lambda s=s: self.across(s, 1).wait_send()
            )

            @pl.when(at.a < s)
            def _(s=s):
                self.up(s).wait_send()

            @pl.when(at.a > s)
            def _(s=s):
                self.down(s).wait_send()


def rope_of(allowed, tokens):
    lane = lax.broadcasted_iota(jnp.int32, (tokens, 128), 1)
    position = jnp.sum(allowed.astype(F32), axis=1, keepdims=True) - 1.0
    half = HEAD_SIZE // 2
    inverse = jnp.exp(-math.log(BASE) * (2.0 * (lane % half).astype(F32) / HEAD_SIZE))
    angle = position * inverse
    return jnp.cos(angle), jnp.sin(angle), lane % HEAD_SIZE < half


def turn(x, cos, sin, first):
    half = HEAD_SIZE // 2
    other = jnp.where(first, -pltpu.roll(x, 128 - half, 1), pltpu.roll(x, half, 1))
    return x * cos + other * sin


def visible(doc, tokens):
    row = lax.broadcasted_iota(jnp.int32, (tokens, tokens), 0)
    col = lax.broadcasted_iota(jnp.int32, (tokens, tokens), 1)
    key_doc = jnp.broadcast_to(doc.astype(F32), (tokens, tokens))
    own = jnp.sum(jnp.where(row == col, key_doc, 0.0), axis=1, keepdims=True)
    return (own == key_doc) & (col <= row)


def picked(routes, lane):
    ids = routes[...].astype(F32).T
    lane = lane.astype(F32)
    chosen = lane == ids[:, :1]
    for i in range(1, TOP):
        chosen = chosen | (lane == ids[:, i : i + 1])
    return chosen


def attend_kernel(sizes, hidden, doc, routes, gain_a, gain_f, *refs):
    shards, owners, tokens, experts = sizes
    shares, cot = refs[:5], refs[5]
    h1, q, k, v, mixed, lse, resid, sent, probs_out = refs[6:15]
    fulls, cot_out, left = refs[15:20], refs[20], refs[21]
    (bufs, cot_all, acc, lsem, xs, xr, ys, yr, ss, sr, cs, cr, ls, lr, own_left) = refs[22:]
    at = Place(shards, owners)
    rg = MODEL_WIDTH // shards
    half, quarter = rg // 2, rg // 4
    f = at.f
    sib = (at.x * 2 + 1 - at.c, at.e)
    over = ((at.x + 1) % at.chips * 2 + at.c, at.e)
    far = over[0]
    other = (at.x + 1) % at.chips * 2 + 1 - at.c
    mine = (at.a + at.b) % 2
    beside = (f, at.a * at.side + (at.b + 1) % at.side)
    step = jnp.where(at.a % 2 == 0, at.side, -at.side)
    along = (f, at.e + step)
    count = len(shares)

    own = [pltpu.make_async_copy(shares[n], bufs[n].at[f], lsem.at[n]) for n in range(count)]
    own.append(pltpu.make_async_copy(cot, cot_all.at[at.e], lsem.at[count]))
    for c in own:
        c.start()

    def piece(n, g, start, size, send, recv, dev):
        ref = bufs[n].at[g, pl.ds(pl.multiple_of(start, quarter), size)]
        return remote(ref, ref, send, recv, dev)

    def begins(i):
        return (mine * half, mine * half + quarter, (1 - mine) * half, (1 - mine) * half + quarter)[i]

    def out_x(n, i):
        start = pl.ds(pl.multiple_of(begins(i), quarter), quarter)
        return remote(
            shares[n].at[start], bufs[n].at[f, start], xs.at[n, i], xr.at[n, i], over
        )

    def in_x(n, i):
        return piece(n, far, begins(i), quarter, xs.at[n, i], xr.at[n, i], over)

    def out_yz(n, i):
        return piece(n, far, begins(i), quarter, ys.at[n, i], yr.at[n, i], (beside, along)[i])

    def in_yz(n, i):
        return piece(n, far, begins(2 + i), quarter, ys.at[n, i], yr.at[n, i], (beside, along)[i])

    def to_sib(n, i, g):
        return piece(n, g, begins(i), quarter, ss.at[n, i], sr.at[n, i], sib)

    def own_sib(n):
        return remote(shares[n], bufs[n].at[f], ss.at[n, 4], sr.at[n, 4], sib)

    def small_x():
        return remote(shares[4], bufs[4].at[f], xs.at[4, 0], xr.at[4, 0], over)

    def small_sib():
        return remote(bufs[4].at[far], bufs[4].at[far], ss.at[4, 0], sr.at[4, 0], sib)

    def pass_x(n, i):
        in_x(n, i).wait_recv()
        out_yz(n, i).start()
        to_sib(n, i, far).start()

    def pass_rest(n):
        for i in range(2):
            in_yz(n, i).wait_recv()
            to_sib(n, 2 + i, far).start()

    def from_sib(n):
        for i in range(4):
            to_sib(n, i, other).wait_recv()

    def lefts(n, i):
        g = (f + i) % shards
        return remote(
            (h1, mixed)[n].at[:, pl.ds(pl.multiple_of(g * rg, 128), rg)],
            left.at[pl.ds(f * tokens, tokens), pl.ds(n * rg, rg)],
            ls.at[n, i - 1], lr.at[n, i - 1], (g, at.e),
        )

    def left_own(n):
        return pltpu.make_async_copy(
            (h1, mixed)[n].at[:, pl.ds(pl.multiple_of(f * rg, 128), rg)],
            left.at[pl.ds(f * tokens, tokens), pl.ds(n * rg, rg)],
            own_left.at[n],
        )

    def send_left(n):
        left_own(n).start()
        for i in range(1, shards):
            lefts(n, i).start()

    at.meet(all_fsdp=True)
    order = (0, 1, 2, 3)
    for n in order[:3]:
        for i in range(2):
            out_x(n, i).start()
        own_sib(n).start()
    small_x().start()
    own_sib(4).start()
    for i in range(2):
        out_x(3, i).start()
    own_sib(3).start()
    cotg = LineGather(at, cot_all, cs, cr)
    own[count].wait()
    cotg.begin()

    x = hidden[...].astype(F32)
    scale = lax.rsqrt(jnp.mean(x * x, axis=1, keepdims=True) + EPS)
    h1[...] = (x * scale * gain_a[...].reshape(1, -1)).astype(BF16)
    allowed = visible(doc[...], tokens)
    cos, sin, first = rope_of(allowed, tokens)

    ends = (0, 1536, 2048, 2560)

    def project(g):
        part = h1[:, pl.ds(pl.multiple_of(g * rg, 128), rg)]
        return [dot(part, bufs[n][g]) for n in range(3)]

    for n in range(3):
        own[n].wait()
        acc[:, ends[n] : ends[n + 1]] = dot(
            h1[:, pl.ds(pl.multiple_of(f * rg, 128), rg)], bufs[n][f]
        )

    def add(g):
        for n, got in enumerate(project(g)):
            acc[:, ends[n] : ends[n + 1]] += got

    for n in range(3):
        own_sib(n).wait_recv()
    add(sib[0])
    pass_x(0, 0)
    cotg.relay_step(1, False)
    cotg.cross(1)
    pass_x(0, 1)
    cotg.relay_step(2, False)
    for n in (1, 2):
        for i in range(2):
            pass_x(n, i)
    cotg.cross(2)
    for n in range(3):
        pass_rest(n)
    pass_x(3, 0)
    cotg.relay_step(3, False)
    cotg.cross(3)
    add(far)
    for n in range(3):
        from_sib(n)
    add(other)
    small_x().wait_recv()
    small_sib().start()
    pass_x(3, 1)
    save = [pltpu.make_async_copy(bufs[n], fulls[n], lsem.at[n]) for n in range(count)]
    for c in save[:3]:
        c.start()

    for j in range(16):
        cols = slice(128 * j, 128 * (j + 1))
        got = turn(acc[:, cols], cos, sin, first).astype(BF16)
        if j < 12:
            q[:, cols] = got
        else:
            k[:, 128 * (j - 12) : 128 * (j - 11)] = got
    v[...] = acc[:, 2048:].astype(BF16)
    ratio = QUERY_HEADS // KEY_VALUE_HEADS
    mask = jnp.concatenate([allowed] * ratio, axis=0)

    def head(ref, h):
        return ref[:, h * HEAD_SIZE : (h + 1) * HEAD_SIZE]

    for g in range(KEY_VALUE_HEADS):
        heads = range(g * ratio, (g + 1) * ratio)
        rows = jnp.concatenate([head(q, h) for h in heads], axis=0)
        s = jnp.where(mask, dot(rows, head(k, g), 1, 1) * SCORE_SCALE, MASKED)
        top = jnp.max(s, axis=1, keepdims=True)
        e = jnp.exp(s - top)
        total = jnp.sum(e, axis=1, keepdims=True)
        o = dot((e / total).astype(BF16), head(v, g)).astype(BF16)
        log_total = top + jnp.log(total)
        for i, h in enumerate(heads):
            mixed[:, h * HEAD_SIZE : (h + 1) * HEAD_SIZE] = o[i * tokens : (i + 1) * tokens]
            lse[:, h : h + 1] = log_total[i * tokens : (i + 1) * tokens]

    send_left(0)
    send_left(1)

    def output(g):
        return dot(mixed[:, pl.ds(pl.multiple_of(g * rg, 128), rg)], bufs[3][g])

    for n in (3, 4):
        own[n].wait()
        own_sib(n).wait_recv()
    resid[...] = x + output(f) + output(sib[0])
    pass_rest(3)
    resid[...] += output(far)
    small_sib().wait_recv()
    from_sib(3)
    total = resid[...] + output(other)
    resid[...] = total
    scale = lax.rsqrt(jnp.mean(total * total, axis=1, keepdims=True) + EPS)
    h2 = (total * scale * gain_f[...].reshape(1, -1)).astype(BF16)
    sent[:, :MODEL_WIDTH] = h2
    logits = dot(h2[:, :rg], bufs[4][0], 1, 1)
    for g in range(1, shards):
        logits = logits + dot(h2[:, g * rg : (g + 1) * rg], bufs[4][g], 1, 1)
    logits = jnp.concatenate([logits, jnp.zeros((tokens, 128 - experts), F32)], axis=1)
    lane = lax.broadcasted_iota(jnp.int32, (tokens, 128), 1)
    live = lane < experts
    logits = jnp.where(live, logits, MASKED)
    e = jnp.where(live, jnp.exp(logits - jnp.max(logits, axis=1, keepdims=True)), 0.0)
    probs = e / jnp.sum(e, axis=1, keepdims=True)
    probs_out[...] = probs
    chosen = picked(routes, lane)
    row = lax.broadcasted_iota(jnp.int32, (tokens, tokens), 0)
    col = lax.broadcasted_iota(jnp.int32, (tokens, tokens), 1)
    below = jnp.where(row > col, 1.0, 0.0).astype(BF16)
    hits = jnp.where(chosen, 1.0, 0.0)
    rank = jnp.where(chosen, dot(below, hits.astype(BF16)), jnp.where(live, -1.0, 0.0))
    gate = jnp.where(chosen, probs, 0.0)
    high = gate.astype(BF16).astype(F32)
    low = gate - high
    meta = rank + pltpu.roll(high, experts, 1) + pltpu.roll(low, 2 * experts, 1)
    sent[:, MODEL_WIDTH:] = meta.astype(BF16)

    for c in save[3:]:
        c.start()
    cotg.rest()
    cotg.finish()
    keep = pltpu.make_async_copy(cot_all, cot_out, lsem.at[count])
    keep.start()
    for n in range(count):
        own_sib(n).wait_send()
    small_x().wait_send()
    small_sib().wait_send()
    for n in order:
        for i in range(2):
            out_x(n, i).wait_send()
            out_yz(n, i).wait_send()
        for i in range(4):
            to_sib(n, i, far).wait_send()
    for n in range(2):
        left_own(n).wait()
        for i in range(1, shards):
            lefts(n, i).wait()
    for c in save:
        c.wait()
    keep.wait()


def attend(sizes, hidden, doc, routes, gain_a, gain_f, shares, cot):
    shards, owners, tokens, experts = sizes
    rg = MODEL_WIDTH // shards
    side = owners // 4
    vm, dma = pltpu.VMEM, pltpu.SemaphoreType.DMA
    vmem, any_ = pl.BlockSpec(memory_space=pltpu.VMEM), pl.BlockSpec(memory_space=pl.ANY)
    n = len(shares)

    def shape(*dims, dtype=BF16):
        return jax.ShapeDtypeStruct(dims, dtype)

    outs = pl.pallas_call(
        functools.partial(attend_kernel, sizes),
        name="attend",
        out_shape=(
            shape(tokens, MODEL_WIDTH),
            shape(tokens, MODEL_WIDTH),
            shape(tokens, KEY_VALUE_HEADS * HEAD_SIZE),
            shape(tokens, KEY_VALUE_HEADS * HEAD_SIZE),
            shape(tokens, MODEL_WIDTH),
            shape(tokens, 128, dtype=F32),
            shape(tokens, MODEL_WIDTH, dtype=F32),
            shape(tokens, MODEL_WIDTH + 128),
            shape(tokens, 128, dtype=F32),
            *[shape(shards, *s.shape) for s in shares],
            shape(owners, tokens, MODEL_WIDTH),
            shape(shards * tokens, 2 * rg),
        ),
        in_specs=[vmem] * 5 + [any_] * (n + 1),
        out_specs=[vmem] * 9 + [any_] * (n + 2),
        scratch_shapes=[
            tuple(vm((shards, *s.shape), BF16) for s in shares),
            vm((owners, tokens, MODEL_WIDTH), BF16),
            vm((tokens, 2560), F32),
            dma((n + 1,)),
            dma((n, 2)),
            dma((n, 2)),
            dma((n, 2)),
            dma((n, 2)),
            dma((n, 5)),
            dma((n, 5)),
            dma((2, side + 2, owners)),
            dma((2, owners)),
            dma((2, shards - 1)),
            dma((2, shards - 1)),
            dma((2,)),
        ],
        compiler_params=pltpu.CompilerParams(
            collective_id=0, has_side_effects=True, vmem_limit_bytes=60 * 2**20
        ),
    )(hidden, doc, routes, gain_a, gain_f, *shares, cot)
    return outs[:9], outs[9 : 9 + n], outs[9 + n], outs[10 + n]


EARLY = 4
AHEAD = 3


def moe_kernel(sizes, sent, cot, wgu, wd, back_out, comb_out, sums, far, away, *scratch):
    shards, owners, tokens, experts, held, pairing = sizes
    (rows_all, cot_buf, taken, cots, made, grads, slot_gate, slot_grad, place, wg_buf, wd_buf,
     acts, dus, gg, gd, turned, from_core, stage, side1, line1, extra1,
     rs, rr, wsem, csem, coresend, corerecv, farsend, farrecv, osem, free, s1, s2, s3, s4, s5,
     ) = scratch
    at = Place(shards, owners)
    groups = held // pairing
    slots = groups * CAP
    half = wd.shape[1]
    rg, rd = MODEL_WIDTH // shards, half // shards
    sibling = (at.x * 2 + 1 - at.c, at.e)

    def weights(g):
        out = []
        for m in range(pairing):
            h, slot = g * pairing + m, g % 2 * pairing + m
            out.append(pltpu.make_async_copy(wgu.at[h], wg_buf.at[slot], wsem.at[0, slot]))
            out.append(pltpu.make_async_copy(wd.at[h], wd_buf.at[slot], wsem.at[1, slot]))
        return out

    mine = pltpu.make_async_copy(sent, rows_all.at[at.e], osem.at[0, 0])
    mine.start()
    for c in weights(0):
        c.start()
    at.meet()
    rows = LineGather(at, rows_all, rs, rr)
    mine.wait()
    rows.begin()

    lane = lax.broadcasted_iota(jnp.int32, (128, slots), 1)
    row = lax.broadcasted_iota(jnp.int32, (128, slots), 0)

    def expert_of(j):
        return (at.e * held + j // CAP * pairing) // 2

    e_lane = expert_of(lane)
    find_rank = (row == e_lane).astype(F32).astype(BF16)
    slot_rank = (lane % CAP).astype(F32)
    e_row = expert_of(lax.broadcasted_iota(jnp.int32, (slots, 128), 0))
    col = lax.broadcasted_iota(jnp.int32, (slots, 128), 1)
    pick_gate = (col == e_row + experts) | (col == e_row + 2 * experts)

    def dispatch(k):
        rank_at = dot(rows_all[k, :, MODEL_WIDTH:], find_rank)
        pt = jnp.where(rank_at == slot_rank, 1.0, 0.0).astype(BF16)
        place[k] = pt
        got = dot(pt, rows_all[k], 0, 0)
        gate = jnp.sum(jnp.where(pick_gate, got[:, MODEL_WIDTH:], 0.0), axis=1, keepdims=True)
        gate = jnp.broadcast_to(gate, (slots, 128))
        to = pl.ds(k * CAP, CAP)
        for g in range(groups):
            taken[g, to, :] = got[g * CAP : (g + 1) * CAP, :MODEL_WIDTH].astype(BF16)
            slot_gate[g, to, :] = gate[g * CAP : (g + 1) * CAP]

    def dispatch_both(k):
        pull = pltpu.make_async_copy(cot.at[k], cot_buf.at[0], csem.at[0])
        pull.start()
        dispatch(k)
        pull.wait()
        got = dot(place[k], cot_buf[0], 0, 0).astype(BF16)
        to = pl.ds(k * CAP, CAP)
        for g in range(groups):
            cots[g, to, :] = got[g * CAP : (g + 1) * CAP]

    rows.each(dispatch_both)
    rows.finish()

    def through(g):
        for c in weights(g):
            c.wait()

        @pl.when(g + 1 < groups)
        def _():
            for c in weights(g + 1):
                c.start()

        gate = slot_gate[g][:, :1]
        total = jnp.zeros((owners * CAP, 1), F32)
        for m in range(pairing):
            h, slot = g * pairing + m, g % 2 * pairing + m
            gu = dot(taken[g], wg_buf[slot])
            a, b = gu[:, :half], gu[:, half:]
            sig = 1.0 / (1.0 + jnp.exp(-a))
            s = a * sig
            act = s * b
            acts[h] = (act * gate).astype(BF16)
            dp = dot(cots[g], wd_buf[slot], 1, 1)
            total = total + jnp.sum(act * dp, axis=1, keepdims=True)
            dact = dp * gate
            dus[h, :, :half] = (dact * b * sig * (1.0 + a * (1.0 - sig))).astype(BF16)
            dus[h, :, half:] = (dact * s).astype(BF16)
        slot_grad[g] = jnp.broadcast_to(total, (owners * CAP, 128))
        n = MODEL_WIDTH // 3
        for i in range(3):
            cols = slice(i * n, (i + 1) * n)
            y = 0.0
            dx = 0.0
            for m in range(pairing):
                h, slot = g * pairing + m, g % 2 * pairing + m
                y = y + dot(acts[h], wd_buf[slot, :, cols])
                dx = dx + dot(dus[h], wg_buf[slot, cols, :], 1, 1)
            made[g, :, cols] = y.astype(BF16)
            grads[g, :, cols] = dx.astype(BF16)

    def to_core(h):
        slot = h % 2
        out = []
        for i in range(at.chips):
            f = 2 * i + 1 - at.c
            for n, (buf, r) in enumerate(((gg, rg), (gd, rd))):
                out.append(
                    remote(
                        buf.at[slot, pl.ds(pl.multiple_of(f * r, r), r)],
                        from_core[n].at[slot, i],
                        coresend.at[slot, n, i],
                        corerecv.at[slot, n, i],
                        sibling,
                    )
                )
        return out

    def to_chips(h):
        return chip_copies(at, h, away, h, far, farsend, farrecv)

    def keep(h):
        slot = h % 2
        out = []
        for n in range(2):
            out.append(pltpu.make_async_copy(stage[n].at[slot, 0], sums[n].at[h], osem.at[n, slot]))
            for i in range(1, at.chips):
                out.append(
                    pltpu.make_async_copy(
                        stage[n].at[slot, i], away[n].at[h, i - 1], osem.at[2 * i + n, slot]
                    )
                )
        return out

    def add(h):
        slot = h % 2
        for c in to_core(h):
            c.wait()

        for i in range(at.chips):
            x = (at.x + i) % at.chips
            f = 2 * x + at.c
            for n, (buf, r) in enumerate(((gg, rg), (gd, rd))):
                own = buf[slot, pl.ds(pl.multiple_of(f * r, r), r)]
                stage[n][slot, i] = own + from_core[n][slot, x]
        for c in keep(h):
            c.start()

        @pl.when(h < held - 2)
        def _():
            pl.semaphore_signal(free, inc=1, device_id=sibling, device_id_type=MESH)

    def leave(h):
        for c in keep(h):
            c.wait()

        @pl.when(h < EARLY)
        def _():
            for c in to_chips(h):
                c.start()

        @pl.when(h == EARLY)
        def _():
            for c in to_chips(h)[0::2]:
                c.start()

    def weigh(h):
        g, slot = h // pairing, h % 2
        n = MODEL_WIDTH // 3

        @pl.when(h % pairing == 0)
        def _():
            turned[...] = taken[g].T

        for i in range(3):
            gg[slot, i * n : (i + 1) * n, :] = dot(
                turned[i * n : (i + 1) * n], dus[h]
            ).astype(BF16)
        gd[slot] = dot(acts[h], cots[g], 0, 0).astype(BF16)

        @pl.when(h >= 2)
        def _():
            pl.semaphore_wait(free, 1)

        for c in to_core(h):
            c.start()

    home = (col == e_row).astype(F32).astype(BF16)
    home_low = (col == e_row + experts).astype(F32).astype(BF16)
    parts = ((0, 512), (512, 1024), (1024, 1536))

    def make_back(k):
        to = pl.ds(k * CAP, CAP)
        dg = jnp.concatenate([slot_grad[g, to, :] for g in range(groups)], axis=0)
        high = dg.astype(BF16)
        low = (dg - high.astype(F32)).astype(BF16)
        pt = place[k]
        for lo, hi in parts:
            dx = jnp.concatenate([grads[g, to, lo:hi] for g in range(groups)], axis=0)
            rows_all[k, :, lo:hi] = dot(pt, dx).astype(BF16)
        rows_all[k, :, MODEL_WIDTH:] = dot(pt, high * home + low * home_low).astype(BF16)

    back = LineScatter(at, rows_all, side1, line1, back_out, extra1, (s1, s2, s3, s4, s5), True)

    def step(i, carry):
        @pl.when((i >= 2) & (i < AHEAD + 2))
        def _():
            leave(i - 2)

        @pl.when(i < groups)
        def _():
            through(i)

        @pl.when(i == groups)
        def _():
            back.begin(make_back)
            back.more(make_back)

        def staged(back, act):
            h = jnp.where(i < groups, i, i - gap) - back
            early = (i >= back) & (i < AHEAD + back) & (back < 2)
            pl.when(early | (i >= groups + back))(lambda: act(h))

        staged(2, leave)
        staged(0, weigh)
        staged(1, add)

        for n in range(2):

            @pl.when(i == groups + 3 + 3 * n)
            def _(n=n):
                back.sum_step(n)

        return carry

    gap = groups - AHEAD
    lax.fori_loop(0, held + gap, step, 0)
    back.sum_step(2)

    def combine(k, carry):
        to = pl.ds(k * CAP, CAP)
        slot = k % 2

        def put(j):
            return pltpu.make_async_copy(cot_buf.at[j % 2], comb_out.at[j], csem.at[j % 2])

        @pl.when(k >= 2)
        def _():
            put(k - 2).wait()

        for lo, hi in parts:
            y = jnp.concatenate([made[g, to, lo:hi] for g in range(groups)], axis=0)
            cot_buf[slot, :, lo:hi] = dot(place[k], y).astype(BF16)
        put(k).start()

        @pl.when(k == owners - 1)
        def _():
            put(k - 1).wait()
            put(k).wait()

        return carry

    back.sum_step(3)
    leave(held - 2)
    add(held - 1)
    lax.fori_loop(0, owners, combine, 0)
    leave(held - 1)
    back.sum_last()
    back.finish()

    def drain(h, carry):
        for c in to_chips(h):
            c.wait()
        return carry

    lax.fori_loop(0, EARLY, drain, 0)
    for c in to_chips(EARLY)[0::2]:
        c.wait()


def chip_copies(at, h, away, j, far, send, recv):
    out = []
    for i in range(1, at.chips):
        back = at.chips - 1 - i
        dev = ((at.x + i) % at.chips * 2 + at.c, at.e)
        for n in range(2):
            out.append(
                remote(
                    away[n].at[h, i - 1], far[n].at[back, h], send.at[n, i - 1, j],
                    recv.at[n, back, j], dev,
                )
            )
    return out


def moe(sizes, sent, cot, wgu, wd):
    shards, owners, tokens, experts, held, pairing = sizes
    groups = held // pairing
    slots, rows = groups * CAP, owners * CAP
    hidden, half = wgu.shape[2], wd.shape[1]
    rg, rd = MODEL_WIDTH // shards, half // shards
    chips = shards // 2
    line = 4
    side = owners // line
    width = MODEL_WIDTH + 128
    vm, dma = pltpu.VMEM, pltpu.SemaphoreType.DMA
    any_, vmem = pl.BlockSpec(memory_space=pl.ANY), pl.BlockSpec(memory_space=pltpu.VMEM)

    def pair(lead):
        return (vm((*lead, rg, hidden), BF16), vm((*lead, rd, MODEL_WIDTH), BF16))

    def outs(lead):
        return (
            jax.ShapeDtypeStruct((*lead, rg, hidden), BF16),
            jax.ShapeDtypeStruct((*lead, rd, MODEL_WIDTH), BF16),
        )

    return pl.pallas_call(
        functools.partial(moe_kernel, sizes),
        name="moe",
        out_shape=(
            jax.ShapeDtypeStruct((tokens, width), F32),
            jax.ShapeDtypeStruct((owners, tokens, MODEL_WIDTH), BF16),
            outs((held,)),
            outs((chips - 1, held)),
            outs((held, chips - 1)),
        ),
        in_specs=[any_] * 4,
        out_specs=(vmem, any_, (any_, any_), (any_, any_), (any_, any_)),
        scratch_shapes=[
            vm((owners, tokens, width), BF16),
            vm((2, tokens, MODEL_WIDTH), BF16),
            vm((groups, rows, MODEL_WIDTH), BF16),
            vm((groups, rows, MODEL_WIDTH), BF16),
            vm((groups, rows, MODEL_WIDTH), BF16),
            vm((groups, rows, MODEL_WIDTH), BF16),
            vm((groups, rows, 128), F32),
            vm((groups, rows, 128), F32),
            vm((owners, tokens, slots), BF16),
            vm((2 * pairing, MODEL_WIDTH, hidden), BF16),
            vm((2 * pairing, half, MODEL_WIDTH), BF16),
            vm((held, rows, half), BF16),
            vm((held, rows, hidden), BF16),
            vm((2, MODEL_WIDTH, hidden), BF16),
            vm((2, half, MODEL_WIDTH), BF16),
            vm((MODEL_WIDTH, rows), BF16),
            pair((2, chips)),
            pair((2, chips)),
            vm((line, tokens, width), BF16),
            vm((line + 1, tokens, width), BF16),
            vm((tokens, width - width // 256 * 128), BF16),
            dma((2, side + 2, owners)),
            dma((2, owners)),
            dma((2, 2 * pairing)),
            dma((2,)),
            dma((2, 2, chips)),
            dma((2, 2, chips)),
            dma((2, chips - 1, EARLY + 1)),
            dma((2, chips - 1, EARLY + 1)),
            dma((2 * chips, 2)),
            pltpu.SemaphoreType.REGULAR,
            dma((line, 2)),
            dma((line, 2)),
            dma((line,)),
            dma((line + 1,)),
            dma((2,)),
        ],
        compiler_params=pltpu.CompilerParams(
            collective_id=1, has_side_effects=True, vmem_limit_bytes=63 * 2**20
        ),
    )(sent, cot, wgu, wd)


def reverse_kernel(sizes, hidden, doc, routes, gain_a, gain_f, cot, q, k, v, mixed, lse, resid, sent,
                   probs, back, wo, wr, wq, wk, wv, comb, left_in, away0, away1, far0, far1, *refs):
    shards, owners, tokens, experts, held = sizes
    block_out, grad_in, out_o, out_q, out_k, out_v, out_r, far = refs[:8]
    (w_bufs, left, turned, rights, dgrad, dattn_f, dqkv, aux, aux_in, comb_part, comb_side, comb_line,
     comb_own, comb_x, part_o, side_o, line_o, own_o, extra_o, part_q, side_q, line_q, own_q, extra_q,
     total_o, total_q, wsem, rsend, rrecv, asend, arecv, farsend, farrecv, *sems) = refs[8:]
    at = Place(shards, owners)
    away = (away0, away1)
    rg = MODEL_WIDTH // shards
    piece = rg // owners
    split = dqkv.shape[1]
    f = at.f
    sibling = (at.x * 2 + 1 - at.c, at.e)
    over = ((at.x + 1) % at.chips * 2 + at.c, at.e)
    ratio = QUERY_HEADS // KEY_VALUE_HEADS

    fulls = (wo, wr, wq, wk, wv)
    loads = [pltpu.make_async_copy(comb, comb_part, wsem.at[0])]
    loads += [pltpu.make_async_copy(w, b, wsem.at[1 + i]) for i, (w, b) in enumerate(zip(fulls, w_bufs))]
    loads.append(pltpu.make_async_copy(left_in, left, wsem.at[6]))
    for c in loads:
        c.start()
    at.meet(all_fsdp=True)

    combine = LineScatter(at, comb_part, comb_side, comb_line, comb_own, comb_x, sems[:5], True)
    outer = LineScatter(at, part_o, side_o, line_o, own_o, extra_o, sems[5:10], True)
    inner = LineScatter(at, part_q, side_q, line_q, own_q, extra_q, sems[10:15], True)
    outer_all = LineGather(at, total_o, sems[15], sems[16])
    inner_all = LineGather(at, total_q, sems[17], sems[18])
    loads[0].wait()
    nothing = lambda k: None
    combine.begin(nothing)

    def rows(i):
        return pl.ds(pl.multiple_of(i * tokens, tokens), tokens)

    def block(chunk, g, send, dev):
        cols = (pl.ds(split, MODEL_WIDTH), pl.ds(0, split))[chunk]
        ref = rights.at[rows(g), cols]
        return remote(ref, ref, rsend.at[chunk, send], rrecv.at[chunk, g], dev)

    def send_rights(chunk):
        block(chunk, f, 0, sibling).start()
        block(chunk, f, 1, over).start()

    def pass_rights(chunk):
        block(chunk, over[0], 0, sibling).wait_recv()
        block(chunk, over[0], 2, sibling).start()

    def take_rights(chunk):
        block(chunk, sibling[0], 0, sibling).wait_recv()
        block(chunk, (at.x + 1) % at.chips * 2 + 1 - at.c, 0, sibling).wait_recv()

    def late(h):
        return chip_copies(at, h, away, h - EARLY, far, farsend, farrecv)

    h2 = sent[:, :MODEL_WIDTH]
    lane = lax.broadcasted_iota(jnp.int32, (tokens, 128), 1)
    chosen = picked(routes, lane)
    meta = back[:, MODEL_WIDTH:]
    dprobs = jnp.where(chosen, meta + pltpu.roll(meta, 128 - experts, 1), 0.0)
    p = probs[...]
    dlogits = (p * (dprobs - jnp.sum(p * dprobs, axis=1, keepdims=True))).astype(BF16)
    loads[1].wait()
    loads[2].wait()
    aux[...] = dot(dlogits, h2, 0, 0)[: aux.shape[0]]

    def full(i):
        return w_bufs[i][...].reshape(MODEL_WIDTH, -1)

    dh = back[:, :MODEL_WIDTH] + jnp.concatenate(
        [dot(dlogits[:, :experts], w_bufs[1][g]) for g in range(shards)], axis=1
    )
    x = resid[...]
    scale = lax.rsqrt(jnp.mean(x * x, axis=1, keepdims=True) + EPS)
    n = x * scale
    aux[experts + 1 : experts + 2, :] = jnp.sum(dh * n, axis=0, keepdims=True)
    dn = dh * gain_f[...].reshape(1, -1)
    dres = cot[...].astype(F32) + scale * (dn - n * jnp.mean(dn * n, axis=1, keepdims=True))
    dgrad[...] = dres
    dattn = dres.astype(BF16)
    rights[rows(f), split:] = dattn
    send_rights(0)
    for c in late(EARLY)[1::2]:
        c.start()
    dattn_f[...] = dot(dattn, full(0), 1, 1).astype(BF16)
    combine.more(nothing)

    allowed = visible(doc[...], tokens)
    cos, sin, first = rope_of(allowed, tokens)
    mask = jnp.concatenate([allowed] * ratio, axis=0)

    def stack(ref, heads):
        return jnp.concatenate(
            [ref[:, h * HEAD_SIZE : (h + 1) * HEAD_SIZE] for h in heads], axis=0
        )

    kept = QUERY_HEADS * HEAD_SIZE
    span = KEY_VALUE_HEADS * HEAD_SIZE
    for g in range(KEY_VALUE_HEADS):
        heads = range(g * ratio, (g + 1) * ratio)
        one = slice(g * HEAD_SIZE, (g + 1) * HEAD_SIZE)
        qs, ks, vs = stack(q, heads), k[:, one], v[:, one]
        dos, os = stack(dattn_f, heads), stack(mixed, heads)
        logs = jnp.concatenate([lse[:, h : h + 1] for h in heads], axis=0)
        s = jnp.where(mask, dot(qs, ks, 1, 1) * SCORE_SCALE, MASKED)
        w = jnp.exp(s - logs)
        low = w.astype(BF16)
        delta = jnp.sum(dos.astype(F32) * os.astype(F32), axis=1, keepdims=True)
        ds = (w * (dot(dos, vs, 1, 1) - delta) * SCORE_SCALE).astype(BF16)
        dq = dot(ds, ks)
        for i, h in enumerate(heads):
            dqkv[:, h * HEAD_SIZE : (h + 1) * HEAD_SIZE] = dq[i * tokens : (i + 1) * tokens]
        dqkv[:, kept + g * HEAD_SIZE : kept + (g + 1) * HEAD_SIZE] = dot(ds, qs, 0, 0)
        at_v = kept + span + g * HEAD_SIZE
        dqkv[:, at_v : at_v + HEAD_SIZE] = dot(low, dos, 0, 0)
        if g == 3:
            combine.sum_step(0)

    for j in range((kept + span) // 128):
        cols = slice(128 * j, 128 * (j + 1))
        rights[rows(f), cols] = turn(dqkv[:, cols], cos, -sin, first).astype(BF16)
    rights[rows(f), kept + span : split] = dqkv[:, kept + span :].astype(BF16)
    send_rights(1)
    pass_rights(0)
    loads[6].wait()
    turned[...] = left[...].T
    take_rights(0)
    step = 512

    def product(part, half, lo, hi):
        for a in range(lo, hi, step):
            got = dot(turned[half * rg : (half + 1) * rg], rights[:, a : a + step]).astype(BF16)
            for i in range(owners):
                part[i, :, a - lo : a - lo + step] = got[i * piece : (i + 1) * piece]

    product(part_o, 1, split, split + MODEL_WIDTH)
    outer.begin(nothing)
    combine.sum_step(1)
    for i in range(3, 6):
        loads[i].wait()
    mine = rights[rows(f), :split]
    dh = dot(mine[:, :kept], full(2), 1, 1)
    dh = dh + dot(mine[:, kept : kept + span], full(3), 1, 1)
    dh = dh + dot(mine[:, kept + span :], full(4), 1, 1)
    x = hidden[...].astype(F32)
    scale = lax.rsqrt(jnp.mean(x * x, axis=1, keepdims=True) + EPS)
    n = x * scale
    aux[experts : experts + 1, :] = jnp.sum(dh * n, axis=0, keepdims=True)
    dn = dh * gain_a[...].reshape(1, -1)
    grad_in[...] = dgrad[...] + scale * (dn - n * jnp.mean(dn * n, axis=1, keepdims=True))

    def cols(g):
        return pl.ds(pl.multiple_of(g * rg, 128), rg)

    def auxes(i):
        g = (f + i) % shards
        return remote(
            aux.at[:, cols(g)], aux_in.at[i], asend.at[i - 1], arecv.at[i - 1], (g, at.e)
        )

    for i in range(1, shards):
        auxes(i).start()
    for h in range(EARLY + 1, held):
        for c in late(h):
            c.start()
    aux_in[0] = aux[:, cols(f)]

    outer.more(nothing)
    combine.sum_step(2)
    combine.sum_step(3)
    pass_rights(1)
    outer.sum_step(0)
    combine.sum_last()
    block_out[...] = (resid[...] + comb_own[...]).astype(BF16)
    take_rights(1)
    extra = aux_in[0]
    for i in range(1, shards):
        auxes(i).wait_recv()
        extra = extra + aux_in[i]
    extra = jnp.concatenate([extra, jnp.zeros((128 - extra.shape[0], rg), F32)], axis=0)
    extra = extra.T.astype(BF16)
    product(part_q, 0, 0, split)
    for i in range(owners):
        part_q[i, :, split:] = extra[i * piece : (i + 1) * piece]
    inner.begin(nothing)
    for i in range(1, 4):
        outer.sum_step(i)
    outer.sum_last()
    inner.more(nothing)
    total_o[at.e] = own_o[...].astype(BF16)
    outer_all.begin()
    inner.sum_step(0)
    outer_all.relay_step(1)
    inner.sum_step(1)
    inner.sum_step(2)
    outer_all.relay_step(2)
    inner.sum_step(3)
    inner.sum_last()
    total_q[at.e] = own_q[...].astype(BF16)
    inner_all.begin()
    outer_all.relay_step(3)
    inner_all.relay()
    outer_all.rest()

    def shown(k, carry):
        to = pl.ds(pl.multiple_of(k * piece, piece), piece)
        out_o[to, :] = total_o[k]
        return carry

    lax.fori_loop(0, owners, shown, 0)
    inner_all.rest()

    def shown_too(k, carry):
        to = pl.ds(pl.multiple_of(k * piece, piece), piece)
        out_q[to, :] = total_q[k, :, :kept]
        out_k[to, :] = total_q[k, :, kept : kept + span]
        out_v[to, :] = total_q[k, :, kept + span : split]
        out_r[to, :] = total_q[k, :, split:]
        return carry

    lax.fori_loop(0, owners, shown_too, 0)
    for chunk in range(2):
        for i in range(3):
            block(chunk, f, i, sibling).wait_send()
    for i in range(1, shards):
        auxes(i).wait_send()
    for t in (combine, outer, inner, outer_all, inner_all):
        t.finish()
    for h in range(EARLY, held):
        for c in late(h)[1::2] if h == EARLY else late(h):
            c.wait()


def reverse(sizes, vmem_args, fulls, comb, left, away, far):
    shards, owners, tokens, experts, held = sizes
    rg = MODEL_WIDTH // shards
    piece = rg // owners
    chips = shards // 2
    line = 4
    side = owners // line
    split = MODEL_WIDTH + 2 * KEY_VALUE_HEADS * HEAD_SIZE
    wide = split + 128
    extra = 48
    vm, dma = pltpu.VMEM, pltpu.SemaphoreType.DMA
    vmem, any_ = pl.BlockSpec(memory_space=pltpu.VMEM), pl.BlockSpec(memory_space=pl.ANY)

    def scatter(rows, width):
        return [
            vm((owners, rows, width), BF16),
            vm((line, rows, width), BF16),
            vm((line + 1, rows, width), BF16),
            vm((rows, width), F32),
            vm((rows, width - width // 256 * 128), BF16),
        ]

    shape = jax.ShapeDtypeStruct
    return pl.pallas_call(
        functools.partial(reverse_kernel, sizes),
        name="reverse",
        out_shape=(
            shape((tokens, MODEL_WIDTH), BF16),
            shape((tokens, MODEL_WIDTH), F32),
            shape((rg, MODEL_WIDTH), BF16),
            shape((rg, MODEL_WIDTH), BF16),
            shape((rg, KEY_VALUE_HEADS * HEAD_SIZE), BF16),
            shape((rg, KEY_VALUE_HEADS * HEAD_SIZE), BF16),
            shape((rg, 128), BF16),
            tuple(shape(r.shape, BF16) for r in far),
        ),
        in_specs=[vmem] * len(vmem_args) + [any_] * 11,
        out_specs=(*[vmem] * 7, (any_, any_)),
        input_output_aliases={len(vmem_args) + 9: 7, len(vmem_args) + 10: 8},
        scratch_shapes=[
            tuple(vm(w.shape, BF16) for w in fulls),
            vm((shards * tokens, 2 * rg), BF16),
            vm((2 * rg, shards * tokens), BF16),
            vm((shards * tokens, split + MODEL_WIDTH), BF16),
            vm((tokens, MODEL_WIDTH), F32),
            vm((tokens, MODEL_WIDTH), BF16),
            vm((tokens, split), F32),
            vm((extra, MODEL_WIDTH), F32),
            vm((shards, extra, rg), F32),
            *scatter(tokens, MODEL_WIDTH),
            *scatter(piece, MODEL_WIDTH),
            *scatter(piece, wide),
            vm((owners, piece, MODEL_WIDTH), BF16),
            vm((owners, piece, wide), BF16),
            dma((7,)),
            dma((2, 3)),
            dma((2, shards)),
            dma((shards - 1,)),
            dma((shards - 1,)),
            dma((2, chips - 1, held - EARLY)),
            dma((2, chips - 1, held - EARLY)),
            *([dma((line, 2)), dma((line, 2)), dma((line,)), dma((line + 1,)), dma((2,))] * 3),
            *([dma((2, side + 2, owners)), dma((2, owners))] * 2),
        ],
        compiler_params=pltpu.CompilerParams(
            collective_id=2, has_side_effects=True, vmem_limit_bytes=63 * 2**20
        ),
    )(*vmem_args, *fulls, comb, left, *away, *far)


def finish_kernel(experts, *refs):
    (s0, r0, s1, r1, q, k, v, o, extra, rows, gradient), outs = refs[:11], refs[11:]
    o0, o1, oq, ok, ov, oo, orouter, oga, ogf, orows, ograd = outs
    for a, b, c in ((s0, r0, o0), (s1, r1, o1)):
        total = a[...].astype(F32)
        for i in range(b.shape[0]):
            total = total + b[i].astype(F32)
        c[...] = total
    for a, b in ((q, oq), (k, ok), (v, ov), (o, oo)):
        b[...] = a[...].astype(F32)
    orows[...] = rows[...]
    ograd[...] = gradient[...]

    @pl.when(pl.program_id(0) == 0)
    def _():
        turned = extra[...].astype(F32).T
        orouter[...] = turned[:experts]
        oga[...] = turned[experts]
        ogf[...] = turned[experts + 1]


def finish(experts, sums, far, grads, extra, rows, gradient):
    steps = 2
    rg = sums[0].shape[1]
    two = [s.reshape(-1, s.shape[2]) for s in sums]
    away = [r.reshape(r.shape[0], -1, r.shape[3]) for r in far]

    def rows_of(a):
        return pl.BlockSpec((a.shape[0] // steps, a.shape[1]), lambda i: (i, 0))

    def deep(a):
        return pl.BlockSpec((a.shape[0], a.shape[1] // steps, a.shape[2]), lambda i: (0, i, 0))

    def whole(shape):
        return pl.BlockSpec(shape, lambda i: (0,) * len(shape))

    shape = jax.ShapeDtypeStruct
    small = [(experts, rg), (rg,), (rg,)]
    out = pl.pallas_call(
        functools.partial(finish_kernel, experts),
        name="finish",
        grid=(steps,),
        out_shape=(
            *[shape(a.shape, F32) for a in two],
            *[shape(a.shape, F32) for a in grads],
            *[shape(a, F32) for a in small],
            shape(rows.shape, rows.dtype),
            shape(gradient.shape, F32),
        ),
        in_specs=[
            rows_of(two[0]), deep(away[0]), rows_of(two[1]), deep(away[1]),
            *[rows_of(a) for a in grads], whole(extra.shape), rows_of(rows), rows_of(gradient),
        ],
        out_specs=(
            *[rows_of(a) for a in two], *[rows_of(a) for a in grads], *[whole(a) for a in small],
            rows_of(rows), rows_of(gradient),
        ),
    )(two[0], away[0], two[1], away[1], *grads, extra, rows, gradient)
    return out[0].reshape(sums[0].shape), out[1].reshape(sums[1].shape), *out[2:]


def plain_local(
    hidden_in,
    doc_ids,
    routes,
    gain_attn,
    w_query,
    key_matrix,
    value_matrix,
    w_output,
    gain_ffn,
    w_router,
    w_gateup,
    w_down,
    cotangent,
):
    tokens = hidden_in.shape[0]
    experts = w_router.shape[1]
    shards = lax.axis_size("fsdp")
    owners = lax.axis_size("expert")
    held = w_gateup.shape[0]
    half = w_down.shape[1]
    hidden_units = w_gateup.shape[2]
    pairing = 2 if held % 2 == 0 else 1
    groups = held // pairing
    slots = groups * CAP
    mine = lax.axis_index("expert")
    f32, bf16 = jnp.float32, jnp.bfloat16

    first = lax.all_gather(
        jnp.concatenate([w_query, key_matrix, value_matrix, w_router], axis=1),
        "fsdp",
        axis=0,
        tiled=True,
    )
    full_query, full_key, full_value, full_router = jnp.split(first, (1536, 2048, 2560), axis=1)
    full_output = lax.all_gather(w_output, "fsdp", axis=0, tiled=True)
    cot_all = lax.all_gather(cotangent, "expert", axis=0)
    weights_attn = (gain_attn, full_query, full_key, full_value, full_output, gain_ffn, full_router)
    state = forward_local(hidden_in, doc_ids[0], routes, *weights_attn)
    resid, ffn_in, probs = state[11], state[12], state[15]

    chosen = jnp.any(
        routes[:, :, None] == jnp.arange(experts, dtype=jnp.int32)[None, None, :], axis=1
    )
    below = jnp.tril(jnp.ones((tokens, tokens), bf16), -1)
    rank = jnp.dot(below, chosen.astype(bf16), preferred_element_type=f32)
    rank = jnp.where(chosen, rank, -1.0)
    gate = jnp.where(chosen, probs, 0.0)
    gate_high = gate.astype(bf16)
    gate_low = (gate - gate_high.astype(f32)).astype(bf16)
    meta = jnp.concatenate([rank.astype(bf16), gate_high, gate_low], axis=1)
    sent = jnp.concatenate(
        [ffn_in, meta, jnp.zeros((tokens, 128 - 3 * experts), bf16)], axis=1
    )
    got = lax.all_gather(sent, "expert", axis=0)
    rows_all = got[:, :, :MODEL_WIDTH]
    meta_all = got[:, :, MODEL_WIDTH:]
    lane = jnp.arange(slots, dtype=jnp.int32)
    slot_expert = (mine * held + (lane // CAP) * pairing) // 2
    spread = (jnp.arange(experts, dtype=jnp.int32)[:, None] == slot_expert[None, :]).astype(bf16)
    rank_at = jnp.dot(meta_all[:, :, :experts], spread, preferred_element_type=f32)
    gate_at = jnp.dot(
        meta_all[:, :, experts : 2 * experts], spread, preferred_element_type=f32
    ) + jnp.dot(meta_all[:, :, 2 * experts : 3 * experts], spread, preferred_element_type=f32)
    place = rank_at == (lane % CAP).astype(f32)[None, None, :]
    onehot = place.astype(bf16)
    gated = jnp.where(place, gate_at, 0.0)
    slot_gate = jnp.sum(gated, axis=1)

    def dispatch(rows):
        out = jnp.einsum("stj,std->sjd", onehot, rows, preferred_element_type=f32)
        return out.reshape(owners, groups, CAP, MODEL_WIDTH)

    taken = dispatch(rows_all).astype(bf16)
    cot_rows = dispatch(cot_all)
    slot_gate_4 = slot_gate.reshape(owners, groups, CAP, 1)
    grads_in = (cot_rows * slot_gate_4).astype(bf16)
    w_pairs = w_gateup.reshape(groups, pairing, MODEL_WIDTH, hidden_units)
    down_pairs = w_down.reshape(groups, pairing, half, MODEL_WIDTH)
    gate_up = jnp.einsum("secd,emdf->emscf", taken, w_pairs, preferred_element_type=f32)
    a, b = gate_up[..., :half], gate_up[..., half:]
    sigma = jax.nn.sigmoid(a)
    acted = (a * sigma * b).astype(bf16)
    made = jnp.einsum("emscf,emfd->secd", acted, down_pairs, preferred_element_type=f32)
    made = made.astype(bf16)
    grad_slot = jnp.sum(made.astype(f32) * cot_rows, axis=-1).reshape(owners, slots)
    grad_gate_back = jnp.where(place, grad_slot[:, None, :], 0.0).reshape(
        owners, tokens, groups, CAP
    )
    grad_gate_back = jnp.sum(grad_gate_back, axis=-1)
    onto = (
        (mine * held + jnp.arange(groups) * pairing)[:, None] // 2
        == jnp.arange(128, dtype=jnp.int32)[None, :]
    ).astype(bf16)
    grad_gate_back = jnp.dot(
        grad_gate_back.astype(bf16), onto, preferred_element_type=f32
    ).astype(bf16)
    weighted = (made.astype(f32) * slot_gate_4).astype(bf16).reshape(owners, slots, MODEL_WIDTH)
    combined = jnp.einsum("stj,sjd->std", onehot, weighted, preferred_element_type=f32)
    grad_acted = jnp.einsum("secd,emfd->emscf", grads_in, down_pairs, preferred_element_type=f32)
    grad_down = jnp.einsum("emscf,secd->emfd", acted, grads_in, preferred_element_type=f32)
    grad_a = grad_acted * b * sigma * (1.0 + a * (1.0 - sigma))
    grad_b = grad_acted * a * sigma
    joined = jnp.concatenate([grad_a, grad_b], axis=-1).astype(bf16)
    grad_gateup = jnp.einsum("secd,emscf->emdf", taken, joined, preferred_element_type=f32)
    grad_rows = jnp.einsum("emscf,emdf->secd", joined, w_pairs, preferred_element_type=f32)
    grad_rows = grad_rows.astype(bf16).reshape(owners, slots, MODEL_WIDTH)
    grad_ffn = jnp.einsum("stj,sjd->std", onehot, grad_rows, preferred_element_type=f32)
    back = jnp.concatenate([grad_ffn.astype(bf16), grad_gate_back], axis=-1)
    back = lax.psum_scatter(
        back.reshape(owners * tokens, -1), "expert", scatter_dimension=0, tiled=True
    ).astype(f32)
    grad_ffn, grad_gate_dense = back[:, :MODEL_WIDTH], back[:, MODEL_WIDTH : MODEL_WIDTH + experts]
    combined = lax.psum_scatter(
        combined.astype(bf16).reshape(owners * tokens, -1),
        "expert",
        scatter_dimension=0,
        tiled=True,
    )
    block_out = (resid + combined.astype(f32)).astype(bf16)
    grad_gateup, grad_down = (
        lax.psum_scatter(
            grad_gateup.reshape(held, MODEL_WIDTH, hidden_units).astype(bf16),
            "fsdp",
            scatter_dimension=1,
            tiled=True,
        ).astype(f32),
        lax.psum_scatter(
            grad_down.reshape(held, half, MODEL_WIDTH).astype(bf16),
            "fsdp",
            scatter_dimension=1,
            tiled=True,
        ).astype(f32),
    )
    grad_input, grads = backward_local(
        state, chosen, cotangent, grad_ffn, grad_gate_dense, *weights_attn
    )
    widths = [g.shape[1] if g.ndim == 2 else 1 for g in grads]
    flat = jnp.concatenate([g if g.ndim == 2 else g[:, None] for g in grads], axis=1)
    share = lax.psum_scatter(flat.astype(bf16), "fsdp", scatter_dimension=0, tiled=True)
    total = lax.psum(share, "expert").astype(f32)
    pieces = jnp.split(total, [sum(widths[: i + 1]) for i in range(len(widths) - 1)], axis=1)
    pieces = [p if g.ndim == 2 else p[:, 0] for p, g in zip(pieces, grads)]
    return (block_out, grad_input, *pieces, grad_gateup, grad_down)


def kernel_local(
    hidden_in,
    doc_ids,
    routes,
    gain_attn,
    w_query,
    key_matrix,
    value_matrix,
    w_output,
    gain_ffn,
    w_router,
    w_gateup,
    w_down,
    cotangent,
):
    tokens = hidden_in.shape[0]
    experts = w_router.shape[1]
    shards = lax.axis_size("fsdp")
    owners = lax.axis_size("expert")
    held = w_gateup.shape[0]
    pairing = 2 if held % 2 == 0 else 1
    f32, bf16 = jnp.float32, jnp.bfloat16

    shares = (w_query, key_matrix, value_matrix, w_output, w_router.T)
    made, fulls, cot_all, left = attend(
        (shards, owners, tokens, experts), hidden_in, doc_ids, routes.T, gain_attn, gain_ffn, shares,
        cotangent,
    )
    h1, q, k, v, mixed, lse, resid, sent, probs = made
    sizes = (shards, owners, tokens, experts, held, pairing)
    back, comb, sums, far, away = moe(sizes, sent, cot_all, w_gateup, w_down)
    wq, wk, wv, wo, wr = fulls
    block_out, grad_input, total_o, total_q, total_k, total_v, total_r, far = reverse(
        (shards, owners, tokens, experts, held),
        (hidden_in, doc_ids, routes.T, gain_attn, gain_ffn, cotangent, q, k, v, mixed,
         lse, resid, sent, probs, back),
        (wo, wr, wq, wk, wv),
        comb,
        left,
        away,
        far,
    )
    out = finish(
        experts, sums, far, (total_q, total_k, total_v, total_o), total_r, block_out, grad_input
    )
    grad_gateup, grad_down, grad_q, grad_k, grad_v, grad_o, grad_r, ga, gf, block, gradient = out
    return (
        block,
        gradient,
        grad_q,
        grad_k,
        grad_v,
        grad_o,
        grad_r.T,
        ga,
        gf,
        grad_gateup,
        grad_down,
    )


def local(*args):
    owners, held = lax.axis_size("expert"), args[10].shape[0]
    groups = held // (2 if held % 2 == 0 else 1)
    if lax.axis_size("fsdp") == 4 and owners == 8 and owners * groups * CAP <= 2048:
        return kernel_local(*args)
    return plain_local(*args)


def solution(mesh):
    in_specs = (
        P(("fsdp", "expert"), None),
        P(("fsdp", "expert"), None),
        P(("fsdp", "expert"), None),
        P(),
        P("fsdp", None),
        P("fsdp", None),
        P("fsdp", None),
        P("fsdp", None),
        P(),
        P("fsdp", None),
        P("expert", None, None),
        P("expert", None, None),
        P(("fsdp", "expert"), None),
    )
    out_specs = (
        P(("fsdp", "expert"), None),
        P(("fsdp", "expert"), None),
        P("fsdp", None),
        P("fsdp", None),
        P("fsdp", None),
        P("fsdp", None),
        P("fsdp", None),
        P("fsdp"),
        P("fsdp"),
        P("expert", "fsdp", None),
        P("expert", "fsdp", None),
    )
    return jax.shard_map(local, mesh=mesh, in_specs=in_specs, out_specs=out_specs, check_vma=False)
```
